8 devices in a mesh: model: 2 (over z, y), data: 4 (over x, core).
Axes of the slice: x: 2, y: 2, z: 1, core: 2. Of those that a mesh axis runs over, the one named last changes fastest.
Arguments:
- h_a: bfloat16 [16384, 2048], P('data')
- h_b: bfloat16 [16384, 2048], P('data')
- w_one: bfloat16 [2048, 2048], P(None, 'model')
- w_two: bfloat16 [2048, 2048], P('model')
- w_three: bfloat16 [2048, 2048], P(None, 'model')
- g_one: float32 [2048], P('model')
- b_one: float32 [2048], P('model')
- g_two: float32 [2048], replicated
- b_two: float32 [2048], replicated
- lam_off: float32 [1], replicated
Outputs:
- output 1: float32 [1], replicated
- output 2: float32 [2048, 2048], P(None, 'model')
- output 3: float32 [2048, 2048], P('model')
- output 4: float32 [2048, 2048], P(None, 'model')
- output 5: float32 [2048], P('model')
- output 6: float32 [2048], P('model')
- output 7: float32 [2048], replicated
- output 8: float32 [2048], replicated
All inputs are finite; a program needn't handle non-finite values.
Results may differ from the reference program's by a relative error of at most 0.001.
Values are sent between devices in bfloat16 or wider.
A program may use at most 1 GiB of HBM per device.

```python
import jax
import jax.numpy as jnp
from jax import lax
import math

N = 16384
F = 2048
D = 2048
SHARDS = 4
BN_EPS = 1e-5


def setup_inputs(seed: int = 0) -> dict:
    root_key = jax.random.key(seed)
    key_list = jax.random.split(root_key, 13)
    shard_rows = N // SHARDS
    shared_img = jax.random.normal(key_list[0], (N, F), jnp.float32)
    shard_shift = 0.5 * jax.random.normal(key_list[1], (SHARDS, 1, F), jnp.float32)
    shard_scale = jnp.exp(0.3 * jax.random.normal(key_list[2], (SHARDS, 1, F), jnp.float32))

    def make_view(view_key):
        noisy_img = shared_img + 0.6 * jax.random.normal(view_key, (N, F), jnp.float32)
        shaped = noisy_img.reshape(SHARDS, shard_rows, F) * shard_scale + shard_shift
        return shaped.reshape(N, F).astype(jnp.bfloat16)

    def make_weight(w_key, fan_in, fan_out):
        return (jax.random.normal(w_key, (fan_in, fan_out), jnp.float32) / math.sqrt(fan_in)).astype(jnp.bfloat16)

    lam_scale = 0.5 * F * N / (D * (N + 2.0 * F))
    return {
        'h_a': make_view(key_list[3]),
        'h_b': make_view(key_list[4]),
        'w_one': make_weight(key_list[5], F, D),
        'w_two': make_weight(key_list[6], D, D),
        'w_three': make_weight(key_list[7], D, D),
        'g_one': 1.0 + 0.25 * jax.random.normal(key_list[8], (D,), jnp.float32),
        'b_one': 0.4 * jax.random.normal(key_list[9], (D,), jnp.float32),
        'g_two': 1.0 + 0.25 * jax.random.normal(key_list[10], (D,), jnp.float32),
        'b_two': 0.4 * jax.random.normal(key_list[11], (D,), jnp.float32),
        'lam_off': lam_scale * (0.5 + jax.random.uniform(key_list[12], (1,), jnp.float32)),
    }


def matmul(left, right):
    return jnp.dot(left, right, preferred_element_type=jnp.float32)


def batch_norm(pre_act):
    mean_val = jnp.sum(pre_act, axis=1, keepdims=True) / N
    mean_sq = jnp.sum(pre_act * pre_act, axis=1, keepdims=True) / N
    inv_std = lax.rsqrt(mean_sq - mean_val * mean_val + BN_EPS)
    return (pre_act - mean_val) * inv_std, inv_std


def bn_backward(d_act, lin_val, norm_val, inv_std, gamma_vec):
    d_lin = jnp.where(lin_val > 0, d_act, 0.0)
    sum_lin = jnp.sum(d_lin, axis=1, keepdims=True)
    sum_norm = jnp.sum(d_lin * norm_val, axis=1, keepdims=True)
    d_pre = gamma_vec * inv_std * (d_lin - (sum_lin + norm_val * sum_norm) / N)
    return d_pre.astype(jnp.bfloat16), jnp.sum(sum_norm, axis=(0, 1)), jnp.sum(sum_lin, axis=(0, 1))


def reference(h_a, h_b, w_one, w_two, w_three, g_one, b_one, g_two, b_two, lam_off):
    view_feats = jnp.concatenate([h_a, h_b], axis=0)
    pre_one = matmul(view_feats, w_one).reshape(2, N, D)
    norm_one, inv_one = batch_norm(pre_one)
    lin_one = g_one * norm_one + b_one
    act_one = jnp.maximum(lin_one, 0.0).astype(jnp.bfloat16)
    pre_two = matmul(act_one.reshape(2 * N, D), w_two).reshape(2, N, D)
    norm_two, inv_two = batch_norm(pre_two)
    lin_two = g_two * norm_two + b_two
    act_two = jnp.maximum(lin_two, 0.0).astype(jnp.bfloat16)
    pre_out = matmul(act_two.reshape(2 * N, D), w_three).reshape(2, N, D)
    norm_out, inv_out = batch_norm(pre_out)
    embed_bf = norm_out.astype(jnp.bfloat16)
    corr_mat = matmul(embed_bf[0].T, embed_bf[1]) / N
    is_diag = jnp.arange(D)[:, None] == jnp.arange(D)[None, :]
    lam_val = lam_off[0]
    loss_val = jnp.sum(jnp.where(is_diag, (1.0 - corr_mat) * (1.0 - corr_mat), lam_val * corr_mat * corr_mat))
    grad_c = jnp.where(is_diag, -2.0 * (1.0 - corr_mat), 2.0 * lam_val * corr_mat).astype(jnp.bfloat16)
    d_emb = jnp.stack([matmul(embed_bf[1], grad_c.T), matmul(embed_bf[0], grad_c)]) / N
    embed_f = embed_bf.astype(jnp.float32)
    sum_g = jnp.sum(d_emb, axis=1, keepdims=True)
    sum_gz = jnp.sum(d_emb * embed_f, axis=1, keepdims=True)
    d_out = (inv_out * (d_emb - (sum_g + embed_f * sum_gz) / N)).astype(jnp.bfloat16)
    dw_three = matmul(act_two.reshape(2 * N, D).T, d_out.reshape(2 * N, D))
    d_act_two = matmul(d_out.reshape(2 * N, D), w_three.T).reshape(2, N, D)
    d_pre_two, dg_two, db_two = bn_backward(d_act_two, lin_two, norm_two, inv_two, g_two)
    dw_two = matmul(act_one.reshape(2 * N, D).T, d_pre_two.reshape(2 * N, D))
    d_act_one = matmul(d_pre_two.reshape(2 * N, D), w_two.T).reshape(2, N, D)
    d_pre_one, dg_one, db_one = bn_backward(d_act_one, lin_one, norm_one, inv_one, g_one)
    dw_one = matmul(view_feats.T, d_pre_one.reshape(2 * N, D))
    return loss_val.reshape(1), dw_one, dw_two, dw_three, dg_one, db_one, dg_two, db_two
```

```python
import jax
import jax.numpy as jnp
from jax import lax
from jax.experimental import pallas as pl
from jax.experimental.pallas import tpu as pltpu
from jax.sharding import PartitionSpec as P

BN_EPS = 1e-5
F32 = jnp.float32
BF16 = jnp.bfloat16
TM = 512
TN = 512
TK = 1024


def mm(left, right):
    return jnp.dot(left, right, preferred_element_type=F32)


def mm_bt(left, right):
    return lax.dot_general(left, right, (((1,), (1,)), ((), ())), preferred_element_type=F32)


def mm_at(left, right):
    return lax.dot_general(left, right, (((0,), (0,)), ((), ())), preferred_element_type=F32)


def mean_inv(sums, total):
    mean = sums[0:1] / total
    var = sums[1:2] / total - mean * mean
    return mean, lax.rsqrt(var + BN_EPS)


def add_sums(ref, first, one, two):
    sums = jnp.concatenate([jnp.sum(one, axis=0, keepdims=True), jnp.sum(two, axis=0, keepdims=True)], axis=0)

    @pl.when(first)
    def _():
        ref[0] = sums

    @pl.when(jnp.logical_not(first))
    def _():
        ref[0] += sums


def call(kernel, name, grid, in_specs, out_specs, out_shape, flops, nbytes, pos, args, scratch=(), aliases=None):
    return pl.pallas_call(
        kernel,
        name=name,
        grid_spec=pltpu.PrefetchScalarGridSpec(
            num_scalar_prefetch=1, grid=grid, in_specs=in_specs, out_specs=out_specs, scratch_shapes=list(scratch)),
        out_shape=out_shape,
        compiler_params=pltpu.CompilerParams(
            dimension_semantics=("arbitrary",) * len(grid), vmem_limit_bytes=60 << 20),
        cost_estimate=pl.CostEstimate(flops=flops, bytes_accessed=nbytes, transcendentals=0),
        input_output_aliases=aliases or {},
    )(pos, *args)


def whole(shape):
    return pl.BlockSpec(shape, lambda *_: (0,) * len(shape), pipeline_mode=pl.Buffered(1))


def sds(shape, dtype):
    return jax.ShapeDtypeStruct(shape, dtype)


def fwd_first(pos, h_a, h_b, w, rows):
    depth, dim = w.shape
    steps = rows // TM

    def kernel(pos_ref, ha_ref, hb_ref, w_ref, u_ref, s_ref):
        i = pl.program_id(0)
        h = lax.select(i < steps, ha_ref[...], hb_ref[...])
        u = mm(h, w_ref[...])
        u_ref[...] = u
        add_sums(s_ref, i % steps == 0, u, u * u)

    return call(
        kernel, "fwd_first", (2 * steps,),
        [pl.BlockSpec((TM, depth), lambda i, p: (p[0] * steps + jnp.minimum(i, steps - 1), 0)),
         pl.BlockSpec((TM, depth), lambda i, p: (p[0] * steps + jnp.maximum(i - steps, 0), 0)),
         whole((depth, dim))],
        [pl.BlockSpec((TM, dim), lambda i, p: (i, 0)), pl.BlockSpec((1, 2, dim), lambda i, p: (i // steps, 0, 0))],
        [sds((2 * rows, dim), F32), sds((2, 2, dim), F32)],
        4 * rows * depth * dim, 2 * rows * (2 * depth + 4 * dim) + 2 * depth * dim, pos, (h_a, h_b, w))


def fwd_next(pos, u, sums, gamma, beta, w, total):
    all_rows, depth = u.shape
    dim = w.shape[1]
    steps = all_rows // 2 // TM

    def kernel(pos_ref, u_ref, s_ref, g_ref, b_ref, w_ref, x_ref, o_ref, so_ref):
        i = pl.program_id(0)
        mean, inv = mean_inv(s_ref[0], total)
        x = jnp.maximum((u_ref[...] - mean) * inv * g_ref[...] + b_ref[...], 0.0).astype(BF16)
        x_ref[...] = x
        out = mm(x, w_ref[...])
        o_ref[...] = out
        add_sums(so_ref, i % steps == 0, out, out * out)

    return call(
        kernel, "fwd_next", (2 * steps,),
        [pl.BlockSpec((TM, depth), lambda i, p: (i, 0)), pl.BlockSpec((1, 2, depth), lambda i, p: (i // steps, 0, 0)),
         whole((1, depth)), whole((1, depth)), whole((depth, dim))],
        [pl.BlockSpec((TM, depth), lambda i, p: (i, 0)), pl.BlockSpec((TM, dim), lambda i, p: (i, 0)),
         pl.BlockSpec((1, 2, dim), lambda i, p: (i // steps, 0, 0))],
        [sds((all_rows, depth), BF16), sds((all_rows, dim), F32), sds((2, 2, dim), F32)],
        2 * all_rows * depth * dim, all_rows * (6 * depth + 4 * dim), pos,
        (u, sums, gamma.reshape(1, depth), beta.reshape(1, depth), w))


def corr(pos, z, sums, total):
    all_rows, dim = z.shape
    steps = all_rows // 2 // TM
    half = dim // 2
    cols = dim // TN

    def kernel(pos_ref, za_ref, zb_ref, s_ref, zh_ref, send_ref, keep_ref, zh_all):
        i = pl.program_id(0)

        @pl.when(i < steps)
        def _():
            for v, ref in ((0, za_ref), (1, zb_ref)):
                mean, inv = mean_inv(s_ref[v], total)
                zh = ((ref[...] - mean) * inv).astype(BF16)
                zh_ref[v] = zh
                zh_all[v, pl.ds(pl.multiple_of(i * TM, TM), TM)] = zh

        @pl.when(i >= steps)
        def _():
            n = pl.multiple_of((i - steps) * TN, TN)
            right = zh_all[1, :, pl.ds(n, TN)]
            for part, ref in ((1 - pos_ref[1], send_ref), (pos_ref[1], keep_ref)):
                ref[...] = mm_at(zh_all[0, :, pl.ds(pl.multiple_of(part * half, half), half)], right)

    col = lambda i, p: (0, jnp.maximum(i - steps, 0))
    row = lambda i: jnp.minimum(i, steps - 1)
    return call(
        kernel, "corr", (steps + cols,),
        [pl.BlockSpec((TM, dim), lambda i, p: (row(i), 0)), pl.BlockSpec((TM, dim), lambda i, p: (row(i) + steps, 0)),
         whole((2, 2, dim))],
        [pl.BlockSpec((2, TM, dim), lambda i, p: (0, row(i), 0)), pl.BlockSpec((half, TN), col),
         pl.BlockSpec((half, TN), col)],
        [sds((2, all_rows // 2, dim), BF16), sds((half, dim), F32), sds((half, dim), F32)],
        all_rows * dim * dim, all_rows * dim * 6 + 4 * dim * dim, pos, (z, z, sums),
        scratch=[pltpu.VMEM((2, all_rows // 2, dim), BF16)])


def emb_grad(pos, zh, grad_c, total):
    _, rows, dim = zh.shape
    steps = rows // TM

    def kernel(pos_ref, other_ref, own_ref, g_ref, d_ref, s_ref):
        i = pl.program_id(0)

        def finish(d):
            d = d / total
            d_ref[...] = d
            add_sums(s_ref, i % steps == 0, d, d * own_ref[0].astype(F32))

        @pl.when(i < steps)
        def _():
            finish(mm_bt(other_ref[0], g_ref[...]))

        @pl.when(i >= steps)
        def _():
            finish(mm(other_ref[0], g_ref[...]))

    return call(
        kernel, "emb_grad", (2 * steps,),
        [pl.BlockSpec((1, TM, dim), lambda i, p: (1 - i // steps, i % steps, 0)),
         pl.BlockSpec((1, TM, dim), lambda i, p: (i // steps, i % steps, 0)), whole((dim, dim))],
        [pl.BlockSpec((TM, dim), lambda i, p: (i, 0)), pl.BlockSpec((1, 2, dim), lambda i, p: (i // steps, 0, 0))],
        [sds((2 * rows, dim), F32), sds((2, 2, dim), F32)],
        4 * rows * dim * dim, rows * dim * 16, pos, (zh, zh, grad_c))


def act_grad(pos, d_pre, w, u, sums, gamma, beta, total):
    all_rows, dim = d_pre.shape
    depth = w.shape[0]
    steps = all_rows // 2 // TM

    def kernel(pos_ref, d_ref, w_ref, u_ref, s_ref, g_ref, b_ref, o_ref, so_ref):
        i = pl.program_id(0)
        mean, inv = mean_inv(s_ref[0], total)
        norm = (u_ref[...] - mean) * inv
        dx = mm_bt(d_ref[...], w_ref[...])
        dy = jnp.where(norm * g_ref[...] + b_ref[...] > 0, dx, 0.0)
        o_ref[...] = dy
        add_sums(so_ref, i % steps == 0, dy, dy * norm)

    return call(
        kernel, "act_grad", (2 * steps,),
        [pl.BlockSpec((TM, dim), lambda i, p: (i, 0)), whole((depth, dim)), pl.BlockSpec((TM, depth), lambda i, p: (i, 0)),
         pl.BlockSpec((1, 2, depth), lambda i, p: (i // steps, 0, 0)), whole((1, depth)), whole((1, depth))],
        [pl.BlockSpec((TM, depth), lambda i, p: (i, 0)), pl.BlockSpec((1, 2, depth), lambda i, p: (i // steps, 0, 0))],
        [sds((all_rows, depth), F32), sds((2, 2, depth), F32)],
        2 * all_rows * depth * dim, all_rows * (8 * depth + 2 * dim), pos,
        (d_pre, w, u, sums, gamma.reshape(1, depth), beta.reshape(1, depth)))


def weight_grad(pos, lefts, pre_args, pre_specs, pre_fn, name, cols_by_core, write_pre):
    dim = pre_args[0].shape[-1]
    all_rows = pre_args[0].shape[-2]
    depth = lefts[0].shape[1]
    half = dim // 2
    ksteps = all_rows // TK
    nh = half // TN

    def slab(n, p):
        mine = p[1] if cols_by_core else p[0]
        return jnp.where(n < nh, (1 - mine) * nh + n, mine * nh + n - nh)

    def kernel(pos_ref, *refs):
        left_refs, refs = refs[:len(lefts)], refs[len(lefts):]
        pre_refs, refs = refs[:len(pre_args)], refs[len(pre_args):]
        outs, refs = refs[:4], refs[4:]
        n, k = pl.program_id(0), pl.program_id(1)
        d = pre_fn(*pre_refs)
        if write_pre:
            refs[0][...] = d
        mine = pos_ref[0] if cols_by_core else pos_ref[1]
        for which, part in ((0, 1 - mine), (1, mine)):
            here = pl.ds(pl.multiple_of(part * half, half), half)
            if len(lefts) == 1:
                left = left_refs[0][pl.ds(pl.multiple_of(k * TK, TK), TK), here]
            else:
                rows = pl.ds(pl.multiple_of(k % (ksteps // 2) * TK, TK), TK)
                left = lax.select(k < ksteps // 2, left_refs[0][rows, here], left_refs[1][rows, here])
            prod = mm_at(left, d)
            for late in (0, 1):
                ref = outs[(which * 2 + late) if not cols_by_core else (late * 1 + which * 2)]

                @pl.when(jnp.logical_and((n >= nh) == bool(late), k == 0))
                def _(ref=ref):
                    ref[...] = prod

                @pl.when(jnp.logical_and((n >= nh) == bool(late), k > 0))
                def _(ref=ref):
                    ref[...] += prod

    early_col = lambda n, k, p: (0, jnp.minimum(n, nh - 1))
    late_col = lambda n, k, p: (0, jnp.maximum(n - nh, 0))
    quarter = sds((half, half), F32)
    out_specs = [pl.BlockSpec((half, TN), early_col), pl.BlockSpec((half, TN), late_col),
                 pl.BlockSpec((half, TN), early_col), pl.BlockSpec((half, TN), late_col)]
    out_shape = [quarter] * 4
    if write_pre:
        out_specs.append(pl.BlockSpec((TK, TN), lambda n, k, p: (k, slab(n, p))))
        out_shape.append(sds((all_rows, dim), BF16))
    if len(lefts) == 1:
        left_specs = [whole((all_rows, depth))]
    else:
        left_specs = [pl.BlockSpec((all_rows // 2, depth), lambda n, k, p: (p[0], 0), pipeline_mode=pl.Buffered(1))] * 2
    res = call(kernel, name, (2 * nh, ksteps), left_specs + pre_specs(slab), out_specs, out_shape,
               2 * all_rows * depth * dim, all_rows * dim * 8, pos, (*lefts, *pre_args))
    if cols_by_core:
        sent_other, kept_other, sent_own, kept_own = res[0], res[1], res[2], res[3]
    else:
        sent_other, sent_own, kept_other, kept_own = res[0], res[1], res[2], res[3]
    return (sent_other, kept_other, sent_own, kept_own), (res[4] if write_pre else None)


def solution(mesh):
    n_model, n_data = mesh.shape['model'], mesh.shape['data']
    axes = ('model', 'data')
    flat = range(n_model * n_data)
    flip_core = [(i, i ^ 1) for i in flat]
    flip_x = [(i, i ^ 2) for i in flat]
    flip_y = [(i, i ^ n_data) for i in flat]
    first_axis = [(i, i ^ (n_data if i % 2 else 2)) for i in flat]
    second_axis = [(i, i ^ (2 if i % 2 else n_data)) for i in flat]

    def send(value, perm):
        return lax.ppermute(value, axes, perm)

    def shard_body(h_a, h_b, w_one, w_two, w_three, g_one, b_one, g_two, b_two, lam_off):
        y, d = lax.axis_index('model'), lax.axis_index('data')
        x, c = d // 2, d % 2
        pos = jnp.stack([y, c]).astype(jnp.int32)
        rows = h_a.shape[0] // n_model
        total = float(h_a.shape[0] * n_data)
        dim = w_three.shape[0]
        half = dim // 2

        def gather_w(w, axis):
            quarter = lax.dynamic_slice_in_dim(w, c * (w.shape[0] // 2), w.shape[0] // 2, 0)
            got = send(quarter, flip_y)
            got2 = send(got, flip_core)
            other = lax.select(c == 0, jnp.concatenate([got, got2], 0), jnp.concatenate([got2, got], 0))
            return lax.select(y == 0, jnp.concatenate([w, other], axis), jnp.concatenate([other, w], axis))

        w1, w2, w3 = gather_w(w_one, 1), gather_w(w_two, 0), gather_w(w_three, 1)
        vec = lax.all_gather(jnp.stack([g_one, b_one]), 'model', axis=1, tiled=True)
        g1, b1 = vec[0], vec[1]

        psum = lambda v: lax.psum(v, axes)
        u1, s1 = fwd_first(pos, h_a, h_b, w1, rows)
        s1 = psum(s1)
        x1, u2, s2 = fwd_next(pos, u1, s1, g1, b1, w2, total)
        s2 = psum(s2)
        x2, z, sz = fwd_next(pos, u2, s2, g_two, b_two, w3, total)
        sz = psum(sz)

        zh, c_send, c_keep = corr(pos, z, sz, total)
        part = c_keep + send(c_send, flip_core)
        bit1 = lax.select(c == 0, x, y)
        bit2 = lax.select(c == 0, y, x)
        piece = lambda v, bit, axis: lax.dynamic_slice_in_dim(v, bit * (v.shape[axis] // 2), v.shape[axis] // 2, axis)
        part = piece(part, bit1, 1) + send(piece(part, 1 - bit1, 1), first_axis)
        part = piece(part, bit2, 0) + send(piece(part, 1 - bit2, 0), second_axis)
        corr_mat = part / total
        n_rows, n_cols = corr_mat.shape
        row_ids = c * half + bit2 * n_rows + lax.broadcasted_iota(jnp.int32, (n_rows, n_cols), 0)
        col_ids = bit1 * n_cols + lax.broadcasted_iota(jnp.int32, (n_rows, n_cols), 1)
        is_diag = row_ids == col_ids
        lam = lam_off[0]
        loss = psum(jnp.sum(jnp.where(is_diag, (1.0 - corr_mat) * (1.0 - corr_mat), lam * corr_mat * corr_mat)))
        grad_c = jnp.where(is_diag, -2.0 * (1.0 - corr_mat), 2.0 * lam * corr_mat).astype(BF16)

        def join(own, got, bit, axis):
            return lax.select(bit == 0, jnp.concatenate([own, got], axis), jnp.concatenate([got, own], axis))

        grad_c = join(grad_c, send(grad_c, second_axis), bit2, 0)
        grad_c = join(grad_c, send(grad_c, first_axis), bit1, 1)
        grad_c = join(grad_c, send(grad_c, flip_core), c, 0)

        d_emb, s_emb = emb_grad(pos, zh, grad_c, total)
        s_emb = psum(s_emb)

        def reduce_dw(parts, axis):
            sent_other, kept_other, sent_own, kept_own = parts
            other = kept_other + send(sent_other, flip_core)
            own = kept_own + send(sent_own, flip_core)
            chunks = 2
            size = half // chunks
            done = []
            for j in range(chunks):
                cut = lambda v: lax.slice_in_dim(v, j * size, (j + 1) * size, axis=0)
                mine = cut(own) + send(cut(other), flip_y)
                done.append(mine + send(mine, flip_x))
            mine = jnp.concatenate(done, 0)
            return join(mine, send(mine, flip_core), c, axis)

        col_spec = lambda slab: pl.BlockSpec((TK, TN), lambda n, k, p: (k, slab(n, p)))
        view = lambda k: k // (2 * rows // TK // 2)
        sum_spec = lambda slab: pl.BlockSpec((1, 2, TN), lambda n, k, p: (view(k), 0, slab(n, p)))
        vec_spec = lambda slab: pl.BlockSpec((1, TN), lambda n, k, p: (0, slab(n, p)))

        def out_pre(d_ref, zh_ref, sz_ref, sd_ref):
            _, inv = mean_inv(sz_ref[0], total)
            sd = sd_ref[0]
            return (inv * (d_ref[...] - sd[0:1] / total - zh_ref[...].astype(F32) * (sd[1:2] / total))).astype(BF16)

        parts3, d_out = weight_grad(
            pos, (x2,), (d_emb, zh.reshape(2 * rows, dim), sz, s_emb),
            lambda slab: [col_spec(slab), col_spec(slab), sum_spec(slab), sum_spec(slab)], out_pre, "dw_three", False, True)
        dw_three = reduce_dw(parts3, 0)

        def bn_pre(d_ref, u_ref, su_ref, sd_ref, g_ref):
            mean, inv = mean_inv(su_ref[0], total)
            sd = sd_ref[0]
            norm = (u_ref[...] - mean) * inv
            return (g_ref[...] * inv * (d_ref[...] - (sd[0:1] + norm * sd[1:2]) / total)).astype(BF16)

        bn_specs = lambda slab: [col_spec(slab), col_spec(slab), sum_spec(slab), sum_spec(slab), vec_spec(slab)]
        dy2, sd2 = act_grad(pos, d_out, w3, u2, s2, g_two, b_two, total)
        sd2 = psum(sd2)
        parts2, d_pre_two = weight_grad(
            pos, (x1,), (dy2, u2, s2, sd2, g_two.reshape(1, dim)), bn_specs, bn_pre, "dw_two", True, True)
        dw_two = reduce_dw(parts2, 1)
        dy1, sd1 = act_grad(pos, d_pre_two, w2, u1, s1, g1, b1, total)
        sd1 = psum(sd1)
        parts1, _ = weight_grad(
            pos, (h_a, h_b), (dy1, u1, s1, sd1, g1.reshape(1, dim)), bn_specs, bn_pre, "dw_one", False, False)
        dw_one = reduce_dw(parts1, 0)

        sum1 = lax.dynamic_slice_in_dim(jnp.sum(sd1, 0), y * half, half, 1)
        sum2 = jnp.sum(sd2, 0)
        return loss.reshape(1), dw_one, dw_two, dw_three, sum1[1], sum1[0], sum2[1], sum2[0]

    in_specs = (P('data', None), P('data', None), P(None, 'model'), P('model', None), P(None, 'model'),
                P('model'), P('model'), P(), P(), P())
    out_specs = (P(), P(None, 'model'), P('model', None), P(None, 'model'), P('model'), P('model'), P(), P())
    return jax.shard_map(shard_body, mesh=mesh, in_specs=in_specs, out_specs=out_specs, check_vma=False)
```

```python
import jax
import jax.numpy as jnp
from jax import lax
from jax.experimental import pallas as pl
from jax.experimental.pallas import tpu as pltpu
from jax.sharding import PartitionSpec as P

BN_EPS = 1e-5
F32 = jnp.float32
BF16 = jnp.bfloat16
TM = 512
TN = 512
TK = 1024


def mm(left, right):
    return jnp.dot(left, right, preferred_element_type=F32)


def mm_bt(left, right):
    return lax.dot_general(left, right, (((1,), (1,)), ((), ())), preferred_element_type=F32)


def mm_at(left, right):
    return lax.dot_general(left, right, (((0,), (0,)), ((), ())), preferred_element_type=F32)


def mean_inv(sums, total):
    mean = sums[0:1] / total
    var = sums[1:2] / total - mean * mean
    return mean, lax.rsqrt(var + BN_EPS)


def coords():
    y, d = lax.axis_index('model'), lax.axis_index('data')
    return y, lax.div(d, 2), lax.rem(d, 2)


def flip(here, which):
    return tuple(1 - p if f else p for p, f in zip(here, which))


PEERS = [(ky, kx, kc) for ky in (0, 1) for kx in (0, 1) for kc in (0, 1)][1:]
Y_PEER, X_PEER, C_PEER = (1, 0, 0), (0, 1, 0), (0, 0, 1)


def flat(here):
    return 4 * here[0] + 2 * here[1] + here[2]


def device(here):
    return (here[0], 2 * here[1] + here[2])


def remote(src, dst, send_sem, recv_sem, there):
    return pltpu.make_async_remote_copy(
        src_ref=src, dst_ref=dst, send_sem=send_sem, recv_sem=recv_sem, device_id=device(there),
        device_id_type=pl.DeviceIdType.MESH)


def arrive():
    here = coords()
    for k in PEERS:
        pl.semaphore_signal(pltpu.get_barrier_semaphore(), inc=1, device_id=device(flip(here, k)),
                            device_id_type=pl.DeviceIdType.MESH)


def all_arrived():
    pl.semaphore_wait(pltpu.get_barrier_semaphore(), len(PEERS))


def share(acc, got, send_sem, recv_sem, b):
    here = coords()
    me = flat(here)
    got[b, me] = acc[b]
    for k, which in enumerate(PEERS):
        remote(acc.at[b], got.at[b, me], send_sem.at[b, k], recv_sem.at[b, me], flip(here, which)).start()


def shared(acc, got, send_sem, recv_sem, b):
    here = coords()
    for k, which in enumerate(PEERS):
        there = flip(here, which)
        copy = remote(acc.at[b], got.at[b, flat(there)], send_sem.at[b, k], recv_sem.at[b, flat(there)], there)
        copy.wait_send()
        copy.wait_recv()
    out = got[b, 0]
    for f in range(1, 8):
        out += got[b, f]
    return out


def share_scratch(n, rows, dim):
    return [pltpu.VMEM((n, rows, dim), F32), pltpu.VMEM((n, 8, rows, dim), F32),
            pltpu.SemaphoreType.DMA((n, 7)), pltpu.SemaphoreType.DMA((n, 8))]


def two_sums(one, two):
    return jnp.concatenate([jnp.sum(one, axis=0, keepdims=True), jnp.sum(two, axis=0, keepdims=True)], axis=0)


def add_share(i, steps, one, two, out_ref, acc, got, send_sem, recv_sem, barrier=True):
    sums = two_sums(one, two)
    v = i // steps

    @pl.when(i % steps == 0)
    def _():
        acc[v] = sums

    @pl.when(i % steps > 0)
    def _():
        acc[v] += sums

    @pl.when(i == steps)
    def _():
        if barrier:
            all_arrived()
        share(acc, got, send_sem, recv_sem, 0)

    @pl.when(i == 2 * steps - 1)
    def _():
        share(acc, got, send_sem, recv_sem, 1)
        for b in (0, 1):
            out_ref[b] = shared(acc, got, send_sem, recv_sem, b)


def call_remote(kernel, name, cid, grid, in_specs, out_specs, out_shape, scratch, flops, nbytes, args, vmem=61 << 20):
    return pl.pallas_call(
        kernel, name=name, grid=grid, in_specs=in_specs, out_specs=out_specs, out_shape=out_shape, scratch_shapes=scratch,
        compiler_params=pltpu.CompilerParams(
            dimension_semantics=("arbitrary",) * len(grid), vmem_limit_bytes=vmem, collective_id=cid,
            has_side_effects=True),
        cost_estimate=pl.CostEstimate(flops=flops, bytes_accessed=nbytes, transcendentals=0))(*args)


ANY = pl.BlockSpec(memory_space=pl.ANY)


def fwd_first(h_a, h_b, w_one, w_two, gb_own):
    depth, half = w_one.shape
    dim = 2 * half
    rows = h_a.shape[0] // 2
    tile, width, quarter = 1024, 512, half // 4
    steps = rows // tile
    ny = 4
    piece = depth // ny

    def block(j):
        y, x, _ = coords()
        return jnp.where(j < 2, 2 * y + j, jnp.where(j == 2, 2 * (1 - y) + x, 2 * (1 - y) + 1 - x))

    def kernel(ha_ref, hb_ref, w_ref, w2_ref, gb_ref, u_ref, s_ref, gbo_ref, w2o_ref,
               w1, gbf, acc, got, ssem, rsem, lsem, ys, yr, xs, xr, cs, cr, y2s, y2r, x2s, x2r, c2s, c2r, gs, gr):
        j, i = pl.program_id(0), pl.program_id(1)
        step = j * 2 * steps + i
        here = coords()
        y, x, c = here
        ypeer, xpeer, cpeer = flip(here, Y_PEER), flip(here, X_PEER), flip(here, C_PEER)
        q_mine, q_x = 2 * x + c, 2 * (1 - x) + c

        def local(b):
            return pltpu.make_async_copy(
                w_ref.at[:, pl.ds(b * width, width)],
                w1.at[:, pl.ds(pl.multiple_of(y * half + b * width, width), width)], lsem.at[b])

        def w1_at(model, q, p):
            return w1.at[pl.ds(p * piece, piece), pl.ds(pl.multiple_of(model * half + q * quarter, quarter), quarter)]

        def w1_y(p):
            return remote(w_ref.at[pl.ds(p * piece, piece), pl.ds(pl.multiple_of(q_mine * quarter, quarter), quarter)],
                          w1_at(y, q_mine, p), ys.at[p], yr.at[p], ypeer)

        def w1_y_got(p):
            return remote(w1_at(1 - y, q_mine, p), w1_at(1 - y, q_mine, p), ys.at[p], yr.at[p], ypeer)

        def w1_x(p):
            return remote(w1_at(1 - y, q_mine, p), w1_at(1 - y, q_mine, p), xs.at[p], xr.at[p], xpeer)

        def w1_x_got(p):
            return remote(w1_at(1 - y, q_x, p), w1_at(1 - y, q_x, p), xs.at[p], xr.at[p], xpeer)

        def w1_c(p, late):
            q = q_x if late else q_mine
            return remote(w1_at(1 - y, q, p), w1_at(1 - y, q, p), cs.at[late, p], cr.at[late, p], cpeer)

        def w1_c_got(p, late):
            q = (2 * (1 - x) if late else 2 * x) + 1 - c
            return remote(w1_at(1 - y, q, p), w1_at(1 - y, q, p), cs.at[late, p], cr.at[late, p], cpeer)

        def w2_at(q):
            return w2o_ref.at[pl.ds(pl.multiple_of(q * quarter, quarter), quarter)]

        w2_y = lambda: remote(w2_ref.at[pl.ds(pl.multiple_of(q_mine * quarter, quarter), quarter)], w2_at(q_mine),
                              y2s, y2r, ypeer)
        w2_y_got = lambda: remote(w2_at(q_mine), w2_at(q_mine), y2s, y2r, ypeer)
        w2_x = lambda: remote(w2_at(q_mine), w2_at(q_mine), x2s, x2r, xpeer)
        w2_x_got = lambda: remote(w2_at(q_x), w2_at(q_x), x2s, x2r, xpeer)

        def w2_c(late):
            q = q_x if late else q_mine
            return remote(w2_at(q), w2_at(q), c2s.at[late], c2r.at[late], cpeer)

        def w2_c_got(late):
            q = (2 * (1 - x) if late else 2 * x) + 1 - c
            return remote(w2_at(q), w2_at(q), c2s.at[late], c2r.at[late], cpeer)

        gb_send = lambda: remote(gb_ref, gbf.at[:, pl.ds(pl.multiple_of(y * half, half), half)], gs, gr, ypeer)
        gb_got = lambda: remote(gb_ref, gbf.at[:, pl.ds(pl.multiple_of((1 - y) * half, half), half)], gs, gr, ypeer)

        def pass_on(p):
            w1_y_got(p).wait_recv()
            w1_x(p).start()
            w1_c(p, 0).start()

        @pl.when(step == 0)
        def _():
            arrive()
            for b in (0, 1):
                local(b).start()
            all_arrived()
            for p in range(ny):
                w1_y(p).start()
            w2_y().start()
            gb_send().start()
            local(0).wait()

        @pl.when(step == 3)
        def _():
            pass_on(0)

        @pl.when(step == 2 * steps)
        def _():
            local(1).wait()

        @pl.when(step == 6)
        def _():
            pass_on(1)

        @pl.when(step == 4 * steps)
        def _():
            pass_on(2)
            for p in (0, 1):
                w1_x_got(p).wait_recv()
                w1_c(p, 1).start()
            pass_on(3)
            for p in range(ny):
                w1_c_got(p, 0).wait_recv()

        @pl.when(step == 4 * steps + 2)
        def _():
            w1_x_got(2).wait_recv()
            w1_c(2, 1).start()

        @pl.when(step == 6 * steps)
        def _():
            w1_x_got(3).wait_recv()
            w1_c(3, 1).start()
            for p in range(ny):
                w1_c_got(p, 1).wait_recv()

        @pl.when(step == 8 * steps - 1)
        def _():
            w2_y_got().wait_recv()
            w2_x().start()
            w2_c(0).start()

        for b in range(3):
            @pl.when(step == (b + 1) * 2 * steps)
            def _(b=b):
                share(acc, got, ssem, rsem, block(b))

        h = lax.select(i < steps, ha_ref[...], hb_ref[...])
        u = mm(h, w1[:, pl.ds(pl.multiple_of(block(j) * width, width), width)])
        u_ref[...] = u
        sums = two_sums(u, u * u)
        v = i // steps

        @pl.when(i % steps == 0)
        def _():
            acc[block(j), v] = sums

        @pl.when(i % steps > 0)
        def _():
            acc[block(j), v] += sums

        @pl.when(step == 8 * steps - 1)
        def _():
            share(acc, got, ssem, rsem, block(3))
            gb_got().wait_recv()
            gb_send().wait_send()
            gbo_ref[...] = gbf[...]
            gbo_ref[:, pl.ds(pl.multiple_of(y * half, half), half)] = gb_ref[...]
            for b in range(4):
                total = shared(acc, got, ssem, rsem, b)
                s_ref[:, :, b * width:(b + 1) * width] = total
            for p in range(ny):
                w1_y(p).wait_send()
                w1_x(p).wait_send()
                w1_c(p, 0).wait_send()
                w1_c(p, 1).wait_send()
            w2_x_got().wait_recv()
            w2_c(1).start()
            w2_y().wait_send()
            w2_x().wait_send()
            for late in (0, 1):
                w2_c(late).wait_send()
                w2_c_got(late).wait_recv()

    dma = pltpu.SemaphoreType.DMA
    return call_remote(
        kernel, "fwd_first", 0, (4, 2 * steps),
        [pl.BlockSpec((tile, depth), lambda j, i: (coords()[0] * steps + jnp.minimum(i, steps - 1), 0)),
         pl.BlockSpec((tile, depth), lambda j, i: (coords()[0] * steps + jnp.maximum(i - steps, 0), 0)),
         ANY, ANY, pl.BlockSpec((2, half), lambda j, i: (0, 0))],
        [pl.BlockSpec((tile, width), lambda j, i: (i, block(j))), pl.BlockSpec((2, 2, dim), lambda j, i: (0, 0, 0)),
         pl.BlockSpec((2, dim), lambda j, i: (0, 0)), ANY],
        [sds((2 * rows, dim), F32), sds((2, 2, dim), F32), sds((2, dim), F32), sds((half, dim), BF16)],
        [pltpu.VMEM((depth, dim), BF16), pltpu.VMEM((2, dim), F32),
         pltpu.VMEM((4, 2, 2, width), F32), pltpu.VMEM((4, 8, 2, 2, width), F32), dma((4, 7)), dma((4, 8)),
         dma((2,)), dma((ny,)), dma((ny,)), dma((ny,)), dma((ny,)), dma((2, ny)), dma((2, ny)),
         dma, dma, dma, dma, dma((2,)), dma((2,)), dma, dma],
        4 * rows * depth * dim, 2 * rows * (8 * depth + 4 * dim), (h_a, h_b, w_one, w_two, gb_own))


def fwd_next(u, sums, gb, w_own, w_other, by_rows, total, cid, w_next=None):
    all_rows, depth = u.shape
    dim = w_own.shape[1] if by_rows else 2 * w_own.shape[1]
    half = dim // 2
    quarter = half // 4
    steps = all_rows // 2 // TM
    slab = dim // (2 * steps)

    def kernel(*refs):
        u_ref, s_ref, gb_ref, wo_ref, wt_ref = refs[:5]
        refs = refs[5:]
        if w_next is not None:
            wn_ref, refs = refs[0], refs[1:]
        x_ref, o_ref, so_ref, wtr_ref = refs[:4]
        refs = refs[4:]
        if w_next is not None:
            wno_ref, refs = refs[0], refs[1:]
        w, acc, got, ssem, rsem, lsem = refs[:6]
        i = pl.program_id(0)
        here = coords()
        y, x, c = here
        ypeer, xpeer, cpeer = flip(here, Y_PEER), flip(here, X_PEER), flip(here, C_PEER)
        q_mine, q_x = 2 * x + c, 2 * (1 - x) + c

        def local(ref, model, b):
            at = pl.ds(pl.multiple_of(model * half, half), half)
            return pltpu.make_async_copy(ref, w.at[at] if by_rows else w.at[:, at], lsem.at[b])

        @pl.when(i == 0)
        def _():
            arrive()
            local(wo_ref, y, 0).start()
            local(wt_ref, 1 - y, 1).start()
            local(wo_ref, y, 0).wait()
            local(wt_ref, 1 - y, 1).wait()

        if w_next is not None:
            y2s, y2r, x2s, x2r, c2s, c2r = refs[6:]
            at = lambda ref, q: ref.at[:, pl.ds(pl.multiple_of(q * quarter, quarter), quarter)]
            wn_y = lambda: remote(at(wn_ref, q_mine), at(wno_ref, q_mine), y2s, y2r, ypeer)
            wn_y_got = lambda: remote(at(wno_ref, q_mine), at(wno_ref, q_mine), y2s, y2r, ypeer)
            wn_x = lambda: remote(at(wno_ref, q_mine), at(wno_ref, q_mine), x2s, x2r, xpeer)
            wn_x_got = lambda: remote(at(wno_ref, q_x), at(wno_ref, q_x), x2s, x2r, xpeer)

            def wn_c(late):
                q = q_x if late else q_mine
                return remote(at(wno_ref, q), at(wno_ref, q), c2s.at[late], c2r.at[late], cpeer)

            def wn_c_got(late):
                q = (2 * (1 - x) if late else 2 * x) + 1 - c
                return remote(at(wno_ref, q), at(wno_ref, q), c2s.at[late], c2r.at[late], cpeer)

        if w_next is not None:
            @pl.when(i == 1)
            def _():
                all_arrived()
                wn_y().start()

            @pl.when(i == 2 * steps - 2)
            def _():
                wn_y_got().wait_recv()
                wn_x().start()
                wn_c(0).start()

        mean, inv = mean_inv(s_ref[0], total)
        act = jnp.maximum((u_ref[...] - mean) * inv * gb_ref[0:1] + gb_ref[1:2], 0.0).astype(BF16)
        x_ref[...] = act
        out = mm(act, w[...])
        o_ref[...] = out
        wtr_ref[...] = w[:, pl.ds(pl.multiple_of(i * slab, slab), slab)].T
        if w_next is not None:
            @pl.when(i == 2 * steps - 1)
            def _():
                wn_x_got().wait_recv()
                wn_c(1).start()
        add_share(i, steps, out, out * out, so_ref, acc, got, ssem, rsem, barrier=w_next is None)
        if w_next is not None:
            @pl.when(i == 2 * steps - 1)
            def _():
                wn_y().wait_send()
                wn_x().wait_send()
                for late in (0, 1):
                    wn_c(late).wait_send()
                    wn_c_got(late).wait_recv()

    dma = pltpu.SemaphoreType.DMA
    more = w_next is not None
    return call_remote(
        kernel, "fwd_next", cid, (2 * steps,),
        [pl.BlockSpec((TM, depth), lambda i: (i, 0)), pl.BlockSpec((1, 2, depth), lambda i: (i // steps, 0, 0)),
         pl.BlockSpec((2, depth), lambda i: (0, 0)), ANY, ANY] + [ANY] * more,
        [pl.BlockSpec((TM, depth), lambda i: (i, 0)), pl.BlockSpec((TM, dim), lambda i: (i, 0)),
         pl.BlockSpec((2, 2, dim), lambda i: (0, 0, 0)), pl.BlockSpec((slab, depth), lambda i: (i, 0))] + [ANY] * more,
        [sds((all_rows, depth), BF16), sds((all_rows, dim), F32), sds((2, 2, dim), F32), sds((dim, depth), BF16)]
        + ([sds(w_next.shape, BF16)] if more else []),
        [pltpu.VMEM((depth, dim), BF16)] + share_scratch(2, 2, dim) + [dma((2,))]
        + ([dma, dma, dma, dma, dma((2,)), dma((2,))] if more else []),
        2 * all_rows * depth * dim, all_rows * (6 * depth + 4 * dim),
        (u, sums, gb, w_own, w_other) + ((w_next,) if more else ()))


def corr_grad(z, sums, lam, total):
    all_rows, dim = z.shape
    rows = all_rows // 2
    half = dim // 2
    quart = half // 2
    n_chunk = 4
    width = half // n_chunk
    pair = 2 * width
    zt = 512
    z_steps = all_rows // zt
    mt = 512
    m_steps = rows // mt

    def kernel(z_ref, s_ref, lam_ref, zho_ref, d_ref, so_ref,
               zh, da, ck, r1, r2, g, stage, acc, got, ssem, rsem, zs, zos,
               d1s, d1r, s1s, s1r, s2s, s2r, a2s, a2r, a1s, a1r, ads, adr, dbs, das):
        here = coords()
        y, x, c = here
        on_x = c == 0
        first = tuple(jnp.where(on_x, a, b) for a, b in zip(flip(here, X_PEER), flip(here, Y_PEER)))
        second = tuple(jnp.where(on_x, a, b) for a, b in zip(flip(here, Y_PEER), flip(here, X_PEER)))
        cpeer = flip(here, C_PEER)
        bit1, bit2 = jnp.where(on_x, x, y), jnp.where(on_x, y, x)
        arrive()
        acc[...] = jnp.zeros_like(acc)

        def load(i, slot):
            return pltpu.make_async_copy(
                z_ref.at[pl.ds(pl.multiple_of(i * zt, zt), zt)],
                ck.at[pl.ds(pl.multiple_of(slot * zt, zt), zt)], zs.at[slot])

        def zh_out(v, r, i):
            at = pl.ds(pl.multiple_of(r * zt, zt), zt)
            return pltpu.make_async_copy(zh.at[v, at], zho_ref.at[v, at], zos.at[i])

        load(0, 0).start()

        def normalise(i, _):
            slot = lax.rem(i, 2)
            v, r = lax.div(i, z_steps // 2), lax.rem(i, z_steps // 2)

            @pl.when(i + 1 < z_steps)
            def _():
                load(i + 1, 1 - slot).start()

            load(i, slot).wait()
            mean, inv = mean_inv(s_ref[v], total)
            at = pl.ds(pl.multiple_of(slot * zt, zt), zt)
            zh[v, pl.ds(pl.multiple_of(r * zt, zt), zt)] = ((ck[at] - mean) * inv).astype(BF16)
            zh_out(v, r, i).start()
            return 0

        lax.fori_loop(0, z_steps, normalise, 0)
        all_arrived()

        chunk = lambda t: pl.ds(pl.multiple_of(t * pair, pair), pair)
        group = lambda t, b: pl.ds(pl.multiple_of(t * pair + b * width, width), width)

        def both(v, rows_at, t):
            return jnp.concatenate(
                [zh[v, rows_at, pl.ds(pl.multiple_of(b * half + t * width, width), width)] for b in (0, 1)], axis=1)

        every = pl.ds(0, rows)
        upper, lower = pl.ds(0, half), pl.ds(half, half)

        def to_core(t):
            return remote(da.at[lower, chunk(t)], da.at[upper, chunk(t)], d1s.at[t], d1r.at[t], cpeer)

        def to_first(t):
            return remote(ck.at[:, group(t, 1 - bit1)], r1.at[t], s1s.at[t], s1r.at[t], first)

        def to_second(t):
            return remote(ck.at[pl.ds(pl.multiple_of((1 - bit2) * quart, quart), quart), group(t, bit1)], r2.at[t],
                          s2s.at[t], s2r.at[t], second)

        def g_rows(core, b, n):
            return pl.ds(pl.multiple_of(core * half + b * quart, n), n)

        g_cols = lambda b: pl.ds(pl.multiple_of(b * width, width), width)

        def g_second(t, b):
            at = g.at[t, g_rows(c, b, quart), g_cols(bit1)]
            return remote(at, at, a2s.at[t], a2r.at[t], second)

        def g_first(t, b):
            at = g.at[t, g_rows(c, 0, half), g_cols(b)]
            return remote(at, at, a1s.at[t], a1r.at[t], first)

        def g_core(t, core):
            at = g.at[t, g_rows(core, 0, half)]
            return remote(at, at, ads.at[t], adr.at[t], cpeer)

        def chip_sum(t):
            to_core(t).wait_recv()
            ck[:, chunk(t)] += da[upper, chunk(t)]

        def corr_part(t, _):
            right = both(1, every, t)
            da[lower, chunk(t)] = mm_at(zh[0, :, pl.ds(pl.multiple_of((1 - c) * half, half), half)], right)
            ck[:, chunk(t)] = mm_at(zh[0, :, pl.ds(pl.multiple_of(c * half, half), half)], right)
            to_core(t).start()

            @pl.when(t > 0)
            def _():
                chip_sum(t - 1)

                @pl.when(t <= 2)
                def _():
                    to_first(t - 1).start()

            return 0

        lax.fori_loop(0, n_chunk, corr_part, 0)
        chip_sum(n_chunk - 1)
        for t in range(n_chunk):
            to_core(t).wait_send()

        def db_out(t, m, slot, b):
            return pltpu.make_async_copy(
                stage.at[slot, :, pl.ds(b * width, width)],
                d_ref.at[1, pl.ds(pl.multiple_of(m * mt, mt), mt),
                         pl.ds(pl.multiple_of(b * half + t * width, width), width)], dbs.at[slot, b])

        def grads(t):
            def rows_of(m, _):
                at = pl.ds(pl.multiple_of(m * mt, mt), mt)
                slot = lax.rem(m, 2)

                @pl.when(t * m_steps + m >= 2)
                def _():
                    for b in (0, 1):
                        db_out(t, m, slot, b).wait()

                db = mm(zh[0, at], g[t]) * (1.0 / total)
                stage[slot] = db
                sums = two_sums(db, db * both(1, at, t).astype(F32))
                for b in (0, 1):
                    cols = pl.ds(pl.multiple_of(b * half + t * width, width), width)
                    acc[1, 0:2, cols] += sums[:, b * width:(b + 1) * width]
                    db_out(t, m, slot, b).start()
                part = mm_bt(both(1, at, t), g[t])
                da[at] = jnp.where(t == 0, 0.0, da[at]) + part
                return 0

            lax.fori_loop(0, m_steps, rows_of, 0)

        def advance(tau, _):
            @pl.when(tau < n_chunk)
            def _():
                to_first(tau).wait_recv()
                ck[:, group(tau, bit1)] += r1[tau]
                to_second(tau).start()

                @pl.when(tau + 2 < n_chunk)
                def _():
                    to_first(tau + 2).start()

            @pl.when(jnp.logical_and(tau >= 1, tau <= n_chunk))
            def _():
                t = tau - 1
                to_second(t).wait_recv()
                corr_mat = (ck[pl.ds(pl.multiple_of(bit2 * quart, quart), quart), group(t, bit1)] + r2[t]) * (1.0 / total)
                row_ids = c * half + bit2 * quart + lax.broadcasted_iota(jnp.int32, (quart, width), 0)
                col_ids = bit1 * half + t * width + lax.broadcasted_iota(jnp.int32, (quart, width), 1)
                is_diag = row_ids == col_ids
                lam_val = lam_ref[0]
                loss = jnp.where(is_diag, (1.0 - corr_mat) * (1.0 - corr_mat), lam_val * corr_mat * corr_mat)
                acc[0, 2:3, 0:width] += jnp.sum(loss, axis=0, keepdims=True)
                grad = jnp.where(is_diag, -2.0 * (1.0 - corr_mat), 2.0 * lam_val * corr_mat).astype(BF16)
                g[t, g_rows(c, bit2, quart), g_cols(bit1)] = grad
                g_second(t, bit2).start()

            @pl.when(jnp.logical_and(tau >= 2, tau <= n_chunk + 1))
            def _():
                t = tau - 2
                g_second(t, 1 - bit2).wait_recv()
                g_first(t, bit1).start()

            @pl.when(tau >= 3)
            def _():
                t = tau - 3
                g_first(t, 1 - bit1).wait_recv()
                g_core(t, c).start()
                g_core(t, 1 - c).wait_recv()
                grads(t)

            return 0

        lax.fori_loop(0, n_chunk + 3, advance, 0)

        def da_out(m):
            at = pl.ds(pl.multiple_of(m * mt, mt), mt)
            return pltpu.make_async_copy(da.at[at], d_ref.at[0, at], das.at[m])

        def finish(m, _):
            at = pl.ds(pl.multiple_of(m * mt, mt), mt)
            d = da[at] * (1.0 / total)
            da[at] = d
            acc[0, 0:2] += two_sums(d, d * zh[0, at].astype(F32))
            da_out(m).start()
            return 0

        share(acc, got, ssem, rsem, 1)
        lax.fori_loop(0, m_steps, finish, 0)
        share(acc, got, ssem, rsem, 0)
        for t in range(n_chunk):
            to_first(t).wait_send()
            to_second(t).wait_send()
            g_second(t, bit2).wait_send()
            g_first(t, bit1).wait_send()
            g_core(t, c).wait_send()
        for b in (1, 0):
            so_ref[b] = shared(acc, got, ssem, rsem, b)
        for i in range(z_steps):
            zh_out(i // (z_steps // 2), i % (z_steps // 2), i).wait()
        for slot in (0, 1):
            for b in (0, 1):
                db_out(0, 0, slot, b).wait()
        for m in range(m_steps):
            da_out(m).wait()

    dma = pltpu.SemaphoreType.DMA
    vmem = pl.BlockSpec(memory_space=pltpu.VMEM)
    pairs = [dma((n_chunk,))] * 12
    return call_remote(
        kernel, "corr_grad", 3, (),
        [ANY, vmem, pl.BlockSpec(memory_space=pltpu.SMEM)], [ANY, ANY, vmem],
        [sds((2, rows, dim), BF16), sds((2, rows, dim), F32), sds((2, 4, dim), F32)],
        [pltpu.VMEM((2, rows, dim), BF16), pltpu.VMEM((rows, dim), F32), pltpu.VMEM((half, dim), F32),
         pltpu.VMEM((n_chunk, half, width), F32), pltpu.VMEM((n_chunk, quart, width), F32),
         pltpu.VMEM((n_chunk, dim, pair), BF16), pltpu.VMEM((2, mt, pair), F32)] + share_scratch(2, 4, dim)
        + [dma((2,)), dma((z_steps,))] + pairs + [dma((2, 2)), dma((m_steps,))],
        all_rows * dim * dim * 3, all_rows * dim * 12, (z, sums, lam), vmem=67043328)


def act_grad(d_pre, w_t, u, sums, gb, total, cid):
    all_rows, dim = d_pre.shape
    depth = w_t.shape[1]
    steps = all_rows // 2 // TM

    def kernel(d_ref, w_ref, u_ref, s_ref, gb_ref, o_ref, so_ref, acc, got, ssem, rsem):
        i = pl.program_id(0)

        @pl.when(i == 0)
        def _():
            arrive()

        mean, inv = mean_inv(s_ref[0], total)
        norm = (u_ref[...] - mean) * inv
        dx = mm(d_ref[...], w_ref[...])
        dy = jnp.where(norm * gb_ref[0:1] + gb_ref[1:2] > 0, dx, 0.0)
        o_ref[...] = dy
        add_share(i, steps, dy, dy * norm, so_ref, acc, got, ssem, rsem)

    return call_remote(
        kernel, "act_grad", cid, (2 * steps,),
        [pl.BlockSpec((TM, dim), lambda i: (i, 0)), whole((dim, depth)), pl.BlockSpec((TM, depth), lambda i: (i, 0)),
         pl.BlockSpec((1, 2, depth), lambda i: (i // steps, 0, 0)), pl.BlockSpec((2, depth), lambda i: (0, 0))],
        [pl.BlockSpec((TM, depth), lambda i: (i, 0)), pl.BlockSpec((2, 2, depth), lambda i: (0, 0, 0))],
        [sds((all_rows, depth), F32), sds((2, 2, depth), F32)], share_scratch(2, 2, depth),
        2 * all_rows * depth * dim, all_rows * (8 * depth + 2 * dim), (d_pre, w_t, u, sums, gb))


def call(kernel, name, grid, in_specs, out_specs, out_shape, flops, nbytes, pos, args, scratch=(), aliases=None):
    return pl.pallas_call(
        kernel,
        name=name,
        grid_spec=pltpu.PrefetchScalarGridSpec(
            num_scalar_prefetch=1, grid=grid, in_specs=in_specs, out_specs=out_specs, scratch_shapes=list(scratch)),
        out_shape=out_shape,
        compiler_params=pltpu.CompilerParams(
            dimension_semantics=("arbitrary",) * len(grid), vmem_limit_bytes=60 << 20),
        cost_estimate=pl.CostEstimate(flops=flops, bytes_accessed=nbytes, transcendentals=0),
        input_output_aliases=aliases or {},
    )(pos, *args)


def whole(shape):
    return pl.BlockSpec(shape, lambda *_: (0,) * len(shape), pipeline_mode=pl.Buffered(1))


def sds(shape, dtype):
    return jax.ShapeDtypeStruct(shape, dtype)


def weight_grad(pos, lefts, pre_args, pre_specs, pre_fn, name, cols_by_core, write_pre):
    dim = pre_args[0].shape[-1]
    all_rows = pre_args[0].shape[-2]
    depth = lefts[0].shape[1]
    half = dim // 2
    ksteps = all_rows // TK
    nh = half // TN

    def slab(n, p):
        mine = p[1] if cols_by_core else p[0]
        return jnp.where(n < nh, (1 - mine) * nh + n, mine * nh + n - nh)

    def kernel(pos_ref, *refs):
        left_refs, refs = refs[:len(lefts)], refs[len(lefts):]
        pre_refs, refs = refs[:len(pre_args)], refs[len(pre_args):]
        outs, refs = refs[:4], refs[4:]
        n, k = pl.program_id(0), pl.program_id(1)
        d = pre_fn(*pre_refs)
        if write_pre:
            refs[0][...] = d
        mine = pos_ref[0] if cols_by_core else pos_ref[1]
        for which, part in ((0, 1 - mine), (1, mine)):
            here = pl.ds(pl.multiple_of(part * half, half), half)
            if len(lefts) == 1:
                left = left_refs[0][pl.ds(pl.multiple_of(k * TK, TK), TK), here]
            else:
                rows = pl.ds(pl.multiple_of(k % (ksteps // 2) * TK, TK), TK)
                left = lax.select(k < ksteps // 2, left_refs[0][rows, here], left_refs[1][rows, here])
            prod = mm_at(left, d)
            for late in (0, 1):
                ref = outs[(which * 2 + late) if not cols_by_core else (late * 1 + which * 2)]

                @pl.when(jnp.logical_and((n >= nh) == bool(late), k == 0))
                def _(ref=ref):
                    ref[...] = prod

                @pl.when(jnp.logical_and((n >= nh) == bool(late), k > 0))
                def _(ref=ref):
                    ref[...] += prod

    early_col = lambda n, k, p: (0, jnp.minimum(n, nh - 1))
    late_col = lambda n, k, p: (0, jnp.maximum(n - nh, 0))
    quarter = sds((half, half), F32)
    out_specs = [pl.BlockSpec((half, TN), early_col), pl.BlockSpec((half, TN), late_col),
                 pl.BlockSpec((half, TN), early_col), pl.BlockSpec((half, TN), late_col)]
    out_shape = [quarter] * 4
    if write_pre:
        out_specs.append(pl.BlockSpec((TK, TN), lambda n, k, p: (k, slab(n, p))))
        out_shape.append(sds((all_rows, dim), BF16))
    if len(lefts) == 1:
        left_specs = [whole((all_rows, depth))]
    else:
        left_specs = [pl.BlockSpec((all_rows // 2, depth), lambda n, k, p: (p[0], 0), pipeline_mode=pl.Buffered(1))] * 2
    res = call(kernel, name, (2 * nh, ksteps), left_specs + pre_specs(slab), out_specs, out_shape,
               2 * all_rows * depth * dim, all_rows * dim * 8, pos, (*lefts, *pre_args))
    if cols_by_core:
        sent_other, kept_other, sent_own, kept_own = res[0], res[1], res[2], res[3]
    else:
        sent_other, sent_own, kept_other, kept_own = res[0], res[1], res[2], res[3]
    return (sent_other, kept_other, sent_own, kept_own), (res[4] if write_pre else None)


def solution(mesh):
    n_model, n_data = mesh.shape['model'], mesh.shape['data']
    axes = ('model', 'data')
    ids = range(n_model * n_data)
    flip_core = [(i, i ^ 1) for i in ids]
    flip_x = [(i, i ^ 2) for i in ids]
    flip_y = [(i, i ^ n_data) for i in ids]

    def send(value, perm):
        return lax.ppermute(value, axes, perm)

    def shard_body(h_a, h_b, w_one, w_two, w_three, g_one, b_one, g_two, b_two, lam_off):
        y, d = lax.axis_index('model'), lax.axis_index('data')
        x, c = d // 2, d % 2
        pos = jnp.stack([y, c]).astype(jnp.int32)
        rows = h_a.shape[0] // n_model
        total = float(h_a.shape[0] * n_data)
        dim = w_three.shape[0]
        half = dim // 2

        u1, s1, gb1, w_two_o = fwd_first(h_a, h_b, w_one, w_two, jnp.stack([g_one, b_one]))
        gb2 = jnp.stack([g_two, b_two])
        x1, u2, s2, w2_t, w_three_o = fwd_next(u1, s1, gb1, w_two, w_two_o, True, total, 1, w_three)
        x2, z, sz, w3_t = fwd_next(u2, s2, gb2, w_three, w_three_o, False, total, 2)
        zh, d_emb, s_emb = corr_grad(z, sz, lam_off, total)
        loss = jnp.sum(s_emb[0, 2])
        d_emb, s_emb = d_emb.reshape(2 * rows, dim), s_emb[:, 0:2]

        def join(own, got, bit, axis):
            return lax.select(bit == 0, jnp.concatenate([own, got], axis), jnp.concatenate([got, own], axis))

        def reduce_dw(parts, axis):
            sent_other, kept_other, sent_own, kept_own = parts
            other = kept_other + send(sent_other, flip_core)
            own = kept_own + send(sent_own, flip_core)
            chunks = 2
            size = half // chunks
            done = []
            for j in range(chunks):
                cut = lambda v: lax.slice_in_dim(v, j * size, (j + 1) * size, axis=0)
                mine = cut(own) + send(cut(other), flip_y)
                done.append(mine + send(mine, flip_x))
            mine = jnp.concatenate(done, 0)
            return join(mine, send(mine, flip_core), c, axis)

        col_spec = lambda slab: pl.BlockSpec((TK, TN), lambda n, k, p: (k, slab(n, p)))
        view = lambda k: k // (2 * rows // TK // 2)
        sum_spec = lambda slab: pl.BlockSpec((1, 2, TN), lambda n, k, p: (view(k), 0, slab(n, p)))
        vec_spec = lambda slab: pl.BlockSpec((1, TN), lambda n, k, p: (0, slab(n, p)))

        def out_pre(d_ref, zh_ref, sz_ref, sd_ref):
            _, inv = mean_inv(sz_ref[0], total)
            sd = sd_ref[0]
            return (inv * (d_ref[...] - sd[0:1] / total - zh_ref[...].astype(F32) * (sd[1:2] / total))).astype(BF16)

        parts3, d_out = weight_grad(
            pos, (x2,), (d_emb, zh.reshape(2 * rows, dim), sz, s_emb),
            lambda slab: [col_spec(slab), col_spec(slab), sum_spec(slab), sum_spec(slab)], out_pre, "dw_three", False, True)
        dw_three = reduce_dw(parts3, 0)

        def bn_pre(d_ref, u_ref, su_ref, sd_ref, g_ref):
            mean, inv = mean_inv(su_ref[0], total)
            sd = sd_ref[0]
            norm = (u_ref[...] - mean) * inv
            return (g_ref[...] * inv * (d_ref[...] - (sd[0:1] + norm * sd[1:2]) / total)).astype(BF16)

        bn_specs = lambda slab: [col_spec(slab), col_spec(slab), sum_spec(slab), sum_spec(slab), vec_spec(slab)]
        dy2, sd2 = act_grad(d_out, w3_t, u2, s2, gb2, total, 4)
        parts2, d_pre_two = weight_grad(
            pos, (x1,), (dy2, u2, s2, sd2, gb2[0:1]), bn_specs, bn_pre, "dw_two", True, True)
        dw_two = reduce_dw(parts2, 1)
        dy1, sd1 = act_grad(d_pre_two, w2_t, u1, s1, gb1, total, 5)
        parts1, _ = weight_grad(
            pos, (h_a, h_b), (dy1, u1, s1, sd1, gb1[0:1]), bn_specs, bn_pre, "dw_one", False, False)
        dw_one = reduce_dw(parts1, 0)

        sum1 = lax.dynamic_slice_in_dim(jnp.sum(sd1, 0), y * half, half, 1)
        sum2 = jnp.sum(sd2, 0)
        return loss.reshape(1), dw_one, dw_two, dw_three, sum1[1], sum1[0], sum2[1], sum2[0]

    in_specs = (P('data', None), P('data', None), P(None, 'model'), P('model', None), P(None, 'model'),
                P('model'), P('model'), P(), P(), P())
    out_specs = (P(), P(None, 'model'), P('model', None), P(None, 'model'), P('model'), P('model'), P(), P())
    return jax.shard_map(shard_body, mesh=mesh, in_specs=in_specs, out_specs=out_specs, check_vma=False)
```

```python
import jax
import jax.numpy as jnp
from jax import lax
from jax.experimental import pallas as pl
from jax.experimental.pallas import tpu as pltpu
from jax.sharding import PartitionSpec as P

BN_EPS = 1e-5
F32 = jnp.float32
BF16 = jnp.bfloat16
TM = 512
MAX_VMEM = 67043328
ANY = pl.BlockSpec(memory_space=pl.ANY)
VMEM = pl.BlockSpec(memory_space=pltpu.VMEM)
DMA = pltpu.SemaphoreType.DMA
TWO_DMA = DMA((2,))
BOTH = (0, 1)
PEERS = [(ky, kx, kc) for ky in BOTH for kx in BOTH for kc in BOTH][1:]
C_PEER, X_PEER, Y_PEER = PEERS[0], PEERS[1], PEERS[3]
N_DEV = len(PEERS) + 1


def mm(left, right):
    return jnp.dot(left, right, preferred_element_type=F32)


def mm_bt(left, right):
    return lax.dot_general(left, right, (((1,), (1,)), ((), ())), preferred_element_type=F32)


def mm_at(left, right):
    return lax.dot_general(left, right, (((0,), (0,)), ((), ())), preferred_element_type=F32)


def other(p):
    return 1 - p


def odd(i):
    return lax.rem(i, 2)


def split(i):
    return lax.div(i, 2), odd(i)


def loop(n, body, start=0):
    def one(i, carry):
        body(i)
        return carry

    lax.fori_loop(start, n, one, 0)


def whole(*shape):
    return pl.BlockSpec(shape, lambda *_: (0,) * len(shape))


def at(i, n):
    return pl.ds(pl.multiple_of(i * n, n), n)


def sds(shape, dtype):
    return jax.ShapeDtypeStruct(shape, dtype)


def mean_inv(sums, total):
    mean = sums[:1] / total
    var = sums[1:2] / total - mean * mean
    return mean, lax.rsqrt(var + BN_EPS)


def two_sums(one, two):
    return jnp.concatenate([jnp.sum(one, axis=0, keepdims=True), jnp.sum(two, axis=0, keepdims=True)], axis=0)


def coords():
    y, d = lax.axis_index('model'), lax.axis_index('data')
    return y, lax.div(d, 2), odd(d)


def flip(here, which):
    return tuple(other(p) if f else p for p, f in zip(here, which))


def flat(here):
    y, x, c = here
    return 4 * y + 2 * x + c


def device(here):
    y, x, c = here
    return (y, 2 * x + c)


def remote(src, dst, send_sem, recv_sem, there):
    return pltpu.make_async_remote_copy(
        src_ref=src, dst_ref=dst, send_sem=send_sem, recv_sem=recv_sem, device_id=device(there),
        device_id_type=pl.DeviceIdType.MESH)


def arrive():
    here = coords()
    for k in PEERS:
        pl.semaphore_signal(pltpu.get_barrier_semaphore(), inc=1, device_id=device(flip(here, k)),
                            device_id_type=pl.DeviceIdType.MESH)


def all_arrived():
    pl.semaphore_wait(pltpu.get_barrier_semaphore(), len(PEERS))


class Share:
    def __init__(self, acc, got, send_sem, recv_sem):
        self.acc, self.got, self.send_sem, self.recv_sem = acc, got, send_sem, recv_sem

    @staticmethod
    def scratch(n, *shape):
        return [pltpu.VMEM((n, *shape), F32), pltpu.VMEM((n, N_DEV, *shape), F32), DMA((n,)), DMA((n,))]

    def start(self, b):
        here = coords()
        me = flat(here)
        self.got[b, me] = self.acc[b]
        for which in PEERS:
            remote(self.acc.at[b], self.got.at[b, me], self.send_sem.at[b], self.recv_sem.at[b],
                   flip(here, which)).start()

    def total(self, b):
        all_of = self.got.at[b, pl.ds(0, len(PEERS))]
        copies = remote(all_of, all_of, self.send_sem.at[b], self.recv_sem.at[b], coords())
        copies.wait_send()
        copies.wait_recv()
        out = self.got[b, 0]
        for f in range(1, N_DEV):
            out += self.got[b, f]
        return out


class Gather:
    def __init__(self, own, dest, n, sems):
        self.own, self.dest, self.n = own, dest, n
        self.ys, self.yr, self.xs, self.xr, self.cs, self.cr = sems
        self.here = coords()
        _, x, c = self.here
        self.mine, self.across = 2 * x + c, 2 * (other(x)) + c
        self.core = (2 * x + other(c), 2 * (other(x)) + other(c))

    @staticmethod
    def scratch(n):
        return [DMA((n,))] * 4 + [DMA((2, n))] * 2

    def y(self, p):
        model = self.here[0]
        return remote(self.own(self.mine, p), self.dest(model, self.mine, p), self.ys.at[p], self.yr.at[p],
                      flip(self.here, Y_PEER))

    def moved(self, q, p, send_sem, recv_sem, which):
        ref = self.dest(1 - self.here[0], q, p)
        return remote(ref, ref, send_sem, recv_sem, flip(self.here, which))

    def x(self, p, q):
        return self.moved(q, p, self.xs.at[p], self.xr.at[p], X_PEER)

    def c(self, p, late, q):
        return self.moved(q, p, self.cs.at[late, p], self.cr.at[late, p], C_PEER)

    def start(self):
        for p in range(self.n):
            self.y(p).start()

    def pass_y(self, p):
        self.moved(self.mine, p, self.ys.at[p], self.yr.at[p], Y_PEER).wait_recv()
        self.x(p, self.mine).start()
        self.c(p, 0, self.mine).start()

    def pass_x(self, p):
        self.x(p, self.across).wait_recv()
        self.c(p, 1, self.across).start()

    def wait_core(self, late):
        for p in range(self.n):
            self.c(p, late, self.core[late]).wait_recv()

    def drain(self):
        for p in range(self.n):
            self.y(p).wait_send()
            self.x(p, self.mine).wait_send()
            self.c(p, 0, self.mine).wait_send()
            self.c(p, 1, self.across).wait_send()


def call(kernel, name, cid, grid, in_specs, out_specs, out_shape, scratch, flops, nbytes, args):
    return pl.pallas_call(
        kernel, name=name, grid=grid, in_specs=in_specs, out_specs=out_specs, out_shape=out_shape, scratch_shapes=scratch,
        compiler_params=pltpu.CompilerParams(vmem_limit_bytes=MAX_VMEM, collective_id=cid, has_side_effects=cid is not None),
        cost_estimate=pl.CostEstimate(flops=flops, bytes_accessed=nbytes, transcendentals=0))(*args)


def fwd_first(h_a, h_b, w_one, w_two, gb_own):
    depth, half = w_one.shape
    dim = 2 * half
    rows = h_a.shape[0] // 2
    tile, width, quarter = 2 * TM, half // 2, half // 4
    steps = rows // tile
    per_block = 2 * steps
    n = 4

    def block(j):
        y, x, _ = coords()
        return jnp.where(j < 2, 2 * y + j, 2 * (other(y)) + jnp.where(j == 2, x, other(x)))

    def kernel(ha_ref, hb_ref, w_ref, w2_ref, gb_ref, u_ref, s_ref, gbo_ref, w2o_ref, w1, gbf, *sems):
        share, sems = Share(*sems[:4]), sems[4:]
        gs, gr, lsem = sems[:3]
        sems = sems[3:]
        j, i = pl.program_id(0), pl.program_id(1)
        step = j * per_block + i
        here = coords()
        y = here[0]
        one = Gather(lambda q, p: w_ref.at[at(p, depth // n), at(q, quarter)],
                     lambda m, q, p: w1.at[at(p, depth // n), at(m * 4 + q, quarter)], n, sems[:6])
        two = Gather(lambda q, p: w2_ref.at[at(q * n + p, quarter // n)],
                     lambda m, q, p: w2o_ref.at[at(q * n + p, quarter // n)], n, sems[6:])

        def local(b):
            return pltpu.make_async_copy(w_ref.at[:, at(b, width)], w1.at[:, at(2 * y + b, width)], lsem.at[b])

        def bn_vectors(m):
            return remote(gb_ref, gbf.at[:, at(m, half)], gs, gr, flip(here, Y_PEER))

        def begin():
            arrive()
            local(0).start()
            local(1).start()
            all_arrived()
            one.start()
            two.start()
            bn_vectors(y).start()
            local(0).wait()

        def late_half():
            for p in range(2, n):
                one.pass_y(p)
            one.pass_x(0)
            one.pass_x(1)
            one.wait_core(0)

        def between():
            one.pass_x(2)
            two.pass_y(0)

        def last_block():
            one.pass_x(n - 1)
            one.wait_core(1)
            two.pass_y(1)
            two.pass_x(0)

        hooks = {0: begin, 3: lambda: one.pass_y(0), per_block: lambda: local(1).wait(), 6: lambda: one.pass_y(1),
                 2 * per_block: late_half, 10: between, 3 * per_block: last_block,
                 14: lambda: two.pass_y(2), 15: lambda: two.pass_x(1)}
        for s in sorted(hooks):
            pl.when(step == s)(hooks[s])
        for b in range(3):
            pl.when(step == (b + 1) * per_block)(lambda b=b: share.start(block(b)))

        h = lax.select(i < steps, ha_ref[...], hb_ref[...])
        u = mm(h, w1[:, at(block(j), width)])
        u_ref[...] = u
        sums = two_sums(u, u * u)
        v = i // steps
        share.acc[block(j), v] = jnp.where(i % steps == 0, 0.0, share.acc[block(j), v]) + sums

        @pl.when(step == 4 * per_block - 1)
        def _():
            share.start(block(3))
            two.pass_y(n - 1)
            for p in range(2, n):
                two.pass_x(p)
            bn_vectors(other(y)).wait_recv()
            bn_vectors(y).wait_send()
            gbo_ref[...] = gbf[...]
            gbo_ref[:, at(y, half)] = gb_ref[...]
            for b in range(4):
                s_ref[:, :, b * width:(b + 1) * width] = share.total(b)
            one.drain()
            two.drain()
            two.wait_core(0)
            two.wait_core(1)

    return call(
        kernel, "fwd_first", 0, (4, per_block),
        [pl.BlockSpec((tile, depth), lambda j, i: (coords()[0] * steps + jnp.minimum(i, steps - 1), 0)),
         pl.BlockSpec((tile, depth), lambda j, i: (coords()[0] * steps + jnp.maximum(i - steps, 0), 0)),
         ANY, ANY, whole(2, half)],
        [pl.BlockSpec((tile, width), lambda j, i: (i, block(j))), whole(2, 2, dim),
         whole(2, dim), ANY],
        [sds((2 * rows, dim), F32), sds((2, 2, dim), F32), sds((2, dim), F32), sds((half, dim), BF16)],
        [pltpu.VMEM((depth, dim), BF16), pltpu.VMEM((2, dim), F32)] + Share.scratch(4, 2, 2, width)
        + [DMA, DMA, TWO_DMA] + Gather.scratch(n) * 2,
        4 * rows * depth * dim, 2 * rows * (8 * depth + 4 * dim), (h_a, h_b, w_one, w_two, gb_own))


def fwd_next(u, sums, gb, w_own, w_other, by_rows, total, cid, w_next=None):
    all_rows, depth = u.shape
    dim = w_own.shape[1] if by_rows else 2 * w_own.shape[1]
    half = dim // 2
    quarter = half // 4
    steps = all_rows // 2 // TM
    last = 2 * steps - 1
    slab = dim // (2 * steps)
    n = 4

    def kernel(u_ref, s_ref, gb_ref, wo_ref, wt_ref, *refs):
        if w_next is not None:
            wn_ref, refs = refs[0], refs[1:]
        x_ref, o_ref, so_ref, wtr_ref, *refs = refs
        if w_next is not None:
            wno_ref, *refs = refs
        w, acc, got, ssem, rsem, lsem, *refs = refs
        share = Share(acc, got, ssem, rsem)
        i = pl.program_id(0)
        y = coords()[0]

        def local(ref, model, b):
            where = at(model, half)
            return pltpu.make_async_copy(ref, w.at[where] if by_rows else w.at[:, where], lsem.at[b])

        if w_next is not None:
            gather = Gather(lambda q, p: wn_ref.at[at(p, depth // n), at(q, quarter)],
                            lambda m, q, p: wno_ref.at[at(p, depth // n), at(q, quarter)], n, refs)

        @pl.when(i == 0)
        def _():
            arrive()
            local(wo_ref, y, 0).start()
            local(wt_ref, other(y), 1).start()
            all_arrived()
            if w_next is not None:
                gather.start()
            local(wo_ref, y, 0).wait()
            local(wt_ref, other(y), 1).wait()

        if w_next is not None:
            for p in range(n):
                pl.when(i == p + 1)(lambda p=p: gather.pass_y(p))
                pl.when(i == p + 3)(lambda p=p: gather.pass_x(p))
        pl.when(i == steps)(lambda: share.start(0))

        mean, inv = mean_inv(s_ref[0], total)
        act = jnp.maximum((u_ref[...] - mean) * inv * gb_ref[:1] + gb_ref[1:], 0.0).astype(BF16)
        x_ref[...] = act
        out = mm(act, w[...])
        o_ref[...] = out
        wtr_ref[...] = w[:, at(i, slab)].T
        v = i // steps
        share.acc[v] = jnp.where(i % steps == 0, 0.0, share.acc[v]) + two_sums(out, out * out)

        @pl.when(i == last)
        def _():
            share.start(1)
            for b in BOTH:
                so_ref[b] = share.total(b)
            if w_next is not None:
                gather.drain()
                gather.wait_core(0)
                gather.wait_core(1)

    more = w_next is not None
    return call(
        kernel, "fwd_next", cid, (2 * steps,),
        [pl.BlockSpec((TM, depth), lambda i: (i, 0)), pl.BlockSpec((1, 2, depth), lambda i: (i // steps, 0, 0)),
         whole(2, depth), ANY, ANY] + [ANY] * more,
        [pl.BlockSpec((TM, depth), lambda i: (i, 0)), pl.BlockSpec((TM, dim), lambda i: (i, 0)),
         whole(2, 2, dim), pl.BlockSpec((slab, depth), lambda i: (i, 0))] + [ANY] * more,
        [sds((all_rows, depth), BF16), sds((all_rows, dim), F32), sds((2, 2, dim), F32), sds((dim, depth), BF16)]
        + ([sds(w_next.shape, BF16)] if more else []),
        [pltpu.VMEM((depth, dim), BF16)] + Share.scratch(2, 2, dim) + [TWO_DMA] + (Gather.scratch(n) if more else []),
        2 * all_rows * depth * dim, all_rows * (6 * depth + 4 * dim),
        (u, sums, gb, w_own, w_other) + ((w_next,) if more else ()))


def corr_grad(z, sums, lam, total):
    all_rows, dim = z.shape
    rows = all_rows // 2
    half = dim // 2
    quart = half // 2
    n_chunk = 8
    width = half // n_chunk
    pair = 2 * width
    zt = mt = TM
    z_steps = all_rows // zt
    m_steps = rows // mt
    scale = 1.0 / total

    def kernel(z_ref, s_ref, lam_ref, zho_ref, d_ref, so_ref, zh, da, ck, r1, r2, g, stage, acc, got, ssem, rsem, zs, zos,
               d1s, d1r, s1s, s1r, s2s, s2r, a2s, a2r, a1s, a1r, ads, adr, dbs, das):
        share = Share(acc, got, ssem, rsem)
        here = coords()
        y, x, c = here
        on_x = c == 0
        by_core = lambda one, two: tuple(jnp.where(on_x, a, b) for a, b in zip(one, two))
        first = by_core(flip(here, X_PEER), flip(here, Y_PEER))
        second = by_core(flip(here, Y_PEER), flip(here, X_PEER))
        cpeer = flip(here, C_PEER)
        bit1, bit2 = by_core((x, y), (y, x))
        arrive()
        acc[...] = jnp.zeros_like(acc)

        def load(i, slot):
            return pltpu.make_async_copy(z_ref.at[at(i, zt)], ck.at[at(slot, zt)], zs.at[slot])

        def zh_out(v, r, i):
            return pltpu.make_async_copy(zh.at[v, at(r, zt)], zho_ref.at[v, at(r, zt)], zos.at[i])

        load(0, 0).start()

        def normalise(i):
            slot = odd(i)
            v, r = lax.div(i, z_steps // 2), lax.rem(i, z_steps // 2)
            pl.when(i + 1 < z_steps)(lambda: load(i + 1, other(slot)).start())
            load(i, slot).wait()
            mean, inv = mean_inv(s_ref[v], total)
            zh[v, at(r, zt)] = ((ck[at(slot, zt)] - mean) * inv).astype(BF16)
            zh_out(v, r, i).start()

        loop(z_steps, normalise)
        all_arrived()

        def both(v, rows_at, t):
            return jnp.concatenate([zh[v, rows_at, at(b * n_chunk + t, width)] for b in BOTH], axis=1)

        every, upper, lower = pl.ds(0, rows), pl.ds(0, half), pl.ds(half, half)
        group = lambda t, b: at(2 * t + b, width)

        def to_core(t):
            return remote(da.at[lower, at(t, pair)], da.at[upper, at(t, pair)], d1s.at[t], d1r.at[t], cpeer)

        def to_first(t):
            return remote(ck.at[:, group(t, other(bit1))], r1.at[t], s1s.at[t], s1r.at[t], first)

        def to_second(t):
            return remote(ck.at[at(other(bit2), quart), group(t, bit1)], r2.at[t], s2s.at[t], s2r.at[t], second)

        def g_second(t, b):
            block = g.at[t, at(2 * c + b, quart), at(bit1, width)]
            return remote(block, block, a2s.at[t], a2r.at[t], second)

        def g_first(t, b):
            block = g.at[t, at(c, half), at(b, width)]
            return remote(block, block, a1s.at[t], a1r.at[t], first)

        def g_core(t, core):
            block = g.at[t, at(core, half)]
            return remote(block, block, ads.at[t], adr.at[t], cpeer)

        def chip_sum(t):
            to_core(t).wait_recv()
            ck[:, at(t, pair)] += da[upper, at(t, pair)]

        def corr_part(t):
            right = both(1, every, t)
            da[lower, at(t, pair)] = mm_at(zh[0, :, at(other(c), half)], right)
            ck[:, at(t, pair)] = mm_at(zh[0, :, at(c, half)], right)
            to_core(t).start()

            @pl.when(t > 0)
            def _():
                chip_sum(t - 1)
                pl.when(t <= 2)(lambda: to_first(t - 1).start())


        loop(n_chunk, corr_part)
        chip_sum(n_chunk - 1)
        for t in range(n_chunk):
            to_core(t).wait_send()

        def db_out(t, m, slot, b):
            return pltpu.make_async_copy(
                stage.at[slot, :, at(b, width)], d_ref.at[1, at(m, mt), at(b * n_chunk + t, width)], dbs.at[slot, b])

        def grads(t):
            def rows_of(m):
                slot = odd(m)

                @pl.when(t * m_steps + m >= 2)
                def _():
                    for b in BOTH:
                        db_out(t, m, slot, b).wait()

                db = mm(zh[0, at(m, mt)], g[t]) * scale
                stage[slot] = db
                own = both(1, at(m, mt), t)
                sums = two_sums(db, db * own.astype(F32))
                for b in BOTH:
                    acc[1, :2, at(b * n_chunk + t, width)] += sums[:, b * width:(b + 1) * width]
                    db_out(t, m, slot, b).start()
                da[at(m, mt)] = jnp.where(t == 0, 0.0, da[at(m, mt)]) + mm_bt(own, g[t])

            loop(m_steps, rows_of)

        def at_first(t):
            to_first(t).wait_recv()
            ck[:, group(t, bit1)] += r1[t]
            to_second(t).start()
            pl.when(t + 2 < n_chunk)(lambda: to_first(t + 2).start())

        def at_second(t):
            to_second(t).wait_recv()
            corr_mat = (ck[at(bit2, quart), group(t, bit1)] + r2[t]) * scale
            row_ids = (2 * c + bit2) * quart + lax.broadcasted_iota(jnp.int32, (quart, width), 0)
            col_ids = (bit1 * n_chunk + t) * width + lax.broadcasted_iota(jnp.int32, (quart, width), 1)
            is_diag = row_ids == col_ids
            lam_val = lam_ref[0]
            loss = jnp.where(is_diag, (1.0 - corr_mat) * (1.0 - corr_mat), lam_val * corr_mat * corr_mat)
            acc[0, 2:3, :width] += jnp.sum(loss, axis=0, keepdims=True)
            grad = jnp.where(is_diag, -2.0 * (1.0 - corr_mat), 2.0 * lam_val * corr_mat).astype(BF16)
            g[t, at(2 * c + bit2, quart), at(bit1, width)] = grad
            g_second(t, bit2).start()

        def back_second(t):
            g_second(t, other(bit2)).wait_recv()
            g_first(t, bit1).start()

        def back_first(t):
            g_first(t, other(bit1)).wait_recv()
            g_core(t, c).start()

        def back_core(t):
            g_core(t, other(c)).wait_recv()
            grads(t)

        stages = (at_first, at_second, back_second, back_first, back_core)

        def advance(tau):
            for lag, stage_fn in enumerate(stages):
                t = tau - lag
                pl.when(jnp.logical_and(t >= 0, t < n_chunk))(lambda t=t, stage_fn=stage_fn: stage_fn(t))

        loop(n_chunk + len(stages) - 1, advance)

        def da_out(m):
            return pltpu.make_async_copy(da.at[at(m, mt)], d_ref.at[0, at(m, mt)], das.at[m])

        def finish(m):
            d = da[at(m, mt)] * scale
            da[at(m, mt)] = d
            acc[0, :2] += two_sums(d, d * zh[0, at(m, mt)].astype(F32))
            da_out(m).start()

        share.start(1)
        loop(m_steps, finish)
        share.start(0)
        for t in range(n_chunk):
            for copy in (to_first(t), to_second(t), g_second(t, bit2), g_first(t, bit1), g_core(t, c)):
                copy.wait_send()
        for b in BOTH:
            so_ref[b] = share.total(b)
            for slot in BOTH:
                db_out(0, 0, slot, b).wait()
        for i in range(z_steps):
            zh_out(i // (z_steps // 2), i % (z_steps // 2), i).wait()
        for m in range(m_steps):
            da_out(m).wait()

    return call(
        kernel, "corr_grad", 3, (), [ANY, VMEM, pl.BlockSpec(memory_space=pltpu.SMEM)], [ANY, ANY, VMEM],
        [sds((2, rows, dim), BF16), sds((2, rows, dim), F32), sds((2, 4, dim), F32)],
        [pltpu.VMEM((2, rows, dim), BF16), pltpu.VMEM((rows, dim), F32), pltpu.VMEM((half, dim), F32),
         pltpu.VMEM((n_chunk, half, width), F32), pltpu.VMEM((n_chunk, quart, width), F32),
         pltpu.VMEM((n_chunk, dim, pair), BF16), pltpu.VMEM((2, mt, pair), F32)] + Share.scratch(2, 4, dim)
        + [TWO_DMA, DMA((z_steps,))] + [DMA((n_chunk,))] * 12 + [DMA((2, 2)), DMA((m_steps,))],
        all_rows * dim * dim * 3, all_rows * dim * 12, (z, sums, lam))


def backward(d_emb, zh, sz, s_emb, layers, x2, h_a, h_b, total):
    all_rows, dim = zh.shape
    rows, half = all_rows // 2, dim // 2
    width = 256
    slabs = dim // width
    items = 2 * slabs
    piece = half // 2
    n_layer = len(layers) + 1
    n_chunk = n_layer * slabs
    (u2, s2, gb2, w3_t, x1), (u1, s1, gb1, w2_t, _) = layers

    def kernel(d_ref, zh_ref, sz_ref, sd_ref, x2_ref, x1_ref, ha_ref, hb_ref, u2_ref, u1_ref, w3_ref, w2_ref,
               s2_ref, s1_ref, gb2_ref, gb1_ref, dw3_ref, dw2_ref, dw1_ref, sum_ref, du_ref, part_ref, ry_ref, rx_ref,
               dbuf, xbuf, wbuf, ubuf, dybuf, dubuf, psend, pkeep, dr, ebuf, mbuf, fbuf, acc, got, ssem, rsem,
               us, ws, xl, dl, dus, ps, pr, pm, ys, yr, xs, xr, es, fs, fcs, fcr, credit):
        share = Share(acc, got, ssem, rsem)
        here = coords()
        y, x, c = here
        ypeer, xpeer, cpeer = flip(here, Y_PEER), flip(here, X_PEER), flip(here, C_PEER)
        arrive()

        def column(k, n):
            side = odd(n + jnp.where(k == 0, other(y), 0))
            return jnp.where(k == 1, n, side * (slabs // 2) + lax.div(n, 2))

        def turn(k):
            return jnp.where(k == 0, 0, other(y))

        def m_slot(j):
            return lax.rem(j, 4)

        def copy(src, dst, sem):
            return pltpu.make_async_copy(src, dst, sem)

        def to_core(s):
            return remote(psend.at[odd(s)], dr.at[odd(s)], ps.at[s], pr.at[s], cpeer)

        def keep_out(s):
            return copy(pkeep.at[odd(s)], part_ref.at[s], pm)

        def chip_sum(s):
            slot = odd(s)
            to_core(s).wait_recv()
            pkeep[slot] += dr[slot]

            @pl.when(s + 2 < n_chunk)
            def _():
                pl.semaphore_signal(credit, inc=1, device_id=device(cpeer), device_id_type=pl.DeviceIdType.MESH)

            to_core(s).wait_send()
            keep_out(s).start()

        def to_y(src, j):
            return remote(src, ry_ref.at[j], ys.at[lax.div(j, slabs)], yr.at[j], ypeer)

        def issue(s):
            keep_out(s).wait()
            k = lax.div(s, slabs)

            @pl.when(k == 1)
            def _():
                to_y(part_ref.at[s, at(other(y), piece)], s).start()

            @pl.when(jnp.logical_and(k != 1, odd(s) == turn(k)))
            def _():
                for b in BOTH:
                    to_y(part_ref.at[s, at(b, piece)], s - turn(k) + b).start()

        def to_x(j):
            return remote(mbuf.at[m_slot(j)], rx_ref.at[j], xs.at[m_slot(j)], xr.at[j], xpeer)

        def result(j, k):
            j = lax.rem(j, slabs)
            if k == 1:
                return dw2_ref.at[at(c, piece), at(j, width)]
            return (dw1_ref if k else dw3_ref).at[at(2 * c + odd(j), piece), at(lax.div(j, 2), width)]

        def put(j, k):
            slot = odd(j)
            return (copy(fbuf.at[slot], result(j, k), fs.at[slot]),
                    remote(fbuf.at[slot], result(j, k), fcs.at[slot], fcr.at[k], cpeer))

        def put_done(j):
            here_copy, there_copy = put(j, 0)
            here_copy.wait()
            there_copy.wait_send()

        def load_y(j):
            return copy(ry_ref.at[j], ebuf.at[0], es.at[0])

        def load_own(j):
            k = lax.div(j, slabs)
            s = jnp.where(k == 1, j, 2 * lax.div(j, 2) + 1 - turn(k))
            row = jnp.where(k == 1, y, odd(j))
            return copy(part_ref.at[s, at(row, piece)], ebuf.at[1], es.at[1])

        def load_x(j):
            return copy(rx_ref.at[j], ebuf.at[2], es.at[2])

        def fetch_x(j):
            to_x(j).wait_recv()
            load_x(j).start()

        def begin(j):
            to_y(ry_ref.at[j], j).wait_recv()
            load_y(j).start()
            load_own(j).start()
            pl.when(j >= 2)(lambda: fetch_x(j - 2))

        def deliver(j):
            load_x(j).wait()

            pl.when(j >= 2)(lambda: put_done(j))
            slot = odd(j)
            fbuf[slot] = mbuf[m_slot(j)] + ebuf[2]
            for k in range(n_layer):
                @pl.when(lax.div(j, slabs) == k)
                def _(k=k):
                    for one in put(j, k):
                        one.start()

        def end(j):
            load_y(j).wait()
            load_own(j).wait()
            pl.when(j >= 4)(lambda: to_x(j).wait_send())
            mbuf[m_slot(j)] = ebuf[0] + ebuf[1]
            to_x(j).start()
            pl.when(j >= 2)(lambda: deliver(j - 2))

        def begun(q):
            early = jnp.maximum(lax.div(q - 1, 4) - 1, 0)
            late = 2 + lax.div(4 * (q - items) + 5, 9)
            return jnp.where(q < items, early, late)

        def events(q):
            now, before, earlier = begun(q), begun(q - 1), begun(q - 2)
            pl.when(before > earlier)(lambda: end(before - 1))
            pl.when(now > before)(lambda: begin(now - 1))

        def left(v, natural, part):
            first = jnp.where(natural, part, 2 * part)
            second = jnp.where(natural, 2 + part, 2 * part + 1)
            return jnp.concatenate([xbuf[at(v, rows), at(b, piece)] for b in (first, second)], axis=1)

        def weight_slab(s, v, natural, d):
            slot = odd(s)
            pl.when(jnp.logical_and(v == 0, s > 0))(lambda: chip_sum(s - 1))
            pl.when(jnp.logical_and(v == 1, s > 0))(lambda: issue(s - 1))
            for buf, part in ((psend, other(c)), (pkeep, c)):
                buf[slot] = jnp.where(v == 0, 0.0, buf[slot]) + mm_at(left(v, natural, part), d)

            @pl.when(v == 1)
            def _():
                pl.when(s >= 2)(lambda: pl.semaphore_wait(credit, 1))
                to_core(s).start()

        def emb_loads(i):
            n, v = split(i)
            cols = at(column(0, n), width)
            return (copy(d_ref.at[at(v, rows), cols], ubuf.at[v], us.at[v]),
                    copy(zh_ref.at[at(v, rows), cols], wbuf.at[v], ws.at[v]))

        def x_load(src, v, src_at):
            return copy(src.at[at(src_at, rows)], xbuf.at[at(v, rows)], xl.at[v])

        def u_load(layer, i, ref=u2_ref):
            slot = lax.rem(layer * items + i, 3)
            n, v = split(i)
            cols = at(column(layer + 1, n), width)
            return copy(ref.at[at(v, rows), cols], ubuf.at[slot], us.at[slot])

        def w_load(layer, n, ref=w3_ref):
            slot = odd(n)
            return copy(ref.at[:, at(column(layer + 1, n), width)], wbuf.at[slot], ws.at[slot])

        def start_u(layer, i):
            for k, ref in enumerate((u2_ref, u1_ref)):
                pl.when(layer == k)(lambda ref=ref: u_load(layer, i, ref).start())

        def start_w(layer, n):
            for k, ref in enumerate((w3_ref, w2_ref)):
                pl.when(layer == k)(lambda ref=ref: w_load(layer, n, ref).start())

        x_load(x2_ref, 0, 0).start()
        for one in emb_loads(0):
            one.start()
        x_load(x2_ref, 1, 1).start()
        all_arrived()

        def emb_item(i):
            n, v = split(i)

            @pl.when(i + 1 < items)
            def _():
                for one in emb_loads(i + 1):
                    one.start()

            @pl.when(i + 1 == items)
            def _():
                u_load(0, 0).start()
                w_load(0, 0).start()

            pl.when(i < 2)(lambda: x_load(x2_ref, v, v).wait())
            for one in emb_loads(i):
                one.wait()
            events(i)
            cols = at(column(0, n), width)
            _, inv = mean_inv(sz_ref[v, :, cols], total)
            sd = sd_ref[v, :2, cols] / total
            d = (inv * (ubuf[v] - sd[:1] - wbuf[v].astype(F32) * sd[1:])).astype(BF16)
            dbuf[at(v, rows), cols] = d
            weight_slab(n, v, False, d)

        loop(items, emb_item)
        for v in BOTH:
            x_load(x1_ref, v, v).start()

        def du_out(i):
            n, v = split(i)
            return copy(dubuf.at[v], du_ref.at[at(v, rows), at(n, width)], dus.at[v])

        most = pl.ds(0, dim - width)
        d_reload = lambda: copy(du_ref.at[:, most], dbuf.at[:, most], dl)

        def stats(layer, v, cols):
            pick = lambda one, two: jnp.where(layer == 0, one, two)
            mean, inv = mean_inv(pick(s2_ref[v, :, cols], s1_ref[v, :, cols]), total)
            gb = pick(gb2_ref[:, cols], gb1_ref[:, cols])
            return mean, inv, gb[:1], gb[1:]

        def step(layer, s):
            natural = layer == 0

            @pl.when(s < items)
            def _():
                i = s
                n, v = split(i)
                g = layer * items + i
                cols = at(column(layer + 1, n), width)
                pl.when(i + 1 < items)(lambda: start_u(layer, i + 1))
                pl.when(jnp.logical_and(v == 0, n + 1 < slabs))(lambda: start_w(layer, n + 1))

                @pl.when(jnp.logical_and(i + 1 == items, natural))
                def _():
                    u_load(1, 0, u1_ref).start()
                    w_load(1, 0, w2_ref).start()

                pl.when(jnp.logical_and(i == 0, layer == 1))(lambda: d_reload().wait())
                u_load(layer, i).wait()
                pl.when(v == 0)(lambda: w_load(layer, n).wait())
                dx = mm(dbuf[at(v, rows)], wbuf[odd(n)])
                mean, inv, gamma, beta = stats(layer, v, cols)
                norm = (ubuf[lax.rem(g, 3)] - mean) * inv
                dy = jnp.where(norm * gamma + beta > 0, dx, 0.0)
                dybuf[v] = dy
                acc[g] = two_sums(dy, dy * norm)
                share.start(g)

                @pl.when(jnp.logical_and(i + 1 == items, natural))
                def _():
                    for one in BOTH:
                        du_out(one).wait()
                    d_reload().start()

            @pl.when(s > 0)
            def _():
                i = s - 1
                n, v = split(i)
                g = layer * items + i
                cols = at(column(layer + 1, n), width)
                pl.when(jnp.logical_and(n == 0, natural))(lambda: x_load(x1_ref, v, v).wait())
                pl.when(jnp.logical_and(n == 0, layer == 1))(lambda: x_load(ha_ref, v, y).wait())
                events(items + g)
                tot = share.total(g)
                sum_ref[layer, v, :, cols] = tot
                mean, inv, gamma, _ = stats(layer, v, cols)
                tot = tot / total
                slope = inv * tot[1:]
                d = (gamma * inv * (dybuf[v] - (tot[:1] + (ubuf[lax.rem(g, 3)] - mean) * slope))).astype(BF16)

                @pl.when(jnp.logical_and(natural, n + 1 < slabs))
                def _():
                    pl.when(n > 0)(lambda: du_out(i).wait())
                    dubuf[v] = d
                    du_out(i).start()

                @pl.when(jnp.logical_and(natural, n + 1 == slabs))
                def _():
                    dbuf[at(v, rows), cols] = d

                weight_slab((layer + 1) * slabs + n, v, natural, d)

            @pl.when(jnp.logical_and(s == items, natural))
            def _():
                x_load(ha_ref, 0, y).start()
                x_load(hb_ref, 1, y).start()

        def layer_steps(k):
            layer = lax.div(k, items + 1)
            step(layer, k - layer * (items + 1))

        loop(len(layers) * (items + 1), layer_steps)

        last = n_chunk - 1
        chip_sum(last)
        issue(last)
        done = 16
        end(done - 1)

        def tail(j):
            begin(j)
            end(j)

        loop(n_chunk, tail, done)
        for j in (last - 1, last):
            fetch_x(j)
            deliver(j)
        put_done(0)
        put_done(1)
        for k in range(n_layer):
            theirs = dw2_ref.at[at(other(c), piece)] if k == 1 else (dw1_ref if k else dw3_ref).at[at(other(c), half)]
            remote(theirs, theirs, fcs.at[0], fcr.at[k], cpeer).wait_recv()
            sent = ry_ref.at[at(k, slabs)]
            remote(sent, sent, ys.at[k], yr.at[0], ypeer).wait_send()
        for j in range(n_chunk - 4, n_chunk):
            to_x(j).wait_send()

    n_item = len(layers) * items
    vm = lambda *shape: pltpu.VMEM(shape, F32)
    bf = lambda *shape: pltpu.VMEM(shape, BF16)
    return call(
        kernel, "backward", 4, (),
        [ANY, ANY, VMEM, VMEM] + [ANY] * 8 + [VMEM] * 4, [ANY] * 3 + [VMEM] + [ANY] * 4,
        [sds((dim, half), F32), sds((half, dim), F32), sds((dim, half), F32), sds((len(layers), 2, 2, dim), F32),
         sds((all_rows, dim), BF16), sds((n_chunk, half, width), F32), sds((n_chunk, piece, width), F32),
         sds((n_chunk, piece, width), F32)],
        [bf(all_rows, dim), bf(all_rows, dim), bf(2, dim, width), vm(3, rows, width), vm(2, rows, width), bf(2, rows, width),
         vm(2, half, width), vm(2, half, width), vm(2, half, width), vm(3, piece, width), vm(4, piece, width),
         vm(2, piece, width)] + Share.scratch(n_item, 2, width)
        + [DMA((3,)), TWO_DMA, TWO_DMA, DMA, TWO_DMA, DMA((n_chunk,)), DMA((n_chunk,)), DMA, DMA((n_layer,)),
           DMA((n_chunk,)), DMA((4,)), DMA((n_chunk,)), DMA((3,)), TWO_DMA, TWO_DMA, DMA((n_layer,)),
           pltpu.SemaphoreType.REGULAR],
        all_rows * dim * dim * 10, all_rows * dim * 40,
        (d_emb, zh, sz, s_emb, x2, x1, h_a, h_b, u2, u1, w3_t, w2_t, s2, s1, gb2, gb1))


def settle(*grads):
    steps = 8

    def kernel(*refs):
        for src, dst in zip(refs[:len(grads)], refs[len(grads):]):
            dst[...] = src[...]

    specs = [pl.BlockSpec((g.shape[0] // steps, g.shape[1]), lambda i: (i, 0)) for g in grads]
    return call(kernel, "settle", None, (steps,), specs, specs, [sds(g.shape, F32) for g in grads], [], 0,
                len(grads) * grads[0].size * 8, grads)


def solution(mesh):
    def shard_body(h_a, h_b, w_one, w_two, w_three, g_one, b_one, g_two, b_two, lam_off):
        y = lax.axis_index('model')
        total = float(h_a.shape[0] * mesh.shape['data'])
        dim, half = w_three.shape
        gb2 = jnp.stack([g_two, b_two])
        u1, s1, gb1, w_two_o = fwd_first(h_a, h_b, w_one, w_two, jnp.stack([g_one, b_one]))
        x1, u2, s2, w2_t, w_three_o = fwd_next(u1, s1, gb1, w_two, w_two_o, True, total, 1, w_three)
        x2, z, sz, w3_t = fwd_next(u2, s2, gb2, w_three, w_three_o, False, total, 2)
        zh, d_emb, s_emb = corr_grad(z, sz, lam_off, total)
        loss = jnp.sum(s_emb[0, 2])
        dw_three, dw_two, dw_one, sums, *_ = backward(
            d_emb.reshape(z.shape), zh.reshape(z.shape), sz, s_emb,
            ((u2, s2, gb2, w3_t, x1), (u1, s1, gb1, w2_t, None)), x2, h_a, h_b, total)
        dw_three, dw_two, dw_one = settle(dw_three, dw_two, dw_one)
        sums = jnp.sum(sums, axis=1)
        sum2 = sums[0]
        sum1 = lax.dynamic_slice_in_dim(sums[1], y * half, half, 1)
        return loss.reshape(1), dw_one, dw_two, dw_three, sum1[1], sum1[0], sum2[1], sum2[0]

    in_specs = (P('data', None), P('data', None), P(None, 'model'), P('model', None), P(None, 'model'),
                P('model'), P('model'), P(), P(), P())
    out_specs = (P(), P(None, 'model'), P('model', None), P(None, 'model'), P('model'), P('model'), P(), P())
    return jax.shard_map(shard_body, mesh=mesh, in_specs=in_specs, out_specs=out_specs, check_vma=False)
```

```python
import jax
import jax.numpy as jnp
from jax import lax
from jax.experimental import pallas as pl
from jax.experimental.pallas import tpu as pltpu
from jax.sharding import PartitionSpec as P

BN_EPS = 1e-5
scope = jax.named_scope
F32 = jnp.float32
BF16 = jnp.bfloat16
TM = 512
MAX_VMEM = 67043328
ANY = pl.BlockSpec(memory_space=pl.ANY)
VMEM = pl.BlockSpec(memory_space=pltpu.VMEM)
DMA = pltpu.SemaphoreType.DMA
TWO_DMA = DMA((2,))
BOTH = (0, 1)
PEERS = [(ky, kx, kc) for ky in BOTH for kx in BOTH for kc in BOTH][1:]
C_PEER, X_PEER, Y_PEER = PEERS[0], PEERS[1], PEERS[3]
N_DEV = len(PEERS) + 1


def mm(left, right):
    return jnp.dot(left, right, preferred_element_type=F32)


def mm_bt(left, right):
    return lax.dot_general(left, right, (((1,), (1,)), ((), ())), preferred_element_type=F32)


def mm_at(left, right):
    return lax.dot_general(left, right, (((0,), (0,)), ((), ())), preferred_element_type=F32)


def other(p):
    return 1 - p


def odd(i):
    return lax.rem(i, 2)


def split(i):
    return lax.div(i, 2), odd(i)


def loop(n, body, start=0):
    def one(i, carry):
        body(i)
        return carry

    lax.fori_loop(start, n, one, 0)


def whole(*shape):
    return pl.BlockSpec(shape, lambda *_: (0,) * len(shape))


def at(i, n):
    return pl.ds(pl.multiple_of(i * n, n), n)


def sds(shape, dtype):
    return jax.ShapeDtypeStruct(shape, dtype)


def mean_inv(sums, total):
    mean = sums[:1] / total
    var = sums[1:2] / total - mean * mean
    return mean, lax.rsqrt(var + BN_EPS)


def two_sums(one, two):
    return jnp.concatenate([jnp.sum(one, axis=0, keepdims=True), jnp.sum(two, axis=0, keepdims=True)], axis=0)


def coords():
    y, d = lax.axis_index('model'), lax.axis_index('data')
    return y, lax.div(d, 2), odd(d)


def flip(here, which):
    return tuple(other(p) if f else p for p, f in zip(here, which))


def flat(here):
    y, x, c = here
    return 4 * y + 2 * x + c


def device(here):
    y, x, c = here
    return (y, 2 * x + c)


def remote(src, dst, send_sem, recv_sem, there):
    return pltpu.make_async_remote_copy(
        src_ref=src, dst_ref=dst, send_sem=send_sem, recv_sem=recv_sem, device_id=device(there),
        device_id_type=pl.DeviceIdType.MESH)


def arrive():
    here = coords()
    for k in PEERS:
        pl.semaphore_signal(pltpu.get_barrier_semaphore(), inc=1, device_id=device(flip(here, k)),
                            device_id_type=pl.DeviceIdType.MESH)


def all_arrived():
    pl.semaphore_wait(pltpu.get_barrier_semaphore(), len(PEERS))


class Share:
    def __init__(self, acc, got, send_sem, recv_sem):
        self.acc, self.got, self.send_sem, self.recv_sem = acc, got, send_sem, recv_sem

    @staticmethod
    def scratch(n, *shape):
        return [pltpu.VMEM((n, *shape), F32), pltpu.VMEM((n, N_DEV, *shape), F32), DMA((n,)), DMA((n,))]

    def start(self, b):
        here = coords()
        me = flat(here)
        self.got[b, me] = self.acc[b]
        for which in PEERS:
            remote(self.acc.at[b], self.got.at[b, me], self.send_sem.at[b], self.recv_sem.at[b],
                   flip(here, which)).start()

    def total(self, b):
        all_of = self.got.at[b, pl.ds(0, len(PEERS))]
        copies = remote(all_of, all_of, self.send_sem.at[b], self.recv_sem.at[b], coords())
        copies.wait_send()
        copies.wait_recv()
        out = self.got[b, 0]
        for f in range(1, N_DEV):
            out += self.got[b, f]
        return out


class Gather:
    def __init__(self, own, dest, n, sems):
        self.own, self.dest, self.n = own, dest, n
        self.ys, self.yr, self.xs, self.xr, self.cs, self.cr = sems
        self.here = coords()
        _, x, c = self.here
        self.mine, self.across = 2 * x + c, 2 * (other(x)) + c
        self.core = (2 * x + other(c), 2 * (other(x)) + other(c))

    @staticmethod
    def scratch(n):
        return [DMA((n,))] * 4 + [DMA((2, n))] * 2

    def y(self, p):
        model = self.here[0]
        return remote(self.own(self.mine, p), self.dest(model, self.mine, p), self.ys.at[p], self.yr.at[p],
                      flip(self.here, Y_PEER))

    def moved(self, q, p, send_sem, recv_sem, which):
        ref = self.dest(1 - self.here[0], q, p)
        return remote(ref, ref, send_sem, recv_sem, flip(self.here, which))

    def x(self, p, q):
        return self.moved(q, p, self.xs.at[p], self.xr.at[p], X_PEER)

    def c(self, p, late, q):
        return self.moved(q, p, self.cs.at[late, p], self.cr.at[late, p], C_PEER)

    def start(self):
        for p in range(self.n):
            self.y(p).start()

    def pass_y(self, p):
        self.moved(self.mine, p, self.ys.at[p], self.yr.at[p], Y_PEER).wait_recv()
        self.x(p, self.mine).start()
        self.c(p, 0, self.mine).start()

    def pass_x(self, p):
        self.x(p, self.across).wait_recv()
        self.c(p, 1, self.across).start()

    def wait_core(self, late):
        for p in range(self.n):
            self.c(p, late, self.core[late]).wait_recv()

    def drain(self):
        for p in range(self.n):
            self.y(p).wait_send()
            self.x(p, self.mine).wait_send()
            self.c(p, 0, self.mine).wait_send()
            self.c(p, 1, self.across).wait_send()


def call(kernel, name, cid, grid, in_specs, out_specs, out_shape, scratch, flops, nbytes, args):
    return pl.pallas_call(
        kernel, name=name, grid=grid, in_specs=in_specs, out_specs=out_specs, out_shape=out_shape, scratch_shapes=scratch,
        compiler_params=pltpu.CompilerParams(vmem_limit_bytes=MAX_VMEM, collective_id=cid, has_side_effects=cid is not None),
        cost_estimate=pl.CostEstimate(flops=flops, bytes_accessed=nbytes, transcendentals=0))(*args)


def fwd_first(h_a, h_b, w_one, w_two, gb_own):
    depth, half = w_one.shape
    dim = 2 * half
    rows = h_a.shape[0] // 2
    tile, width, quarter = 2 * TM, half // 2, half // 4
    steps = rows // tile
    per_block = 2 * steps
    n = 4

    def block(j):
        y, x, _ = coords()
        return jnp.where(j < 2, 2 * y + j, 2 * (other(y)) + jnp.where(j == 2, x, other(x)))

    def tile_of(j, i):
        return jnp.where(odd(j) == 0, i, per_block - 1 - i)

    def kernel(ha_ref, hb_ref, w_ref, w2_ref, gb_ref, u_ref, s_ref, gbo_ref, w2o_ref, w1, gbf, *sems):
        share, sems = Share(*sems[:4]), sems[4:]
        gs, gr, lsem = sems[:3]
        sems = sems[3:]
        j, i = pl.program_id(0), pl.program_id(1)
        step = j * per_block + i
        here = coords()
        y = here[0]
        one = Gather(lambda q, p: w_ref.at[at(p, depth // n), at(q, quarter)],
                     lambda m, q, p: w1.at[at(p, depth // n), at(m * 4 + q, quarter)], n, sems[:6])
        two = Gather(lambda q, p: w2_ref.at[at(q * n + p, quarter // n)],
                     lambda m, q, p: w2o_ref.at[at(q * n + p, quarter // n)], n, sems[6:])

        def local(b):
            return pltpu.make_async_copy(w_ref.at[:, at(b, width)], w1.at[:, at(2 * y + b, width)], lsem.at[b])

        def bn_vectors(m):
            return remote(gb_ref, gbf.at[:, at(m, half)], gs, gr, flip(here, Y_PEER))

        def begin():
            arrive()
            local(0).start()
            local(1).start()
            all_arrived()
            one.start()
            two.start()
            bn_vectors(y).start()
            local(0).wait()

        def late_half():
            one.pass_x(0)
            one.pass_y(n - 1)
            one.wait_core(0)

        def last_block():
            one.pass_x(n - 1)
            two.pass_y(0)
            one.wait_core(1)

        def second_block():
            local(1).wait()
            one.pass_y(1)

        hooks = {0: begin, 2: lambda: one.pass_y(0), per_block: second_block, 6: lambda: one.pass_y(2),
                 2 * per_block: late_half, 9: lambda: one.pass_x(1), 11: lambda: one.pass_x(2), 3 * per_block: last_block,
                 13: lambda: two.pass_y(1), 15: lambda: two.pass_x(0)}
        for s in sorted(hooks):
            pl.when(step == s)(scope(f'hook{s}')(hooks[s]))
        for b in range(3):
            pl.when(step == (b + 1) * per_block)(lambda b=b: share.start(block(b)))

        tile_at = tile_of(j, i)
        h = lax.select(tile_at < steps, ha_ref[...], hb_ref[...])
        u = mm(h, w1[:, at(block(j), width)])
        u_ref[...] = u
        sums = two_sums(u, u * u)
        v = tile_at // steps
        share.acc[block(j), v] = jnp.where(i % steps == 0, 0.0, share.acc[block(j), v]) + sums

        @pl.when(step == 4 * per_block - 1)
        @scope('f1end')
        def _():
            share.start(block(3))
            two.pass_y(2)
            two.pass_x(1)
            two.pass_y(n - 1)
            for p in range(2, n):
                two.pass_x(p)
            bn_vectors(other(y)).wait_recv()
            bn_vectors(y).wait_send()
            gbo_ref[...] = gbf[...]
            gbo_ref[:, at(y, half)] = gb_ref[...]
            for b in range(4):
                s_ref[:, :, b * width:(b + 1) * width] = share.total(b)
            one.drain()
            two.drain()
            two.wait_core(0)
            two.wait_core(1)

    return call(
        kernel, "fwd_first", 0, (4, per_block),
        [pl.BlockSpec((tile, depth), lambda j, i: (coords()[0] * steps + jnp.minimum(tile_of(j, i), steps - 1), 0)),
         pl.BlockSpec((tile, depth), lambda j, i: (coords()[0] * steps + jnp.maximum(tile_of(j, i) - steps, 0), 0)),
         ANY, ANY, whole(2, half)],
        [pl.BlockSpec((tile, width), lambda j, i: (tile_of(j, i), block(j))), whole(2, 2, dim),
         whole(2, dim), ANY],
        [sds((2 * rows, dim), F32), sds((2, 2, dim), F32), sds((2, dim), F32), sds((half, dim), BF16)],
        [pltpu.VMEM((depth, dim), BF16), pltpu.VMEM((2, dim), F32)] + Share.scratch(4, 2, 2, width)
        + [DMA, DMA, TWO_DMA] + Gather.scratch(n) * 2,
        4 * rows * depth * dim, 2 * rows * (8 * depth + 4 * dim), (h_a, h_b, w_one, w_two, gb_own))


def fwd_next(u, sums, gb, w_own, w_other, by_rows, total, cid, w_next=None):
    all_rows, depth = u.shape
    dim = w_own.shape[1] if by_rows else 2 * w_own.shape[1]
    half = dim // 2
    quarter = half // 4
    steps = all_rows // 2 // TM
    last = 2 * steps - 1
    slab = dim // (2 * steps)
    n = 4

    def kernel(u_ref, s_ref, gb_ref, wo_ref, wt_ref, *refs):
        if w_next is not None:
            wn_ref, refs = refs[0], refs[1:]
        x_ref, o_ref, so_ref, wtr_ref, *refs = refs
        if w_next is not None:
            wno_ref, *refs = refs
        w, acc, got, ssem, rsem, lsem, *refs = refs
        share = Share(acc, got, ssem, rsem)
        i = pl.program_id(0)
        y = coords()[0]

        def local(ref, model, b):
            where = at(model, half)
            return pltpu.make_async_copy(ref, w.at[where] if by_rows else w.at[:, where], lsem.at[b])

        if w_next is not None:
            gather = Gather(lambda q, p: wn_ref.at[at(p, depth // n), at(q, quarter)],
                            lambda m, q, p: wno_ref.at[at(p, depth // n), at(q, quarter)], n, refs)

        @pl.when(i == 0)
        def _():
            arrive()
            local(wo_ref, y, 0).start()
            local(wt_ref, other(y), 1).start()
            all_arrived()
            if w_next is not None:
                gather.start()
            local(wo_ref, y, 0).wait()
            local(wt_ref, other(y), 1).wait()

        if w_next is not None:
            for p in range(n):
                pl.when(i == p + 1)(lambda p=p: gather.pass_y(p))
                pl.when(i == p + 3)(lambda p=p: gather.pass_x(p))
        pl.when(i == steps)(lambda: share.start(0))

        mean, inv = mean_inv(s_ref[0], total)
        act = jnp.maximum((u_ref[...] - mean) * inv * gb_ref[:1] + gb_ref[1:], 0.0).astype(BF16)
        x_ref[...] = act
        out = mm(act, w[...])
        o_ref[...] = out
        wtr_ref[...] = w[:, at(i, slab)].T
        v = i // steps
        share.acc[v] = jnp.where(i % steps == 0, 0.0, share.acc[v]) + two_sums(out, out * out)

        @pl.when(i == last)
        def _():
            share.start(1)
            with scope('wait_last'):
                for b in BOTH:
                    so_ref[b] = share.total(b)
            if w_next is not None:
                gather.drain()
                gather.wait_core(0)
                gather.wait_core(1)

    more = w_next is not None
    return call(
        kernel, "fwd_next", cid, (2 * steps,),
        [pl.BlockSpec((TM, depth), lambda i: (i, 0)), pl.BlockSpec((1, 2, depth), lambda i: (i // steps, 0, 0)),
         whole(2, depth), ANY, ANY] + [ANY] * more,
        [pl.BlockSpec((TM, depth), lambda i: (i, 0)), pl.BlockSpec((TM, dim), lambda i: (i, 0)),
         whole(2, 2, dim), pl.BlockSpec((slab, depth), lambda i: (i, 0))] + [ANY] * more,
        [sds((all_rows, depth), BF16), sds((all_rows, dim), F32), sds((2, 2, dim), F32), sds((dim, depth), BF16)]
        + ([sds(w_next.shape, BF16)] if more else []),
        [pltpu.VMEM((depth, dim), BF16)] + Share.scratch(2, 2, dim) + [TWO_DMA] + (Gather.scratch(n) if more else []),
        2 * all_rows * depth * dim, all_rows * (6 * depth + 4 * dim),
        (u, sums, gb, w_own, w_other) + ((w_next,) if more else ()))


def corr_grad(z, sums, lam, total):
    all_rows, dim = z.shape
    rows = all_rows // 2
    half = dim // 2
    quart = half // 2
    n_chunk = 8
    width = half // n_chunk
    pair = 2 * width
    mt = TM
    zt = TM // 2
    ahead = 3
    z_steps = all_rows // zt
    m_steps = rows // mt
    scale = 1.0 / total

    def kernel(z_ref, s_ref, lam_ref, zho_ref, d_ref, so_ref, zh, da, ck, r1, r2, g, stage, dsend, drecv, acc, got, ssem, rsem, zs, zos,
               d1s, d1r, s1s, s1r, s2s, s2r, a2s, a2r, a1s, a1r, ads, adr, dbs, das):
        share = Share(acc, got, ssem, rsem)
        here = coords()
        y, x, c = here
        on_x = c == 0
        by_core = lambda one, two: tuple(jnp.where(on_x, a, b) for a, b in zip(one, two))
        first = by_core(flip(here, X_PEER), flip(here, Y_PEER))
        second = by_core(flip(here, Y_PEER), flip(here, X_PEER))
        cpeer = flip(here, C_PEER)
        bit1, bit2 = by_core((x, y), (y, x))
        arrive()
        acc[...] = jnp.zeros_like(acc)

        def load(i, slot):
            return pltpu.make_async_copy(z_ref.at[at(i, zt)], ck.at[at(slot, zt)], zs.at[slot])

        def zh_out(v, r, i):
            return pltpu.make_async_copy(zh.at[v, at(r, zt)], zho_ref.at[v, at(r, zt)], zos.at[i])

        z_slots = half // zt
        for i in range(ahead):
            load(i, i).start()

        @scope('normalise')
        def normalise(i):
            slot = lax.rem(i, z_slots)
            v, r = lax.div(i, z_steps // 2), lax.rem(i, z_steps // 2)
            pl.when(i + ahead < z_steps)(lambda: load(i + ahead, lax.rem(i + ahead, z_slots)).start())
            load(i, slot).wait()
            mean, inv = mean_inv(s_ref[v], total)
            zh[v, at(r, zt)] = ((ck[at(slot, zt)] - mean) * inv).astype(BF16)
            zh_out(v, r, i).start()

        loop(z_steps, normalise)
        all_arrived()

        def both(v, rows_at, t):
            return jnp.concatenate([zh[v, rows_at, at(b * n_chunk + t, width)] for b in BOTH], axis=1)

        group = lambda t, b: at(2 * t + b, width)

        def to_core(t):
            return remote(dsend.at[odd(t)], drecv.at[odd(t)], d1s.at[t], d1r.at[t], cpeer)

        def to_first(t):
            return remote(ck.at[:, group(t, other(bit1))], r1.at[t], s1s.at[t], s1r.at[t], first)

        def to_second(t):
            return remote(ck.at[at(other(bit2), quart), group(t, bit1)], r2.at[t], s2s.at[t], s2r.at[t], second)

        def g_second(t, b):
            block = g.at[t, at(2 * c + b, quart), at(bit1, width)]
            return remote(block, block, a2s.at[t], a2r.at[t], second)

        def g_first(t, b):
            block = g.at[t, at(c, half), at(b, width)]
            return remote(block, block, a1s.at[t], a1r.at[t], first)

        def g_core(t, core):
            block = g.at[t, at(core, half)]
            return remote(block, block, ads.at[t], adr.at[t], cpeer)

        @scope('chip_sum')
        def chip_sum(t):
            to_core(t).wait_recv()
            to_core(t).wait_send()
            ck[:, at(t, pair)] += drecv[odd(t)]
            to_first(t).start()

        @scope('corr_part')
        def corr_part(t):
            right = both(1, pl.ds(0, rows), t)
            dsend[odd(t)] = mm_at(zh[0, :, at(other(c), half)], right)
            ck[:, at(t, pair)] = mm_at(zh[0, :, at(c, half)], right)
            to_core(t).start()

        def db_out(t, m, slot, b):
            return pltpu.make_async_copy(
                stage.at[slot, :, at(b, width)], d_ref.at[1, at(m, mt), at(b * n_chunk + t, width)], dbs.at[slot, b])

        def da_out(m):
            return pltpu.make_async_copy(da.at[at(m, mt)], d_ref.at[0, at(m, mt)], das.at[m])

        def finish(m):
            d = da[at(m, mt)] * scale
            da[at(m, mt)] = d
            acc[0, :2] += two_sums(d, d * zh[0, at(m, mt)].astype(F32))
            da_out(m).start()

        def grads(t):
            @scope('rows_of')
            def rows_of(m):
                slot = odd(m)

                @pl.when(t * m_steps + m >= 2)
                def _():
                    for b in BOTH:
                        db_out(t, m, slot, b).wait()

                db = mm(zh[0, at(m, mt)], g[t]) * scale
                stage[slot] = db
                own = both(1, at(m, mt), t)
                sums = two_sums(db, db * own.astype(F32))
                for b in BOTH:
                    acc[1, :2, at(b * n_chunk + t, width)] += sums[:, b * width:(b + 1) * width]
                    db_out(t, m, slot, b).start()
                da[at(m, mt)] = jnp.where(t == 0, 0.0, da[at(m, mt)]) + mm_bt(own, g[t])
                pl.when(t == n_chunk - 1)(lambda: finish(m))

            loop(m_steps, rows_of)

        @scope('at_first')
        def at_first(t):
            to_first(t).wait_recv()
            ck[:, group(t, bit1)] += r1[t]
            to_second(t).start()

        @scope('at_second')
        def at_second(t):
            to_second(t).wait_recv()
            corr_mat = (ck[at(bit2, quart), group(t, bit1)] + r2[t]) * scale
            row_ids = (2 * c + bit2) * quart + lax.broadcasted_iota(jnp.int32, (quart, width), 0)
            col_ids = (bit1 * n_chunk + t) * width + lax.broadcasted_iota(jnp.int32, (quart, width), 1)
            is_diag = row_ids == col_ids
            lam_val = lam_ref[0]
            loss = jnp.where(is_diag, (1.0 - corr_mat) * (1.0 - corr_mat), lam_val * corr_mat * corr_mat)
            acc[0, 2:3, :width] += jnp.sum(loss, axis=0, keepdims=True)
            grad = jnp.where(is_diag, -2.0 * (1.0 - corr_mat), 2.0 * lam_val * corr_mat).astype(BF16)
            g[t, at(2 * c + bit2, quart), at(bit1, width)] = grad
            g_second(t, bit2).start()

        @scope('back_second')
        def back_second(t):
            g_second(t, other(bit2)).wait_recv()
            g_first(t, bit1).start()

        @scope('back_first')
        def back_first(t):
            g_first(t, other(bit1)).wait_recv()
            g_core(t, c).start()

        def back_core(t):
            g_core(t, other(c)).wait_recv()
            grads(t)

        lead = 3

        def advance(tau):
            for lag, stage_fn in ((lead, at_first), (lead + 1, back_first), (lead + 2, back_core), (lead, at_second),
                                  (1, chip_sum), (0, corr_part), (lead, back_second)):
                t = tau - lag
                pl.when(jnp.logical_and(t >= 0, t < n_chunk))(lambda t=t, stage_fn=stage_fn: stage_fn(t))

        loop(n_chunk + lead + 2, advance)
        share.start(1)
        share.start(0)
        for t in range(n_chunk):
            for copy in (to_first(t), to_second(t), g_second(t, bit2), g_first(t, bit1), g_core(t, c)):
                copy.wait_send()
        for b in BOTH:
            so_ref[b] = share.total(b)
            for slot in BOTH:
                db_out(0, 0, slot, b).wait()
        for i in range(z_steps):
            zh_out(i // (z_steps // 2), i % (z_steps // 2), i).wait()
        for m in range(m_steps):
            da_out(m).wait()

    return call(
        kernel, "corr_grad", 3, (), [ANY, VMEM, pl.BlockSpec(memory_space=pltpu.SMEM)], [ANY, ANY, VMEM],
        [sds((2, rows, dim), BF16), sds((2, rows, dim), F32), sds((2, 4, dim), F32)],
        [pltpu.VMEM((2, rows, dim), BF16), pltpu.VMEM((rows, dim), F32), pltpu.VMEM((half, dim), F32),
         pltpu.VMEM((n_chunk, half, width), F32), pltpu.VMEM((n_chunk, quart, width), F32),
         pltpu.VMEM((n_chunk, dim, pair), BF16), pltpu.VMEM((2, mt, pair), F32)]
        + [pltpu.VMEM((2, half, pair), F32)] * 2 + Share.scratch(2, 4, dim)
        + [DMA((half // zt,)), DMA((z_steps,))] + [DMA((n_chunk,))] * 12 + [DMA((2, 2)), DMA((m_steps,))],
        all_rows * dim * dim * 3, all_rows * dim * 12, (z, sums, lam))


def backward(d_emb, zh, sz, s_emb, layers, x2, h_a, h_b, total):
    all_rows, dim = zh.shape
    rows, half = all_rows // 2, dim // 2
    width = 256
    slabs = dim // width
    items = 2 * slabs
    piece = width
    side = half // 2 // piece
    per_slab = half // piece
    n_layer = len(layers) + 1
    n_slab = n_layer * slabs
    per_layer = slabs * side
    n_chunk = n_layer * per_layer
    ahead = 3
    (u2, s2, gb2, w3_t, x1), (u1, s1, gb1, w2_t, _) = layers

    def kernel(d_ref, zh_ref, sz_ref, sd_ref, x2_ref, x1_ref, ha_ref, hb_ref, u2_ref, u1_ref, w3_ref, w2_ref,
               s2_ref, s1_ref, gb2_ref, gb1_ref, dw3_ref, dw2_ref, dw1_ref, sum_ref, dy_ref, part_ref, ry_ref, rx_ref,
               dbuf, xbuf, wbuf, ubuf, dybuf, dyout, psend, pkeep, dr, ebuf, mbuf, fbuf, acc, got, ssem, rsem,
               us, ws, ds, dos, xl, ps, pr, pm, ys, yr, xs, xr, es, fs, fcs, fcr, credit):
        share = Share(acc, got, ssem, rsem)
        here = coords()
        y, x, c = here
        ypeer, xpeer, cpeer = flip(here, Y_PEER), flip(here, X_PEER), flip(here, C_PEER)
        arrive()

        def column(k, n):
            model = odd(n + jnp.where(k == 0, other(y), 0))
            return jnp.where(k == 1, n, model * (slabs // 2) + lax.div(n, 2))

        def turn(k):
            return jnp.where(k == 0, 0, other(y))

        def m_slot(j):
            return lax.rem(j, 4)

        def copy(src, dst, sem):
            return pltpu.make_async_copy(src, dst, sem)

        def sent_by(q):
            k = lax.div(q, items)
            run = lax.rem(q, items)
            first = per_slab * lax.div(run + 2, 4)
            middle = per_layer + side * lax.div(run, 2)
            last = 2 * per_layer + per_slab * lax.div(run, 4)
            done = per_layer * lax.div(k + 1, 2)
            return jnp.where(k == 0, first, jnp.where(k == 2, middle, jnp.where(k == 4, last, done)))

        def begun(q):
            paced = jnp.clip(lax.div(5 * q - items, 9), 0, 2 * per_layer)
            return jnp.where(q < 4 * items + 4, paced, 2 * per_layer + q - 4 * items - 3)

        def to_core(s):
            return remote(psend.at[odd(s)], dr.at[odd(s)], ps.at[s], pr.at[s], cpeer)

        def keep_out(s):
            return copy(pkeep.at[odd(s)], part_ref.at[s], pm)

        @scope('chip_sum')
        def chip_sum(s):
            to_core(s).wait_recv()
            pkeep[odd(s)] += dr[odd(s)]

            @pl.when(s + 2 < n_slab)
            def _():
                pl.semaphore_signal(credit, inc=1, device_id=device(cpeer), device_id_type=pl.DeviceIdType.MESH)

            to_core(s).wait_send()
            keep_out(s).start()

        def home(j, own):
            k = lax.div(j, per_layer)
            i = lax.rem(j, per_layer)
            model = y if own else other(y)
            turned = other(turn(k)) if own else turn(k)
            s = jnp.where(k == 1, lax.div(i, side), 2 * lax.div(i, per_slab) + turned)
            place = jnp.where(k == 1, model * side + lax.rem(i, side), lax.rem(i, per_slab))
            return part_ref.at[k * slabs + s, at(place, piece)]

        def to_y(j):
            return remote(home(j, False), ry_ref.at[j], ys.at[lax.div(j, per_layer)], yr.at[j], ypeer)

        @scope('issue')
        def issue(s, q):
            keep_out(s).wait()
            k, n = lax.div(s, slabs), lax.rem(s, slabs)
            for mine, fire, first, count in (
                    (k == 1, True, n * side, side), (k != 1, odd(n) == jnp.where(k == 0, 0, 1), lax.div(n, 2) * per_slab, per_slab)):
                for r in range(count):
                    j = k * per_layer + first + r
                    pl.when(mine & fire & (j < begun(q - 1) + ahead))(lambda j=j: to_y(j).start())

        def to_x(j):
            return remote(mbuf.at[m_slot(j)], rx_ref.at[j], xs.at[m_slot(j)], xr.at[j], xpeer)

        def result(j, k):
            i = lax.rem(j, per_layer)
            if k == 1:
                return dw2_ref.at[at(c * side + lax.rem(i, side), piece), at(lax.div(i, side), width)]
            return (dw1_ref if k else dw3_ref).at[at(c * per_slab + lax.rem(i, per_slab), piece), at(lax.div(i, per_slab), width)]

        def put(j, k):
            slot = odd(j)
            return (copy(fbuf.at[slot], result(j, k), fs.at[slot]),
                    remote(fbuf.at[slot], result(j, k), fcs.at[slot], fcr.at[k], cpeer))

        def put_done(j):
            here_copy, there_copy = put(j, 0)
            here_copy.wait()
            there_copy.wait_send()

        def load_part(j, which):
            src = (lambda: ry_ref.at[j], lambda: home(j, True), lambda: rx_ref.at[j])[which]()
            return copy(src, ebuf.at[which], es.at[which])

        @scope('fetch_x')
        def fetch_x(j):
            to_x(j).wait_recv()
            load_part(j, 2).start()

        @scope('begin')
        def begin(j, q):
            remote(ry_ref.at[j], ry_ref.at[j], ys.at[0], yr.at[j], ypeer).wait_recv()
            load_part(j, 0).start()
            load_part(j, 1).start()
            pl.when(j + ahead < sent_by(q))(lambda: to_y(j + ahead).start())
            pl.when(j >= 2)(lambda: fetch_x(j - 2))

        @scope('deliver')
        def deliver(j):
            load_part(j, 2).wait()
            pl.when(j >= 2)(lambda: put_done(j))
            fbuf[odd(j)] = mbuf[m_slot(j)] + ebuf[2]
            for k in range(n_layer):
                @pl.when(lax.div(j, per_layer) == k)
                def _(k=k):
                    for one in put(j, k):
                        one.start()

        @scope('end')
        def end(j):
            load_part(j, 0).wait()
            load_part(j, 1).wait()
            pl.when(j >= 4)(lambda: to_x(j).wait_send())
            mbuf[m_slot(j)] = ebuf[0] + ebuf[1]
            to_x(j).start()
            pl.when(j >= 2)(lambda: deliver(j - 2))

        def events(q):
            now, before, earlier = begun(q), begun(q - 1), begun(q - 2)
            pl.when(before > earlier)(lambda: end(before - 1))
            pl.when(now > before)(lambda: begin(now - 1, q))

        def left(v, natural, part):
            first = jnp.where(natural, part, 2 * part)
            second = first + jnp.where(natural, 2, 1)
            return jnp.concatenate([xbuf[at(v, rows), at(b, half // 2)] for b in (first, second)], axis=1)

        @scope('weight_slab')
        def weight_slab(k, n, v, d):
            s = k * slabs + n
            slot = odd(s)

            def one(buf, part):
                buf[slot] = jnp.where(v == 0, 0.0, buf[slot]) + mm_at(left(v, k == 1, part), d)

            one(psend, other(c))

            @pl.when(v == 1)
            def _():
                pl.when(s >= 2)(lambda: pl.semaphore_wait(credit, 1))
                to_core(s).start()

            one(pkeep, c)
            pl.when(v == 1)(lambda: chip_sum(s))

        def tick(k, n, v, q):
            pl.when((v == 0) & (n > 0))(lambda: issue(k * slabs + n - 1, q))
            events(q)

        def emb_loads(i):
            n, v = split(i)
            cols = at(column(0, n), width)
            return (copy(d_ref.at[at(v, rows), cols], ubuf.at[v], us.at[v]),
                    copy(zh_ref.at[at(v, rows), cols], wbuf.at[v], ws.at[v]))

        def x_load(src, v, src_at):
            return copy(src.at[at(src_at, rows)], xbuf.at[at(v, rows)], xl.at[v])

        def slab_of(ref, layer, i, buf, sem):
            n, v = split(i)
            return copy(ref.at[at(v, rows), at(column(layer + 1, n), width)], buf.at[v], sem.at[v])

        def u_load(layer, i, ref=u2_ref):
            return slab_of(ref, layer, i, ubuf, us)

        def dy_load(layer, i):
            return slab_of(dy_ref, layer, i, dybuf, ds)

        def dy_out(layer, i):
            n, v = split(i)
            return copy(dyout.at[v], dy_ref.at[at(v, rows), at(column(layer + 1, n), width)], dos.at[v])

        def w_load(layer, n, ref=w3_ref):
            return copy(ref.at[:, at(column(layer + 1, n), width)], wbuf.at[odd(n)], ws.at[odd(n)])

        def start_u(layer, i):
            for k, ref in enumerate((u2_ref, u1_ref)):
                pl.when(layer == k)(lambda ref=ref: u_load(layer, i, ref).start())

        def start_w(layer, n):
            for k, ref in enumerate((w3_ref, w2_ref)):
                pl.when(layer == k)(lambda ref=ref: w_load(layer, n, ref).start())

        x_load(x2_ref, 0, 0).start()
        for one in emb_loads(0):
            one.start()
        x_load(x2_ref, 1, 1).start()
        all_arrived()

        def emb_item(i):
            n, v = split(i)

            @pl.when(i + 1 < items)
            def _():
                for one in emb_loads(i + 1):
                    one.start()

            @pl.when(i + 1 == items)
            def _():
                u_load(0, 0).start()
                w_load(0, 0).start()

            pl.when(i < 2)(lambda: x_load(x2_ref, v, v).wait())
            for one in emb_loads(i):
                one.wait()
            tick(0, n, v, i)
            cols = at(column(0, n), width)
            _, inv = mean_inv(sz_ref[v, :, cols], total)
            sd = sd_ref[v, :2, cols] / total
            d = (inv * (ubuf[v] - sd[:1] - wbuf[v].astype(F32) * sd[1:])).astype(BF16)
            dbuf[at(v, rows), cols] = d
            weight_slab(0, n, v, d)

        loop(items, emb_item)
        issue(slabs - 1, items)
        for v in BOTH:
            x_load(x1_ref, v, v).start()

        def stats(layer, v, cols):
            pick = lambda one, two: jnp.where(layer == 0, one, two)
            mean, inv = mean_inv(pick(s2_ref[v, :, cols], s1_ref[v, :, cols]), total)
            gb = pick(gb2_ref[:, cols], gb1_ref[:, cols])
            return mean, inv, gb[:1], gb[1:]

        def bn_layer(layer):
            start = (2 * layer + 1) * items

            def dx_item(i):
                n, v = split(i)
                cols = at(column(layer + 1, n), width)

                @pl.when(i + 1 < items)
                def _():
                    start_u(layer, i + 1)
                    pl.when((v == 0) & (n + 1 < slabs))(lambda: start_w(layer, n + 1))

                @pl.when(i + 1 == items)
                def _():
                    start_u(layer, 0)
                    dy_load(layer, 0).start()

                scope('wait_u')(u_load(layer, i).wait)()
                pl.when(v == 0)(lambda: w_load(layer, n).wait())
                events(start + i)
                with scope('mm_dx'):
                    dx = mm(dbuf[at(v, rows)], wbuf[odd(n)])
                mean, inv, gamma, beta = stats(layer, v, cols)
                norm = (ubuf[v] - mean) * inv
                dy = jnp.where(norm * gamma + beta > 0, dx, 0.0)
                pl.when(n > 0)(lambda: dy_out(layer, i).wait())
                dyout[v] = dy
                dy_out(layer, i).start()
                g = layer * items + i
                acc[g] = two_sums(dy, dy * norm)
                share.start(g)

            def dw_item(i):
                n, v = split(i)
                cols = at(column(layer + 1, n), width)

                @pl.when(i + 1 < items)
                def _():
                    start_u(layer, i + 1)
                    dy_load(layer, i + 1).start()

                @pl.when((i + 1 == items) & (layer == 0))
                def _():
                    u_load(1, 0, u1_ref).start()
                    w_load(1, 0, w2_ref).start()

                pl.when((n == 0) & (layer == 0))(lambda: x_load(x1_ref, v, v).wait())
                pl.when((n == 0) & (layer == 1))(lambda: x_load(ha_ref, v, y).wait())
                u_load(layer, i).wait()
                scope('wait_dy')(dy_load(layer, i).wait)()
                tick(layer + 1, n, v, start + items + i)
                with scope('wait_stats'):
                    tot = share.total(layer * items + i)
                sum_ref[layer, v, :, cols] = tot
                mean, inv, gamma, _ = stats(layer, v, cols)
                tot = tot / total
                d = (gamma * inv * (dybuf[v] - (tot[:1] + (ubuf[v] - mean) * (inv * tot[1:])))).astype(BF16)
                dbuf[at(v, rows), cols] = d
                weight_slab(layer + 1, n, v, d)

            loop(items, dx_item)
            for v in BOTH:
                dy_out(layer, v).wait()
            loop(items, dw_item)
            issue((layer + 2) * slabs - 1, start + 2 * items)

            @pl.when(layer == 0)
            def _():
                for v, ref in enumerate((ha_ref, hb_ref)):
                    x_load(ref, v, y).start()

        loop(len(layers), bn_layer)

        ticks = (2 * n_layer - 1) * items
        ended = 2 * per_layer + items - 4
        end(ended - 1)

        def tail(j):
            begin(j, ticks)
            end(j)

        loop(n_chunk, tail, ended)
        for j in range(n_chunk - 2, n_chunk):
            fetch_x(j)
            deliver(j)
        for j in BOTH:
            put_done(j)
        for k in range(n_layer):
            theirs = dw2_ref.at[at(other(c), half // 2)] if k == 1 else (dw1_ref if k else dw3_ref).at[at(other(c), half)]
            remote(theirs, theirs, fcs.at[0], fcr.at[k], cpeer).wait_recv()
            sent = ry_ref.at[at(k, per_layer)]
            remote(sent, sent, ys.at[k], yr.at[0], ypeer).wait_send()
        for j in range(n_chunk - 4, n_chunk):
            to_x(j).wait_send()

    n_item = len(layers) * items
    vm = lambda *shape: pltpu.VMEM(shape, F32)
    bf = lambda *shape: pltpu.VMEM(shape, BF16)
    return call(
        kernel, "backward", 4, (),
        [ANY, ANY, VMEM, VMEM] + [ANY] * 8 + [VMEM] * 4, [ANY] * 3 + [VMEM] + [ANY] * 4,
        [sds((dim, half), F32), sds((half, dim), F32), sds((dim, half), F32), sds((len(layers), 2, 2, dim), F32),
         sds((all_rows, dim), F32), sds((n_slab, half, width), F32), sds((n_chunk, piece, width), F32),
         sds((n_chunk, piece, width), F32)],
        [bf(all_rows, dim), bf(all_rows, dim), bf(2, dim, width), vm(2, rows, width), vm(2, rows, width), vm(2, rows, width),
         vm(2, half, width), vm(2, half, width), vm(2, half, width), vm(3, piece, width), vm(4, piece, width),
         vm(2, piece, width)] + Share.scratch(n_item, 2, width)
        + [TWO_DMA, TWO_DMA, TWO_DMA, TWO_DMA, TWO_DMA, DMA((n_slab,)), DMA((n_slab,)), DMA, DMA((n_layer,)),
           DMA((n_chunk,)), DMA((4,)), DMA((n_chunk,)), DMA((3,)), TWO_DMA, TWO_DMA, DMA((n_layer,)),
           pltpu.SemaphoreType.REGULAR],
        all_rows * dim * dim * 10, all_rows * dim * 40,
        (d_emb, zh, sz, s_emb, x2, x1, h_a, h_b, u2, u1, w3_t, w2_t, s2, s1, gb2, gb1))


def settle(*grads):
    steps = 8

    def kernel(*refs):
        for src, dst in zip(refs[:len(grads)], refs[len(grads):]):
            dst[...] = src[...]

    specs = [pl.BlockSpec((g.shape[0] // steps, g.shape[1]), lambda i: (i, 0)) for g in grads]
    return call(kernel, "settle", None, (steps,), specs, specs, [sds(g.shape, F32) for g in grads], [], 0,
                len(grads) * grads[0].size * 8, grads)


def solution(mesh):
    def shard_body(h_a, h_b, w_one, w_two, w_three, g_one, b_one, g_two, b_two, lam_off):
        y = lax.axis_index('model')
        total = float(h_a.shape[0] * mesh.shape['data'])
        dim, half = w_three.shape
        gb2 = jnp.stack([g_two, b_two])
        u1, s1, gb1, w_two_o = fwd_first(h_a, h_b, w_one, w_two, jnp.stack([g_one, b_one]))
        x1, u2, s2, w2_t, w_three_o = fwd_next(u1, s1, gb1, w_two, w_two_o, True, total, 1, w_three)
        x2, z, sz, w3_t = fwd_next(u2, s2, gb2, w_three, w_three_o, False, total, 2)
        zh, d_emb, s_emb = corr_grad(z, sz, lam_off, total)
        loss = jnp.sum(s_emb[0, 2])
        dw_three, dw_two, dw_one, sums, *_ = backward(
            d_emb.reshape(z.shape), zh.reshape(z.shape), sz, s_emb,
            ((u2, s2, gb2, w3_t, x1), (u1, s1, gb1, w2_t, None)), x2, h_a, h_b, total)
        dw_three, dw_two, dw_one = settle(dw_three, dw_two, dw_one)
        sums = jnp.sum(sums, axis=1)
        sum2 = sums[0]
        sum1 = lax.dynamic_slice_in_dim(sums[1], y * half, half, 1)
        return loss.reshape(1), dw_one, dw_two, dw_three, sum1[1], sum1[0], sum2[1], sum2[0]

    in_specs = (P('data', None), P('data', None), P(None, 'model'), P('model', None), P(None, 'model'),
                P('model'), P('model'), P(), P(), P())
    out_specs = (P(), P(None, 'model'), P('model', None), P(None, 'model'), P('model'), P('model'), P(), P())
    return jax.shard_map(shard_body, mesh=mesh, in_specs=in_specs, out_specs=out_specs, check_vma=False)
```

```python
import jax
import jax.numpy as jnp
from jax import lax
from jax.experimental import pallas as pl
from jax.experimental.pallas import tpu as pltpu
from jax.sharding import PartitionSpec as P

BN_EPS = 1e-5
scope = jax.named_scope
F32 = jnp.float32
BF16 = jnp.bfloat16
TM = 512
MAX_VMEM = 67043328
ANY = pl.BlockSpec(memory_space=pl.ANY)
VMEM = pl.BlockSpec(memory_space=pltpu.VMEM)
DMA = pltpu.SemaphoreType.DMA
TWO_DMA = DMA((2,))
BOTH = (0, 1)
PEERS = [(ky, kx, kc) for ky in BOTH for kx in BOTH for kc in BOTH][1:]
C_PEER, X_PEER, Y_PEER = PEERS[0], PEERS[1], PEERS[3]
N_DEV = len(PEERS) + 1


def mm(left, right):
    return jnp.dot(left, right, preferred_element_type=F32)


def mm_bt(left, right):
    return lax.dot_general(left, right, (((1,), (1,)), ((), ())), preferred_element_type=F32)


def mm_at(left, right):
    return lax.dot_general(left, right, (((0,), (0,)), ((), ())), preferred_element_type=F32)


def other(p):
    return 1 - p


def odd(i):
    return lax.rem(i, 2)


def split(i):
    return lax.div(i, 2), odd(i)


def loop(n, body, start=0):
    def one(i, carry):
        body(i)
        return carry

    lax.fori_loop(start, n, one, 0)


def whole(*shape):
    return pl.BlockSpec(shape, lambda *_: (0,) * len(shape))


def at(i, n):
    return pl.ds(pl.multiple_of(i * n, n), n)


def sds(shape, dtype):
    return jax.ShapeDtypeStruct(shape, dtype)


def mean_inv(sums, total):
    mean = sums[:1] / total
    var = sums[1:2] / total - mean * mean
    return mean, lax.rsqrt(var + BN_EPS)


def two_sums(one, two):
    return jnp.concatenate([jnp.sum(one, axis=0, keepdims=True), jnp.sum(two, axis=0, keepdims=True)], axis=0)


def coords():
    y, d = lax.axis_index('model'), lax.axis_index('data')
    return y, lax.div(d, 2), odd(d)


def flip(here, which):
    return tuple(other(p) if f else p for p, f in zip(here, which))


def flat(here):
    y, x, c = here
    return 4 * y + 2 * x + c


def device(here):
    y, x, c = here
    return (y, 2 * x + c)


def remote(src, dst, send_sem, recv_sem, there):
    return pltpu.make_async_remote_copy(
        src_ref=src, dst_ref=dst, send_sem=send_sem, recv_sem=recv_sem, device_id=device(there),
        device_id_type=pl.DeviceIdType.MESH)


def arrive():
    here = coords()
    for k in PEERS:
        pl.semaphore_signal(pltpu.get_barrier_semaphore(), inc=1, device_id=device(flip(here, k)),
                            device_id_type=pl.DeviceIdType.MESH)


def all_arrived():
    pl.semaphore_wait(pltpu.get_barrier_semaphore(), len(PEERS))


class Share:
    def __init__(self, acc, got, send_sem, recv_sem):
        self.acc, self.got, self.send_sem, self.recv_sem = acc, got, send_sem, recv_sem

    @staticmethod
    def scratch(n, *shape):
        return [pltpu.VMEM((n, *shape), F32), pltpu.VMEM((n, N_DEV, *shape), F32), DMA((n,)), DMA((n,))]

    def start(self, b):
        here = coords()
        me = flat(here)
        self.got[b, me] = self.acc[b]
        for which in PEERS:
            remote(self.acc.at[b], self.got.at[b, me], self.send_sem.at[b], self.recv_sem.at[b],
                   flip(here, which)).start()

    def total(self, b):
        all_of = self.got.at[b, pl.ds(0, len(PEERS))]
        copies = remote(all_of, all_of, self.send_sem.at[b], self.recv_sem.at[b], coords())
        copies.wait_send()
        copies.wait_recv()
        out = self.got[b, 0]
        for f in range(1, N_DEV):
            out += self.got[b, f]
        return out


class Gather:
    def __init__(self, own, dest, n, sems):
        self.own, self.dest, self.n = own, dest, n
        self.ys, self.yr, self.xs, self.xr, self.cs, self.cr = sems
        self.here = coords()
        _, x, c = self.here
        self.mine, self.across = 2 * x + c, 2 * (other(x)) + c
        self.core = (2 * x + other(c), 2 * (other(x)) + other(c))

    @staticmethod
    def scratch(n):
        return [DMA((n,))] * 4 + [DMA((2, n))] * 2

    def y(self, p):
        model = self.here[0]
        return remote(self.own(self.mine, p), self.dest(model, self.mine, p), self.ys.at[p], self.yr.at[p],
                      flip(self.here, Y_PEER))

    def moved(self, q, p, send_sem, recv_sem, which):
        ref = self.dest(1 - self.here[0], q, p)
        return remote(ref, ref, send_sem, recv_sem, flip(self.here, which))

    def x(self, p, q):
        return self.moved(q, p, self.xs.at[p], self.xr.at[p], X_PEER)

    def c(self, p, late, q):
        return self.moved(q, p, self.cs.at[late, p], self.cr.at[late, p], C_PEER)

    def start(self):
        for p in range(self.n):
            self.y(p).start()

    def pass_y(self, p):
        self.moved(self.mine, p, self.ys.at[p], self.yr.at[p], Y_PEER).wait_recv()
        self.x(p, self.mine).start()
        self.c(p, 0, self.mine).start()

    def pass_x(self, p):
        self.x(p, self.across).wait_recv()
        self.c(p, 1, self.across).start()

    def wait_core(self, late):
        for p in range(self.n):
            self.c(p, late, self.core[late]).wait_recv()

    def drain(self):
        for p in range(self.n):
            self.y(p).wait_send()
            self.x(p, self.mine).wait_send()
            self.c(p, 0, self.mine).wait_send()
            self.c(p, 1, self.across).wait_send()


def call(kernel, name, cid, grid, in_specs, out_specs, out_shape, scratch, flops, nbytes, args):
    return pl.pallas_call(
        kernel, name=name, grid=grid, in_specs=in_specs, out_specs=out_specs, out_shape=out_shape, scratch_shapes=scratch,
        compiler_params=pltpu.CompilerParams(vmem_limit_bytes=MAX_VMEM, collective_id=cid, has_side_effects=cid is not None),
        cost_estimate=pl.CostEstimate(flops=flops, bytes_accessed=nbytes, transcendentals=0))(*args)


def fwd_first(h_a, h_b, w_one, w_two, gb_own):
    depth, half = w_one.shape
    dim = 2 * half
    rows = h_a.shape[0] // 2
    tile, width, quarter = 2 * TM, half // 2, half // 4
    steps = rows // tile
    per_block = 2 * steps
    n = 4

    def block(j):
        y, x, _ = coords()
        return jnp.where(j < 2, 2 * y + j, 2 * (other(y)) + jnp.where(j == 2, x, other(x)))

    def tile_of(j, i):
        return jnp.where(odd(j) == 0, i, per_block - 1 - i)

    def kernel(ha_ref, hb_ref, w_ref, w2_ref, gb_ref, u_ref, s_ref, gbo_ref, w2o_ref, ht_ref, w1, gbf, *sems):
        share, sems = Share(*sems[:4]), sems[4:]
        gs, gr, lsem = sems[:3]
        sems = sems[3:]
        j, i = pl.program_id(0), pl.program_id(1)
        step = j * per_block + i
        here = coords()
        y = here[0]
        one = Gather(lambda q, p: w_ref.at[at(p, depth // n), at(q, quarter)],
                     lambda m, q, p: w1.at[at(p, depth // n), at(m * 4 + q, quarter)], n, sems[:6])
        two = Gather(lambda q, p: w2_ref.at[at(q * n + p, quarter // n)],
                     lambda m, q, p: w2o_ref.at[at(q * n + p, quarter // n)], n, sems[6:])

        def local(b):
            return pltpu.make_async_copy(w_ref.at[:, at(b, width)], w1.at[:, at(2 * y + b, width)], lsem.at[b])

        def bn_vectors(m):
            return remote(gb_ref, gbf.at[:, at(m, half)], gs, gr, flip(here, Y_PEER))

        def begin():
            arrive()
            local(0).start()
            local(1).start()
            all_arrived()
            one.start()
            two.start()
            bn_vectors(y).start()
            local(0).wait()

        def late_half():
            one.pass_x(0)
            one.pass_y(n - 1)
            one.wait_core(0)

        def last_block():
            one.pass_x(n - 1)
            two.pass_y(0)
            one.wait_core(1)

        def second_block():
            local(1).wait()
            one.pass_y(1)

        hooks = {0: begin, 2: lambda: one.pass_y(0), per_block: second_block, 6: lambda: one.pass_y(2),
                 2 * per_block: late_half, 9: lambda: one.pass_x(1), 11: lambda: one.pass_x(2), 3 * per_block: last_block,
                 13: lambda: two.pass_y(1), 15: lambda: two.pass_x(0)}
        for s in sorted(hooks):
            pl.when(step == s)(scope(f'hook{s}')(hooks[s]))
        for b in range(3):
            pl.when(step == (b + 1) * per_block)(lambda b=b: share.start(block(b)))

        tile_at = tile_of(j, i)
        first_view = tile_at < steps
        h = lax.select(first_view, ha_ref[...], hb_ref[...])
        cols = at(j, width)
        ht_ref[...] = lax.select(first_view, ha_ref[:, cols], hb_ref[:, cols]).T
        u = mm(h, w1[:, at(block(j), width)])
        u_ref[...] = u
        sums = two_sums(u, u * u)
        v = tile_at // steps
        share.acc[block(j), v] = jnp.where(i % steps == 0, 0.0, share.acc[block(j), v]) + sums

        @pl.when(step == 4 * per_block - 1)
        @scope('f1end')
        def _():
            share.start(block(3))
            two.pass_y(2)
            two.pass_x(1)
            two.pass_y(n - 1)
            for p in range(2, n):
                two.pass_x(p)
            bn_vectors(other(y)).wait_recv()
            bn_vectors(y).wait_send()
            gbo_ref[...] = gbf[...]
            gbo_ref[:, at(y, half)] = gb_ref[...]
            for b in range(4):
                s_ref[:, :, b * width:(b + 1) * width] = share.total(b)
            one.drain()
            two.drain()
            two.wait_core(0)
            two.wait_core(1)

    return call(
        kernel, "fwd_first", 0, (4, per_block),
        [pl.BlockSpec((tile, depth), lambda j, i: (coords()[0] * steps + jnp.minimum(tile_of(j, i), steps - 1), 0)),
         pl.BlockSpec((tile, depth), lambda j, i: (coords()[0] * steps + jnp.maximum(tile_of(j, i) - steps, 0), 0)),
         ANY, ANY, whole(2, half)],
        [pl.BlockSpec((tile, width), lambda j, i: (tile_of(j, i), block(j))), whole(2, 2, dim),
         whole(2, dim), ANY, pl.BlockSpec((width, tile), lambda j, i: (j, tile_of(j, i)))],
        [sds((2 * rows, dim), F32), sds((2, 2, dim), F32), sds((2, dim), F32), sds((half, dim), BF16),
         sds((depth, 2 * rows), BF16)],
        [pltpu.VMEM((depth, dim), BF16), pltpu.VMEM((2, dim), F32)] + Share.scratch(4, 2, 2, width)
        + [DMA, DMA, TWO_DMA] + Gather.scratch(n) * 2,
        4 * rows * depth * dim, 2 * rows * (8 * depth + 4 * dim), (h_a, h_b, w_one, w_two, gb_own))


def fwd_next(u, sums, gb, w_own, w_other, by_rows, total, cid, w_next=None):
    all_rows, depth = u.shape
    dim = w_own.shape[1] if by_rows else 2 * w_own.shape[1]
    half = dim // 2
    quarter = half // 4
    steps = all_rows // 2 // TM
    last = 2 * steps - 1
    slab = dim // (2 * steps)
    n = 4

    def kernel(u_ref, s_ref, gb_ref, wo_ref, wt_ref, *refs):
        if w_next is not None:
            wn_ref, refs = refs[0], refs[1:]
        x_ref, o_ref, so_ref, wtr_ref, *refs = refs
        if w_next is not None:
            wno_ref, *refs = refs
        w, acc, got, ssem, rsem, lsem, *refs = refs
        share = Share(acc, got, ssem, rsem)
        i = pl.program_id(0)
        y = coords()[0]

        def local(ref, model, b):
            where = at(model, half)
            return pltpu.make_async_copy(ref, w.at[where] if by_rows else w.at[:, where], lsem.at[b])

        if w_next is not None:
            gather = Gather(lambda q, p: wn_ref.at[at(p, depth // n), at(q, quarter)],
                            lambda m, q, p: wno_ref.at[at(p, depth // n), at(q, quarter)], n, refs)

        @pl.when(i == 0)
        def _():
            arrive()
            local(wo_ref, y, 0).start()
            local(wt_ref, other(y), 1).start()
            all_arrived()
            if w_next is not None:
                gather.start()
            local(wo_ref, y, 0).wait()
            local(wt_ref, other(y), 1).wait()

        if w_next is not None:
            for p in range(n):
                pl.when(i == p + 1)(lambda p=p: gather.pass_y(p))
                pl.when(i == p + 3)(lambda p=p: gather.pass_x(p))
        pl.when(i == steps)(lambda: share.start(0))

        mean, inv = mean_inv(s_ref[0], total)
        act = jnp.maximum((u_ref[...] - mean) * inv * gb_ref[:1] + gb_ref[1:], 0.0).astype(BF16)
        x_ref[...] = act.T
        out = mm(act, w[...])
        o_ref[...] = out
        wtr_ref[...] = w[:, at(i, slab)].T
        v = i // steps
        share.acc[v] = jnp.where(i % steps == 0, 0.0, share.acc[v]) + two_sums(out, out * out)

        @pl.when(i == last)
        def _():
            share.start(1)
            with scope('wait_last'):
                for b in BOTH:
                    so_ref[b] = share.total(b)
            if w_next is not None:
                gather.drain()
                gather.wait_core(0)
                gather.wait_core(1)

    more = w_next is not None
    return call(
        kernel, "fwd_next", cid, (2 * steps,),
        [pl.BlockSpec((TM, depth), lambda i: (i, 0)), pl.BlockSpec((1, 2, depth), lambda i: (i // steps, 0, 0)),
         whole(2, depth), ANY, ANY] + [ANY] * more,
        [pl.BlockSpec((depth, TM), lambda i: (0, i)), pl.BlockSpec((TM, dim), lambda i: (i, 0)),
         whole(2, 2, dim), pl.BlockSpec((slab, depth), lambda i: (i, 0))] + [ANY] * more,
        [sds((depth, all_rows), BF16), sds((all_rows, dim), F32), sds((2, 2, dim), F32), sds((dim, depth), BF16)]
        + ([sds(w_next.shape, BF16)] if more else []),
        [pltpu.VMEM((depth, dim), BF16)] + Share.scratch(2, 2, dim) + [TWO_DMA] + (Gather.scratch(n) if more else []),
        2 * all_rows * depth * dim, all_rows * (6 * depth + 4 * dim),
        (u, sums, gb, w_own, w_other) + ((w_next,) if more else ()))


def corr_grad(z, sums, lam, total):
    all_rows, dim = z.shape
    rows = all_rows // 2
    half = dim // 2
    quart = half // 2
    n_chunk = 8
    width = half // n_chunk
    pair = 2 * width
    mt = TM
    zt = TM // 2
    ahead = 3
    z_steps = all_rows // zt
    m_steps = rows // mt
    scale = 1.0 / total

    def kernel(z_ref, s_ref, lam_ref, zho_ref, d_ref, so_ref, zh, da, ck, r1, r2, g, stage, dsend, drecv, acc, got, ssem, rsem, zs, zos,
               d1s, d1r, s1s, s1r, s2s, s2r, a2s, a2r, a1s, a1r, ads, adr, dbs, das):
        share = Share(acc, got, ssem, rsem)
        here = coords()
        y, x, c = here
        on_x = c == 0
        by_core = lambda one, two: tuple(jnp.where(on_x, a, b) for a, b in zip(one, two))
        first = by_core(flip(here, X_PEER), flip(here, Y_PEER))
        second = by_core(flip(here, Y_PEER), flip(here, X_PEER))
        cpeer = flip(here, C_PEER)
        bit1, bit2 = by_core((x, y), (y, x))
        arrive()
        acc[...] = jnp.zeros_like(acc)

        def load(i, slot):
            return pltpu.make_async_copy(z_ref.at[at(i, zt)], ck.at[at(slot, zt)], zs.at[slot])

        def zh_out(i):
            v, r = lax.div(i, n_chunk // 2), lax.rem(i, n_chunk // 2)
            return pltpu.make_async_copy(zh.at[v, at(r, TM)], zho_ref.at[v, at(r, TM)], zos.at[i])

        z_slots = half // zt
        for i in range(ahead):
            load(i, i).start()

        @scope('normalise')
        def normalise(i):
            slot = lax.rem(i, z_slots)
            v, r = lax.div(i, z_steps // 2), lax.rem(i, z_steps // 2)
            pl.when(i + ahead < z_steps)(lambda: load(i + ahead, lax.rem(i + ahead, z_slots)).start())
            load(i, slot).wait()
            mean, inv = mean_inv(s_ref[v], total)
            zh[v, at(r, zt)] = ((ck[at(slot, zt)] - mean) * inv).astype(BF16)

        loop(z_steps, normalise)
        all_arrived()

        def both(v, rows_at, t):
            return jnp.concatenate([zh[v, rows_at, at(b * n_chunk + t, width)] for b in BOTH], axis=1)

        group = lambda t, b: at(2 * t + b, width)

        def to_core(t):
            return remote(dsend.at[odd(t)], drecv.at[odd(t)], d1s.at[t], d1r.at[t], cpeer)

        def to_first(t):
            return remote(ck.at[:, group(t, other(bit1))], r1.at[t], s1s.at[t], s1r.at[t], first)

        def to_second(t):
            return remote(ck.at[at(other(bit2), quart), group(t, bit1)], r2.at[t], s2s.at[t], s2r.at[t], second)

        def g_second(t, b):
            block = g.at[t, at(2 * c + b, quart), at(bit1, width)]
            return remote(block, block, a2s.at[t], a2r.at[t], second)

        def g_first(t, b):
            block = g.at[t, at(c, half), at(b, width)]
            return remote(block, block, a1s.at[t], a1r.at[t], first)

        def g_core(t, core):
            block = g.at[t, at(core, half)]
            return remote(block, block, ads.at[t], adr.at[t], cpeer)

        @scope('chip_sum')
        def chip_sum(t):
            to_core(t).wait_recv()
            to_core(t).wait_send()
            ck[:, at(t, pair)] += drecv[odd(t)]
            to_first(t).start()

        @scope('corr_part')
        def corr_part(t):
            zh_out(t).start()
            right = both(1, pl.ds(0, rows), t)
            dsend[odd(t)] = mm_at(zh[0, :, at(other(c), half)], right)
            ck[:, at(t, pair)] = mm_at(zh[0, :, at(c, half)], right)
            to_core(t).start()

        def db_out(t, m, slot, b):
            return pltpu.make_async_copy(
                stage.at[slot, :, at(b, width)], d_ref.at[1, at(m, mt), at(b * n_chunk + t, width)], dbs.at[slot, b])

        def da_out(m):
            return pltpu.make_async_copy(da.at[at(m, mt)], d_ref.at[0, at(m, mt)], das.at[m])

        def finish(m):
            d = da[at(m, mt)] * scale
            da[at(m, mt)] = d
            acc[0, :2] += two_sums(d, d * zh[0, at(m, mt)].astype(F32))
            da_out(m).start()

        def grads(t):
            @scope('rows_of')
            def rows_of(m):
                slot = odd(m)

                @pl.when(t * m_steps + m >= 2)
                def _():
                    for b in BOTH:
                        db_out(t, m, slot, b).wait()

                db = mm(zh[0, at(m, mt)], g[t]) * scale
                stage[slot] = db
                own = both(1, at(m, mt), t)
                sums = two_sums(db, db * own.astype(F32))
                for b in BOTH:
                    acc[1, :2, at(b * n_chunk + t, width)] += sums[:, b * width:(b + 1) * width]
                    db_out(t, m, slot, b).start()
                da[at(m, mt)] = jnp.where(t == 0, 0.0, da[at(m, mt)]) + mm_bt(own, g[t])
                pl.when(t == n_chunk - 1)(lambda: finish(m))

            loop(m_steps, rows_of)

        @scope('at_first')
        def at_first(t):
            to_first(t).wait_recv()
            ck[:, group(t, bit1)] += r1[t]
            to_second(t).start()

        @scope('at_second')
        def at_second(t):
            to_second(t).wait_recv()
            corr_mat = (ck[at(bit2, quart), group(t, bit1)] + r2[t]) * scale
            row_ids = (2 * c + bit2) * quart + lax.broadcasted_iota(jnp.int32, (quart, width), 0)
            col_ids = (bit1 * n_chunk + t) * width + lax.broadcasted_iota(jnp.int32, (quart, width), 1)
            is_diag = row_ids == col_ids
            lam_val = lam_ref[0]
            loss = jnp.where(is_diag, (1.0 - corr_mat) * (1.0 - corr_mat), lam_val * corr_mat * corr_mat)
            acc[0, 2:3, :width] += jnp.sum(loss, axis=0, keepdims=True)
            grad = jnp.where(is_diag, -2.0 * (1.0 - corr_mat), 2.0 * lam_val * corr_mat).astype(BF16)
            g[t, at(2 * c + bit2, quart), at(bit1, width)] = grad
            g_second(t, bit2).start()

        @scope('back_second')
        def back_second(t):
            g_second(t, other(bit2)).wait_recv()
            g_first(t, bit1).start()

        @scope('back_first')
        def back_first(t):
            g_first(t, other(bit1)).wait_recv()
            g_core(t, c).start()

        def back_core(t):
            g_core(t, other(c)).wait_recv()
            grads(t)

        lead = 3

        def advance(tau):
            for lag, stage_fn in ((lead, at_first), (lead + 1, back_second), (lead + 2, back_first), (lead + 3, back_core),
                                  (lead, at_second), (1, chip_sum), (0, corr_part)):
                t = tau - lag
                pl.when(jnp.logical_and(t >= 0, t < n_chunk))(lambda t=t, stage_fn=stage_fn: stage_fn(t))

        loop(n_chunk + lead + 3, advance)
        share.start(1)
        share.start(0)
        for t in range(n_chunk):
            for copy in (to_first(t), to_second(t), g_second(t, bit2), g_first(t, bit1), g_core(t, c)):
                copy.wait_send()
        for b in BOTH:
            so_ref[b] = share.total(b)
            for slot in BOTH:
                db_out(0, 0, slot, b).wait()
        for i in range(n_chunk):
            zh_out(i).wait()
        for m in range(m_steps):
            da_out(m).wait()

    return call(
        kernel, "corr_grad", 3, (), [ANY, VMEM, pl.BlockSpec(memory_space=pltpu.SMEM)], [ANY, ANY, VMEM],
        [sds((2, rows, dim), BF16), sds((2, rows, dim), F32), sds((2, 4, dim), F32)],
        [pltpu.VMEM((2, rows, dim), BF16), pltpu.VMEM((rows, dim), F32), pltpu.VMEM((half, dim), F32),
         pltpu.VMEM((n_chunk, half, width), F32), pltpu.VMEM((n_chunk, quart, width), F32),
         pltpu.VMEM((n_chunk, dim, pair), BF16), pltpu.VMEM((2, mt, pair), F32)]
        + [pltpu.VMEM((2, half, pair), F32)] * 2 + Share.scratch(2, 4, dim)
        + [DMA((half // zt,)), DMA((n_chunk,))] + [DMA((n_chunk,))] * 12 + [DMA((2, 2)), DMA((m_steps,))],
        all_rows * dim * dim * 3, all_rows * dim * 12, (z, sums, lam))


def backward(d_emb, zh, sz, s_emb, layers, x2_t, total):
    all_rows, dim = zh.shape
    rows, half = all_rows // 2, dim // 2
    width = 256
    slabs = dim // width
    items = 2 * slabs
    piece = width
    side = half // 2 // piece
    per_slab = half // piece
    n_layer = len(layers) + 1
    n_slab = n_layer * slabs
    per_layer = slabs * side
    n_chunk = n_layer * per_layer
    ahead = 3
    (u2, s2, gb2, w3_t, x1_t), (u1, s1, gb1, w2_t, h_t) = layers

    def kernel(d_ref, zh_ref, sz_ref, sd_ref, x2_ref, x1_ref, h_ref, u2_ref, u1_ref, w3_ref, w2_ref,
               s2_ref, s1_ref, gb2_ref, gb1_ref, dw3_ref, dw2_ref, dw1_ref, sum_ref, dy_ref, part_ref, ry_ref, rx_ref,
               dbuf, xbuf, wbuf, ubuf, dybuf, dyout, psend, pkeep, dr, ebuf, mbuf, fbuf, acc, got, ssem, rsem,
               us, ws, ds, dos, xl, ps, pr, pm, ys, yr, xs, xr, es, fs, fcs, fcr, credit):
        share = Share(acc, got, ssem, rsem)
        here = coords()
        y, x, c = here
        ypeer, xpeer, cpeer = flip(here, Y_PEER), flip(here, X_PEER), flip(here, C_PEER)
        arrive()

        def column(k, n):
            model = odd(n + jnp.where(k == 0, other(y), 0))
            return jnp.where(k == 1, n, model * (slabs // 2) + lax.div(n, 2))

        def turn(k):
            return jnp.where(k == 0, 0, other(y))

        def m_slot(j):
            return lax.rem(j, 4)

        def copy(src, dst, sem):
            return pltpu.make_async_copy(src, dst, sem)

        def sent_by(q):
            first = jnp.minimum(per_slab * lax.div(q, 4), per_layer)
            middle = jnp.clip(side * lax.div(q - 2 * items - 2, 2), 0, per_layer)
            last = jnp.clip(per_slab * lax.div(q - 4 * items - 2, 4), 0, per_layer)
            return first + middle + last

        def begun(q):
            return jnp.maximum(lax.div(7 * q - 33, 16), 0)

        def to_core(s):
            return remote(psend.at[odd(s)], dr.at[odd(s)], ps.at[s], pr.at[s], cpeer)

        def keep_out(s):
            return copy(pkeep.at[odd(s)], part_ref.at[s], pm)

        @scope('chip_sum')
        def chip_sum(s):
            to_core(s).wait_recv()
            pkeep[odd(s)] += dr[odd(s)]

            @pl.when(s + 2 < n_slab)
            def _():
                pl.semaphore_signal(credit, inc=1, device_id=device(cpeer), device_id_type=pl.DeviceIdType.MESH)

            to_core(s).wait_send()
            keep_out(s).start()

        def home(j, own):
            k = lax.div(j, per_layer)
            i = lax.rem(j, per_layer)
            model = y if own else other(y)
            turned = other(turn(k)) if own else turn(k)
            s = jnp.where(k == 1, lax.div(i, side), 2 * lax.div(i, per_slab) + turned)
            place = jnp.where(k == 1, model * side + lax.rem(i, side), lax.rem(i, per_slab))
            return part_ref.at[k * slabs + s, at(place, piece)]

        def to_y(j):
            return remote(home(j, False), ry_ref.at[j], ys.at[lax.div(j, per_layer)], yr.at[j], ypeer)

        @scope('issue')
        def issue(s, q):
            keep_out(s).wait()
            k, n = lax.div(s, slabs), lax.rem(s, slabs)
            for mine, fire, first, count in (
                    (k == 1, True, n * side, side), (k != 1, odd(n) == jnp.where(k == 0, 0, 1), lax.div(n, 2) * per_slab, per_slab)):
                for r in range(count):
                    j = k * per_layer + first + r
                    pl.when(mine & fire & (j < begun(q) + ahead))(lambda j=j: to_y(j).start())

        def to_x(j):
            return remote(mbuf.at[m_slot(j)], rx_ref.at[j], xs.at[m_slot(j)], xr.at[j], xpeer)

        def result(j, k):
            i = lax.rem(j, per_layer)
            if k == 1:
                return dw2_ref.at[at(c * side + lax.rem(i, side), piece), at(lax.div(i, side), width)]
            return (dw1_ref if k else dw3_ref).at[at(c * per_slab + lax.rem(i, per_slab), piece), at(lax.div(i, per_slab), width)]

        def put(j, k):
            slot = odd(j)
            return (copy(fbuf.at[slot], result(j, k), fs.at[slot]),
                    remote(fbuf.at[slot], result(j, k), fcs.at[slot], fcr.at[k], cpeer))

        def put_done(j):
            here_copy, there_copy = put(j, 0)
            here_copy.wait()
            there_copy.wait_send()

        def load_part(j, which):
            src = (lambda: ry_ref.at[j], lambda: home(j, True), lambda: rx_ref.at[j])[which]()
            return copy(src, ebuf.at[which], es.at[which])

        @scope('fetch_x')
        def fetch_x(j):
            to_x(j).wait_recv()
            load_part(j, 2).start()

        @scope('begin')
        def begin(j, q):
            remote(ry_ref.at[j], ry_ref.at[j], ys.at[0], yr.at[j], ypeer).wait_recv()
            load_part(j, 0).start()
            load_part(j, 1).start()
            pl.when(j + ahead < sent_by(q))(lambda: to_y(j + ahead).start())
            pl.when(j >= 2)(lambda: fetch_x(j - 2))

        @scope('deliver')
        def deliver(j):
            load_part(j, 2).wait()
            pl.when(j >= 2)(lambda: put_done(j))
            fbuf[odd(j)] = mbuf[m_slot(j)] + ebuf[2]
            for k in range(n_layer):
                @pl.when(lax.div(j, per_layer) == k)
                def _(k=k):
                    for one in put(j, k):
                        one.start()

        @scope('end')
        def end(j):
            load_part(j, 0).wait()
            load_part(j, 1).wait()
            pl.when(j >= 4)(lambda: to_x(j).wait_send())
            mbuf[m_slot(j)] = ebuf[0] + ebuf[1]
            to_x(j).start()
            pl.when(j >= 2)(lambda: deliver(j - 2))

        def events(q):
            now, before, earlier = begun(q), begun(q - 1), begun(q - 2)
            pl.when(before > earlier)(lambda: end(before - 1))
            pl.when(now > before)(lambda: begin(now - 1, q))

        @scope('weight_slab')
        def weight_slab(k, n, v, d):
            s = k * slabs + n
            for buf, part in ((psend, other(c)), (pkeep, c)):
                first = jnp.where(k == 1, part, 2 * part)
                for b in BOTH:
                    left = xbuf[at(first + b * jnp.where(k == 1, 2, 1), half // 2), at(v, rows)]
                    here_at = at(b, half // 2)
                    buf[odd(s), here_at] = jnp.where(v == 0, 0.0, buf[odd(s), here_at]) + mm(left, d)

        def after(k, n, v, q):
            s = k * slabs + n
            pl.when((v == 0) & (n > 0))(lambda: chip_sum(s - 1))

            @pl.when(v == 1)
            def _():
                pl.when(s >= 2)(lambda: pl.semaphore_wait(credit, 1))
                to_core(s).start()
                pl.when(n > 0)(lambda: issue(s - 1, q))

        def emb_loads(i):
            n, v = split(i)
            cols = at(column(0, n), width)
            return (copy(d_ref.at[at(v, rows), cols], ubuf.at[v], us.at[v]),
                    copy(zh_ref.at[at(v, rows), cols], wbuf.at[v], ws.at[v]))

        def x_load(src, v):
            return copy(src.at[:, at(v, rows)], xbuf.at[:, at(v, rows)], xl.at[v])

        def slab_of(ref, layer, i, buf, sem):
            n, v = split(i)
            return copy(ref.at[at(v, rows), at(column(layer + 1, n), width)], buf.at[v], sem.at[v])

        def u_load(layer, i, ref=u2_ref):
            return slab_of(ref, layer, i, ubuf, us)

        def dy_load(layer, i):
            return slab_of(dy_ref, layer, i, dybuf, ds)

        def dy_out(layer, i):
            n, v = split(i)
            return copy(dyout.at[v], dy_ref.at[at(v, rows), at(column(layer + 1, n), width)], dos.at[v])

        def w_load(layer, n, ref=w3_ref):
            return copy(ref.at[:, at(column(layer + 1, n), width)], wbuf.at[odd(n)], ws.at[odd(n)])

        def start_u(layer, i):
            for k, ref in enumerate((u2_ref, u1_ref)):
                pl.when(layer == k)(lambda ref=ref: u_load(layer, i, ref).start())

        def start_w(layer, n):
            for k, ref in enumerate((w3_ref, w2_ref)):
                pl.when(layer == k)(lambda ref=ref: w_load(layer, n, ref).start())

        for one in (x_load(x2_ref, 0), *emb_loads(0), x_load(x2_ref, 1)):
            one.start()
        all_arrived()

        def emb_item(i):
            n, v = split(i)

            @pl.when(i + 1 < items)
            def _():
                for one in emb_loads(i + 1):
                    one.start()

            @pl.when(i + 1 == items)
            def _():
                u_load(0, 0).start()
                w_load(0, 0).start()

            pl.when(n == 0)(lambda: x_load(x2_ref, v).wait())
            for one in emb_loads(i):
                one.wait()
            events(i)
            cols = at(column(0, n), width)
            _, inv = mean_inv(sz_ref[v, :, cols], total)
            sd = sd_ref[v, :2, cols] / total
            d = (inv * (ubuf[v] - sd[:1] - wbuf[v].astype(F32) * sd[1:])).astype(BF16)
            dbuf[at(v, rows), cols] = d
            weight_slab(0, n, v, d)
            after(0, n, v, i)

        loop(items, emb_item)
        for v in BOTH:
            x_load(x1_ref, v).start()

        def stats(layer, v, cols):
            pick = lambda one, two: jnp.where(layer == 0, one, two)
            mean, inv = mean_inv(pick(s2_ref[v, :, cols], s1_ref[v, :, cols]), total)
            gb = pick(gb2_ref[:, cols], gb1_ref[:, cols])
            return mean, inv, gb[:1], gb[1:]

        def bn_layer(layer):
            start = (2 * layer + 1) * items

            def dx_item(i):
                n, v = split(i)
                cols = at(column(layer + 1, n), width)

                @pl.when(i + 1 < items)
                def _():
                    start_u(layer, i + 1)
                    pl.when((v == 0) & (n + 1 < slabs))(lambda: start_w(layer, n + 1))

                @pl.when(i + 1 == items)
                def _():
                    start_u(layer, 0)
                    dy_load(layer, 0).start()

                scope('wait_u')(u_load(layer, i).wait)()
                pl.when(v == 0)(lambda: w_load(layer, n).wait())
                events(start + i)
                pl.when(n > 0)(lambda: dy_out(layer, i).wait())
                with scope('dx'):
                    mean, inv, gamma, beta = stats(layer, v, cols)
                    sums = 0.0
                    for b in range(rows // TM):
                        some = at(b, TM)
                        dx = mm(dbuf[at(v * (rows // TM) + b, TM)], wbuf[odd(n)])
                        norm = (ubuf[v, some] - mean) * inv
                        dy = jnp.where(norm * gamma + beta > 0, dx, 0.0)
                        dyout[v, some] = dy
                        sums += two_sums(dy, dy * norm)
                dy_out(layer, i).start()
                g = layer * items + i
                acc[g] = sums
                share.start(g)
                before = (layer + 1) * slabs - 1
                pl.when(i == 0)(lambda: chip_sum(before))
                pl.when(i == 1)(lambda: issue(before, start + i))

            def dw_item(i):
                n, v = split(i)
                cols = at(column(layer + 1, n), width)

                @pl.when(i + 1 < items)
                def _():
                    start_u(layer, i + 1)
                    dy_load(layer, i + 1).start()

                @pl.when((i + 1 == items) & (layer == 0))
                def _():
                    u_load(1, 0, u1_ref).start()
                    w_load(1, 0, w2_ref).start()

                pl.when(n == 0)(lambda: x_load(x1_ref, v).wait())
                u_load(layer, i).wait()
                dy_load(layer, i).wait()
                events(start + items + i)
                with scope('wait_stats'):
                    tot = share.total(layer * items + i)
                sum_ref[layer, v, :, cols] = tot
                mean, inv, gamma, _ = stats(layer, v, cols)
                tot = tot / total
                d = (gamma * inv * (dybuf[v] - (tot[:1] + (ubuf[v] - mean) * (inv * tot[1:])))).astype(BF16)
                dbuf[at(v, rows), cols] = d
                weight_slab(layer + 1, n, v, d)
                after(layer + 1, n, v, start + items + i)

            loop(items, dx_item)
            for v in BOTH:
                dy_out(layer, v).wait()
            loop(items, dw_item)

            @pl.when(layer == 0)
            def _():
                for v in BOTH:
                    x_load(h_ref, v).start()

        loop(len(layers), bn_layer)

        ticks = (2 * n_layer - 1) * items
        chip_sum(n_slab - 1)
        issue(n_slab - 1, ticks)
        ended = 2 * per_layer

        def tail(j):
            begin(j, ticks + 2)
            end(j)

        loop(n_chunk, tail, ended)
        for j in range(n_chunk - 2, n_chunk):
            fetch_x(j)
            deliver(j)
        for j in BOTH:
            put_done(j)
        for k in range(n_layer):
            theirs = dw2_ref.at[at(other(c), half // 2)] if k == 1 else (dw1_ref if k else dw3_ref).at[at(other(c), half)]
            remote(theirs, theirs, fcs.at[0], fcr.at[k], cpeer).wait_recv()
            sent = ry_ref.at[at(k, per_layer)]
            remote(sent, sent, ys.at[k], yr.at[0], ypeer).wait_send()
        for j in range(n_chunk - 4, n_chunk):
            to_x(j).wait_send()

    n_item = len(layers) * items
    vm = lambda *shape: pltpu.VMEM(shape, F32)
    bf = lambda *shape: pltpu.VMEM(shape, BF16)
    return call(
        kernel, "backward", 4, (),
        [ANY, ANY, VMEM, VMEM] + [ANY] * 7 + [VMEM] * 4, [ANY] * 3 + [VMEM] + [ANY] * 4,
        [sds((dim, half), F32), sds((half, dim), F32), sds((dim, half), F32), sds((len(layers), 2, 2, dim), F32),
         sds((all_rows, dim), F32), sds((n_slab, half, width), F32), sds((n_chunk, piece, width), F32),
         sds((n_chunk, piece, width), F32)],
        [bf(all_rows, dim), bf(dim, all_rows), bf(2, dim, width), vm(2, rows, width), vm(2, rows, width), vm(2, rows, width),
         vm(2, half, width), vm(2, half, width), vm(2, half, width), vm(3, piece, width), vm(4, piece, width),
         vm(2, piece, width)] + Share.scratch(n_item, 2, width)
        + [TWO_DMA, TWO_DMA, TWO_DMA, TWO_DMA, TWO_DMA, DMA((n_slab,)), DMA((n_slab,)), DMA, DMA((n_layer,)),
           DMA((n_chunk,)), DMA((4,)), DMA((n_chunk,)), DMA((3,)), TWO_DMA, TWO_DMA, DMA((n_layer,)),
           pltpu.SemaphoreType.REGULAR],
        all_rows * dim * dim * 10, all_rows * dim * 40,
        (d_emb, zh, sz, s_emb, x2_t, x1_t, h_t, u2, u1, w3_t, w2_t, s2, s1, gb2, gb1))


def settle(*grads):
    steps = 8

    def kernel(*refs):
        for src, dst in zip(refs[:len(grads)], refs[len(grads):]):
            dst[...] = src[...]

    specs = [pl.BlockSpec((g.shape[0] // steps, g.shape[1]), lambda i: (i, 0)) for g in grads]
    return call(kernel, "settle", None, (steps,), specs, specs, [sds(g.shape, F32) for g in grads], [], 0,
                len(grads) * grads[0].size * 8, grads)


def solution(mesh):
    def shard_body(h_a, h_b, w_one, w_two, w_three, g_one, b_one, g_two, b_two, lam_off):
        y = lax.axis_index('model')
        total = float(h_a.shape[0] * mesh.shape['data'])
        dim, half = w_three.shape
        gb2 = jnp.stack([g_two, b_two])
        u1, s1, gb1, w_two_o, h_t = fwd_first(h_a, h_b, w_one, w_two, jnp.stack([g_one, b_one]))
        x1_t, u2, s2, w2_t, w_three_o = fwd_next(u1, s1, gb1, w_two, w_two_o, True, total, 1, w_three)
        x2_t, z, sz, w3_t = fwd_next(u2, s2, gb2, w_three, w_three_o, False, total, 2)
        zh, d_emb, s_emb = corr_grad(z, sz, lam_off, total)
        loss = jnp.sum(s_emb[0, 2])
        dw_three, dw_two, dw_one, sums, *_ = backward(
            d_emb.reshape(z.shape), zh.reshape(z.shape), sz, s_emb,
            ((u2, s2, gb2, w3_t, x1_t), (u1, s1, gb1, w2_t, h_t)), x2_t, total)
        dw_three, dw_two, dw_one = settle(dw_three, dw_two, dw_one)
        sums = jnp.sum(sums, axis=1)
        sum2 = sums[0]
        sum1 = lax.dynamic_slice_in_dim(sums[1], y * half, half, 1)
        return loss.reshape(1), dw_one, dw_two, dw_three, sum1[1], sum1[0], sum2[1], sum2[0]

    in_specs = (P('data', None), P('data', None), P(None, 'model'), P('model', None), P(None, 'model'),
                P('model'), P('model'), P(), P(), P())
    out_specs = (P(), P(None, 'model'), P('model', None), P(None, 'model'), P('model'), P('model'), P(), P())
    return jax.shard_map(shard_body, mesh=mesh, in_specs=in_specs, out_specs=out_specs, check_vma=False)
```

```python
import functools

import jax
import jax.numpy as jnp
from jax import lax
from jax.experimental import pallas as pl
from jax.experimental.pallas import tpu as pltpu
from jax.sharding import PartitionSpec as P

BN_EPS = 1e-5
F32 = jnp.float32
BF16 = jnp.bfloat16
TM = 512
MAX_VMEM = 67043328
ANY = pl.BlockSpec(memory_space=pl.ANY)
VMEM = pl.BlockSpec(memory_space=pltpu.VMEM)
DMA = pltpu.SemaphoreType.DMA
TWO_DMA = DMA((2,))
BOTH = (0, 1)
PEERS = [(ky, kx, kc) for ky in BOTH for kx in BOTH for kc in BOTH][1:]
C_PEER, X_PEER, Y_PEER = PEERS[0], PEERS[1], PEERS[3]
N_DEV = len(PEERS) + 1


def mm(left, right):
    return jnp.dot(left, right, preferred_element_type=F32)


def mm_bt(left, right):
    return lax.dot_general(left, right, (((1,), (1,)), ((), ())), preferred_element_type=F32)


def mm_at(left, right):
    return lax.dot_general(left, right, (((0,), (0,)), ((), ())), preferred_element_type=F32)


def other(p):
    return 1 - p


def odd(i):
    return lax.rem(i, 2)


def split(i):
    return lax.div(i, 2), odd(i)


def loop(n, body, start=0):
    def one(i, carry):
        body(i)
        return carry

    lax.fori_loop(start, n, one, 0)


def whole(*shape):
    return pl.BlockSpec(shape, lambda *_: (0,) * len(shape))


def at(i, n):
    return pl.ds(pl.multiple_of(i * n, n), n)


def sds(shape, dtype):
    return jax.ShapeDtypeStruct(shape, dtype)


def mean_inv(sums, total):
    mean = sums[:1] / total
    var = sums[1:2] / total - mean * mean
    return mean, lax.rsqrt(var + BN_EPS)


def two_sums(one, two):
    return jnp.concatenate([jnp.sum(one, axis=0, keepdims=True), jnp.sum(two, axis=0, keepdims=True)], axis=0)


def coords():
    y, d = lax.axis_index('model'), lax.axis_index('data')
    return y, lax.div(d, 2), odd(d)


def flip(here, which):
    return tuple(other(p) if f else p for p, f in zip(here, which))


def flat(here):
    y, x, c = here
    return 4 * y + 2 * x + c


def device(here):
    y, x, c = here
    return (y, 2 * x + c)


def remote(src, dst, send_sem, recv_sem, there):
    return pltpu.make_async_remote_copy(
        src_ref=src, dst_ref=dst, send_sem=send_sem, recv_sem=recv_sem, device_id=device(there),
        device_id_type=pl.DeviceIdType.MESH)


def arrive():
    here = coords()
    for k in PEERS:
        pl.semaphore_signal(pltpu.get_barrier_semaphore(), inc=1, device_id=device(flip(here, k)),
                            device_id_type=pl.DeviceIdType.MESH)


def all_arrived():
    pl.semaphore_wait(pltpu.get_barrier_semaphore(), len(PEERS))


class Share:
    def __init__(self, acc, got, send_sem, recv_sem):
        self.acc, self.got, self.send_sem, self.recv_sem = acc, got, send_sem, recv_sem

    @staticmethod
    def scratch(n, *shape):
        return [pltpu.VMEM((n, *shape), F32), pltpu.VMEM((n, N_DEV, *shape), F32), DMA((n,)), DMA((n,))]

    def start(self, b):
        here = coords()
        me = flat(here)
        self.got[b, me] = self.acc[b]
        for which in PEERS:
            remote(self.acc.at[b], self.got.at[b, me], self.send_sem.at[b], self.recv_sem.at[b],
                   flip(here, which)).start()

    def total(self, b):
        all_of = self.got.at[b, pl.ds(0, len(PEERS))]
        copies = remote(all_of, all_of, self.send_sem.at[b], self.recv_sem.at[b], coords())
        copies.wait_send()
        copies.wait_recv()
        out = self.got[b, 0]
        for f in range(1, N_DEV):
            out += self.got[b, f]
        return out


class Gather:
    def __init__(self, own, dest, n, sems):
        self.own, self.dest, self.n = own, dest, n
        self.ys, self.yr, self.xs, self.xr, self.cs, self.cr = sems
        self.here = coords()
        _, x, c = self.here
        self.mine, self.across = 2 * x + c, 2 * (other(x)) + c
        self.core = (2 * x + other(c), 2 * (other(x)) + other(c))

    @staticmethod
    def scratch(n):
        return [DMA((n,))] * 4 + [DMA((2, n))] * 2

    def y(self, p):
        model = self.here[0]
        return remote(self.own(self.mine, p), self.dest(model, self.mine, p), self.ys.at[p], self.yr.at[p],
                      flip(self.here, Y_PEER))

    def moved(self, q, p, send_sem, recv_sem, which):
        ref = self.dest(1 - self.here[0], q, p)
        return remote(ref, ref, send_sem, recv_sem, flip(self.here, which))

    def x(self, p, q):
        return self.moved(q, p, self.xs.at[p], self.xr.at[p], X_PEER)

    def c(self, p, late, q):
        return self.moved(q, p, self.cs.at[late, p], self.cr.at[late, p], C_PEER)

    def start(self):
        for p in range(self.n):
            self.y(p).start()

    def pass_y(self, p):
        self.moved(self.mine, p, self.ys.at[p], self.yr.at[p], Y_PEER).wait_recv()
        self.x(p, self.mine).start()
        self.c(p, 0, self.mine).start()

    def pass_x(self, p):
        self.x(p, self.across).wait_recv()
        self.c(p, 1, self.across).start()

    def wait_core(self, late):
        for p in range(self.n):
            self.c(p, late, self.core[late]).wait_recv()

    def drain(self):
        for p in range(self.n):
            self.y(p).wait_send()
            self.x(p, self.mine).wait_send()
            self.c(p, 0, self.mine).wait_send()
            self.c(p, 1, self.across).wait_send()


def call(kernel, name, cid, grid, in_specs, out_specs, out_shape, scratch, flops, nbytes, args):
    return pl.pallas_call(
        kernel, name=name, grid=grid, in_specs=in_specs, out_specs=out_specs, out_shape=out_shape, scratch_shapes=scratch,
        compiler_params=pltpu.CompilerParams(vmem_limit_bytes=MAX_VMEM, collective_id=cid, has_side_effects=cid is not None),
        cost_estimate=pl.CostEstimate(flops=flops, bytes_accessed=nbytes, transcendentals=0))(*args)


def fwd_first(h_a, h_b, w_one, w_two, gb_own):
    depth, half = w_one.shape
    dim = 2 * half
    rows = h_a.shape[0] // 2
    tile, width, quarter = 2 * TM, half // 2, half // 4
    steps = rows // tile
    per_block = 2 * steps
    n, n2 = 4, 8

    def block(j):
        y, x, _ = coords()
        return jnp.where(j < 2, 2 * y + j, 2 * (other(y)) + jnp.where(j == 2, x, other(x)))

    def tile_of(j, i):
        return jnp.where(odd(j) == 0, i, per_block - 1 - i)

    def kernel(ha_ref, hb_ref, w_ref, w2_ref, gb_ref, u_ref, s_ref, gbo_ref, w2o_ref, ht_ref, w1, gbf, *sems):
        share, sems = Share(*sems[:4]), sems[4:]
        gs, gr, lsem = sems[:3]
        sems = sems[3:]
        j, i = pl.program_id(0), pl.program_id(1)
        step = j * per_block + i
        here = coords()
        y = here[0]
        one = Gather(lambda q, p: w_ref.at[at(p, depth // n), at(q, quarter)],
                     lambda m, q, p: w1.at[at(p, depth // n), at(m * 4 + q, quarter)], n, sems[:6])
        two = Gather(lambda q, p: w2_ref.at[at(q * n2 + p, quarter // n2)],
                     lambda m, q, p: w2o_ref.at[at(q * n2 + p, quarter // n2)], n2, sems[6:])

        def local(b):
            return pltpu.make_async_copy(w_ref.at[:, at(b, width)], w1.at[:, at(2 * y + b, width)], lsem.at[b])

        def bn_vectors(m):
            return remote(gb_ref, gbf.at[:, at(m, half)], gs, gr, flip(here, Y_PEER))

        def begin():
            arrive()
            local(0).start()
            local(1).start()
            all_arrived()
            one.start()
            two.start()
            bn_vectors(y).start()
            local(0).wait()

        def late_half():
            one.pass_x(0)
            one.pass_y(n - 1)
            one.wait_core(0)

        hooks = [(0, begin), (per_block, lambda: local(1).wait()), (2 * per_block, late_half)]
        hooks += [(2 * p + 3, functools.partial(one.pass_y, p)) for p in range(n - 1)]
        hooks += [(p + 2 * per_block, functools.partial(one.pass_x, p)) for p in range(1, n)]
        hooks += [(3 * per_block, lambda: one.wait_core(1))]
        hooks += [(p + 9, functools.partial(two.pass_y, p)) for p in range(n2 - 1)]
        hooks += [(13 + (p + 1) // 2, functools.partial(two.pass_x, p)) for p in range(n2 // 2)]
        for s, hook in hooks:
            pl.when(step == s)(hook)
        for b in range(3):
            pl.when(step == (b + 1) * per_block)(lambda b=b: share.start(block(b)))

        tile_at = tile_of(j, i)
        first_view = tile_at < steps
        h = lax.select(first_view, ha_ref[...], hb_ref[...])
        cols = at(j, width)
        ht_ref[...] = lax.select(first_view, ha_ref[:, cols], hb_ref[:, cols]).T
        u = mm(h, w1[:, at(block(j), width)])
        u_ref[...] = u
        sums = two_sums(u, u * u)
        v = tile_at // steps
        share.acc[block(j), v] = jnp.where(i % steps == 0, 0.0, share.acc[block(j), v]) + sums

        @pl.when(step == 4 * per_block - 1)
        def _():
            share.start(block(3))
            two.pass_y(n2 - 1)
            for p in range(n2 // 2, n2):
                two.pass_x(p)
            bn_vectors(other(y)).wait_recv()
            bn_vectors(y).wait_send()
            gbo_ref[...] = gbf[...]
            gbo_ref[:, at(y, half)] = gb_ref[...]
            for b in range(4):
                s_ref[:, :, b * width:(b + 1) * width] = share.total(b)
            one.drain()
            two.drain()
            two.wait_core(0)
            two.wait_core(1)

    return call(
        kernel, "fwd_first", 0, (4, per_block),
        [pl.BlockSpec((tile, depth), lambda j, i: (coords()[0] * steps + jnp.minimum(tile_of(j, i), steps - 1), 0)),
         pl.BlockSpec((tile, depth), lambda j, i: (coords()[0] * steps + jnp.maximum(tile_of(j, i) - steps, 0), 0)),
         ANY, ANY, whole(2, half)],
        [pl.BlockSpec((tile, width), lambda j, i: (tile_of(j, i), block(j))), whole(2, 2, dim),
         whole(2, dim), ANY, pl.BlockSpec((width, tile), lambda j, i: (j, tile_of(j, i)))],
        [sds((2 * rows, dim), F32), sds((2, 2, dim), F32), sds((2, dim), F32), sds((half, dim), BF16),
         sds((depth, 2 * rows), BF16)],
        [pltpu.VMEM((depth, dim), BF16), pltpu.VMEM((2, dim), F32)] + Share.scratch(4, 2, 2, width)
        + [DMA, DMA, TWO_DMA] + Gather.scratch(n) + Gather.scratch(n2),
        4 * rows * depth * dim, 2 * rows * (8 * depth + 4 * dim), (h_a, h_b, w_one, w_two, gb_own))


def fwd_next(u, sums, gb, w_own, w_other, by_rows, total, cid, w_next=None):
    all_rows, depth = u.shape
    dim = w_own.shape[1] if by_rows else 2 * w_own.shape[1]
    half = dim // 2
    quarter = half // 4
    steps = all_rows // 2 // TM
    last = 2 * steps - 1
    slab = dim // (2 * steps)
    n = 4

    def kernel(u_ref, s_ref, gb_ref, wo_ref, wt_ref, *refs):
        if w_next is not None:
            wn_ref, refs = refs[0], refs[1:]
        x_ref, o_ref, so_ref, wtr_ref, *refs = refs
        if w_next is not None:
            wno_ref, *refs = refs
        w, acc, got, ssem, rsem, lsem, *refs = refs
        share = Share(acc, got, ssem, rsem)
        i = pl.program_id(0)
        y = coords()[0]

        def local(ref, model, b):
            where = at(model, half)
            return pltpu.make_async_copy(ref, w.at[where] if by_rows else w.at[:, where], lsem.at[b])

        if w_next is not None:
            gather = Gather(lambda q, p: wn_ref.at[at(p, depth // n), at(q, quarter)],
                            lambda m, q, p: wno_ref.at[at(p, depth // n), at(q, quarter)], n, refs)

        @pl.when(i == 0)
        def _():
            arrive()
            local(wo_ref, y, 0).start()
            local(wt_ref, other(y), 1).start()
            all_arrived()
            if w_next is not None:
                gather.start()
            local(wo_ref, y, 0).wait()
            local(wt_ref, other(y), 1).wait()

        if w_next is not None:
            for p in range(n):
                pl.when(i == p + 1)(lambda p=p: gather.pass_y(p))
                pl.when(i == p + 3)(lambda p=p: gather.pass_x(p))
        pl.when(i == steps)(lambda: share.start(0))

        mean, inv = mean_inv(s_ref[0], total)
        act = jnp.maximum((u_ref[...] - mean) * inv * gb_ref[:1] + gb_ref[1:], 0.0).astype(BF16)
        x_ref[...] = act.T
        out = mm(act, w[...])
        o_ref[...] = out
        wtr_ref[...] = w[:, at(i, slab)].T
        v = i // steps
        share.acc[v] = jnp.where(i % steps == 0, 0.0, share.acc[v]) + two_sums(out, out * out)

        @pl.when(i == last)
        def _():
            share.start(1)
            for b in BOTH:
                so_ref[b] = share.total(b)
            if w_next is not None:
                gather.drain()
                gather.wait_core(0)
                gather.wait_core(1)

    more = w_next is not None
    return call(
        kernel, "fwd_next", cid, (2 * steps,),
        [pl.BlockSpec((TM, depth), lambda i: (i, 0)), pl.BlockSpec((1, 2, depth), lambda i: (i // steps, 0, 0)),
         whole(2, depth), ANY, ANY] + [ANY] * more,
        [pl.BlockSpec((depth, TM), lambda i: (0, i)), pl.BlockSpec((TM, dim), lambda i: (i, 0)),
         whole(2, 2, dim), pl.BlockSpec((slab, depth), lambda i: (i, 0))] + [ANY] * more,
        [sds((depth, all_rows), BF16), sds((all_rows, dim), F32), sds((2, 2, dim), F32), sds((dim, depth), BF16)]
        + ([sds(w_next.shape, BF16)] if more else []),
        [pltpu.VMEM((depth, dim), BF16)] + Share.scratch(2, 2, dim) + [TWO_DMA] + (Gather.scratch(n) if more else []),
        2 * all_rows * depth * dim, all_rows * (6 * depth + 4 * dim),
        (u, sums, gb, w_own, w_other) + ((w_next,) if more else ()))


def corr_grad(z, sums, lam, total):
    all_rows, dim = z.shape
    rows = all_rows // 2
    half = dim // 2
    quart = half // 2
    n_chunk = 8
    width = half // n_chunk
    pair = 2 * width
    mt = TM
    zt = TM // 2
    ahead = 3
    lead = 3
    z_steps = all_rows // zt
    m_steps = rows // mt
    scale = 1.0 / total

    def kernel(z_ref, s_ref, lam_ref, zho_ref, d_ref, so_ref, zh, da, ck, r1, r2, g, stage, dsend, drecv, acc, got, ssem, rsem, zs, zos,
               d1s, d1r, s1s, s1r, s2s, s2r, a2s, a2r, a1s, a1r, ads, adr, dbs, das):
        share = Share(acc, got, ssem, rsem)
        here = coords()
        y, x, c = here
        on_x = c == 0
        by_core = lambda one, two: tuple(jnp.where(on_x, a, b) for a, b in zip(one, two))
        first = by_core(flip(here, X_PEER), flip(here, Y_PEER))
        second = by_core(flip(here, Y_PEER), flip(here, X_PEER))
        cpeer = flip(here, C_PEER)
        bit1, bit2 = by_core((x, y), (y, x))
        arrive()
        acc[...] = jnp.zeros_like(acc)

        def load(i, slot):
            return pltpu.make_async_copy(z_ref.at[at(i, zt)], ck.at[at(slot, zt)], zs.at[slot])

        def zh_out(i):
            v, r = lax.div(i, n_chunk // 2), lax.rem(i, n_chunk // 2)
            return pltpu.make_async_copy(zh.at[v, at(r, TM)], zho_ref.at[v, at(r, TM)], zos.at[i])

        z_slots = half // zt
        for i in range(ahead):
            load(i, i).start()

        def normalise(i):
            slot = lax.rem(i, z_slots)
            v, r = lax.div(i, z_steps // 2), lax.rem(i, z_steps // 2)
            pl.when(i + ahead < z_steps)(lambda: load(i + ahead, lax.rem(i + ahead, z_slots)).start())
            load(i, slot).wait()
            mean, inv = mean_inv(s_ref[v], total)
            zh[v, at(r, zt)] = ((ck[at(slot, zt)] - mean) * inv).astype(BF16)

        loop(z_steps, normalise)
        all_arrived()

        def both(v, rows_at, t):
            return jnp.concatenate([zh[v, rows_at, at(b * n_chunk + t, width)] for b in BOTH], axis=1)

        group = lambda t, b: at(2 * t + b, width)

        def to_core(t):
            return remote(dsend.at[odd(t)], drecv.at[odd(t)], d1s.at[t], d1r.at[t], cpeer)

        def to_first(t):
            return remote(ck.at[:, group(t, other(bit1))], r1.at[t], s1s.at[t], s1r.at[t], first)

        def to_second(t):
            return remote(ck.at[at(other(bit2), quart), group(t, bit1)], r2.at[t], s2s.at[t], s2r.at[t], second)

        def g_second(t, b):
            block = g.at[t, at(2 * c + b, quart), at(bit1, width)]
            return remote(block, block, a2s.at[t], a2r.at[t], second)

        def g_first(t, b):
            block = g.at[t, at(c, half), at(b, width)]
            return remote(block, block, a1s.at[t], a1r.at[t], first)

        def g_core(t, core):
            block = g.at[t, at(core, half)]
            return remote(block, block, ads.at[t], adr.at[t], cpeer)

        def chip_sum(t):
            to_core(t).wait_recv()
            to_core(t).wait_send()
            ck[:, at(t, pair)] += drecv[odd(t)]
            pl.when(t < lead - 1)(lambda: to_first(t).start())

        def corr_part(t):
            zh_out(t).start()
            right = both(1, pl.ds(0, rows), t)
            dsend[odd(t)] = mm_at(zh[0, :, at(other(c), half)], right)
            ck[:, at(t, pair)] = mm_at(zh[0, :, at(c, half)], right)
            to_core(t).start()

        def db_out(t, m, slot, b):
            return pltpu.make_async_copy(
                stage.at[slot, :, at(b, width)], d_ref.at[1, at(m, mt), at(b * n_chunk + t, width)], dbs.at[slot, b])

        def da_out(m):
            return pltpu.make_async_copy(da.at[at(m, mt)], d_ref.at[0, at(m, mt)], das.at[m])

        def finish(m):
            d = da[at(m, mt)] * scale
            da[at(m, mt)] = d
            acc[0, :2] += two_sums(d, d * zh[0, at(m, mt)].astype(F32))
            da_out(m).start()

        def grads(t):
            def rows_of(m):
                slot = odd(m)

                @pl.when(t * m_steps + m >= 2)
                def _():
                    for b in BOTH:
                        db_out(t, m, slot, b).wait()

                db = mm(zh[0, at(m, mt)], g[t]) * scale
                stage[slot] = db
                own = both(1, at(m, mt), t)
                sums = two_sums(db, db * own.astype(F32))
                for b in BOTH:
                    acc[1, :2, at(b * n_chunk + t, width)] += sums[:, b * width:(b + 1) * width]
                    db_out(t, m, slot, b).start()
                da[at(m, mt)] = jnp.where(t == 0, 0.0, da[at(m, mt)]) + mm_bt(own, g[t])
                pl.when(t == n_chunk - 1)(lambda: finish(m))

            loop(m_steps, rows_of)

        def at_first(t):
            to_first(t).wait_recv()
            ck[:, group(t, bit1)] += r1[t]
            to_second(t).start()

        def at_second(t):
            to_second(t).wait_recv()
            corr_mat = (ck[at(bit2, quart), group(t, bit1)] + r2[t]) * scale
            row_ids = (2 * c + bit2) * quart + lax.broadcasted_iota(jnp.int32, (quart, width), 0)
            col_ids = (bit1 * n_chunk + t) * width + lax.broadcasted_iota(jnp.int32, (quart, width), 1)
            is_diag = row_ids == col_ids
            lam_val = lam_ref[0]
            loss = jnp.where(is_diag, (1.0 - corr_mat) * (1.0 - corr_mat), lam_val * corr_mat * corr_mat)
            acc[0, 2:3, :width] += jnp.sum(loss, axis=0, keepdims=True)
            grad = jnp.where(is_diag, -2.0 * (1.0 - corr_mat), 2.0 * lam_val * corr_mat).astype(BF16)
            g[t, at(2 * c + bit2, quart), at(bit1, width)] = grad
            g_second(t, bit2).start()

        def back_second(t):
            g_second(t, other(bit2)).wait_recv()
            g_first(t, bit1).start()
            pl.when(t + lead - 1 < n_chunk)(lambda: to_first(t + lead - 1).start())

        def back_first(t):
            g_first(t, other(bit1)).wait_recv()
            g_core(t, c).start()

        def back_core(t):
            g_core(t, other(c)).wait_recv()
            grads(t)

        def advance(tau):
            for lag, stage_fn in ((lead, at_first), (lead + 2, back_core), (lead + 1, back_first), (lead, at_second),
                                  (1, chip_sum), (0, corr_part), (lead, back_second)):
                t = tau - lag
                pl.when(jnp.logical_and(t >= 0, t < n_chunk))(lambda t=t, stage_fn=stage_fn: stage_fn(t))

        loop(n_chunk + lead + 2, advance)
        share.start(1)
        share.start(0)
        for t in range(n_chunk):
            for copy in (to_first(t), to_second(t), g_second(t, bit2), g_first(t, bit1), g_core(t, c)):
                copy.wait_send()
        for b in BOTH:
            so_ref[b] = share.total(b)
            for slot in BOTH:
                db_out(0, 0, slot, b).wait()
        for i in range(n_chunk):
            zh_out(i).wait()
        for m in range(m_steps):
            da_out(m).wait()

    return call(
        kernel, "corr_grad", 3, (), [ANY, VMEM, pl.BlockSpec(memory_space=pltpu.SMEM)], [ANY, ANY, VMEM],
        [sds((2, rows, dim), BF16), sds((2, rows, dim), F32), sds((2, 4, dim), F32)],
        [pltpu.VMEM((2, rows, dim), BF16), pltpu.VMEM((rows, dim), F32), pltpu.VMEM((half, dim), F32),
         pltpu.VMEM((n_chunk, half, width), F32), pltpu.VMEM((n_chunk, quart, width), F32),
         pltpu.VMEM((n_chunk, dim, pair), BF16), pltpu.VMEM((2, mt, pair), F32)]
        + [pltpu.VMEM((2, half, pair), F32)] * 2 + Share.scratch(2, 4, dim)
        + [DMA((half // zt,)), DMA((n_chunk,))] + [DMA((n_chunk,))] * 12 + [DMA((2, 2)), DMA((m_steps,))],
        all_rows * dim * dim * 3, all_rows * dim * 12, (z, sums, lam))


def backward(d_emb, zh, sz, s_emb, layers, x2_t, total):
    all_rows, dim = zh.shape
    rows, half = all_rows // 2, dim // 2
    width = 256
    slabs = dim // width
    items = 2 * slabs
    piece = width
    side = half // 2 // piece
    per_slab = half // piece
    n_layer = len(layers) + 1
    n_slab = n_layer * slabs
    per_layer = slabs * side
    n_chunk = n_layer * per_layer
    ahead = 3
    (u2, s2, gb2, w3_t, x1_t), (u1, s1, gb1, w2_t, h_t) = layers

    def kernel(d_ref, zh_ref, sz_ref, sd_ref, x2_ref, x1_ref, h_ref, u2_ref, u1_ref, w3_ref, w2_ref,
               s2_ref, s1_ref, gb2_ref, gb1_ref, dw3_ref, dw2_ref, dw1_ref, sum_ref, dy_ref, part_ref, ry_ref, rx_ref,
               dbuf, xbuf, wbuf, ubuf, dybuf, dyout, psend, pkeep, dr, ebuf, mbuf, fbuf, acc, got, ssem, rsem,
               us, ws, ds, dos, xl, ps, pr, pm, ys, yr, xs, xr, es, fs, fcs, fcr, credit):
        share = Share(acc, got, ssem, rsem)
        here = coords()
        y, x, c = here
        ypeer, xpeer, cpeer = flip(here, Y_PEER), flip(here, X_PEER), flip(here, C_PEER)
        arrive()

        def column(k, n):
            model = odd(n + jnp.where(k == 0, other(y), 0))
            return jnp.where(k == 1, n, model * (slabs // 2) + lax.div(n, 2))

        def turn(k):
            return jnp.where(k == 0, 0, other(y))

        def m_slot(j):
            return lax.rem(j, 4)

        def copy(src, dst, sem):
            return pltpu.make_async_copy(src, dst, sem)

        def sent_by(q):
            first = jnp.minimum(per_slab * lax.div(q, 4), per_layer)
            middle = jnp.clip(side * lax.div(q - 2 * items - 2, 2), 0, per_layer)
            last = jnp.clip(per_slab * lax.div(q - 4 * items - 2, 4), 0, per_layer)
            return first + middle + last

        def begun(q):
            paced = jnp.maximum(lax.div(5 * q - 26, 9), 0)
            return jnp.minimum(paced, 2 * per_layer + jnp.maximum(q - 4 * items - 5, 0))

        def to_core(s):
            return remote(psend.at[odd(s)], dr.at[odd(s)], ps.at[s], pr.at[s], cpeer)

        def keep_out(s):
            return copy(pkeep.at[odd(s)], part_ref.at[s], pm)

        def chip_sum(s):
            to_core(s).wait_recv()
            pkeep[odd(s)] += dr[odd(s)]

            @pl.when(s + 2 < n_slab)
            def _():
                pl.semaphore_signal(credit, inc=1, device_id=device(cpeer), device_id_type=pl.DeviceIdType.MESH)

            to_core(s).wait_send()
            keep_out(s).start()

        def home(j, own):
            k = lax.div(j, per_layer)
            i = lax.rem(j, per_layer)
            model = y if own else other(y)
            turned = other(turn(k)) if own else turn(k)
            s = jnp.where(k == 1, lax.div(i, side), 2 * lax.div(i, per_slab) + turned)
            place = jnp.where(k == 1, model * side + lax.rem(i, side), lax.rem(i, per_slab))
            return part_ref.at[k * slabs + s, at(place, piece)]

        def to_y(j):
            return remote(home(j, False), ry_ref.at[j], ys.at[lax.div(j, per_layer)], yr.at[j], ypeer)

        def issue(s, q):
            keep_out(s).wait()
            k, n = lax.div(s, slabs), lax.rem(s, slabs)
            for mine, fire, first, count in (
                    (k == 1, True, n * side, side), (k != 1, odd(n) == jnp.where(k == 0, 0, 1), lax.div(n, 2) * per_slab, per_slab)):
                for r in range(count):
                    j = k * per_layer + first + r
                    pl.when(mine & fire & (j < begun(q) + ahead))(lambda j=j: to_y(j).start())

        def to_x(j):
            return remote(mbuf.at[m_slot(j)], rx_ref.at[j], xs.at[m_slot(j)], xr.at[j], xpeer)

        def result(j, k):
            i = lax.rem(j, per_layer)
            if k == 1:
                return dw2_ref.at[at(c * side + lax.rem(i, side), piece), at(lax.div(i, side), width)]
            return (dw1_ref if k else dw3_ref).at[at(c * per_slab + lax.rem(i, per_slab), piece), at(lax.div(i, per_slab), width)]

        def put(j, k):
            slot = odd(j)
            return (copy(fbuf.at[slot], result(j, k), fs.at[slot]),
                    remote(fbuf.at[slot], result(j, k), fcs.at[slot], fcr.at[k], cpeer))

        def put_done(j):
            here_copy, there_copy = put(j, 0)
            here_copy.wait()
            there_copy.wait_send()

        def load_part(j, which):
            src = (lambda: ry_ref.at[j], lambda: home(j, True), lambda: rx_ref.at[j])[which]()
            return copy(src, ebuf.at[which], es.at[which])

        def fetch_x(j):
            to_x(j).wait_recv()
            load_part(j, 2).start()

        def begin(j, q):
            remote(ry_ref.at[j], ry_ref.at[j], ys.at[0], yr.at[j], ypeer).wait_recv()
            load_part(j, 0).start()
            load_part(j, 1).start()
            pl.when(j + ahead < sent_by(q))(lambda: to_y(j + ahead).start())
            pl.when(j >= 2)(lambda: fetch_x(j - 2))

        def deliver(j):
            load_part(j, 2).wait()
            pl.when(j >= 2)(lambda: put_done(j))
            fbuf[odd(j)] = mbuf[m_slot(j)] + ebuf[2]
            for k in range(n_layer):
                @pl.when(lax.div(j, per_layer) == k)
                def _(k=k):
                    for one in put(j, k):
                        one.start()

        def end(j):
            load_part(j, 0).wait()
            load_part(j, 1).wait()
            pl.when(j >= 4)(lambda: to_x(j).wait_send())
            mbuf[m_slot(j)] = ebuf[0] + ebuf[1]
            to_x(j).start()
            pl.when(j >= 2)(lambda: deliver(j - 2))

        def events(q):
            now, before, earlier = begun(q), begun(q - 1), begun(q - 2)
            pl.when(before > earlier)(lambda: end(before - 1))
            pl.when(now > before)(lambda: begin(now - 1, q))

        def weight_slab(k, n, v, d):
            s = k * slabs + n
            for buf, part in ((psend, other(c)), (pkeep, c)):
                first = jnp.where(k == 1, part, 2 * part)
                for b in BOTH:
                    left = xbuf[at(first + b * jnp.where(k == 1, 2, 1), half // 2), at(v, rows)]
                    here_at = at(b, half // 2)
                    buf[odd(s), here_at] = jnp.where(v == 0, 0.0, buf[odd(s), here_at]) + mm(left, d)

        def after(k, n, v, q):
            s = k * slabs + n
            pl.when((v == 0) & (n > 0))(lambda: chip_sum(s - 1))

            @pl.when(v == 1)
            def _():
                pl.when(s >= 2)(lambda: pl.semaphore_wait(credit, 1))
                to_core(s).start()
                pl.when(n > 0)(lambda: issue(s - 1, q))

        def emb_loads(i):
            n, v = split(i)
            cols = at(column(0, n), width)
            return (copy(d_ref.at[at(v, rows), cols], ubuf.at[v], us.at[v]),
                    copy(zh_ref.at[at(v, rows), cols], wbuf.at[v], ws.at[v]))

        def x_load(src, v):
            return copy(src.at[:, at(v, rows)], xbuf.at[:, at(v, rows)], xl.at[v])

        def slab_of(ref, layer, i, buf, sem):
            n, v = split(i)
            return copy(ref.at[at(v, rows), at(column(layer + 1, n), width)], buf.at[v], sem.at[v])

        def u_load(layer, i, ref=u2_ref):
            return slab_of(ref, layer, i, ubuf, us)

        def dy_load(layer, i):
            return slab_of(dy_ref, layer, i, dybuf, ds)

        def dy_out(layer, i):
            n, v = split(i)
            return copy(dyout.at[v], dy_ref.at[at(v, rows), at(column(layer + 1, n), width)], dos.at[v])

        def w_load(layer, n, ref=w3_ref):
            return copy(ref.at[:, at(column(layer + 1, n), width)], wbuf.at[odd(n)], ws.at[odd(n)])

        def start_u(layer, i):
            for k, ref in enumerate((u2_ref, u1_ref)):
                pl.when(layer == k)(lambda ref=ref: u_load(layer, i, ref).start())

        def start_w(layer, n):
            for k, ref in enumerate((w3_ref, w2_ref)):
                pl.when(layer == k)(lambda ref=ref: w_load(layer, n, ref).start())

        for one in (x_load(x2_ref, 0), *emb_loads(0), x_load(x2_ref, 1)):
            one.start()
        all_arrived()

        def emb_item(i):
            n, v = split(i)

            @pl.when(i + 1 < items)
            def _():
                for one in emb_loads(i + 1):
                    one.start()

            @pl.when(i + 1 == items)
            def _():
                u_load(0, 0).start()
                w_load(0, 0).start()

            pl.when(n == 0)(lambda: x_load(x2_ref, v).wait())
            for one in emb_loads(i):
                one.wait()
            events(i)
            cols = at(column(0, n), width)
            _, inv = mean_inv(sz_ref[v, :, cols], total)
            sd = sd_ref[v, :2, cols] / total
            d = (inv * (ubuf[v] - sd[:1] - wbuf[v].astype(F32) * sd[1:])).astype(BF16)
            dbuf[at(v, rows), cols] = d
            weight_slab(0, n, v, d)
            after(0, n, v, i)

        loop(items, emb_item)

        def stats(layer, v, cols):
            pick = lambda one, two: jnp.where(layer == 0, one, two)
            mean, inv = mean_inv(pick(s2_ref[v, :, cols], s1_ref[v, :, cols]), total)
            gb = pick(gb2_ref[:, cols], gb1_ref[:, cols])
            return mean, inv, gb[:1], gb[1:]

        def bn_layer(layer):
            start = (2 * layer + 1) * items

            def dx_item(i):
                n, v = split(i)
                cols = at(column(layer + 1, n), width)

                @pl.when(i + 1 < items)
                def _():
                    start_u(layer, i + 1)
                    pl.when((v == 0) & (n + 1 < slabs))(lambda: start_w(layer, n + 1))

                @pl.when(i + 1 == items)
                def _():
                    start_u(layer, 0)
                    dy_load(layer, 0).start()

                u_load(layer, i).wait()
                pl.when(v == 0)(lambda: w_load(layer, n).wait())
                events(start + i)
                for k, ref in enumerate((x1_ref, h_ref)):
                    pl.when((layer == k) & ((i == 4) | (i == 9)))(lambda ref=ref: x_load(ref, v).start())
                pl.when(n > 0)(lambda: dy_out(layer, i).wait())
                mean, inv, gamma, beta = stats(layer, v, cols)
                sums = 0.0
                for b in range(rows // TM):
                    some = at(b, TM)
                    dx = mm(dbuf[at(v * (rows // TM) + b, TM)], wbuf[odd(n)])
                    norm = (ubuf[v, some] - mean) * inv
                    dy = jnp.where(norm * gamma + beta > 0, dx, 0.0)
                    dyout[v, some] = dy
                    sums += two_sums(dy, dy * norm)
                dy_out(layer, i).start()
                g = layer * items + i
                acc[g] = sums
                share.start(g)
                before = (layer + 1) * slabs - 1
                pl.when(i == 0)(lambda: chip_sum(before))
                pl.when(i == 1)(lambda: issue(before, start + i))

            def dw_item(i):
                n, v = split(i)
                cols = at(column(layer + 1, n), width)

                @pl.when(i + 1 < items)
                def _():
                    start_u(layer, i + 1)
                    dy_load(layer, i + 1).start()

                @pl.when((i + 1 == items) & (layer == 0))
                def _():
                    u_load(1, 0, u1_ref).start()
                    w_load(1, 0, w2_ref).start()

                pl.when(n == 0)(lambda: x_load(x1_ref, v).wait())
                u_load(layer, i).wait()
                dy_load(layer, i).wait()
                events(start + items + i)
                tot = share.total(layer * items + i)
                sum_ref[layer, v, :, cols] = tot
                mean, inv, gamma, _ = stats(layer, v, cols)
                tot = tot / total
                d = (gamma * inv * (dybuf[v] - (tot[:1] + (ubuf[v] - mean) * (inv * tot[1:])))).astype(BF16)
                dbuf[at(v, rows), cols] = d
                weight_slab(layer + 1, n, v, d)
                after(layer + 1, n, v, start + items + i)

            loop(items, dx_item)
            for v in BOTH:
                dy_out(layer, v).wait()
            loop(items, dw_item)

        loop(len(layers), bn_layer)

        ticks = (2 * n_layer - 1) * items
        chip_sum(n_slab - 1)
        issue(n_slab - 1, ticks)
        ended = 41
        end(ended - 1)

        def tail(j):
            begin(j, ticks + 2)
            end(j)

        loop(n_chunk, tail, ended)
        for j in range(n_chunk - 2, n_chunk):
            fetch_x(j)
            deliver(j)
        for j in BOTH:
            put_done(j)
        for k in range(n_layer):
            theirs = dw2_ref.at[at(other(c), half // 2)] if k == 1 else (dw1_ref if k else dw3_ref).at[at(other(c), half)]
            remote(theirs, theirs, fcs.at[0], fcr.at[k], cpeer).wait_recv()
            sent = ry_ref.at[at(k, per_layer)]
            remote(sent, sent, ys.at[k], yr.at[0], ypeer).wait_send()
        for j in range(n_chunk - 4, n_chunk):
            to_x(j).wait_send()

    n_item = len(layers) * items
    vm = lambda *shape: pltpu.VMEM(shape, F32)
    bf = lambda *shape: pltpu.VMEM(shape, BF16)
    return call(
        kernel, "backward", 4, (),
        [ANY, ANY, VMEM, VMEM] + [ANY] * 7 + [VMEM] * 4, [ANY] * 3 + [VMEM] + [ANY] * 4,
        [sds((dim, half), F32), sds((half, dim), F32), sds((dim, half), F32), sds((len(layers), 2, 2, dim), F32),
         sds((all_rows, dim), F32), sds((n_slab, half, width), F32), sds((n_chunk, piece, width), F32),
         sds((n_chunk, piece, width), F32)],
        [bf(all_rows, dim), bf(dim, all_rows), bf(2, dim, width), vm(2, rows, width), vm(2, rows, width), vm(2, rows, width),
         vm(2, half, width), vm(2, half, width), vm(2, half, width), vm(3, piece, width), vm(4, piece, width),
         vm(2, piece, width)] + Share.scratch(n_item, 2, width)
        + [TWO_DMA, TWO_DMA, TWO_DMA, TWO_DMA, TWO_DMA, DMA((n_slab,)), DMA((n_slab,)), DMA, DMA((n_layer,)),
           DMA((n_chunk,)), DMA((4,)), DMA((n_chunk,)), DMA((3,)), TWO_DMA, TWO_DMA, DMA((n_layer,)),
           pltpu.SemaphoreType.REGULAR],
        all_rows * dim * dim * 10, all_rows * dim * 40,
        (d_emb, zh, sz, s_emb, x2_t, x1_t, h_t, u2, u1, w3_t, w2_t, s2, s1, gb2, gb1))


def settle(*grads):
    steps = 8

    def kernel(*refs):
        for src, dst in zip(refs[:len(grads)], refs[len(grads):]):
            dst[...] = src[...]

    specs = [pl.BlockSpec((g.shape[0] // steps, g.shape[1]), lambda i: (i, 0)) for g in grads]
    return call(kernel, "settle", None, (steps,), specs, specs, [sds(g.shape, F32) for g in grads], [], 0,
                len(grads) * grads[0].size * 8, grads)


def solution(mesh):
    def shard_body(h_a, h_b, w_one, w_two, w_three, g_one, b_one, g_two, b_two, lam_off):
        y = lax.axis_index('model')
        total = float(h_a.shape[0] * mesh.shape['data'])
        dim, half = w_three.shape
        gb2 = jnp.stack([g_two, b_two])
        u1, s1, gb1, w_two_o, h_t = fwd_first(h_a, h_b, w_one, w_two, jnp.stack([g_one, b_one]))
        x1_t, u2, s2, w2_t, w_three_o = fwd_next(u1, s1, gb1, w_two, w_two_o, True, total, 1, w_three)
        x2_t, z, sz, w3_t = fwd_next(u2, s2, gb2, w_three, w_three_o, False, total, 2)
        zh, d_emb, s_emb = corr_grad(z, sz, lam_off, total)
        loss = jnp.sum(s_emb[0, 2])
        dw_three, dw_two, dw_one, sums, *_ = backward(
            d_emb.reshape(z.shape), zh.reshape(z.shape), sz, s_emb,
            ((u2, s2, gb2, w3_t, x1_t), (u1, s1, gb1, w2_t, h_t)), x2_t, total)
        dw_three, dw_two, dw_one = settle(dw_three, dw_two, dw_one)
        sums = jnp.sum(sums, axis=1)
        sum2 = sums[0]
        sum1 = lax.dynamic_slice_in_dim(sums[1], y * half, half, 1)
        return loss.reshape(1), dw_one, dw_two, dw_three, sum1[1], sum1[0], sum2[1], sum2[0]

    in_specs = (P('data', None), P('data', None), P(None, 'model'), P('model', None), P(None, 'model'),
                P('model'), P('model'), P(), P(), P())
    out_specs = (P(), P(None, 'model'), P('model', None), P(None, 'model'), P('model'), P('model'), P(), P())
    return jax.shard_map(shard_body, mesh=mesh, in_specs=in_specs, out_specs=out_specs, check_vma=False)
```

```python
import functools

import jax
import jax.numpy as jnp
from jax import lax
from jax.experimental import pallas as pl
from jax.experimental.pallas import tpu as pltpu
from jax.sharding import PartitionSpec as P

BN_EPS = 1e-5
scope = jax.named_scope
F32 = jnp.float32
BF16 = jnp.bfloat16
TM = 512
MAX_VMEM = 67043328
ANY = pl.BlockSpec(memory_space=pl.ANY)
VMEM = pl.BlockSpec(memory_space=pltpu.VMEM)
DMA = pltpu.SemaphoreType.DMA
TWO_DMA = DMA((2,))
BOTH = (0, 1)
PEERS = [(ky, kx, kc) for ky in BOTH for kx in BOTH for kc in BOTH][1:]
C_PEER, X_PEER, Y_PEER = PEERS[0], PEERS[1], PEERS[3]
N_DEV = len(PEERS) + 1


def mm(left, right):
    return jnp.dot(left, right, preferred_element_type=F32)


def mm_bt(left, right):
    return lax.dot_general(left, right, (((1,), (1,)), ((), ())), preferred_element_type=F32)


def mm_at(left, right):
    return lax.dot_general(left, right, (((0,), (0,)), ((), ())), preferred_element_type=F32)


def other(p):
    return 1 - p


def odd(i):
    return lax.rem(i, 2)


def split(i):
    return lax.div(i, 2), odd(i)


def loop(n, body, start=0):
    def one(i, carry):
        body(i)
        return carry

    lax.fori_loop(start, n, one, 0)


def whole(*shape):
    return pl.BlockSpec(shape, lambda *_: (0,) * len(shape))


def at(i, n):
    return pl.ds(pl.multiple_of(i * n, n), n)


def sds(shape, dtype):
    return jax.ShapeDtypeStruct(shape, dtype)


def mean_inv(sums, total):
    mean = sums[:1] / total
    var = sums[1:2] / total - mean * mean
    return mean, lax.rsqrt(var + BN_EPS)


def two_sums(one, two):
    return jnp.concatenate([jnp.sum(one, axis=0, keepdims=True), jnp.sum(two, axis=0, keepdims=True)], axis=0)


def coords():
    y, d = lax.axis_index('model'), lax.axis_index('data')
    return y, lax.div(d, 2), odd(d)


def flip(here, which):
    return tuple(other(p) if f else p for p, f in zip(here, which))


def flat(here):
    y, x, c = here
    return 4 * y + 2 * x + c


def device(here):
    y, x, c = here
    return (y, 2 * x + c)


def remote(src, dst, send_sem, recv_sem, there):
    return pltpu.make_async_remote_copy(
        src_ref=src, dst_ref=dst, send_sem=send_sem, recv_sem=recv_sem, device_id=device(there),
        device_id_type=pl.DeviceIdType.MESH)


def arrive():
    here = coords()
    for k in PEERS:
        pl.semaphore_signal(pltpu.get_barrier_semaphore(), inc=1, device_id=device(flip(here, k)),
                            device_id_type=pl.DeviceIdType.MESH)


def all_arrived():
    pl.semaphore_wait(pltpu.get_barrier_semaphore(), len(PEERS))


class Share:
    def __init__(self, acc, got, send_sem, recv_sem):
        self.acc, self.got, self.send_sem, self.recv_sem = acc, got, send_sem, recv_sem

    @staticmethod
    def scratch(n, *shape):
        return [pltpu.VMEM((n, *shape), F32), pltpu.VMEM((n, N_DEV, *shape), F32), DMA((n,)), DMA((n,))]

    def start(self, b):
        here = coords()
        me = flat(here)
        self.got[b, me] = self.acc[b]
        for which in PEERS:
            remote(self.acc.at[b], self.got.at[b, me], self.send_sem.at[b], self.recv_sem.at[b],
                   flip(here, which)).start()

    def total(self, b):
        all_of = self.got.at[b, pl.ds(0, len(PEERS))]
        copies = remote(all_of, all_of, self.send_sem.at[b], self.recv_sem.at[b], coords())
        copies.wait_send()
        copies.wait_recv()
        out = self.got[b, 0]
        for f in range(1, N_DEV):
            out += self.got[b, f]
        return out


class Gather:
    def __init__(self, own, dest, n, sems):
        self.own, self.dest, self.n = own, dest, n
        self.ys, self.yr, self.xs, self.xr, self.cs, self.cr = sems
        self.here = coords()
        _, x, c = self.here
        self.mine, self.across = 2 * x + c, 2 * (other(x)) + c
        self.core = (2 * x + other(c), 2 * (other(x)) + other(c))

    @staticmethod
    def scratch(n):
        return [DMA((n,))] * 4 + [DMA((2, n))] * 2

    def y(self, p):
        model = self.here[0]
        return remote(self.own(self.mine, p), self.dest(model, self.mine, p), self.ys.at[p], self.yr.at[p],
                      flip(self.here, Y_PEER))

    def moved(self, q, p, send_sem, recv_sem, which):
        ref = self.dest(1 - self.here[0], q, p)
        return remote(ref, ref, send_sem, recv_sem, flip(self.here, which))

    def x(self, p, q):
        return self.moved(q, p, self.xs.at[p], self.xr.at[p], X_PEER)

    def c(self, p, late, q):
        return self.moved(q, p, self.cs.at[late, p], self.cr.at[late, p], C_PEER)

    def start(self):
        for p in range(self.n):
            self.y(p).start()

    def pass_y(self, p):
        self.moved(self.mine, p, self.ys.at[p], self.yr.at[p], Y_PEER).wait_recv()
        self.x(p, self.mine).start()
        self.c(p, 0, self.mine).start()

    def pass_x(self, p):
        self.x(p, self.across).wait_recv()
        self.c(p, 1, self.across).start()

    def wait_core(self, late):
        for p in range(self.n):
            self.c(p, late, self.core[late]).wait_recv()

    def drain(self):
        for p in range(self.n):
            self.y(p).wait_send()
            self.x(p, self.mine).wait_send()
            self.c(p, 0, self.mine).wait_send()
            self.c(p, 1, self.across).wait_send()


def call(kernel, name, cid, grid, in_specs, out_specs, out_shape, scratch, flops, nbytes, args):
    return pl.pallas_call(
        kernel, name=name, grid=grid, in_specs=in_specs, out_specs=out_specs, out_shape=out_shape, scratch_shapes=scratch,
        compiler_params=pltpu.CompilerParams(vmem_limit_bytes=MAX_VMEM, collective_id=cid, has_side_effects=cid is not None),
        cost_estimate=pl.CostEstimate(flops=flops, bytes_accessed=nbytes, transcendentals=0))(*args)


def fwd_first(h_a, h_b, w_one, w_two, gb_own):
    depth, half = w_one.shape
    dim = 2 * half
    rows = h_a.shape[0] // 2
    tile, width, quarter = 2 * TM, half // 2, half // 4
    steps = rows // tile
    per_block = 2 * steps
    n, n2 = 4, 8

    def block(j):
        y, x, _ = coords()
        return jnp.where(j < 2, 2 * y + j, 2 * (other(y)) + jnp.where(j == 2, x, other(x)))

    def tile_of(j, i):
        return jnp.where(odd(j) == 0, i, per_block - 1 - i)

    def kernel(ha_ref, hb_ref, w_ref, w2_ref, gb_ref, u_ref, s_ref, gbo_ref, w2o_ref, ht_ref, w1, gbf, *sems):
        share, sems = Share(*sems[:4]), sems[4:]
        gs, gr, lsem = sems[:3]
        sems = sems[3:]
        j, i = pl.program_id(0), pl.program_id(1)
        step = j * per_block + i
        here = coords()
        y = here[0]
        one = Gather(lambda q, p: w_ref.at[at(p, depth // n), at(q, quarter)],
                     lambda m, q, p: w1.at[at(p, depth // n), at(m * 4 + q, quarter)], n, sems[:6])
        two = Gather(lambda q, p: w2_ref.at[at(q * n2 + p, quarter // n2)],
                     lambda m, q, p: w2o_ref.at[at(q * n2 + p, quarter // n2)], n2, sems[6:])

        def local(b):
            return pltpu.make_async_copy(w_ref.at[:, at(b, width)], w1.at[:, at(2 * y + b, width)], lsem.at[b])

        def bn_vectors(m):
            return remote(gb_ref, gbf.at[:, at(m, half)], gs, gr, flip(here, Y_PEER))

        def begin():
            arrive()
            local(0).start()
            local(1).start()
            all_arrived()
            one.start()
            two.start()
            bn_vectors(y).start()
            local(0).wait()

        def late_half():
            one.pass_x(0)
            one.pass_y(n - 1)
            one.wait_core(0)

        hooks = [(0, begin), (per_block, lambda: local(1).wait()), (2 * per_block, late_half)]
        hooks += [(2 * p + 3, functools.partial(one.pass_y, p)) for p in range(n - 1)]
        hooks += [(p + 2 * per_block, functools.partial(one.pass_x, p)) for p in range(1, n)]
        hooks += [(3 * per_block, lambda: one.wait_core(1))]
        hooks += [(p + 9, functools.partial(two.pass_y, p)) for p in range(n2 - 1)]
        hooks += [(13 + (p + 1) // 2, functools.partial(two.pass_x, p)) for p in range(n2 // 2)]
        for s, hook in hooks:
            pl.when(step == s)(scope(f'hook{s}')(hook))
        for b in range(3):
            pl.when(step == (b + 1) * per_block)(lambda b=b: share.start(block(b)))

        tile_at = tile_of(j, i)
        first_view = tile_at < steps
        h = lax.select(first_view, ha_ref[...], hb_ref[...])
        cols = at(j, width)
        ht_ref[...] = lax.select(first_view, ha_ref[:, cols], hb_ref[:, cols]).T
        u = mm(h, w1[:, at(block(j), width)])
        u_ref[...] = u
        sums = two_sums(u, u * u)
        v = tile_at // steps
        share.acc[block(j), v] = jnp.where(i % steps == 0, 0.0, share.acc[block(j), v]) + sums

        @pl.when(step == 4 * per_block - 1)
        @scope('f1end')
        def _():
            share.start(block(3))
            two.pass_y(n2 - 1)
            for p in range(n2 // 2, n2):
                two.pass_x(p)
            bn_vectors(other(y)).wait_recv()
            bn_vectors(y).wait_send()
            gbo_ref[...] = gbf[...]
            gbo_ref[:, at(y, half)] = gb_ref[...]
            for b in range(4):
                s_ref[:, :, b * width:(b + 1) * width] = share.total(b)
            one.drain()
            two.drain()
            two.wait_core(0)
            two.wait_core(1)

    return call(
        kernel, "fwd_first", 0, (4, per_block),
        [pl.BlockSpec((tile, depth), lambda j, i: (coords()[0] * steps + jnp.minimum(tile_of(j, i), steps - 1), 0)),
         pl.BlockSpec((tile, depth), lambda j, i: (coords()[0] * steps + jnp.maximum(tile_of(j, i) - steps, 0), 0)),
         ANY, ANY, whole(2, half)],
        [pl.BlockSpec((tile, width), lambda j, i: (tile_of(j, i), block(j))), whole(2, 2, dim),
         whole(2, dim), ANY, pl.BlockSpec((width, tile), lambda j, i: (j, tile_of(j, i)))],
        [sds((2 * rows, dim), F32), sds((2, 2, dim), F32), sds((2, dim), F32), sds((half, dim), BF16),
         sds((depth, 2 * rows), BF16)],
        [pltpu.VMEM((depth, dim), BF16), pltpu.VMEM((2, dim), F32)] + Share.scratch(4, 2, 2, width)
        + [DMA, DMA, TWO_DMA] + Gather.scratch(n) + Gather.scratch(n2),
        4 * rows * depth * dim, 2 * rows * (8 * depth + 4 * dim), (h_a, h_b, w_one, w_two, gb_own))


def fwd_next(u, sums, gb, w_own, w_other, by_rows, total, cid, w_next=None):
    all_rows, depth = u.shape
    dim = w_own.shape[1] if by_rows else 2 * w_own.shape[1]
    half = dim // 2
    quarter = half // 4
    steps = all_rows // 2 // TM
    last = 2 * steps - 1
    slab = dim // (2 * steps)
    n = 4

    def kernel(u_ref, s_ref, gb_ref, wo_ref, wt_ref, *refs):
        if w_next is not None:
            wn_ref, refs = refs[0], refs[1:]
        x_ref, o_ref, so_ref, wtr_ref, *refs = refs
        if w_next is not None:
            wno_ref, *refs = refs
        w, acc, got, ssem, rsem, lsem, *refs = refs
        share = Share(acc, got, ssem, rsem)
        i = pl.program_id(0)
        y = coords()[0]

        def local(ref, model, b):
            where = at(model, half)
            return pltpu.make_async_copy(ref, w.at[where] if by_rows else w.at[:, where], lsem.at[b])

        if w_next is not None:
            gather = Gather(lambda q, p: wn_ref.at[at(p, depth // n), at(q, quarter)],
                            lambda m, q, p: wno_ref.at[at(p, depth // n), at(q, quarter)], n, refs)

        @pl.when(i == 0)
        def _():
            arrive()
            local(wo_ref, y, 0).start()
            local(wt_ref, other(y), 1).start()
            all_arrived()
            if w_next is not None:
                gather.start()
            local(wo_ref, y, 0).wait()
            local(wt_ref, other(y), 1).wait()

        if w_next is not None:
            for p in range(n):
                pl.when(i == p + 1)(lambda p=p: gather.pass_y(p))
                pl.when(i == p + 3)(lambda p=p: gather.pass_x(p))
        pl.when(i == steps)(lambda: share.start(0))

        mean, inv = mean_inv(s_ref[0], total)
        act = jnp.maximum((u_ref[...] - mean) * inv * gb_ref[:1] + gb_ref[1:], 0.0).astype(BF16)
        x_ref[...] = act.T
        out = mm(act, w[...])
        o_ref[...] = out
        wtr_ref[...] = w[:, at(i, slab)].T
        v = i // steps
        share.acc[v] = jnp.where(i % steps == 0, 0.0, share.acc[v]) + two_sums(out, out * out)

        @pl.when(i == last)
        def _():
            share.start(1)
            with scope('wait_last'):
                for b in BOTH:
                    so_ref[b] = share.total(b)
            if w_next is not None:
                gather.drain()
                gather.wait_core(0)
                gather.wait_core(1)

    more = w_next is not None
    return call(
        kernel, "fwd_next", cid, (2 * steps,),
        [pl.BlockSpec((TM, depth), lambda i: (i, 0)), pl.BlockSpec((1, 2, depth), lambda i: (i // steps, 0, 0)),
         whole(2, depth), ANY, ANY] + [ANY] * more,
        [pl.BlockSpec((depth, TM), lambda i: (0, i)), pl.BlockSpec((TM, dim), lambda i: (i, 0)),
         whole(2, 2, dim), pl.BlockSpec((slab, depth), lambda i: (i, 0))] + [ANY] * more,
        [sds((depth, all_rows), BF16), sds((all_rows, dim), F32), sds((2, 2, dim), F32), sds((dim, depth), BF16)]
        + ([sds(w_next.shape, BF16)] if more else []),
        [pltpu.VMEM((depth, dim), BF16)] + Share.scratch(2, 2, dim) + [TWO_DMA] + (Gather.scratch(n) if more else []),
        2 * all_rows * depth * dim, all_rows * (6 * depth + 4 * dim),
        (u, sums, gb, w_own, w_other) + ((w_next,) if more else ()))


def corr_grad(z, sums, lam, total):
    all_rows, dim = z.shape
    rows = all_rows // 2
    half = dim // 2
    quart = half // 2
    n_chunk = 8
    width = half // n_chunk
    pair = 2 * width
    mt = TM
    zt = TM // 2
    ahead = 3
    lead = 4
    z_steps = all_rows // zt
    m_steps = rows // mt
    scale = 1.0 / total

    def kernel(z_ref, s_ref, lam_ref, zho_ref, d_ref, so_ref, lo_ref, zh, da, ck, r1, r2, g, stage, dsend, drecv, acc, got, ssem, rsem, loss_acc, loss_got, lsem, lrsem, zs, zos,
               d1s, d1r, s1s, s1r, s2s, s2r, a2s, a2r, a1s, a1r, ads, adr, dbs, das):
        share = Share(acc, got, ssem, rsem)
        share_loss = Share(loss_acc, loss_got, lsem, lrsem)
        here = coords()
        y, x, c = here
        on_x = c == 0
        by_core = lambda one, two: tuple(jnp.where(on_x, a, b) for a, b in zip(one, two))
        first = by_core(flip(here, X_PEER), flip(here, Y_PEER))
        second = by_core(flip(here, Y_PEER), flip(here, X_PEER))
        cpeer = flip(here, C_PEER)
        bit1, bit2 = by_core((x, y), (y, x))
        arrive()
        acc[...] = jnp.zeros_like(acc)
        loss_acc[...] = jnp.zeros_like(loss_acc)

        def load(i, slot):
            return pltpu.make_async_copy(z_ref.at[at(i, zt)], ck.at[at(slot, zt)], zs.at[slot])

        def zh_out(i):
            v, r = lax.div(i, n_chunk // 2), lax.rem(i, n_chunk // 2)
            return pltpu.make_async_copy(zh.at[v, at(r, TM)], zho_ref.at[v, at(r, TM)], zos.at[i])

        z_slots = half // zt
        for i in range(ahead):
            load(i, i).start()

        @scope('normalise')
        def normalise(i):
            slot = lax.rem(i, z_slots)
            v, r = lax.div(i, z_steps // 2), lax.rem(i, z_steps // 2)
            pl.when(i + ahead < z_steps)(lambda: load(i + ahead, lax.rem(i + ahead, z_slots)).start())
            load(i, slot).wait()
            mean, inv = mean_inv(s_ref[v], total)
            zh[v, at(r, zt)] = ((ck[at(slot, zt)] - mean) * inv).astype(BF16)

        loop(z_steps, normalise)
        all_arrived()

        def both(v, rows_at, t):
            return jnp.concatenate([zh[v, rows_at, at(b * n_chunk + t, width)] for b in BOTH], axis=1)

        group = lambda t, b: at(2 * t + b, width)

        def to_core(t):
            return remote(dsend.at[odd(t)], drecv.at[odd(t)], d1s.at[t], d1r.at[t], cpeer)

        def to_first(t):
            return remote(ck.at[:, group(t, other(bit1))], r1.at[t], s1s.at[t], s1r.at[t], first)

        def to_second(t):
            return remote(ck.at[at(other(bit2), quart), group(t, bit1)], r2.at[t], s2s.at[t], s2r.at[t], second)

        def g_second(t, b):
            block = g.at[t, at(2 * c + b, quart), at(bit1, width)]
            return remote(block, block, a2s.at[t], a2r.at[t], second)

        def g_first(t, b):
            block = g.at[t, at(c, half), at(b, width)]
            return remote(block, block, a1s.at[t], a1r.at[t], first)

        def g_core(t, core):
            block = g.at[t, at(core, half)]
            return remote(block, block, ads.at[t], adr.at[t], cpeer)

        @scope('chip_sum')
        def chip_sum(t):
            to_core(t).wait_recv()
            to_core(t).wait_send()
            ck[:, at(t, pair)] += drecv[odd(t)]
            pl.when(t < lead - 1)(lambda: to_first(t).start())

        def corr_part(t):
            zh_out(t).start()
            right = both(1, pl.ds(0, rows), t)
            dsend[odd(t)] = mm_at(zh[0, :, at(other(c), half)], right)
            ck[:, at(t, pair)] = mm_at(zh[0, :, at(c, half)], right)
            to_core(t).start()

        def db_out(t, m, slot, b):
            return pltpu.make_async_copy(
                stage.at[slot, :, at(b, width)], d_ref.at[1, at(m, mt), at(b * n_chunk + t, width)], dbs.at[slot, b])

        def da_out(m):
            return pltpu.make_async_copy(da.at[at(m, mt)], d_ref.at[0, at(m, mt)], das.at[m])

        def finish(m):
            d = da[at(m, mt)] * scale
            da[at(m, mt)] = d
            acc[0] += two_sums(d, d * zh[0, at(m, mt)].astype(F32))
            da_out(m).start()

        def grads(t):
            @scope('rows_of')
            def rows_of(m):
                slot = odd(m)

                @pl.when(t * m_steps + m >= 2)
                def _():
                    for b in BOTH:
                        db_out(t, m, slot, b).wait()

                db = mm(zh[0, at(m, mt)], g[t]) * scale
                stage[slot] = db
                own = both(1, at(m, mt), t)
                sums = two_sums(db, db * own.astype(F32))
                for b in BOTH:
                    acc[1, :, at(b * n_chunk + t, width)] += sums[:, b * width:(b + 1) * width]
                    db_out(t, m, slot, b).start()
                da[at(m, mt)] = jnp.where(t == 0, 0.0, da[at(m, mt)]) + mm_bt(own, g[t])
                pl.when(t == n_chunk - 1)(lambda: finish(m))

            loop(m_steps, rows_of)

        @scope('at_first')
        def at_first(t):
            to_first(t).wait_recv()
            ck[:, group(t, bit1)] += r1[t]
            to_second(t).start()

        @scope('at_second')
        def at_second(t):
            to_second(t).wait_recv()
            corr_mat = (ck[at(bit2, quart), group(t, bit1)] + r2[t]) * scale
            row_ids = (2 * c + bit2) * quart + lax.broadcasted_iota(jnp.int32, (quart, width), 0)
            col_ids = (bit1 * n_chunk + t) * width + lax.broadcasted_iota(jnp.int32, (quart, width), 1)
            is_diag = row_ids == col_ids
            lam_val = lam_ref[0]
            loss = jnp.where(is_diag, (1.0 - corr_mat) * (1.0 - corr_mat), lam_val * corr_mat * corr_mat)
            loss_acc[0] += jnp.sum(loss, axis=0, keepdims=True)
            pl.when(t == n_chunk - 1)(lambda: share_loss.start(0))
            grad = jnp.where(is_diag, -2.0 * (1.0 - corr_mat), 2.0 * lam_val * corr_mat).astype(BF16)
            g[t, at(2 * c + bit2, quart), at(bit1, width)] = grad
            g_second(t, bit2).start()

        @scope('back_second')
        def back_second(t):
            g_second(t, other(bit2)).wait_recv()
            g_first(t, bit1).start()
            pl.when(t + lead - 1 < n_chunk)(lambda: to_first(t + lead - 1).start())

        @scope('back_first')
        def back_first(t):
            g_first(t, other(bit1)).wait_recv()
            g_core(t, c).start()

        def back_core(t):
            g_core(t, other(c)).wait_recv()
            grads(t)

        def advance(tau):
            for lag, stage_fn in ((lead, at_first), (lead + 2, back_core), (lead + 1, back_first), (lead, at_second),
                                  (1, chip_sum), (0, corr_part), (lead, back_second)):
                t = tau - lag
                pl.when(jnp.logical_and(t >= 0, t < n_chunk))(lambda t=t, stage_fn=stage_fn: stage_fn(t))

        loop(n_chunk + lead + 2, advance)
        share.start(1)
        share.start(0)
        for t in range(n_chunk):
            for copy in (to_first(t), to_second(t), g_second(t, bit2), g_first(t, bit1), g_core(t, c)):
                copy.wait_send()
        for b in BOTH:
            so_ref[b] = share.total(b)
            for slot in BOTH:
                db_out(0, 0, slot, b).wait()
        lo_ref[...] = share_loss.total(0)
        for i in range(n_chunk):
            zh_out(i).wait()
        for m in range(m_steps):
            da_out(m).wait()

    return call(
        kernel, "corr_grad", 3, (), [ANY, VMEM, pl.BlockSpec(memory_space=pltpu.SMEM)], [ANY, ANY, VMEM, VMEM],
        [sds((2, rows, dim), BF16), sds((2, rows, dim), F32), sds((2, 2, dim), F32), sds((1, width), F32)],
        [pltpu.VMEM((2, rows, dim), BF16), pltpu.VMEM((rows, dim), F32), pltpu.VMEM((half, dim), F32),
         pltpu.VMEM((n_chunk, half, width), F32), pltpu.VMEM((n_chunk, quart, width), F32),
         pltpu.VMEM((n_chunk, dim, pair), BF16), pltpu.VMEM((2, mt, pair), F32)]
        + [pltpu.VMEM((2, half, pair), F32)] * 2 + Share.scratch(2, 2, dim) + Share.scratch(1, 1, width)
        + [DMA((half // zt,)), DMA((n_chunk,))] + [DMA((n_chunk,))] * 12 + [DMA((2, 2)), DMA((m_steps,))],
        all_rows * dim * dim * 3, all_rows * dim * 12, (z, sums, lam))


def backward(d_emb, zh, sz, s_emb, layers, x2_t, total):
    all_rows, dim = zh.shape
    rows, half = all_rows // 2, dim // 2
    width = 256
    slabs = dim // width
    items = 2 * slabs
    piece = width
    side = half // 2 // piece
    per_slab = half // piece
    n_layer = len(layers) + 1
    n_slab = n_layer * slabs
    per_layer = slabs * side
    n_chunk = n_layer * per_layer
    ahead = 3
    (u2, s2, gb2, w3_t, x1_t), (u1, s1, gb1, w2_t, h_t) = layers

    def kernel(d_ref, zh_ref, sz_ref, sd_ref, x2_ref, x1_ref, h_ref, u2_ref, u1_ref, w3_ref, w2_ref,
               s2_ref, s1_ref, gb2_ref, gb1_ref, dw3_ref, dw2_ref, dw1_ref, sum_ref, dy_ref, part_ref, ry_ref, rx_ref,
               dbuf, xbuf, d0, d1, wbuf, ubuf, dybuf, dyout, psend, pkeep, dr, ebuf, mbuf, fbuf, acc, got, ssem, rsem,
               us, ws, ds, dos, xl, ps, pr, pm, ys, yr, xs, xr, es, fs, fcs, fcr, credit):
        share = Share(acc, got, ssem, rsem)
        here = coords()
        y, x, c = here
        ypeer, xpeer, cpeer = flip(here, Y_PEER), flip(here, X_PEER), flip(here, C_PEER)
        arrive()

        def column(k, n):
            model = odd(n + jnp.where(k == 0, other(y), 0))
            return jnp.where(k == 1, n, model * (slabs // 2) + lax.div(n, 2))

        def turn(k):
            return jnp.where(k == 0, 0, other(y))

        def m_slot(j):
            return lax.rem(j, 4)

        def copy(src, dst, sem):
            return pltpu.make_async_copy(src, dst, sem)

        def sent_by(q):
            first = jnp.minimum(per_slab * lax.div(q, 4), per_layer)
            middle = jnp.clip(side * lax.div(q - 2 * items - 2, 2), 0, per_layer)
            last = jnp.clip(per_slab * lax.div(q - 4 * items - 2, 4), 0, per_layer)
            return first + middle + last

        def begun(q):
            return jnp.maximum(lax.div(q - 6, 2), 0)

        def to_core(s):
            return remote(psend.at[odd(s)], dr.at[odd(s)], ps.at[s], pr.at[s], cpeer)

        def keep_out(s):
            return copy(pkeep.at[odd(s)], part_ref.at[s], pm)

        @scope('chip_sum')
        def chip_sum(s):
            to_core(s).wait_recv()
            pkeep[odd(s)] += dr[odd(s)]

            @pl.when(s + 2 < n_slab)
            def _():
                pl.semaphore_signal(credit, inc=1, device_id=device(cpeer), device_id_type=pl.DeviceIdType.MESH)

            to_core(s).wait_send()
            keep_out(s).start()

        def home(j, own):
            k = lax.div(j, per_layer)
            i = lax.rem(j, per_layer)
            model = y if own else other(y)
            turned = other(turn(k)) if own else turn(k)
            s = jnp.where(k == 1, lax.div(i, side), 2 * lax.div(i, per_slab) + turned)
            place = jnp.where(k == 1, model * side + lax.rem(i, side), lax.rem(i, per_slab))
            return part_ref.at[k * slabs + s, at(place, piece)]

        def to_y(j):
            return remote(home(j, False), ry_ref.at[j], ys.at[lax.div(j, per_layer)], yr.at[j], ypeer)

        @scope('issue')
        def issue(s, q):
            keep_out(s).wait()
            k, n = lax.div(s, slabs), lax.rem(s, slabs)
            for mine, fire, first, count in (
                    (k == 1, True, n * side, side), (k != 1, odd(n) == jnp.where(k == 0, 0, 1), lax.div(n, 2) * per_slab, per_slab)):
                for r in range(count):
                    j = k * per_layer + first + r
                    pl.when(mine & fire & (j < begun(q) + ahead))(lambda j=j: to_y(j).start())

        def to_x(j):
            return remote(mbuf.at[m_slot(j)], rx_ref.at[j], xs.at[m_slot(j)], xr.at[j], xpeer)

        def result(j, k):
            i = lax.rem(j, per_layer)
            if k == 1:
                return dw2_ref.at[at(c * side + lax.rem(i, side), piece), at(lax.div(i, side), width)]
            return (dw1_ref if k else dw3_ref).at[at(c * per_slab + lax.rem(i, per_slab), piece), at(lax.div(i, per_slab), width)]

        def put(j, k):
            slot = odd(j)
            return (copy(fbuf.at[slot], result(j, k), fs.at[slot]),
                    remote(fbuf.at[slot], result(j, k), fcs.at[slot], fcr.at[k], cpeer))

        def put_done(j):
            here_copy, there_copy = put(j, 0)
            here_copy.wait()
            there_copy.wait_send()

        def load_part(j, which):
            src = (lambda: ry_ref.at[j], lambda: home(j, True), lambda: rx_ref.at[j])[which]()
            return copy(src, ebuf.at[which], es.at[which])

        @scope('fetch_x')
        def fetch_x(j):
            to_x(j).wait_recv()
            load_part(j, 2).start()

        @scope('begin')
        def begin(j, q):
            remote(ry_ref.at[j], ry_ref.at[j], ys.at[0], yr.at[j], ypeer).wait_recv()
            load_part(j, 0).start()
            load_part(j, 1).start()
            pl.when(j + ahead < sent_by(q))(lambda: to_y(j + ahead).start())
            pl.when(j >= 2)(lambda: fetch_x(j - 2))

        @scope('deliver')
        def deliver(j):
            load_part(j, 2).wait()
            pl.when(j >= 2)(lambda: put_done(j))
            fbuf[odd(j)] = mbuf[m_slot(j)] + ebuf[2]
            for k in range(n_layer):
                @pl.when(lax.div(j, per_layer) == k)
                def _(k=k):
                    for one in put(j, k):
                        one.start()

        @scope('end')
        def end(j):
            load_part(j, 0).wait()
            load_part(j, 1).wait()
            pl.when(j >= 4)(lambda: to_x(j).wait_send())
            mbuf[m_slot(j)] = ebuf[0] + ebuf[1]
            to_x(j).start()
            pl.when(j >= 2)(lambda: deliver(j - 2))

        def events(q):
            now, before, earlier = begun(q), begun(q - 1), begun(q - 2)
            pl.when(before > earlier)(lambda: end(before - 1))
            pl.when(now > before)(lambda: begin(now - 1, q))

        def weight_slab(k, n, v, d):
            slot = odd(k * slabs + n)
            for buf, part in ((psend, other(c)), (pkeep, c)):
                first = jnp.where(k == 1, part, 2 * part)
                for b in BOTH:
                    left = xbuf[at(first + b * jnp.where(k == 1, 2, 1), half // 2), pl.ds(v * rows, rows)]
                    here_at = at(b, half // 2)
                    prod = mm(left, d)
                    buf[slot, here_at] = buf[slot, here_at] + prod if v else prod

        @scope('after')
        def after(k, n, v, q):
            s = k * slabs + n
            if v == 0:
                pl.when(n > 0)(lambda: chip_sum(s - 1))
            else:
                pl.when(s >= 2)(lambda: pl.semaphore_wait(credit, 1))
                to_core(s).start()
                pl.when(n > 0)(lambda: issue(s - 1, q))

        def dw_pass(k, q, ready, fetch, pre, ahead_of_next):
            ready(0)
            fetch(1)
            d0[...] = pre(0, 0)

            def slab(n):
                for v, d_ref, d_next in ((0, d0, d1), (1, d1, d0)):
                    i = 2 * n + v
                    pl.when(i + 1 < items)(lambda: ready(i + 1))
                    pl.when(i + 2 < items)(lambda: fetch(i + 2))
                    pl.when(n == 0)(lambda: x_load(x2_ref, v).wait())
                    if v:
                        pl.when(n == slabs - 1)(ahead_of_next)
                    events(q + i)
                    d = d_ref[...]
                    dbuf[pl.ds(v * rows, rows), at(column(k, n), width)] = d
                    weight_slab(k, n, v, d)
                    d_next[...] = pre(jnp.minimum(n + v, slabs - 1), other(v))
                    after(k, n, v, q + i)

            loop(slabs, slab)

        def emb_loads(i):
            n, v = split(i)
            cols = at(column(0, n), width)
            return (copy(d_ref.at[at(v, rows), cols], ubuf.at[v], us.at[v]),
                    copy(zh_ref.at[at(v, rows), cols], wbuf.at[v], ws.at[v]))

        def emb_fetch(i):
            for one in emb_loads(i):
                one.start()

        def emb_ready(i):
            for one in emb_loads(i):
                one.wait()

        def emb_pre(n, v):
            cols = at(column(0, n), width)
            _, inv = mean_inv(sz_ref[v, :, cols], total)
            sd = sd_ref[v, :, cols] / total
            return (inv * (ubuf[v] - sd[:1] - wbuf[v].astype(F32) * sd[1:])).astype(BF16)

        def x_load(src, v):
            return copy(src.at[:, at(v, rows)], xbuf.at[:, at(v, rows)], xl.at[v])

        def u_slot(layer, v):
            return jnp.where(layer == 0, other(v), v)

        def slab_of(ref, layer, i, buf, sem, slot):
            n, v = split(i)
            return copy(ref.at[at(v, rows), at(column(layer + 1, n), width)], buf.at[slot], sem.at[slot])

        def u_load(layer, i, ref=u2_ref):
            return slab_of(ref, layer, i, ubuf, us, u_slot(layer, odd(i)))

        def dy_load(layer, i):
            return slab_of(dy_ref, layer, i, dybuf, ds, odd(i))

        def dy_out(layer, i):
            n, v = split(i)
            return copy(dyout.at[v], dy_ref.at[at(v, rows), at(column(layer + 1, n), width)], dos.at[v])

        def w_load(layer, n, ref=w3_ref):
            slot = odd(n + 1)
            return copy(ref.at[:, at(column(layer + 1, n), width)], wbuf.at[slot], ws.at[slot])

        def by_layer(layer, make, refs):
            for k, ref in enumerate(refs):
                pl.when(layer == k)(lambda ref=ref: make(ref).start())

        def start_u(layer, i):
            by_layer(layer, lambda ref: u_load(layer, i, ref), (u2_ref, u1_ref))

        def start_w(layer, n):
            by_layer(layer, lambda ref: w_load(layer, n, ref), (w3_ref, w2_ref))

        def next_layer(layer):
            start_u(layer, 0)
            start_w(layer, 0)

        for one in (x_load(x2_ref, 0), *emb_loads(0), x_load(x2_ref, 1)):
            one.start()
        all_arrived()
        dw_pass(0, 0, emb_ready, emb_fetch, emb_pre, lambda: next_layer(0))

        def stats(layer, v, cols):
            pick = lambda one, two: jnp.where(layer == 0, one, two)
            mean, inv = mean_inv(pick(s2_ref[v, :, cols], s1_ref[v, :, cols]), total)
            gb = pick(gb2_ref[:, cols], gb1_ref[:, cols])
            return mean, inv, gb[:1], gb[1:]

        def bn_layer(layer):
            start = (2 * layer + 1) * items

            def dx_item(i):
                n, v = split(i)
                slot = u_slot(layer, v)
                cols = at(column(layer + 1, n), width)

                @pl.when(i + 1 < items)
                def _():
                    start_u(layer, i + 1)
                    pl.when((v == 0) & (n + 1 < slabs))(lambda: start_w(layer, n + 1))

                @pl.when(i + 1 == items)
                def _():
                    start_u(layer, 0)
                    dy_load(layer, 0).start()

                scope('wait_u')(u_load(layer, i).wait)()
                pl.when(v == 0)(lambda: w_load(layer, n).wait())
                events(start + i)
                pl.when((i == 4) | (i == 9))(lambda: by_layer(layer, lambda ref: x_load(ref, v), (x1_ref, h_ref)))
                pl.when(n > 0)(lambda: dy_out(layer, i).wait())
                mean, inv, gamma, beta = stats(layer, v, cols)
                sums = 0.0
                for b in range(rows // TM):
                    some = at(b, TM)
                    dx = mm(dbuf[at(v * (rows // TM) + b, TM)], wbuf[odd(n + 1)])
                    norm = (ubuf[slot, some] - mean) * inv
                    dy = jnp.where(norm * gamma + beta > 0, dx, 0.0)
                    dyout[v, some] = dy
                    sums += two_sums(dy, dy * norm)
                dy_out(layer, i).start()
                g = layer * items + i
                acc[g] = sums
                share.start(g)
                before = (layer + 1) * slabs - 1
                pl.when(i == 0)(lambda: chip_sum(before))
                pl.when(i == 1)(lambda: issue(before, start + i))

            def fetch(i):
                start_u(layer, i)
                dy_load(layer, i).start()

            def ready(i):
                n, v = split(i)
                u_load(layer, i).wait()
                dy_load(layer, i).wait()
                sum_ref[layer, v, :, at(column(layer + 1, n), width)] = share.total(layer * items + i)

            def pre(n, v):
                cols = at(column(layer + 1, n), width)
                tot = sum_ref[layer, v, :, cols] / total
                mean, inv, gamma, _ = stats(layer, v, cols)
                return (gamma * inv * (dybuf[v] - (tot[:1] + (ubuf[u_slot(layer, v)] - mean) * (inv * tot[1:])))).astype(BF16)

            loop(items, dx_item)
            for v in BOTH:
                dy_out(layer, v).wait()
            dw_pass(layer + 1, start + items, ready, fetch, pre, lambda: pl.when(layer == 0)(lambda: next_layer(1)))

        loop(len(layers), bn_layer)

        ticks = (2 * n_layer - 1) * items
        chip_sum(n_slab - 1)
        issue(n_slab - 1, ticks)
        ended = 36

        def tail(j):
            begin(j, ticks + 2)
            end(j)

        loop(n_chunk, tail, ended)
        for j in range(n_chunk - 2, n_chunk):
            fetch_x(j)
            deliver(j)
        for j in BOTH:
            put_done(j)
        for k in range(n_layer):
            theirs = dw2_ref.at[at(other(c), half // 2)] if k == 1 else (dw1_ref if k else dw3_ref).at[at(other(c), half)]
            remote(theirs, theirs, fcs.at[0], fcr.at[k], cpeer).wait_recv()
            sent = ry_ref.at[at(k, per_layer)]
            remote(sent, sent, ys.at[k], yr.at[0], ypeer).wait_send()
        for j in range(n_chunk - 4, n_chunk):
            to_x(j).wait_send()

    n_item = len(layers) * items
    vm = lambda *shape: pltpu.VMEM(shape, F32)
    bf = lambda *shape: pltpu.VMEM(shape, BF16)
    return call(
        kernel, "backward", 4, (),
        [ANY, ANY, VMEM, VMEM] + [ANY] * 7 + [VMEM] * 4, [ANY] * 3 + [VMEM] + [ANY] * 4,
        [sds((dim, half), F32), sds((half, dim), F32), sds((dim, half), F32), sds((len(layers), 2, 2, dim), F32),
         sds((all_rows, dim), F32), sds((n_slab, half, width), F32), sds((n_chunk, piece, width), F32),
         sds((n_chunk, piece, width), F32)],
        [bf(all_rows, dim), bf(dim, all_rows), bf(rows, width), bf(rows, width), bf(2, dim, width),
         vm(2, rows, width), vm(2, rows, width), vm(2, rows, width),
         vm(2, half, width), vm(2, half, width), vm(2, half, width), vm(3, piece, width), vm(4, piece, width),
         vm(2, piece, width)] + Share.scratch(n_item, 2, width)
        + [TWO_DMA, TWO_DMA, TWO_DMA, TWO_DMA, TWO_DMA, DMA((n_slab,)), DMA((n_slab,)), DMA, DMA((n_layer,)),
           DMA((n_chunk,)), DMA((4,)), DMA((n_chunk,)), DMA((3,)), TWO_DMA, TWO_DMA, DMA((n_layer,)),
           pltpu.SemaphoreType.REGULAR],
        all_rows * dim * dim * 10, all_rows * dim * 40,
        (d_emb, zh, sz, s_emb, x2_t, x1_t, h_t, u2, u1, w3_t, w2_t, s2, s1, gb2, gb1))


def settle(*grads):
    steps = 8

    def kernel(*refs):
        for src, dst in zip(refs[:len(grads)], refs[len(grads):]):
            dst[...] = src[...]

    specs = [pl.BlockSpec((g.shape[0] // steps, g.shape[1]), lambda i: (i, 0)) for g in grads]
    return call(kernel, "settle", None, (steps,), specs, specs, [sds(g.shape, F32) for g in grads], [], 0,
                len(grads) * grads[0].size * 8, grads)


def solution(mesh):
    def shard_body(h_a, h_b, w_one, w_two, w_three, g_one, b_one, g_two, b_two, lam_off):
        y = lax.axis_index('model')
        total = float(h_a.shape[0] * mesh.shape['data'])
        dim, half = w_three.shape
        gb2 = jnp.stack([g_two, b_two])
        u1, s1, gb1, w_two_o, h_t = fwd_first(h_a, h_b, w_one, w_two, jnp.stack([g_one, b_one]))
        x1_t, u2, s2, w2_t, w_three_o = fwd_next(u1, s1, gb1, w_two, w_two_o, True, total, 1, w_three)
        x2_t, z, sz, w3_t = fwd_next(u2, s2, gb2, w_three, w_three_o, False, total, 2)
        zh, d_emb, s_emb, loss = corr_grad(z, sz, lam_off, total)
        loss = jnp.sum(loss)
        dw_three, dw_two, dw_one, sums, *_ = backward(
            d_emb.reshape(z.shape), zh.reshape(z.shape), sz, s_emb,
            ((u2, s2, gb2, w3_t, x1_t), (u1, s1, gb1, w2_t, h_t)), x2_t, total)
        dw_three, dw_two, dw_one = settle(dw_three, dw_two, dw_one)
        sums = jnp.sum(sums, axis=1)
        sum2 = sums[0]
        sum1 = lax.dynamic_slice_in_dim(sums[1], y * half, half, 1)
        return loss.reshape(1), dw_one, dw_two, dw_three, sum1[1], sum1[0], sum2[1], sum2[0]

    in_specs = (P('data', None), P('data', None), P(None, 'model'), P('model', None), P(None, 'model'),
                P('model'), P('model'), P(), P(), P())
    out_specs = (P(), P(None, 'model'), P('model', None), P(None, 'model'), P('model'), P('model'), P(), P())
    return jax.shard_map(shard_body, mesh=mesh, in_specs=in_specs, out_specs=out_specs, check_vma=False)
```

```python
import functools

import jax
import jax.numpy as jnp
from jax import lax
from jax.experimental import pallas as pl
from jax.experimental.pallas import tpu as pltpu
from jax.sharding import PartitionSpec as P

BN_EPS = 1e-5
F32 = jnp.float32
BF16 = jnp.bfloat16
PIECE = 64
LANES = 256
SUBLANES = 8
TM = 512
MAX_VMEM = 67043328
ANY = pl.BlockSpec(memory_space=pl.ANY)
VMEM = pl.BlockSpec(memory_space=pltpu.VMEM)
DMA = pltpu.SemaphoreType.DMA
TWO_DMA = DMA((2,))
BOTH = (0, 1)
PEERS = [(ky, kx, kc) for ky in BOTH for kx in BOTH for kc in BOTH][1:]
C_PEER, X_PEER, Y_PEER = PEERS[0], PEERS[1], PEERS[3]
N_DEV = len(PEERS) + 1


def mm(left, right):
    return jnp.dot(left, right, preferred_element_type=F32)


def mm_bt(left, right):
    return lax.dot_general(left, right, (((1,), (1,)), ((), ())), preferred_element_type=F32)


def mm_at(left, right):
    return lax.dot_general(left, right, (((0,), (0,)), ((), ())), preferred_element_type=F32)


def other(p):
    return 1 - p


def odd(i):
    return lax.rem(i, 2)


def split(i):
    return lax.div(i, 2), odd(i)


def loop(n, body, start=0):
    def one(i, carry):
        body(i)
        return carry

    lax.fori_loop(start, n, one, 0)


def whole(*shape):
    return pl.BlockSpec(shape, lambda *_: (0,) * len(shape))


def at(i, n):
    return pl.ds(pl.multiple_of(i * n, n), n)


def sds(shape, dtype):
    return jax.ShapeDtypeStruct(shape, dtype)


def mean_inv(sums, total):
    mean = sums[:1] / total
    var = sums[1:2] / total - mean * mean
    return mean, lax.rsqrt(var + BN_EPS)


def fold(v):
    return jnp.sum(v.reshape(-1, SUBLANES, v.shape[1]), axis=0)


def runs(n, size):
    return [pl.ds(r, size) for r in range(0, n, size)]


def two_sums(pairs):
    one = two = 0.0
    for a, b in pairs:
        one, two = one + fold(a), two + fold(b)
    return jnp.concatenate([jnp.sum(t, axis=0, keepdims=True) for t in (one, two)], axis=0)


def moments(ref, cols):
    pieces = (ref[r, cols] for r in runs(ref.shape[0], PIECE))
    return two_sums((u, u * u) for u in pieces)


def coords():
    y, d = lax.axis_index('model'), lax.axis_index('data')
    return y, lax.div(d, 2), odd(d)


def flip(here, which):
    return tuple(other(p) if f else p for p, f in zip(here, which))


def flat(here):
    y, x, c = here
    return 4 * y + 2 * x + c


def device(here):
    y, x, c = here
    return (y, 2 * x + c)


def remote(src, dst, send_sem, recv_sem, there):
    return pltpu.make_async_remote_copy(
        src_ref=src, dst_ref=dst, send_sem=send_sem, recv_sem=recv_sem, device_id=device(there),
        device_id_type=pl.DeviceIdType.MESH)


def arrive():
    here = coords()
    for k in PEERS:
        pl.semaphore_signal(pltpu.get_barrier_semaphore(), inc=1, device_id=device(flip(here, k)),
                            device_id_type=pl.DeviceIdType.MESH)


def all_arrived():
    pl.semaphore_wait(pltpu.get_barrier_semaphore(), len(PEERS))


class Share:
    def __init__(self, acc, got, send_sem, recv_sem):
        self.acc, self.got, self.send_sem, self.recv_sem = acc, got, send_sem, recv_sem

    @staticmethod
    def scratch(n, *shape):
        return [pltpu.VMEM((n, *shape), F32), pltpu.VMEM((n, N_DEV, *shape), F32), DMA((n,)), DMA((n,))]

    def start(self, b):
        here = coords()
        me = flat(here)
        self.got[b, me] = self.acc[b]
        for which in PEERS:
            remote(self.acc.at[b], self.got.at[b, me], self.send_sem.at[b], self.recv_sem.at[b],
                   flip(here, which)).start()

    def total(self, b):
        all_of = self.got.at[b, pl.ds(0, len(PEERS))]
        copies = remote(all_of, all_of, self.send_sem.at[b], self.recv_sem.at[b], coords())
        copies.wait_send()
        copies.wait_recv()
        out = self.got[b, 0]
        for f in range(1, N_DEV):
            out += self.got[b, f]
        return out


class Gather:
    def __init__(self, own, dest, n, sems):
        self.own, self.dest, self.n = own, dest, n
        self.ys, self.yr, self.xs, self.xr, self.cs, self.cr = sems
        self.here = coords()
        _, x, c = self.here
        self.mine, self.across = 2 * x + c, 2 * (other(x)) + c
        self.core = (2 * x + other(c), 2 * (other(x)) + other(c))

    @staticmethod
    def scratch(n):
        return [DMA((n,))] * 4 + [DMA((2, n))] * 2

    def y(self, p):
        model = self.here[0]
        return remote(self.own(self.mine, p), self.dest(model, self.mine, p), self.ys.at[p], self.yr.at[p],
                      flip(self.here, Y_PEER))

    def moved(self, q, p, send_sem, recv_sem, which):
        ref = self.dest(1 - self.here[0], q, p)
        return remote(ref, ref, send_sem, recv_sem, flip(self.here, which))

    def x(self, p, q):
        return self.moved(q, p, self.xs.at[p], self.xr.at[p], X_PEER)

    def c(self, p, late, q):
        return self.moved(q, p, self.cs.at[late, p], self.cr.at[late, p], C_PEER)

    def start(self):
        for p in range(self.n):
            self.y(p).start()

    def pass_y(self, p):
        self.moved(self.mine, p, self.ys.at[p], self.yr.at[p], Y_PEER).wait_recv()
        self.x(p, self.mine).start()
        self.c(p, 0, self.mine).start()

    def pass_x(self, p):
        self.x(p, self.across).wait_recv()
        self.c(p, 1, self.across).start()

    def wait_core(self, late):
        for p in range(self.n):
            self.c(p, late, self.core[late]).wait_recv()

    def drain(self):
        for p in range(self.n):
            self.y(p).wait_send()
            self.x(p, self.mine).wait_send()
            self.c(p, 0, self.mine).wait_send()
            self.c(p, 1, self.across).wait_send()


def call(kernel, name, cid, grid, in_specs, out_specs, out_shape, scratch, flops, nbytes, args):
    return pl.pallas_call(
        kernel, name=name, grid=grid, in_specs=in_specs, out_specs=out_specs, out_shape=out_shape, scratch_shapes=scratch,
        compiler_params=pltpu.CompilerParams(vmem_limit_bytes=MAX_VMEM, collective_id=cid, has_side_effects=cid is not None),
        cost_estimate=pl.CostEstimate(flops=flops, bytes_accessed=nbytes, transcendentals=0))(*args)


def fwd_first(h_a, h_b, w_one, w_two, gb_own):
    depth, half = w_one.shape
    dim = 2 * half
    rows = h_a.shape[0] // 2
    tile, width, quarter = 2 * TM, half // 2, half // 4
    steps = rows // tile
    per_block = 2 * steps
    n, n2 = 4, 8

    def block(j):
        y, x, _ = coords()
        return jnp.where(j < 2, 2 * y + j, 2 * (other(y)) + jnp.where(j == 2, x, other(x)))

    def tile_of(j, i):
        return jnp.where(odd(j) == 0, i, per_block - 1 - i)

    def kernel(ha_ref, hb_ref, w_ref, w2_ref, gb_ref, u_ref, s_ref, gbo_ref, w2o_ref, ht_ref, w1, gbf, *sems):
        share, sems = Share(*sems[:4]), sems[4:]
        gs, gr, lsem = sems[:3]
        sems = sems[3:]
        j, i = pl.program_id(0), pl.program_id(1)
        step = j * per_block + i
        here = coords()
        y = here[0]
        one = Gather(lambda q, p: w_ref.at[at(p, depth // n), at(q, quarter)],
                     lambda m, q, p: w1.at[at(p, depth // n), at(m * 4 + q, quarter)], n, sems[:6])
        two = Gather(lambda q, p: w2_ref.at[at(q * n2 + p, quarter // n2)],
                     lambda m, q, p: w2o_ref.at[at(q * n2 + p, quarter // n2)], n2, sems[6:])

        def local(b):
            return pltpu.make_async_copy(w_ref.at[:, at(b, width)], w1.at[:, at(2 * y + b, width)], lsem.at[b])

        def bn_vectors(m):
            return remote(gb_ref, gbf.at[:, at(m, half)], gs, gr, flip(here, Y_PEER))

        def begin():
            arrive()
            local(0).start()
            local(1).start()
            all_arrived()
            one.start()
            two.start()
            bn_vectors(y).start()
            local(0).wait()

        def late_half():
            one.pass_x(0)
            one.pass_y(n - 1)
            one.wait_core(0)

        hooks = [(0, begin), (per_block, lambda: local(1).wait()), (2 * per_block, late_half)]
        hooks += [(2 * p + 3, functools.partial(one.pass_y, p)) for p in range(n - 1)]
        hooks += [(p + 2 * per_block, functools.partial(one.pass_x, p)) for p in range(1, n)]
        hooks += [(3 * per_block, lambda: one.wait_core(1))]
        hooks += [(p + 9, functools.partial(two.pass_y, p)) for p in range(n2 - 1)]
        hooks += [(13 + (p + 1) // 2, functools.partial(two.pass_x, p)) for p in range(n2 // 2)]
        for s, hook in hooks:
            pl.when(step == s)(hook)
        for b in range(3):
            pl.when(step == (b + 1) * per_block)(lambda b=b: share.start(block(b)))

        tile_at = tile_of(j, i)
        first_view = tile_at < steps
        cols = at(j, width)
        ht_ref[...] = lax.select(first_view, ha_ref[:, cols], hb_ref[:, cols]).T
        for r in runs(tile, TM):
            u_ref[r] = mm(lax.select(first_view, ha_ref[r], hb_ref[r]), w1[:, at(block(j), width)])
        sums = jnp.concatenate([moments(u_ref, cols) for cols in runs(width, LANES)], axis=1)
        v = tile_at // steps
        share.acc[block(j), v] = jnp.where(i % steps == 0, 0.0, share.acc[block(j), v]) + sums

        @pl.when(step == 4 * per_block - 1)
        def _():
            share.start(block(3))
            two.pass_y(n2 - 1)
            for p in range(n2 // 2, n2):
                two.pass_x(p)
            bn_vectors(other(y)).wait_recv()
            bn_vectors(y).wait_send()
            gbo_ref[...] = gbf[...]
            gbo_ref[:, at(y, half)] = gb_ref[...]
            for b in range(4):
                s_ref[:, :, b * width:(b + 1) * width] = share.total(b)
            one.drain()
            two.drain()
            two.wait_core(0)
            two.wait_core(1)

    return call(
        kernel, "fwd_first", 0, (4, per_block),
        [pl.BlockSpec((tile, depth), lambda j, i: (coords()[0] * steps + jnp.minimum(tile_of(j, i), steps - 1), 0)),
         pl.BlockSpec((tile, depth), lambda j, i: (coords()[0] * steps + jnp.maximum(tile_of(j, i) - steps, 0), 0)),
         ANY, ANY, whole(2, half)],
        [pl.BlockSpec((tile, width), lambda j, i: (tile_of(j, i), block(j))), whole(2, 2, dim),
         whole(2, dim), ANY, pl.BlockSpec((width, tile), lambda j, i: (j, tile_of(j, i)))],
        [sds((2 * rows, dim), F32), sds((2, 2, dim), F32), sds((2, dim), F32), sds((half, dim), BF16),
         sds((depth, 2 * rows), BF16)],
        [pltpu.VMEM((depth, dim), BF16), pltpu.VMEM((2, dim), F32)] + Share.scratch(4, 2, 2, width)
        + [DMA, DMA, TWO_DMA] + Gather.scratch(n) + Gather.scratch(n2),
        4 * rows * depth * dim, 2 * rows * (8 * depth + 4 * dim), (h_a, h_b, w_one, w_two, gb_own))


def fwd_next(u, sums, gb, w_own, w_other, by_rows, total, cid, w_next=None):
    all_rows, depth = u.shape
    dim = w_own.shape[1] if by_rows else 2 * w_own.shape[1]
    half = dim // 2
    quarter = half // 4
    steps = all_rows // 2 // TM
    last = 2 * steps - 1
    slab = dim // (2 * steps)
    n = 4

    def kernel(u_ref, s_ref, gb_ref, wo_ref, wt_ref, *refs):
        if w_next is not None:
            wn_ref, refs = refs[0], refs[1:]
        x_ref, o_ref, so_ref, wtr_ref, *refs = refs
        if w_next is not None:
            wno_ref, *refs = refs
        w, act, acc, got, ssem, rsem, lsem, *refs = refs
        share = Share(acc, got, ssem, rsem)
        i = pl.program_id(0)
        y = coords()[0]

        def local(ref, model, b):
            where = at(model, half)
            return pltpu.make_async_copy(ref, w.at[where] if by_rows else w.at[:, where], lsem.at[b])

        if w_next is not None:
            gather = Gather(lambda q, p: wn_ref.at[at(p, depth // n), at(q, quarter)],
                            lambda m, q, p: wno_ref.at[at(p, depth // n), at(q, quarter)], n, refs)

        @pl.when(i == 0)
        def _():
            arrive()
            acc[...] = jnp.zeros_like(acc)
            local(wo_ref, y, 0).start()
            local(wt_ref, other(y), 1).start()
            all_arrived()
            if w_next is not None:
                gather.start()
            local(wo_ref, y, 0).wait()
            local(wt_ref, other(y), 1).wait()

        if w_next is not None:
            for p in range(n):
                pl.when(i == p + 1)(lambda p=p: gather.pass_y(p))
                pl.when(i == p + 3)(lambda p=p: gather.pass_x(p))
        pl.when(i == steps)(lambda: share.start(0))

        mean, inv = mean_inv(s_ref[0], total)
        for k, cols in enumerate(runs(depth, LANES)):
            m, r, g, b = (t[:, k * LANES:(k + 1) * LANES] for t in (mean, inv, gb_ref[:1], gb_ref[1:]))
            for piece in runs(TM, PIECE):
                act[piece, cols] = jnp.maximum((u_ref[piece, cols] - m) * r * g + b, 0.0).astype(BF16)
        x_ref[...] = act[...].T
        wtr_ref[...] = w[:, at(i, slab)].T
        v = i // steps
        keep = jnp.where(i % steps == 0, 0.0, 1.0)
        for some in runs(dim, TM):
            o_ref[:, some] = mm(act[...], w[:, some])
            for cols in runs(TM, LANES):
                cols = pl.ds(some.start + cols.start, LANES)
                share.acc[v, :, cols] = keep * share.acc[v, :, cols] + moments(o_ref, cols)

        @pl.when(i == last)
        def _():
            share.start(1)
            for b in BOTH:
                so_ref[b] = share.total(b)
            if w_next is not None:
                gather.drain()
                gather.wait_core(0)
                gather.wait_core(1)

    more = w_next is not None
    return call(
        kernel, "fwd_next", cid, (2 * steps,),
        [pl.BlockSpec((TM, depth), lambda i: (i, 0)), pl.BlockSpec((1, 2, depth), lambda i: (i // steps, 0, 0)),
         whole(2, depth), ANY, ANY] + [ANY] * more,
        [pl.BlockSpec((depth, TM), lambda i: (0, i)), pl.BlockSpec((TM, dim), lambda i: (i, 0)),
         whole(2, 2, dim), pl.BlockSpec((slab, depth), lambda i: (i, 0))] + [ANY] * more,
        [sds((depth, all_rows), BF16), sds((all_rows, dim), F32), sds((2, 2, dim), F32), sds((dim, depth), BF16)]
        + ([sds(w_next.shape, BF16)] if more else []),
        [pltpu.VMEM((depth, dim), BF16), pltpu.VMEM((TM, depth), BF16)] + Share.scratch(2, 2, dim) + [TWO_DMA] + (Gather.scratch(n) if more else []),
        2 * all_rows * depth * dim, all_rows * (6 * depth + 4 * dim),
        (u, sums, gb, w_own, w_other) + ((w_next,) if more else ()))


def corr_grad(z, sums, lam, total):
    all_rows, dim = z.shape
    rows = all_rows // 2
    half = dim // 2
    quart = half // 2
    n_chunk = 8
    width = half // n_chunk
    pair = 2 * width
    mt = TM
    zt = TM // 2
    ahead = 3
    lead = 4
    z_steps = all_rows // zt
    m_steps = rows // mt
    scale = 1.0 / total

    def kernel(z_ref, s_ref, lam_ref, zho_ref, d_ref, so_ref, lo_ref, zh, da, ck, r1, r2, g, stage, dsend, drecv, acc, got, ssem, rsem, loss_acc, loss_got, lsem, lrsem, zs, zos,
               d1s, d1r, s1s, s1r, s2s, s2r, a2s, a2r, a1s, a1r, ads, adr, dbs, das):
        share = Share(acc, got, ssem, rsem)
        share_loss = Share(loss_acc, loss_got, lsem, lrsem)
        here = coords()
        y, x, c = here
        on_x = c == 0
        by_core = lambda one, two: tuple(jnp.where(on_x, a, b) for a, b in zip(one, two))
        first = by_core(flip(here, X_PEER), flip(here, Y_PEER))
        second = by_core(flip(here, Y_PEER), flip(here, X_PEER))
        cpeer = flip(here, C_PEER)
        bit1, bit2 = by_core((x, y), (y, x))
        arrive()
        acc[...] = jnp.zeros_like(acc)
        loss_acc[...] = jnp.zeros_like(loss_acc)

        def load(i, slot):
            return pltpu.make_async_copy(z_ref.at[at(i, zt)], ck.at[at(slot, zt)], zs.at[slot])

        def zh_out(i):
            v, r = lax.div(i, n_chunk // 2), lax.rem(i, n_chunk // 2)
            return pltpu.make_async_copy(zh.at[v, at(r, TM)], zho_ref.at[v, at(r, TM)], zos.at[i])

        z_slots = half // zt
        for i in range(ahead):
            load(i, i).start()

        def normalise(i):
            slot = lax.rem(i, z_slots)
            v, r = lax.div(i, z_steps // 2), lax.rem(i, z_steps // 2)
            pl.when(i + ahead < z_steps)(lambda: load(i + ahead, lax.rem(i + ahead, z_slots)).start())
            load(i, slot).wait()
            mean, inv = mean_inv(s_ref[v], total)
            for k, cols in enumerate(runs(dim, LANES)):
                m, s = (t[:, k * LANES:(k + 1) * LANES] for t in (mean, inv))
                for p in range(zt // PIECE):
                    zh[v, at(r * (zt // PIECE) + p, PIECE), cols] = (
                        (ck[at(slot * (zt // PIECE) + p, PIECE), cols] - m) * s).astype(BF16)
            da[at(i, rows // z_steps)] = jnp.zeros((rows // z_steps, dim), F32)

        loop(z_steps, normalise)
        all_arrived()

        def both(v, rows_at, t):
            return jnp.concatenate([zh[v, rows_at, at(b * n_chunk + t, width)] for b in BOTH], axis=1)

        group = lambda t, b: at(2 * t + b, width)

        def to_core(t):
            return remote(dsend.at[odd(t)], drecv.at[odd(t)], d1s.at[t], d1r.at[t], cpeer)

        def to_first(t):
            return remote(ck.at[:, group(t, other(bit1))], r1.at[t], s1s.at[t], s1r.at[t], first)

        def to_second(t):
            return remote(ck.at[at(other(bit2), quart), group(t, bit1)], r2.at[t], s2s.at[t], s2r.at[t], second)

        def g_second(t, b):
            block = g.at[t, at(2 * c + b, quart), at(bit1, width)]
            return remote(block, block, a2s.at[t], a2r.at[t], second)

        def g_first(t, b):
            block = g.at[t, at(c, half), at(b, width)]
            return remote(block, block, a1s.at[t], a1r.at[t], first)

        def g_core(t, core):
            block = g.at[t, at(core, half)]
            return remote(block, block, ads.at[t], adr.at[t], cpeer)

        def chip_sum(t):
            to_core(t).wait_recv()
            to_core(t).wait_send()
            ck[:, at(t, pair)] += drecv[odd(t)]
            pl.when(t < lead - 1)(lambda: to_first(t).start())

        def corr_part(t):
            zh_out(t).start()
            right = both(1, pl.ds(0, rows), t)
            dsend[odd(t)] = mm_at(zh[0, :, at(other(c), half)], right)
            ck[:, at(t, pair)] = mm_at(zh[0, :, at(c, half)], right)
            to_core(t).start()

        def db_out(t, m, slot, b):
            return pltpu.make_async_copy(
                stage.at[slot, :, at(b, width)], d_ref.at[1, at(m, mt), at(b * n_chunk + t, width)], dbs.at[slot, b])

        def da_out(m):
            return pltpu.make_async_copy(da.at[at(m, mt)], d_ref.at[0, at(m, mt)], das.at[m])

        def finish(m):
            def scaled(cols):
                for p in range(mt // PIECE):
                    some = at(m * (mt // PIECE) + p, PIECE)
                    d = da[some, cols] * scale
                    da[some, cols] = d
                    yield d, d * zh[0, some, cols].astype(F32)

            for cols in runs(dim, LANES):
                acc[0, :, cols] += two_sums(scaled(cols))
            da_out(m).start()

        def grads(t):
            def rows_of(m):
                slot = odd(m)

                @pl.when(t * m_steps + m >= 2)
                def _():
                    for b in BOTH:
                        db_out(t, m, slot, b).wait()

                own = both(1, at(m, mt), t)
                stage[slot] = mm(zh[0, at(m, mt)], g[t]) * scale
                sums = two_sums((stage[slot, r], stage[slot, r] * both(1, at(m * (mt // PIECE) + p, PIECE), t).astype(F32))
                                for p, r in enumerate(runs(mt, PIECE)))
                for b in BOTH:
                    acc[1, :, at(b * n_chunk + t, width)] += sums[:, b * width:(b + 1) * width]
                    db_out(t, m, slot, b).start()
                for cols in runs(dim, LANES):
                    da[at(m, mt), cols] += mm_bt(own, g[t, cols])
                pl.when(t == n_chunk - 1)(lambda: finish(m))

            loop(m_steps, rows_of)

        def at_first(t):
            to_first(t).wait_recv()
            ck[:, group(t, bit1)] += r1[t]
            to_second(t).start()

        def at_second(t):
            to_second(t).wait_recv()
            corr_mat = (ck[at(bit2, quart), group(t, bit1)] + r2[t]) * scale
            row_ids = (2 * c + bit2) * quart + lax.broadcasted_iota(jnp.int32, (quart, width), 0)
            col_ids = (bit1 * n_chunk + t) * width + lax.broadcasted_iota(jnp.int32, (quart, width), 1)
            is_diag = row_ids == col_ids
            lam_val = lam_ref[0]
            loss = jnp.where(is_diag, (1.0 - corr_mat) * (1.0 - corr_mat), lam_val * corr_mat * corr_mat)
            loss_acc[0] += jnp.sum(loss, axis=0, keepdims=True)
            pl.when(t == n_chunk - 1)(lambda: share_loss.start(0))
            grad = jnp.where(is_diag, -2.0 * (1.0 - corr_mat), 2.0 * lam_val * corr_mat).astype(BF16)
            g[t, at(2 * c + bit2, quart), at(bit1, width)] = grad
            g_second(t, bit2).start()

        def back_second(t):
            g_second(t, other(bit2)).wait_recv()
            g_first(t, bit1).start()
            pl.when(t + lead - 1 < n_chunk)(lambda: to_first(t + lead - 1).start())

        def back_first(t):
            g_first(t, other(bit1)).wait_recv()
            g_core(t, c).start()

        def back_core(t):
            g_core(t, other(c)).wait_recv()
            grads(t)

        def advance(tau):
            for lag, stage_fn in ((lead, at_first), (lead + 2, back_core), (lead + 1, back_first), (lead, at_second),
                                  (1, chip_sum), (0, corr_part), (lead, back_second)):
                t = tau - lag
                pl.when(jnp.logical_and(t >= 0, t < n_chunk))(lambda t=t, stage_fn=stage_fn: stage_fn(t))

        loop(n_chunk + lead + 2, advance)
        share.start(1)
        share.start(0)
        for t in range(n_chunk):
            for copy in (to_first(t), to_second(t), g_second(t, bit2), g_first(t, bit1), g_core(t, c)):
                copy.wait_send()
        for b in BOTH:
            so_ref[b] = share.total(b)
            for slot in BOTH:
                db_out(0, 0, slot, b).wait()
        lo_ref[...] = share_loss.total(0)
        for i in range(n_chunk):
            zh_out(i).wait()
        for m in range(m_steps):
            da_out(m).wait()

    return call(
        kernel, "corr_grad", 3, (), [ANY, VMEM, pl.BlockSpec(memory_space=pltpu.SMEM)], [ANY, ANY, VMEM, VMEM],
        [sds((2, rows, dim), BF16), sds((2, rows, dim), F32), sds((2, 2, dim), F32), sds((1, width), F32)],
        [pltpu.VMEM((2, rows, dim), BF16), pltpu.VMEM((rows, dim), F32), pltpu.VMEM((half, dim), F32),
         pltpu.VMEM((n_chunk, half, width), F32), pltpu.VMEM((n_chunk, quart, width), F32),
         pltpu.VMEM((n_chunk, dim, pair), BF16), pltpu.VMEM((2, mt, pair), F32)]
        + [pltpu.VMEM((2, half, pair), F32)] * 2 + Share.scratch(2, 2, dim) + Share.scratch(1, 1, width)
        + [DMA((half // zt,)), DMA((n_chunk,))] + [DMA((n_chunk,))] * 12 + [DMA((2, 2)), DMA((m_steps,))],
        all_rows * dim * dim * 3, all_rows * dim * 12, (z, sums, lam))


def backward(d_emb, zh, sz, s_emb, layers, x2_t, total):
    all_rows, dim = zh.shape
    rows, half = all_rows // 2, dim // 2
    width = 256
    slabs = dim // width
    items = 2 * slabs
    piece = width
    side = half // 2 // piece
    per_slab = half // piece
    n_layer = len(layers) + 1
    n_slab = n_layer * slabs
    per_layer = slabs * side
    n_chunk = n_layer * per_layer
    ahead = 3
    (u2, s2, gb2, w3_t, x1_t), (u1, s1, gb1, w2_t, h_t) = layers

    def kernel(d_ref, zh_ref, sz_ref, sd_ref, x2_ref, x1_ref, h_ref, u2_ref, u1_ref, w3_ref, w2_ref,
               s2_ref, s1_ref, gb2_ref, gb1_ref, dw3_ref, dw2_ref, dw1_ref, sum_ref, dy_ref, part_ref, ry_ref, rx_ref,
               dbuf, xbuf, d0, d1, wbuf, ubuf, dybuf, dyout, psend, pkeep, dr, ebuf, mbuf, fbuf, acc, got, ssem, rsem,
               us, ws, ds, dos, xl, ps, pr, pm, ys, yr, xs, xr, es, fs, fcs, fcr, credit):
        share = Share(acc, got, ssem, rsem)
        here = coords()
        y, x, c = here
        ypeer, xpeer, cpeer = flip(here, Y_PEER), flip(here, X_PEER), flip(here, C_PEER)
        arrive()

        def column(k, n):
            model = odd(n + jnp.where(k == 0, other(y), 0))
            return jnp.where(k == 1, n, model * (slabs // 2) + lax.div(n, 2))

        def turn(k):
            return jnp.where(k == 0, 0, other(y))

        def m_slot(j):
            return lax.rem(j, 4)

        def copy(src, dst, sem):
            return pltpu.make_async_copy(src, dst, sem)

        def sent_by(q):
            first = jnp.minimum(per_slab * lax.div(q, 4), per_layer)
            middle = jnp.clip(side * lax.div(q - 2 * items - 2, 2), 0, per_layer)
            last = jnp.clip(per_slab * lax.div(q - 4 * items - 2, 4), 0, per_layer)
            return first + middle + last

        def begun(q):
            return jnp.maximum(lax.div(q - 6, 2), 0)

        def to_core(s):
            return remote(psend.at[odd(s)], dr.at[odd(s)], ps.at[s], pr.at[s], cpeer)

        def keep_out(s):
            return copy(pkeep.at[odd(s)], part_ref.at[s], pm)

        def chip_sum(s):
            to_core(s).wait_recv()
            pkeep[odd(s)] += dr[odd(s)]

            @pl.when(s + 2 < n_slab)
            def _():
                pl.semaphore_signal(credit, inc=1, device_id=device(cpeer), device_id_type=pl.DeviceIdType.MESH)

            to_core(s).wait_send()
            keep_out(s).start()

        def home(j, own):
            k = lax.div(j, per_layer)
            i = lax.rem(j, per_layer)
            model = y if own else other(y)
            turned = other(turn(k)) if own else turn(k)
            s = jnp.where(k == 1, lax.div(i, side), 2 * lax.div(i, per_slab) + turned)
            place = jnp.where(k == 1, model * side + lax.rem(i, side), lax.rem(i, per_slab))
            return part_ref.at[k * slabs + s, at(place, piece)]

        def to_y(j):
            return remote(home(j, False), ry_ref.at[j], ys.at[lax.div(j, per_layer)], yr.at[j], ypeer)

        def issue(s, q):
            keep_out(s).wait()
            k, n = lax.div(s, slabs), lax.rem(s, slabs)
            for mine, fire, first, count in (
                    (k == 1, True, n * side, side), (k != 1, odd(n) == jnp.where(k == 0, 0, 1), lax.div(n, 2) * per_slab, per_slab)):
                for r in range(count):
                    j = k * per_layer + first + r
                    pl.when(mine & fire & (j < begun(q) + ahead))(lambda j=j: to_y(j).start())

        def to_x(j):
            return remote(mbuf.at[m_slot(j)], rx_ref.at[j], xs.at[m_slot(j)], xr.at[j], xpeer)

        def result(j, k):
            i = lax.rem(j, per_layer)
            if k == 1:
                return dw2_ref.at[at(c * side + lax.rem(i, side), piece), at(lax.div(i, side), width)]
            return (dw1_ref if k else dw3_ref).at[at(c * per_slab + lax.rem(i, per_slab), piece), at(lax.div(i, per_slab), width)]

        def put(j, k):
            slot = odd(j)
            return (copy(fbuf.at[slot], result(j, k), fs.at[slot]),
                    remote(fbuf.at[slot], result(j, k), fcs.at[slot], fcr.at[k], cpeer))

        def put_done(j):
            here_copy, there_copy = put(j, 0)
            here_copy.wait()
            there_copy.wait_send()

        def load_part(j, which):
            src = (lambda: ry_ref.at[j], lambda: home(j, True), lambda: rx_ref.at[j])[which]()
            return copy(src, ebuf.at[which], es.at[which])

        def fetch_x(j):
            to_x(j).wait_recv()
            load_part(j, 2).start()

        def begin(j, q):
            remote(ry_ref.at[j], ry_ref.at[j], ys.at[0], yr.at[j], ypeer).wait_recv()
            load_part(j, 0).start()
            load_part(j, 1).start()
            pl.when(j + ahead < sent_by(q))(lambda: to_y(j + ahead).start())
            pl.when(j >= 2)(lambda: fetch_x(j - 2))

        def deliver(j):
            load_part(j, 2).wait()
            pl.when(j >= 2)(lambda: put_done(j))
            fbuf[odd(j)] = mbuf[m_slot(j)] + ebuf[2]
            for k in range(n_layer):
                @pl.when(lax.div(j, per_layer) == k)
                def _(k=k):
                    for one in put(j, k):
                        one.start()

        def end(j):
            load_part(j, 0).wait()
            load_part(j, 1).wait()
            pl.when(j >= 4)(lambda: to_x(j).wait_send())
            mbuf[m_slot(j)] = ebuf[0] + ebuf[1]
            to_x(j).start()
            pl.when(j >= 2)(lambda: deliver(j - 2))

        def events(q):
            now, before, earlier = begun(q), begun(q - 1), begun(q - 2)
            pl.when(before > earlier)(lambda: end(before - 1))
            pl.when(now > before)(lambda: begin(now - 1, q))

        def weight_slab(k, n, v, d):
            slot = odd(k * slabs + n)
            for buf, part in ((psend, other(c)), (pkeep, c)):
                first = jnp.where(k == 1, part, 2 * part)
                for b in BOTH:
                    left = xbuf[at(first + b * jnp.where(k == 1, 2, 1), half // 2), pl.ds(v * rows, rows)]
                    here_at = at(b, half // 2)
                    prod = mm(left, d)
                    buf[slot, here_at] = buf[slot, here_at] + prod if v else prod

        def after(k, n, v, q):
            s = k * slabs + n
            if v == 0:
                pl.when(n > 0)(lambda: chip_sum(s - 1))
            else:
                pl.when(s >= 2)(lambda: pl.semaphore_wait(credit, 1))
                to_core(s).start()
                pl.when(n > 0)(lambda: issue(s - 1, q))

        def dw_pass(k, q, ready, fetch, pre, ahead_of_next):
            ready(0)
            fetch(1)
            pre(d0, 0, 0)

            def slab(n):
                for v, d_ref, d_next in ((0, d0, d1), (1, d1, d0)):
                    i = 2 * n + v
                    pl.when(i + 1 < items)(lambda: ready(i + 1))
                    pl.when(i + 2 < items)(lambda: fetch(i + 2))
                    pl.when(n == 0)(lambda: x_load(x2_ref, v).wait())
                    if v:
                        pl.when(n == slabs - 1)(ahead_of_next)
                    events(q + i)
                    for r in runs(rows, TM):
                        dbuf[pl.ds(v * rows + r.start, TM), at(column(k, n), width)] = d_ref[r]
                    weight_slab(k, n, v, d_ref[...])
                    pre(d_next, jnp.minimum(n + v, slabs - 1), other(v))
                    after(k, n, v, q + i)

            loop(slabs, slab)

        def emb_loads(i):
            n, v = split(i)
            cols = at(column(0, n), width)
            return (copy(d_ref.at[at(v, rows), cols], ubuf.at[v], us.at[v]),
                    copy(zh_ref.at[at(v, rows), cols], wbuf.at[v], ws.at[v]))

        def emb_fetch(i):
            for one in emb_loads(i):
                one.start()

        def emb_ready(i):
            for one in emb_loads(i):
                one.wait()

        def emb_pre(d_out, n, v):
            cols = at(column(0, n), width)
            _, inv = mean_inv(sz_ref[v, :, cols], total)
            sd = sd_ref[v, :, cols] / total
            for r in runs(rows, PIECE):
                d_out[r] = (inv * (ubuf[v, r] - sd[:1] - wbuf[v, r].astype(F32) * sd[1:])).astype(BF16)

        def x_load(src, v):
            return copy(src.at[:, at(v, rows)], xbuf.at[:, at(v, rows)], xl.at[v])

        def u_slot(layer, v):
            return jnp.where(layer == 0, other(v), v)

        def slab_of(ref, layer, i, buf, sem, slot):
            n, v = split(i)
            return copy(ref.at[at(v, rows), at(column(layer + 1, n), width)], buf.at[slot], sem.at[slot])

        def u_load(layer, i, ref=u2_ref):
            return slab_of(ref, layer, i, ubuf, us, u_slot(layer, odd(i)))

        def dy_load(layer, i):
            return slab_of(dy_ref, layer, i, dybuf, ds, odd(i))

        def dy_out(layer, i):
            n, v = split(i)
            return copy(dyout.at[v], dy_ref.at[at(v, rows), at(column(layer + 1, n), width)], dos.at[v])

        def w_load(layer, n, ref=w3_ref):
            slot = odd(n + 1)
            return copy(ref.at[:, at(column(layer + 1, n), width)], wbuf.at[slot], ws.at[slot])

        def by_layer(layer, make, refs):
            for k, ref in enumerate(refs):
                pl.when(layer == k)(lambda ref=ref: make(ref).start())

        def start_u(layer, i):
            by_layer(layer, lambda ref: u_load(layer, i, ref), (u2_ref, u1_ref))

        def start_w(layer, n):
            by_layer(layer, lambda ref: w_load(layer, n, ref), (w3_ref, w2_ref))

        def next_layer(layer):
            start_u(layer, 0)
            start_w(layer, 0)

        for one in (x_load(x2_ref, 0), *emb_loads(0), x_load(x2_ref, 1)):
            one.start()
        all_arrived()
        dw_pass(0, 0, emb_ready, emb_fetch, emb_pre, lambda: next_layer(0))

        def stats(layer, v, cols):
            pick = lambda one, two: jnp.where(layer == 0, one, two)
            mean, inv = mean_inv(pick(s2_ref[v, :, cols], s1_ref[v, :, cols]), total)
            gb = pick(gb2_ref[:, cols], gb1_ref[:, cols])
            return mean, inv, gb[:1], gb[1:]

        def bn_layer(layer):
            start = (2 * layer + 1) * items

            def dx_item(i):
                n, v = split(i)
                slot = u_slot(layer, v)
                cols = at(column(layer + 1, n), width)

                @pl.when(i + 1 < items)
                def _():
                    start_u(layer, i + 1)
                    pl.when((v == 0) & (n + 1 < slabs))(lambda: start_w(layer, n + 1))

                @pl.when(i + 1 == items)
                def _():
                    start_u(layer, 0)
                    dy_load(layer, 0).start()

                u_load(layer, i).wait()
                pl.when(v == 0)(lambda: w_load(layer, n).wait())
                events(start + i)
                pl.when((i == 4) | (i == 9))(lambda: by_layer(layer, lambda ref: x_load(ref, v), (x1_ref, h_ref)))
                pl.when(n > 0)(lambda: dy_out(layer, i).wait())
                mean, inv, gamma, beta = stats(layer, v, cols)

                def pieces():
                    for b in range(rows // TM):
                        dx = mm(dbuf[at(v * (rows // TM) + b, TM)], wbuf[odd(n + 1)])
                        for p in range(0, TM, PIECE):
                            some = pl.ds(b * TM + p, PIECE)
                            norm = (ubuf[slot, some] - mean) * inv
                            dy = jnp.where(norm * gamma + beta > 0, dx[p:p + PIECE], 0.0)
                            dyout[v, some] = dy
                            yield dy, dy * norm

                g = layer * items + i
                acc[g] = two_sums(pieces())
                dy_out(layer, i).start()
                share.start(g)
                before = (layer + 1) * slabs - 1
                pl.when(i == 0)(lambda: chip_sum(before))
                pl.when(i == 1)(lambda: issue(before, start + i))

            def fetch(i):
                start_u(layer, i)
                dy_load(layer, i).start()

            def ready(i):
                n, v = split(i)
                u_load(layer, i).wait()
                dy_load(layer, i).wait()
                sum_ref[layer, v, :, at(column(layer + 1, n), width)] = share.total(layer * items + i)

            def pre(d_out, n, v):
                cols = at(column(layer + 1, n), width)
                tot = sum_ref[layer, v, :, cols] / total
                mean, inv, gamma, _ = stats(layer, v, cols)
                slope, front, slot = inv * tot[1:], gamma * inv, u_slot(layer, v)
                for r in runs(rows, PIECE):
                    d_out[r] = (front * (dybuf[v, r] - (tot[:1] + (ubuf[slot, r] - mean) * slope))).astype(BF16)

            loop(items, dx_item)
            for v in BOTH:
                dy_out(layer, v).wait()
            dw_pass(layer + 1, start + items, ready, fetch, pre, lambda: pl.when(layer == 0)(lambda: next_layer(1)))

        loop(len(layers), bn_layer)

        ticks = (2 * n_layer - 1) * items
        chip_sum(n_slab - 1)
        issue(n_slab - 1, ticks)
        ended = 36

        def tail(j):
            begin(j, ticks + 2)
            end(j)

        loop(n_chunk, tail, ended)
        for j in range(n_chunk - 2, n_chunk):
            fetch_x(j)
            deliver(j)
        for j in BOTH:
            put_done(j)
        for k in range(n_layer):
            theirs = dw2_ref.at[at(other(c), half // 2)] if k == 1 else (dw1_ref if k else dw3_ref).at[at(other(c), half)]
            remote(theirs, theirs, fcs.at[0], fcr.at[k], cpeer).wait_recv()
            sent = ry_ref.at[at(k, per_layer)]
            remote(sent, sent, ys.at[k], yr.at[0], ypeer).wait_send()
        for j in range(n_chunk - 4, n_chunk):
            to_x(j).wait_send()

    n_item = len(layers) * items
    vm = lambda *shape: pltpu.VMEM(shape, F32)
    bf = lambda *shape: pltpu.VMEM(shape, BF16)
    return call(
        kernel, "backward", 4, (),
        [ANY, ANY, VMEM, VMEM] + [ANY] * 7 + [VMEM] * 4, [ANY] * 3 + [VMEM] + [ANY] * 4,
        [sds((dim, half), F32), sds((half, dim), F32), sds((dim, half), F32), sds((len(layers), 2, 2, dim), F32),
         sds((all_rows, dim), F32), sds((n_slab, half, width), F32), sds((n_chunk, piece, width), F32),
         sds((n_chunk, piece, width), F32)],
        [bf(all_rows, dim), bf(dim, all_rows), bf(rows, width), bf(rows, width), bf(2, dim, width),
         vm(2, rows, width), vm(2, rows, width), vm(2, rows, width),
         vm(2, half, width), vm(2, half, width), vm(2, half, width), vm(3, piece, width), vm(4, piece, width),
         vm(2, piece, width)] + Share.scratch(n_item, 2, width)
        + [TWO_DMA, TWO_DMA, TWO_DMA, TWO_DMA, TWO_DMA, DMA((n_slab,)), DMA((n_slab,)), DMA, DMA((n_layer,)),
           DMA((n_chunk,)), DMA((4,)), DMA((n_chunk,)), DMA((3,)), TWO_DMA, TWO_DMA, DMA((n_layer,)),
           pltpu.SemaphoreType.REGULAR],
        all_rows * dim * dim * 10, all_rows * dim * 40,
        (d_emb, zh, sz, s_emb, x2_t, x1_t, h_t, u2, u1, w3_t, w2_t, s2, s1, gb2, gb1))


def settle(*grads):
    steps = 8

    def kernel(*refs):
        for src, dst in zip(refs[:len(grads)], refs[len(grads):]):
            dst[...] = src[...]

    specs = [pl.BlockSpec((g.shape[0] // steps, g.shape[1]), lambda i: (i, 0)) for g in grads]
    return call(kernel, "settle", None, (steps,), specs, specs, [sds(g.shape, F32) for g in grads], [], 0,
                len(grads) * grads[0].size * 8, grads)


def solution(mesh):
    def shard_body(h_a, h_b, w_one, w_two, w_three, g_one, b_one, g_two, b_two, lam_off):
        y = lax.axis_index('model')
        total = float(h_a.shape[0] * mesh.shape['data'])
        dim, half = w_three.shape
        gb2 = jnp.stack([g_two, b_two])
        u1, s1, gb1, w_two_o, h_t = fwd_first(h_a, h_b, w_one, w_two, jnp.stack([g_one, b_one]))
        x1_t, u2, s2, w2_t, w_three_o = fwd_next(u1, s1, gb1, w_two, w_two_o, True, total, 1, w_three)
        x2_t, z, sz, w3_t = fwd_next(u2, s2, gb2, w_three, w_three_o, False, total, 2)
        zh, d_emb, s_emb, loss = corr_grad(z, sz, lam_off, total)
        loss = jnp.sum(loss)
        dw_three, dw_two, dw_one, sums, *_ = backward(
            d_emb.reshape(z.shape), zh.reshape(z.shape), sz, s_emb,
            ((u2, s2, gb2, w3_t, x1_t), (u1, s1, gb1, w2_t, h_t)), x2_t, total)
        dw_three, dw_two, dw_one = settle(dw_three, dw_two, dw_one)
        sums = jnp.sum(sums, axis=1)
        sum2 = sums[0]
        sum1 = lax.dynamic_slice_in_dim(sums[1], y * half, half, 1)
        return loss.reshape(1), dw_one, dw_two, dw_three, sum1[1], sum1[0], sum2[1], sum2[0]

    in_specs = (P('data', None), P('data', None), P(None, 'model'), P('model', None), P(None, 'model'),
                P('model'), P('model'), P(), P(), P())
    out_specs = (P(), P(None, 'model'), P('model', None), P(None, 'model'), P('model'), P('model'), P(), P())
    return jax.shard_map(shard_body, mesh=mesh, in_specs=in_specs, out_specs=out_specs, check_vma=False)
```

```python
import functools

import jax
import jax.numpy as jnp
from jax import lax
from jax.experimental import pallas as pl
from jax.experimental.pallas import tpu as pltpu
from jax.sharding import PartitionSpec as P

BN_EPS = 1e-5
F32 = jnp.float32
BF16 = jnp.bfloat16
PIECE = 64
LANES = 256
SUBLANES = 8
TM = 512
MAX_VMEM = 67043328
ANY = pl.BlockSpec(memory_space=pl.ANY)
VMEM = pl.BlockSpec(memory_space=pltpu.VMEM)
DMA = pltpu.SemaphoreType.DMA
TWO_DMA = DMA((2,))
BOTH = (0, 1)
PEERS = [(ky, kx, kc) for ky in BOTH for kx in BOTH for kc in BOTH][1:]
C_PEER, X_PEER, Y_PEER = PEERS[0], PEERS[1], PEERS[3]
N_DEV = len(PEERS) + 1


def mm(left, right):
    return jnp.dot(left, right, preferred_element_type=F32)


def mm_bt(left, right):
    return lax.dot_general(left, right, (((1,), (1,)), ((), ())), preferred_element_type=F32)


def mm_at(left, right):
    return lax.dot_general(left, right, (((0,), (0,)), ((), ())), preferred_element_type=F32)


def other(p):
    return 1 - p


def odd(i):
    return lax.rem(i, 2)


def split(i):
    return lax.div(i, 2), odd(i)


def loop(n, body, start=0):
    def one(i, carry):
        body(i)
        return carry

    lax.fori_loop(start, n, one, 0)


def whole(*shape):
    return pl.BlockSpec(shape, lambda *_: (0,) * len(shape))


def at(i, n):
    return pl.ds(pl.multiple_of(i * n, n), n)


def sds(shape, dtype):
    return jax.ShapeDtypeStruct(shape, dtype)


def mean_inv(sums, total):
    mean = sums[:1] / total
    var = sums[1:2] / total - mean * mean
    return mean, lax.rsqrt(var + BN_EPS)


def fold(v):
    return jnp.sum(v.reshape(-1, SUBLANES, v.shape[1]), axis=0)


def runs(n, size):
    return [pl.ds(r, size) for r in range(0, n, size)]


def two_sums(pairs):
    one = two = 0.0
    for a, b in pairs:
        one, two = one + fold(a), two + fold(b)
    return jnp.concatenate([jnp.sum(t, axis=0, keepdims=True) for t in (one, two)], axis=0)


def moments(ref, cols):
    pieces = (ref[r, cols] for r in runs(ref.shape[0], PIECE))
    return two_sums((u, u * u) for u in pieces)


def coords():
    y, d = lax.axis_index('model'), lax.axis_index('data')
    return y, lax.div(d, 2), odd(d)


def flip(here, which):
    return tuple(other(p) if f else p for p, f in zip(here, which))


def flat(here):
    y, x, c = here
    return 4 * y + 2 * x + c


def device(here):
    y, x, c = here
    return (y, 2 * x + c)


def remote(src, dst, send_sem, recv_sem, there):
    return pltpu.make_async_remote_copy(
        src_ref=src, dst_ref=dst, send_sem=send_sem, recv_sem=recv_sem, device_id=device(there),
        device_id_type=pl.DeviceIdType.MESH)


def arrive():
    here = coords()
    for k in PEERS:
        pl.semaphore_signal(pltpu.get_barrier_semaphore(), inc=1, device_id=device(flip(here, k)),
                            device_id_type=pl.DeviceIdType.MESH)


def all_arrived():
    pl.semaphore_wait(pltpu.get_barrier_semaphore(), len(PEERS))


class Share:
    def __init__(self, acc, got, send_sem, recv_sem):
        self.acc, self.got, self.send_sem, self.recv_sem = acc, got, send_sem, recv_sem

    @staticmethod
    def scratch(n, *shape):
        return [pltpu.VMEM((n, *shape), F32), pltpu.VMEM((n, N_DEV, *shape), F32), DMA((n,)), DMA((n,))]

    def start(self, b):
        here = coords()
        me = flat(here)
        self.got[b, me] = self.acc[b]
        for which in PEERS:
            remote(self.acc.at[b], self.got.at[b, me], self.send_sem.at[b], self.recv_sem.at[b],
                   flip(here, which)).start()

    def total(self, b):
        all_of = self.got.at[b, pl.ds(0, len(PEERS))]
        copies = remote(all_of, all_of, self.send_sem.at[b], self.recv_sem.at[b], coords())
        copies.wait_send()
        copies.wait_recv()
        out = self.got[b, 0]
        for f in range(1, N_DEV):
            out += self.got[b, f]
        return out


class Gather:
    def __init__(self, own, dest, n, sems):
        self.own, self.dest, self.n = own, dest, n
        self.ys, self.yr, self.xs, self.xr, self.cs, self.cr = sems
        self.here = coords()
        _, x, c = self.here
        self.mine, self.across = 2 * x + c, 2 * (other(x)) + c
        self.core = (2 * x + other(c), 2 * (other(x)) + other(c))

    @staticmethod
    def scratch(n):
        return [DMA((n,))] * 4 + [DMA((2, n))] * 2

    def y(self, p):
        model = self.here[0]
        return remote(self.own(self.mine, p), self.dest(model, self.mine, p), self.ys.at[p], self.yr.at[p],
                      flip(self.here, Y_PEER))

    def moved(self, q, p, send_sem, recv_sem, which):
        ref = self.dest(1 - self.here[0], q, p)
        return remote(ref, ref, send_sem, recv_sem, flip(self.here, which))

    def x(self, p, q):
        return self.moved(q, p, self.xs.at[p], self.xr.at[p], X_PEER)

    def c(self, p, late, q):
        return self.moved(q, p, self.cs.at[late, p], self.cr.at[late, p], C_PEER)

    def start(self):
        for p in range(self.n):
            self.y(p).start()

    def pass_y(self, p):
        self.moved(self.mine, p, self.ys.at[p], self.yr.at[p], Y_PEER).wait_recv()
        self.x(p, self.mine).start()
        self.c(p, 0, self.mine).start()

    def pass_x(self, p):
        self.x(p, self.across).wait_recv()
        self.c(p, 1, self.across).start()

    def wait_core(self, late):
        for p in range(self.n):
            self.c(p, late, self.core[late]).wait_recv()

    def drain(self):
        for p in range(self.n):
            self.y(p).wait_send()
            self.x(p, self.mine).wait_send()
            self.c(p, 0, self.mine).wait_send()
            self.c(p, 1, self.across).wait_send()


def call(kernel, name, cid, grid, in_specs, out_specs, out_shape, scratch, flops, nbytes, args):
    return pl.pallas_call(
        kernel, name=name, grid=grid, in_specs=in_specs, out_specs=out_specs, out_shape=out_shape, scratch_shapes=scratch,
        compiler_params=pltpu.CompilerParams(vmem_limit_bytes=MAX_VMEM, collective_id=cid, has_side_effects=cid is not None),
        cost_estimate=pl.CostEstimate(flops=flops, bytes_accessed=nbytes, transcendentals=0))(*args)


def fwd_first(h_a, h_b, w_one, w_two, *vectors):
    depth, half = w_one.shape
    dim = 2 * half
    rows = h_a.shape[0] // 2
    tile, width, quarter = 2 * TM, half // 2, half // 4
    steps = rows // tile
    per_block = 2 * steps
    n, n2 = 4, 8

    def block(j):
        y, x, _ = coords()
        return jnp.where(j < 2, 2 * y + j, 2 * (other(y)) + jnp.where(j == 2, x, other(x)))

    def tile_of(j, i):
        return jnp.where(odd(j) == 0, i, per_block - 1 - i)

    def kernel(ha_ref, hb_ref, w_ref, w2_ref, g1_ref, b1_ref, g2_ref, b2_ref, u_ref, s_ref, gbo_ref, gb2_ref, w2o_ref, ht_ref,
               w1, gbf, *sems):
        share, sems = Share(*sems[:4]), sems[4:]
        gs, gr, lsem = sems[:3]
        sems = sems[3:]
        j, i = pl.program_id(0), pl.program_id(1)
        step = j * per_block + i
        here = coords()
        y = here[0]
        one = Gather(lambda q, p: w_ref.at[at(p, depth // n), at(q, quarter)],
                     lambda m, q, p: w1.at[at(p, depth // n), at(m * 4 + q, quarter)], n, sems[:6])
        two = Gather(lambda q, p: w2_ref.at[at(q * n2 + p, quarter // n2)],
                     lambda m, q, p: w2o_ref.at[at(q * n2 + p, quarter // n2)], n2, sems[6:])

        def local(b):
            return pltpu.make_async_copy(w_ref.at[:, at(b, width)], w1.at[:, at(2 * y + b, width)], lsem.at[b])

        def bn_vectors(m):
            return remote(gbf.at[:, at(m, half)], gbf.at[:, at(m, half)], gs, gr, flip(here, Y_PEER))

        def begin():
            arrive()
            local(0).start()
            local(1).start()
            all_arrived()
            one.start()
            two.start()
            for r, (one_ref, two_ref) in enumerate(((g1_ref, g2_ref), (b1_ref, b2_ref))):
                row = pl.ds(r, 1)
                gbf[row, at(y, half)] = one_ref[...]
                gb2_ref[row] = two_ref[...]
            local(0).wait()

        def late_half():
            one.pass_x(0)
            one.pass_y(n - 1)
            one.wait_core(0)

        hooks = [(0, begin), (1, lambda: bn_vectors(y).start()), (per_block, lambda: local(1).wait()), (2 * per_block, late_half)]
        hooks += [(2 * p + 3, functools.partial(one.pass_y, p)) for p in range(n - 1)]
        hooks += [(p + 2 * per_block, functools.partial(one.pass_x, p)) for p in range(1, n)]
        hooks += [(3 * per_block, lambda: one.wait_core(1))]
        hooks += [(p + 9, functools.partial(two.pass_y, p)) for p in range(n2 - 1)]
        hooks += [(13 + (p + 1) // 2, functools.partial(two.pass_x, p)) for p in range(n2 // 2)]
        for s, hook in hooks:
            pl.when(step == s)(hook)
        for b in range(3):
            pl.when(step == (b + 1) * per_block)(lambda b=b: share.start(block(b)))

        tile_at = tile_of(j, i)
        first_view = tile_at < steps
        cols = at(j, width)
        ht_ref[...] = lax.select(first_view, ha_ref[:, cols], hb_ref[:, cols]).T
        for r in runs(tile, TM):
            u_ref[r] = mm(lax.select(first_view, ha_ref[r], hb_ref[r]), w1[:, at(block(j), width)])
        sums = jnp.concatenate([moments(u_ref, cols) for cols in runs(width, LANES)], axis=1)
        v = tile_at // steps
        share.acc[block(j), v] = jnp.where(i % steps == 0, 0.0, share.acc[block(j), v]) + sums

        @pl.when(step == 4 * per_block - 1)
        def _():
            share.start(block(3))
            two.pass_y(n2 - 1)
            for p in range(n2 // 2, n2):
                two.pass_x(p)
            bn_vectors(other(y)).wait_recv()
            bn_vectors(y).wait_send()
            gbo_ref[...] = gbf[...]
            for b in range(4):
                s_ref[:, :, b * width:(b + 1) * width] = share.total(b)
            one.drain()
            two.drain()
            two.wait_core(0)
            two.wait_core(1)

    return call(
        kernel, "fwd_first", 0, (4, per_block),
        [pl.BlockSpec((tile, depth), lambda j, i: (coords()[0] * steps + jnp.minimum(tile_of(j, i), steps - 1), 0)),
         pl.BlockSpec((tile, depth), lambda j, i: (coords()[0] * steps + jnp.maximum(tile_of(j, i) - steps, 0), 0)),
         ANY, ANY] + [whole(*t.shape) for t in vectors],
        [pl.BlockSpec((tile, width), lambda j, i: (tile_of(j, i), block(j))), whole(2, 2, dim),
         whole(2, dim), whole(2, dim), ANY, pl.BlockSpec((width, tile), lambda j, i: (j, tile_of(j, i)))],
        [sds((2 * rows, dim), F32), sds((2, 2, dim), F32), sds((2, dim), F32), sds((2, dim), F32),
         sds((half, dim), BF16), sds((depth, 2 * rows), BF16)],
        [pltpu.VMEM((depth, dim), BF16), pltpu.VMEM((2, dim), F32)] + Share.scratch(4, 2, 2, width)
        + [DMA, DMA, TWO_DMA] + Gather.scratch(n) + Gather.scratch(n2),
        4 * rows * depth * dim, 2 * rows * (8 * depth + 4 * dim), (h_a, h_b, w_one, w_two, *vectors))


def fwd_next(u, sums, gb, w_own, w_other, by_rows, total, cid, w_next=None):
    all_rows, depth = u.shape
    dim = w_own.shape[1] if by_rows else 2 * w_own.shape[1]
    half = dim // 2
    quarter = half // 4
    steps = all_rows // 2 // TM
    last = 2 * steps - 1
    slab = dim // (2 * steps)
    n = 4
    more = w_next is not None

    def kernel(u_ref, s_ref, gb_ref, wo_ref, wt_ref, *refs):
        if more:
            wn_ref, refs = refs[0], refs[1:]
        x_ref, o_ref, so_ref, wtr_ref, *refs = refs
        if more:
            wno_ref, *refs = refs
        w, act, acc, got, ssem, rsem, lsem, *refs = refs
        share = Share(acc, got, ssem, rsem)
        i = pl.program_id(0)
        y = coords()[0]

        def local(ref, model, b):
            where = at(model, half)
            return pltpu.make_async_copy(ref, w.at[where] if by_rows else w.at[:, where], lsem.at[b])

        if more:
            gather = Gather(lambda q, p: wn_ref.at[at(p, depth // n), at(q, quarter)],
                            lambda m, q, p: wno_ref.at[at(p, depth // n), at(q, quarter)], n, refs)

        @pl.when(i == 0)
        def _():
            arrive()
            acc[...] = jnp.zeros_like(acc)
            local(wo_ref, y, 0).start()
            local(wt_ref, other(y), 1).start()
            all_arrived()
            if more:
                gather.start()
            local(wo_ref, y, 0).wait()
            local(wt_ref, other(y), 1).wait()

        if more:
            for p in range(n):
                pl.when(i == p + 2)(lambda p=p: gather.pass_y(p))
                pl.when(i == p + 4)(lambda p=p: gather.pass_x(p))
        pl.when(i == steps)(lambda: share.start(0))

        mean, inv = mean_inv(s_ref[0], total)
        for k, cols in enumerate(runs(depth, LANES)):
            m, r, g, b = (t[:, k * LANES:(k + 1) * LANES] for t in (mean, inv, gb_ref[:1], gb_ref[1:]))
            for piece in runs(TM, PIECE):
                act[piece, cols] = jnp.maximum((u_ref[piece, cols] - m) * r * g + b, 0.0).astype(BF16)
        x_ref[...] = act[...].T
        wtr_ref[...] = w[:, at(i, slab)].T
        v = i // steps
        keep = jnp.where(i % steps == 0, 0.0, 1.0)
        for some in runs(dim, TM):
            o_ref[:, some] = mm(act[...], w[:, some])
            for cols in runs(TM, LANES):
                cols = pl.ds(some.start + cols.start, LANES)
                share.acc[v, :, cols] = keep * share.acc[v, :, cols] + moments(o_ref, cols)

        @pl.when(i == last)
        def _():
            share.start(1)
            for b in BOTH:
                so_ref[b] = share.total(b)
            if more:
                gather.drain()
                gather.wait_core(0)
                gather.wait_core(1)

    return call(
        kernel, "fwd_next", cid, (2 * steps,),
        [pl.BlockSpec((TM, depth), lambda i: (i, 0)), pl.BlockSpec((1, 2, depth), lambda i: (i // steps, 0, 0)),
         whole(2, depth), ANY, ANY] + [ANY] * more,
        [pl.BlockSpec((depth, TM), lambda i: (0, i)), pl.BlockSpec((TM, dim), lambda i: (i, 0)),
         whole(2, 2, dim), pl.BlockSpec((slab, depth), lambda i: (i, 0))] + [ANY] * more,
        [sds((depth, all_rows), BF16), sds((all_rows, dim), F32), sds((2, 2, dim), F32), sds((dim, depth), BF16)]
        + ([sds(w_next.shape, BF16)] if more else []),
        [pltpu.VMEM((depth, dim), BF16), pltpu.VMEM((TM, depth), BF16)] + Share.scratch(2, 2, dim) + [TWO_DMA] + (Gather.scratch(n) if more else []),
        2 * all_rows * depth * dim, all_rows * (6 * depth + 4 * dim),
        (u, sums, gb, w_own, w_other) + ((w_next,) if more else ()))


def corr_grad(z, sums, lam, total):
    all_rows, dim = z.shape
    rows = all_rows // 2
    half = dim // 2
    quart = half // 2
    n_chunk = 8
    width = half // n_chunk
    pair = 2 * width
    mt = TM
    zt = TM // 2
    ahead = 3
    lead = 3
    z_steps = all_rows // zt
    m_steps = rows // mt
    scale = 1.0 / total

    def kernel(z_ref, s_ref, lam_ref, zho_ref, d_ref, so_ref, lo_ref, zh, da, ck, r1, r2, g, stage, dsend, drecv, acc, got, ssem, rsem, loss_acc, loss_got, lsem, lrsem, zs, zos,
               d1s, d1r, s1s, s1r, s2s, s2r, a2s, a2r, a1s, a1r, ads, adr, dbs, das):
        share = Share(acc, got, ssem, rsem)
        share_loss = Share(loss_acc, loss_got, lsem, lrsem)
        here = coords()
        y, x, c = here
        on_x = c == 0
        by_core = lambda one, two: tuple(jnp.where(on_x, a, b) for a, b in zip(one, two))
        first = by_core(flip(here, X_PEER), flip(here, Y_PEER))
        second = by_core(flip(here, Y_PEER), flip(here, X_PEER))
        cpeer = flip(here, C_PEER)
        bit1, bit2 = by_core((x, y), (y, x))
        arrive()
        acc[...] = jnp.zeros_like(acc)
        loss_acc[...] = jnp.zeros_like(loss_acc)

        def load(i, slot):
            return pltpu.make_async_copy(z_ref.at[at(i, zt)], ck.at[at(slot, zt)], zs.at[slot])

        def zh_out(i):
            v, r = lax.div(i, n_chunk // 2), lax.rem(i, n_chunk // 2)
            return pltpu.make_async_copy(zh.at[v, at(r, TM)], zho_ref.at[v, at(r, TM)], zos.at[i])

        z_slots = half // zt
        for i in range(ahead):
            load(i, i).start()

        def normalise(i):
            slot = lax.rem(i, z_slots)
            v, r = lax.div(i, z_steps // 2), lax.rem(i, z_steps // 2)
            pl.when(i + ahead < z_steps)(lambda: load(i + ahead, lax.rem(i + ahead, z_slots)).start())
            load(i, slot).wait()
            mean, inv = mean_inv(s_ref[v], total)
            for k, cols in enumerate(runs(dim, LANES)):
                m, s = (t[:, k * LANES:(k + 1) * LANES] for t in (mean, inv))
                for p in range(zt // PIECE):
                    zh[v, at(r * (zt // PIECE) + p, PIECE), cols] = (
                        (ck[at(slot * (zt // PIECE) + p, PIECE), cols] - m) * s).astype(BF16)
            da[at(i, rows // z_steps)] = jnp.zeros((rows // z_steps, dim), F32)

        loop(z_steps, normalise)
        all_arrived()

        def both(v, rows_at, t):
            return jnp.concatenate([zh[v, rows_at, at(b * n_chunk + t, width)] for b in BOTH], axis=1)

        group = lambda t, b: at(2 * t + b, width)

        def to_core(t):
            return remote(dsend.at[odd(t)], drecv.at[odd(t)], d1s.at[t], d1r.at[t], cpeer)

        def to_first(t):
            return remote(ck.at[:, group(t, other(bit1))], r1.at[t], s1s.at[t], s1r.at[t], first)

        def to_second(t):
            return remote(ck.at[at(other(bit2), quart), group(t, bit1)], r2.at[t], s2s.at[t], s2r.at[t], second)

        def g_second(t, b):
            block = g.at[t, at(2 * c + b, quart), at(bit1, width)]
            return remote(block, block, a2s.at[t], a2r.at[t], second)

        def g_first(t, b):
            block = g.at[t, at(c, half), at(b, width)]
            return remote(block, block, a1s.at[t], a1r.at[t], first)

        def g_core(t, core):
            block = g.at[t, at(core, half)]
            return remote(block, block, ads.at[t], adr.at[t], cpeer)

        def chip_sum(t):
            to_core(t).wait_recv()
            to_core(t).wait_send()
            ck[:, at(t, pair)] += drecv[odd(t)]
            to_first(t).start()

        def corr_part(t):
            zh_out(t).start()
            right = both(1, pl.ds(0, rows), t)
            dsend[odd(t)] = mm_at(zh[0, :, at(other(c), half)], right)
            ck[:, at(t, pair)] = mm_at(zh[0, :, at(c, half)], right)
            to_core(t).start()

        def db_out(t, m, slot, b):
            return pltpu.make_async_copy(
                stage.at[slot, :, at(b, width)], d_ref.at[1, at(m, mt), at(b * n_chunk + t, width)], dbs.at[slot, b])

        def da_out(m):
            return pltpu.make_async_copy(da.at[at(m, mt)], d_ref.at[0, at(m, mt)], das.at[m])

        def finish(m):
            def scaled(cols):
                for p in range(mt // PIECE):
                    some = at(m * (mt // PIECE) + p, PIECE)
                    d = da[some, cols] * scale
                    da[some, cols] = d
                    yield d, d * zh[0, some, cols].astype(F32)

            for cols in runs(dim, LANES):
                acc[0, :, cols] += two_sums(scaled(cols))
            da_out(m).start()

        def grads(t):
            def rows_of(m):
                slot = odd(m)

                @pl.when(t * m_steps + m >= 2)
                def _():
                    for b in BOTH:
                        db_out(t, m, slot, b).wait()

                own = both(1, at(m, mt), t)
                stage[slot] = mm(zh[0, at(m, mt)], g[t]) * scale
                sums = two_sums((stage[slot, r], stage[slot, r] * both(1, at(m * (mt // PIECE) + p, PIECE), t).astype(F32))
                                for p, r in enumerate(runs(mt, PIECE)))
                for b in BOTH:
                    acc[1, :, at(b * n_chunk + t, width)] += sums[:, b * width:(b + 1) * width]
                    db_out(t, m, slot, b).start()
                for cols in runs(dim, LANES):
                    da[at(m, mt), cols] += mm_bt(own, g[t, cols])
                pl.when(t == n_chunk - 1)(lambda: finish(m))

            loop(m_steps, rows_of)

        def at_first(t):
            to_first(t).wait_recv()
            ck[:, group(t, bit1)] += r1[t]
            to_second(t).start()

        def at_second(t):
            to_second(t).wait_recv()
            corr_mat = (ck[at(bit2, quart), group(t, bit1)] + r2[t]) * scale
            row_ids = (2 * c + bit2) * quart + lax.broadcasted_iota(jnp.int32, (quart, width), 0)
            col_ids = (bit1 * n_chunk + t) * width + lax.broadcasted_iota(jnp.int32, (quart, width), 1)
            is_diag = row_ids == col_ids
            lam_val = lam_ref[0]
            loss = jnp.where(is_diag, (1.0 - corr_mat) * (1.0 - corr_mat), lam_val * corr_mat * corr_mat)
            loss_acc[0] += jnp.sum(loss, axis=0, keepdims=True)
            pl.when(t == n_chunk - 1)(lambda: share_loss.start(0))
            grad = jnp.where(is_diag, -2.0 * (1.0 - corr_mat), 2.0 * lam_val * corr_mat).astype(BF16)
            g[t, at(2 * c + bit2, quart), at(bit1, width)] = grad
            g_second(t, bit2).start()

        def back_second(t):
            g_second(t, other(bit2)).wait_recv()
            g_first(t, bit1).start()

        def back_first(t):
            g_first(t, other(bit1)).wait_recv()
            g_core(t, c).start()

        def back_core(t):
            g_core(t, other(c)).wait_recv()
            grads(t)

        def advance(tau):
            for lag, stage_fn in ((lead, at_first), (lead + 1, back_second), (lead + 2, back_first), (lead + 3, back_core),
                                  (lead, at_second), (1, chip_sum), (0, corr_part)):
                t = tau - lag
                pl.when(jnp.logical_and(t >= 0, t < n_chunk))(lambda t=t, stage_fn=stage_fn: stage_fn(t))

        loop(n_chunk + lead + 3, advance)
        share.start(1)
        share.start(0)
        for t in range(n_chunk):
            for copy in (to_first(t), to_second(t), g_second(t, bit2), g_first(t, bit1), g_core(t, c)):
                copy.wait_send()
        for b in BOTH:
            so_ref[b] = share.total(b)
            for slot in BOTH:
                db_out(0, 0, slot, b).wait()
        lo_ref[...] = share_loss.total(0)
        for i in range(n_chunk):
            zh_out(i).wait()
        for m in range(m_steps):
            da_out(m).wait()

    return call(
        kernel, "corr_grad", 3, (), [ANY, VMEM, pl.BlockSpec(memory_space=pltpu.SMEM)], [ANY, ANY, VMEM, VMEM],
        [sds((2, rows, dim), BF16), sds((2, rows, dim), F32), sds((2, 2, dim), F32), sds((1, width), F32)],
        [pltpu.VMEM((2, rows, dim), BF16), pltpu.VMEM((rows, dim), F32), pltpu.VMEM((half, dim), F32),
         pltpu.VMEM((n_chunk, half, width), F32), pltpu.VMEM((n_chunk, quart, width), F32),
         pltpu.VMEM((n_chunk, dim, pair), BF16), pltpu.VMEM((2, mt, pair), F32)]
        + [pltpu.VMEM((2, half, pair), F32)] * 2 + Share.scratch(2, 2, dim) + Share.scratch(1, 1, width)
        + [DMA((half // zt,)), DMA((n_chunk,))] + [DMA((n_chunk,))] * 12 + [DMA((2, 2)), DMA((m_steps,))],
        all_rows * dim * dim * 3, all_rows * dim * 12, (z, sums, lam))


def backward(d_emb, zh, sz, s_emb, layers, x2_t, total):
    all_rows, dim = zh.shape
    rows, half = all_rows // 2, dim // 2
    width = 256
    slabs = dim // width
    items = 2 * slabs
    piece = width
    side = half // 2 // piece
    per_slab = half // piece
    n_layer = len(layers) + 1
    n_slab = n_layer * slabs
    per_layer = slabs * side
    n_chunk = n_layer * per_layer
    ahead = 3
    (u2, s2, gb2, w3_t, x1_t), (u1, s1, gb1, w2_t, h_t) = layers

    def kernel(d_ref, zh_ref, sz_ref, sd_ref, x2_ref, x1_ref, h_ref, u2_ref, u1_ref, w3_ref, w2_ref,
               s2_ref, s1_ref, gb2_ref, gb1_ref, dw3_ref, dw2_ref, dw1_ref, sum_ref, dy_ref, part_ref, ry_ref, rx_ref,
               dbuf, xbuf, d0, d1, wbuf, ubuf, dybuf, dyout, psend, pkeep, dr, ebuf, mbuf, fbuf, acc, got, ssem, rsem,
               us, ws, ds, dos, xl, ps, pr, pm, ys, yr, xs, xr, es, fs, fcs, fcr, credit):
        share = Share(acc, got, ssem, rsem)
        here = coords()
        y, x, c = here
        ypeer, xpeer, cpeer = flip(here, Y_PEER), flip(here, X_PEER), flip(here, C_PEER)
        arrive()

        def column(k, n):
            model = odd(n + jnp.where(k == 0, other(y), 0))
            return jnp.where(k == 1, n, model * (slabs // 2) + lax.div(n, 2))

        def turn(k):
            return jnp.where(k == 0, 0, other(y))

        def m_slot(j):
            return lax.rem(j, 4)

        def copy(src, dst, sem):
            return pltpu.make_async_copy(src, dst, sem)

        def sent_by(q):
            first = jnp.minimum(per_slab * lax.div(q, 4), per_layer)
            middle = jnp.clip(side * lax.div(q - 2 * items - 2, 2), 0, per_layer)
            last = jnp.clip(per_slab * lax.div(q - 4 * items - 2, 4), 0, per_layer)
            return first + middle + last

        def begun(q):
            return jnp.maximum(lax.div(q - 6, 2), 0)

        def to_core(s):
            return remote(psend.at[odd(s)], dr.at[odd(s)], ps.at[s], pr.at[s], cpeer)

        def keep_out(s):
            return copy(pkeep.at[odd(s)], part_ref.at[s], pm)

        def chip_sum(s):
            to_core(s).wait_recv()
            pkeep[odd(s)] += dr[odd(s)]

            @pl.when(s + 2 < n_slab)
            def _():
                pl.semaphore_signal(credit, inc=1, device_id=device(cpeer), device_id_type=pl.DeviceIdType.MESH)

            to_core(s).wait_send()
            keep_out(s).start()

        def home(j, own):
            k = lax.div(j, per_layer)
            i = lax.rem(j, per_layer)
            model = y if own else other(y)
            turned = other(turn(k)) if own else turn(k)
            s = jnp.where(k == 1, lax.div(i, side), 2 * lax.div(i, per_slab) + turned)
            place = jnp.where(k == 1, model * side + lax.rem(i, side), lax.rem(i, per_slab))
            return part_ref.at[k * slabs + s, at(place, piece)]

        def to_y(j):
            return remote(home(j, False), ry_ref.at[j], ys.at[lax.div(j, per_layer)], yr.at[j], ypeer)

        def issue(s, q):
            keep_out(s).wait()
            k, n = lax.div(s, slabs), lax.rem(s, slabs)
            for mine, fire, first, count in (
                    (k == 1, True, n * side, side), (k != 1, odd(n) == jnp.where(k == 0, 0, 1), lax.div(n, 2) * per_slab, per_slab)):
                for r in range(count):
                    j = k * per_layer + first + r
                    pl.when(mine & fire & (j < begun(q) + ahead))(lambda j=j: to_y(j).start())

        def to_x(j):
            return remote(mbuf.at[m_slot(j)], rx_ref.at[j], xs.at[m_slot(j)], xr.at[j], xpeer)

        def result(j, k):
            i = lax.rem(j, per_layer)
            if k == 1:
                return dw2_ref.at[at(c * side + lax.rem(i, side), piece), at(lax.div(i, side), width)]
            return (dw1_ref if k else dw3_ref).at[at(c * per_slab + lax.rem(i, per_slab), piece), at(lax.div(i, per_slab), width)]

        def put(j, k):
            slot = odd(j)
            return (copy(fbuf.at[slot], result(j, k), fs.at[slot]),
                    remote(fbuf.at[slot], result(j, k), fcs.at[slot], fcr.at[k], cpeer))

        def put_done(j):
            here_copy, there_copy = put(j, 0)
            here_copy.wait()
            there_copy.wait_send()

        def load_part(j, which):
            src = (lambda: ry_ref.at[j], lambda: home(j, True), lambda: rx_ref.at[j])[which]()
            return copy(src, ebuf.at[which], es.at[which])

        def fetch_x(j):
            to_x(j).wait_recv()
            load_part(j, 2).start()

        def begin(j, q):
            remote(ry_ref.at[j], ry_ref.at[j], ys.at[0], yr.at[j], ypeer).wait_recv()
            load_part(j, 0).start()
            load_part(j, 1).start()
            pl.when(j + ahead < sent_by(q))(lambda: to_y(j + ahead).start())
            pl.when(j >= 2)(lambda: fetch_x(j - 2))

        def deliver(j):
            load_part(j, 2).wait()
            pl.when(j >= 2)(lambda: put_done(j))
            fbuf[odd(j)] = mbuf[m_slot(j)] + ebuf[2]
            for k in range(n_layer):
                @pl.when(lax.div(j, per_layer) == k)
                def _(k=k):
                    for one in put(j, k):
                        one.start()

        def end(j):
            load_part(j, 0).wait()
            load_part(j, 1).wait()
            pl.when(j >= 4)(lambda: to_x(j).wait_send())
            mbuf[m_slot(j)] = ebuf[0] + ebuf[1]
            to_x(j).start()
            pl.when(j >= 2)(lambda: deliver(j - 2))

        def events(q):
            now, before, earlier = begun(q), begun(q - 1), begun(q - 2)
            pl.when(before > earlier)(lambda: end(before - 1))
            pl.when(now > before)(lambda: begin(now - 1, q))

        def weight_slab(k, n, v, d):
            slot = odd(k * slabs + n)
            for buf, part in ((psend, other(c)), (pkeep, c)):
                first = jnp.where(k == 1, part, 2 * part)
                for b in BOTH:
                    left = xbuf[at(first + b * jnp.where(k == 1, 2, 1), half // 2), pl.ds(v * rows, rows)]
                    here_at = at(b, half // 2)
                    prod = mm(left, d)
                    buf[slot, here_at] = buf[slot, here_at] + prod if v else prod

        def after(k, n, v, q):
            s = k * slabs + n
            if v == 0:
                pl.when(n > 0)(lambda: chip_sum(s - 1))
            else:
                pl.when(s >= 2)(lambda: pl.semaphore_wait(credit, 1))
                to_core(s).start()
                pl.when(n > 0)(lambda: issue(s - 1, q))

        def dw_pass(k, q, ready, fetch, pre, ahead_of_next):
            ready(0)
            fetch(1)
            pre(d0, 0, 0)

            def slab(n):
                for v, d_ref, d_next in ((0, d0, d1), (1, d1, d0)):
                    i = 2 * n + v
                    pl.when(i + 1 < items)(lambda: ready(i + 1))
                    pl.when(i + 2 < items)(lambda: fetch(i + 2))
                    pl.when(n == 0)(lambda: x_load(x2_ref, v).wait())
                    if v:
                        pl.when(n == slabs - 1)(ahead_of_next)
                    events(q + i)
                    for r in runs(rows, TM):
                        dbuf[pl.ds(v * rows + r.start, TM), at(column(k, n), width)] = d_ref[r]
                    weight_slab(k, n, v, d_ref[...])
                    pre(d_next, jnp.minimum(n + v, slabs - 1), other(v))
                    after(k, n, v, q + i)

            loop(slabs, slab)

        def emb_loads(i):
            n, v = split(i)
            cols = at(column(0, n), width)
            return (copy(d_ref.at[at(v, rows), cols], ubuf.at[v], us.at[v]),
                    copy(zh_ref.at[at(v, rows), cols], wbuf.at[v], ws.at[v]))

        def emb_fetch(i):
            for one in emb_loads(i):
                one.start()

        def emb_ready(i):
            for one in emb_loads(i):
                one.wait()

        def emb_pre(d_out, n, v):
            cols = at(column(0, n), width)
            _, inv = mean_inv(sz_ref[v, :, cols], total)
            sd = sd_ref[v, :, cols] / total
            for r in runs(rows, PIECE):
                d_out[r] = (inv * (ubuf[v, r] - sd[:1] - wbuf[v, r].astype(F32) * sd[1:])).astype(BF16)

        def x_load(src, v, rows_at=pl.ds(0, dim)):
            return copy(src.at[rows_at, at(v, rows)], xbuf.at[rows_at, at(v, rows)], xl.at[v])

        def u_slot(layer, v):
            return jnp.where(layer == 0, other(v), v)

        def slab_of(ref, layer, i, buf, sem, slot):
            n, v = split(i)
            return copy(ref.at[at(v, rows), at(column(layer + 1, n), width)], buf.at[slot], sem.at[slot])

        def u_load(layer, i, ref=u2_ref):
            return slab_of(ref, layer, i, ubuf, us, u_slot(layer, odd(i)))

        def dy_load(layer, i):
            return slab_of(dy_ref, layer, i, dybuf, ds, odd(i))

        def dy_out(layer, i):
            n, v = split(i)
            return copy(dyout.at[v], dy_ref.at[at(v, rows), at(column(layer + 1, n), width)], dos.at[v])

        def w_load(layer, n, ref=w3_ref):
            slot = odd(n + 1)
            return copy(ref.at[:, at(column(layer + 1, n), width)], wbuf.at[slot], ws.at[slot])

        def by_layer(layer, make, refs):
            for k, ref in enumerate(refs):
                pl.when(layer == k)(lambda ref=ref: make(ref).start())

        def start_u(layer, i):
            by_layer(layer, lambda ref: u_load(layer, i, ref), (u2_ref, u1_ref))

        def start_w(layer, n):
            by_layer(layer, lambda ref: w_load(layer, n, ref), (w3_ref, w2_ref))

        def next_layer(layer):
            start_u(layer, 0)
            start_w(layer, 0)

        for one in (x_load(x2_ref, 0), *emb_loads(0), x_load(x2_ref, 1)):
            one.start()
        all_arrived()
        dw_pass(0, 0, emb_ready, emb_fetch, emb_pre, lambda: next_layer(0))

        def stats(layer, v, cols):
            pick = lambda one, two: jnp.where(layer == 0, one, two)
            mean, inv = mean_inv(pick(s2_ref[v, :, cols], s1_ref[v, :, cols]), total)
            gb = pick(gb2_ref[:, cols], gb1_ref[:, cols])
            return mean, inv, gb[:1], gb[1:]

        def bn_layer(layer):
            start = (2 * layer + 1) * items

            def dx_item(i):
                n, v = split(i)
                slot = u_slot(layer, v)
                cols = at(column(layer + 1, n), width)

                @pl.when(i + 1 < items)
                def _():
                    start_u(layer, i + 1)
                    pl.when((v == 0) & (n + 1 < slabs))(lambda: start_w(layer, n + 1))

                @pl.when(i + 1 == items)
                def _():
                    start_u(layer, 0)
                    dy_load(layer, 0).start()

                u_load(layer, i).wait()
                pl.when(v == 0)(lambda: w_load(layer, n).wait())
                events(start + i)
                pl.when((i > 2) & (i < 11))(lambda: by_layer(
                    layer, lambda ref: x_load(ref, v, at(lax.div(i - 3, 2), half // 2)), (x1_ref, h_ref)))
                pl.when(n > 0)(lambda: dy_out(layer, i).wait())
                mean, inv, gamma, beta = stats(layer, v, cols)

                def pieces():
                    for b in range(rows // TM):
                        dx = mm(dbuf[at(v * (rows // TM) + b, TM)], wbuf[odd(n + 1)])
                        for p in range(0, TM, PIECE):
                            some = pl.ds(b * TM + p, PIECE)
                            norm = (ubuf[slot, some] - mean) * inv
                            dy = jnp.where(norm * gamma + beta > 0, dx[p:p + PIECE], 0.0)
                            dyout[v, some] = dy
                            yield dy, dy * norm

                g = layer * items + i
                acc[g] = two_sums(pieces())
                dy_out(layer, i).start()
                share.start(g)
                before = (layer + 1) * slabs - 1
                pl.when(i == 0)(lambda: chip_sum(before))
                pl.when(i == 1)(lambda: issue(before, start + i))

            def fetch(i):
                start_u(layer, i)
                dy_load(layer, i).start()

            def ready(i):
                n, v = split(i)
                u_load(layer, i).wait()
                dy_load(layer, i).wait()
                sum_ref[layer, v, :, at(column(layer + 1, n), width)] = share.total(layer * items + i)

            def pre(d_out, n, v):
                cols = at(column(layer + 1, n), width)
                tot = sum_ref[layer, v, :, cols] / total
                mean, inv, gamma, _ = stats(layer, v, cols)
                slope, front, slot = inv * tot[1:], gamma * inv, u_slot(layer, v)
                for r in runs(rows, PIECE):
                    d_out[r] = (front * (dybuf[v, r] - (tot[:1] + (ubuf[slot, r] - mean) * slope))).astype(BF16)

            loop(items, dx_item)
            for v in BOTH:
                dy_out(layer, v).wait()
            dw_pass(layer + 1, start + items, ready, fetch, pre, lambda: pl.when(layer == 0)(lambda: next_layer(1)))

        loop(len(layers), bn_layer)

        ticks = (2 * n_layer - 1) * items
        chip_sum(n_slab - 1)
        issue(n_slab - 1, ticks)
        ended = 36

        def tail(j):
            begin(j, ticks + 2)
            end(j)

        loop(n_chunk, tail, ended)
        for j in range(n_chunk - 2, n_chunk):
            fetch_x(j)
            deliver(j)
        for j in BOTH:
            put_done(j)
        for k in range(n_layer):
            theirs = dw2_ref.at[at(other(c), half // 2)] if k == 1 else (dw1_ref if k else dw3_ref).at[at(other(c), half)]
            remote(theirs, theirs, fcs.at[0], fcr.at[k], cpeer).wait_recv()
            sent = ry_ref.at[at(k, per_layer)]
            remote(sent, sent, ys.at[k], yr.at[0], ypeer).wait_send()
        for j in range(n_chunk - 4, n_chunk):
            to_x(j).wait_send()

    n_item = len(layers) * items
    vm = lambda *shape: pltpu.VMEM(shape, F32)
    bf = lambda *shape: pltpu.VMEM(shape, BF16)
    return call(
        kernel, "backward", 4, (),
        [ANY, ANY, VMEM, VMEM] + [ANY] * 7 + [VMEM] * 4, [ANY] * 3 + [VMEM] + [ANY] * 4,
        [sds((dim, half), F32), sds((half, dim), F32), sds((dim, half), F32), sds((len(layers), 2, 2, dim), F32),
         sds((all_rows, dim), F32), sds((n_slab, half, width), F32), sds((n_chunk, piece, width), F32),
         sds((n_chunk, piece, width), F32)],
        [bf(all_rows, dim), bf(dim, all_rows), bf(rows, width), bf(rows, width), bf(2, dim, width),
         vm(2, rows, width), vm(2, rows, width), vm(2, rows, width),
         vm(2, half, width), vm(2, half, width), vm(2, half, width), vm(3, piece, width), vm(4, piece, width),
         vm(2, piece, width)] + Share.scratch(n_item, 2, width)
        + [TWO_DMA, TWO_DMA, TWO_DMA, TWO_DMA, TWO_DMA, DMA((n_slab,)), DMA((n_slab,)), DMA, DMA((n_layer,)),
           DMA((n_chunk,)), DMA((4,)), DMA((n_chunk,)), DMA((3,)), TWO_DMA, TWO_DMA, DMA((n_layer,)),
           pltpu.SemaphoreType.REGULAR],
        all_rows * dim * dim * 10, all_rows * dim * 40,
        (d_emb, zh, sz, s_emb, x2_t, x1_t, h_t, u2, u1, w3_t, w2_t, s2, s1, gb2, gb1))


def settle(*grads):
    steps = 16

    def kernel(*refs):
        for src, dst in zip(refs[:len(grads)], refs[len(grads):]):
            dst[...] = src[...]

    specs = [pl.BlockSpec((g.shape[0] // steps, g.shape[1]), lambda i: (i, 0)) for g in grads]
    return call(kernel, "settle", None, (steps,), specs, specs, [sds(g.shape, F32) for g in grads], [], 0,
                len(grads) * grads[0].size * 8, grads)


def solution(mesh):
    def shard_body(h_a, h_b, w_one, w_two, w_three, g_one, b_one, g_two, b_two, lam_off):
        y = lax.axis_index('model')
        total = float(h_a.shape[0] * mesh.shape['data'])
        dim, half = w_three.shape
        rowed = [t.reshape(1, -1) for t in (g_one, b_one, g_two, b_two)]
        u1, s1, gb1, gb2, w_two_o, h_t = fwd_first(h_a, h_b, w_one, w_two, *rowed)
        x1_t, u2, s2, w2_t, w_three_o = fwd_next(u1, s1, gb1, w_two, w_two_o, True, total, 1, w_three)
        x2_t, z, sz, w3_t = fwd_next(u2, s2, gb2, w_three, w_three_o, False, total, 2)
        zh, d_emb, s_emb, loss = corr_grad(z, sz, lam_off, total)
        loss = jnp.sum(loss)
        dw_three, dw_two, dw_one, sums, *_ = backward(
            d_emb.reshape(z.shape), zh.reshape(z.shape), sz, s_emb,
            ((u2, s2, gb2, w3_t, x1_t), (u1, s1, gb1, w2_t, h_t)), x2_t, total)
        dw_three, dw_two, dw_one = settle(dw_three, dw_two, dw_one)
        sums = jnp.sum(sums, axis=1)
        sum2 = sums[0]
        sum1 = lax.dynamic_slice_in_dim(sums[1], y * half, half, 1)
        return loss.reshape(1), dw_one, dw_two, dw_three, sum1[1], sum1[0], sum2[1], sum2[0]

    in_specs = (P('data', None), P('data', None), P(None, 'model'), P('model', None), P(None, 'model'),
                P('model'), P('model'), P(), P(), P())
    out_specs = (P(), P(None, 'model'), P('model', None), P(None, 'model'), P('model'), P('model'), P(), P())
    return jax.shard_map(shard_body, mesh=mesh, in_specs=in_specs, out_specs=out_specs, check_vma=False)
```

```python
import functools

import jax
import jax.numpy as jnp
from jax import lax
from jax.experimental import pallas as pl
from jax.experimental.pallas import tpu as pltpu
from jax.sharding import PartitionSpec as P

BN_EPS = 1e-5
F32 = jnp.float32
BF16 = jnp.bfloat16
PIECE = 64
LANES = 256
SUBLANES = 8
TM = 512
MAX_VMEM = 67043328
ANY = pl.BlockSpec(memory_space=pl.ANY)
VMEM = pl.BlockSpec(memory_space=pltpu.VMEM)
DMA = pltpu.SemaphoreType.DMA
TWO_DMA = DMA((2,))
BOTH = (0, 1)
PEERS = [(ky, kx, kc) for ky in BOTH for kx in BOTH for kc in BOTH][1:]
C_PEER, X_PEER, Y_PEER = PEERS[0], PEERS[1], PEERS[3]
N_DEV = len(PEERS) + 1


def mm(left, right):
    return jnp.dot(left, right, preferred_element_type=F32)


def mm_bt(left, right):
    return lax.dot_general(left, right, (((1,), (1,)), ((), ())), preferred_element_type=F32)


def mm_at(left, right):
    return lax.dot_general(left, right, (((0,), (0,)), ((), ())), preferred_element_type=F32)


def other(p):
    return 1 - p


def odd(i):
    return lax.rem(i, 2)


def split(i):
    return lax.div(i, 2), odd(i)


def loop(n, body, start=0):
    def one(i, carry):
        body(i)
        return carry

    lax.fori_loop(start, n, one, 0)


def whole(*shape):
    return pl.BlockSpec(shape, lambda *_: (0,) * len(shape))


def at(i, n):
    return pl.ds(pl.multiple_of(i * n, n), n)


def sds(shape, dtype):
    return jax.ShapeDtypeStruct(shape, dtype)


def mean_inv(sums, total):
    mean = sums[:1] / total
    var = sums[1:2] / total - mean * mean
    return mean, lax.rsqrt(var + BN_EPS)


def fold(v):
    return jnp.sum(v.reshape(-1, SUBLANES, v.shape[1]), axis=0)


def runs(n, size):
    return [pl.ds(r, size) for r in range(0, n, size)]


def two_sums(pairs):
    one = two = 0.0
    for a, b in pairs:
        one, two = one + fold(a), two + fold(b)
    return jnp.concatenate([jnp.sum(t, axis=0, keepdims=True) for t in (one, two)], axis=0)


def moments(ref, cols):
    pieces = (ref[r, cols] for r in runs(ref.shape[0], PIECE))
    return two_sums((u, u * u) for u in pieces)


def coords():
    y, d = lax.axis_index('model'), lax.axis_index('data')
    return y, lax.div(d, 2), odd(d)


def flip(here, which):
    return tuple(other(p) if f else p for p, f in zip(here, which))


def flat(here):
    y, x, c = here
    return 4 * y + 2 * x + c


def device(here):
    y, x, c = here
    return (y, 2 * x + c)


def remote(src, dst, send_sem, recv_sem, there):
    return pltpu.make_async_remote_copy(
        src_ref=src, dst_ref=dst, send_sem=send_sem, recv_sem=recv_sem, device_id=device(there),
        device_id_type=pl.DeviceIdType.MESH)


def arrive():
    here = coords()
    for k in PEERS:
        pl.semaphore_signal(pltpu.get_barrier_semaphore(), inc=1, device_id=device(flip(here, k)),
                            device_id_type=pl.DeviceIdType.MESH)


def all_arrived():
    pl.semaphore_wait(pltpu.get_barrier_semaphore(), len(PEERS))


class Share:
    def __init__(self, acc, got, send_sem, recv_sem):
        self.acc, self.got, self.send_sem, self.recv_sem = acc, got, send_sem, recv_sem

    @staticmethod
    def scratch(n, *shape):
        return [pltpu.VMEM((n, *shape), F32), pltpu.VMEM((n, N_DEV, *shape), F32), DMA((n,)), DMA((n,))]

    def start(self, b):
        here = coords()
        me = flat(here)
        self.got[b, me] = self.acc[b]
        for which in PEERS:
            remote(self.acc.at[b], self.got.at[b, me], self.send_sem.at[b], self.recv_sem.at[b],
                   flip(here, which)).start()

    def total(self, b):
        all_of = self.got.at[b, pl.ds(0, len(PEERS))]
        copies = remote(all_of, all_of, self.send_sem.at[b], self.recv_sem.at[b], coords())
        copies.wait_send()
        copies.wait_recv()
        out = self.got[b, 0]
        for f in range(1, N_DEV):
            out += self.got[b, f]
        return out


class Gather:
    def __init__(self, own, dest, n, sems):
        self.own, self.dest, self.n = own, dest, n
        self.ys, self.yr, self.xs, self.xr, self.cs, self.cr = sems
        self.here = coords()
        _, x, c = self.here
        self.mine, self.across = 2 * x + c, 2 * (other(x)) + c
        self.core = (2 * x + other(c), 2 * (other(x)) + other(c))

    @staticmethod
    def scratch(n):
        return [DMA((n,))] * 4 + [DMA((2, n))] * 2

    def y(self, p):
        model = self.here[0]
        return remote(self.own(self.mine, p), self.dest(model, self.mine, p), self.ys.at[p], self.yr.at[p],
                      flip(self.here, Y_PEER))

    def moved(self, q, p, send_sem, recv_sem, which):
        ref = self.dest(1 - self.here[0], q, p)
        return remote(ref, ref, send_sem, recv_sem, flip(self.here, which))

    def x(self, p, q):
        return self.moved(q, p, self.xs.at[p], self.xr.at[p], X_PEER)

    def c(self, p, late, q):
        return self.moved(q, p, self.cs.at[late, p], self.cr.at[late, p], C_PEER)

    def start(self):
        for p in range(self.n):
            self.y(p).start()

    def pass_y(self, p):
        self.moved(self.mine, p, self.ys.at[p], self.yr.at[p], Y_PEER).wait_recv()
        self.x(p, self.mine).start()
        self.c(p, 0, self.mine).start()

    def pass_x(self, p):
        self.x(p, self.across).wait_recv()
        self.c(p, 1, self.across).start()

    def wait_core(self, late):
        for p in range(self.n):
            self.c(p, late, self.core[late]).wait_recv()

    def drain(self):
        for p in range(self.n):
            self.y(p).wait_send()
            self.x(p, self.mine).wait_send()
            self.c(p, 0, self.mine).wait_send()
            self.c(p, 1, self.across).wait_send()


def call(kernel, name, cid, grid, in_specs, out_specs, out_shape, scratch, flops, nbytes, args):
    return pl.pallas_call(
        kernel, name=name, grid=grid, in_specs=in_specs, out_specs=out_specs, out_shape=out_shape, scratch_shapes=scratch,
        compiler_params=pltpu.CompilerParams(vmem_limit_bytes=MAX_VMEM, collective_id=cid, has_side_effects=cid is not None),
        cost_estimate=pl.CostEstimate(flops=flops, bytes_accessed=nbytes, transcendentals=0))(*args)


def fwd_first(h_a, h_b, w_one, w_two, *vectors):
    depth, half = w_one.shape
    dim = 2 * half
    rows = h_a.shape[0] // 2
    tile, width, quarter = 2 * TM, half // 2, half // 4
    steps = rows // tile
    per_block = 2 * steps
    n, n2 = 4, 8

    def block(j):
        y, x, _ = coords()
        return jnp.where(j < 2, 2 * y + j, 2 * (other(y)) + jnp.where(j == 2, x, other(x)))

    def tile_of(j, i):
        return jnp.where(odd(j) == 0, i, per_block - 1 - i)

    def kernel(ha_ref, hb_ref, w_ref, w2_ref, g1_ref, b1_ref, g2_ref, b2_ref, u_ref, s_ref, gbo_ref, gb2_ref, w2o_ref, ht_ref,
               w1, gbf, *sems):
        share, sems = Share(*sems[:4]), sems[4:]
        gs, gr, lsem = sems[:3]
        sems = sems[3:]
        j, i = pl.program_id(0), pl.program_id(1)
        step = j * per_block + i
        here = coords()
        y = here[0]
        one = Gather(lambda q, p: w_ref.at[at(p, depth // n), at(q, quarter)],
                     lambda m, q, p: w1.at[at(p, depth // n), at(m * 4 + q, quarter)], n, sems[:6])
        two = Gather(lambda q, p: w2_ref.at[at(q * n2 + p, quarter // n2)],
                     lambda m, q, p: w2o_ref.at[at(q * n2 + p, quarter // n2)], n2, sems[6:])

        def local(b):
            return pltpu.make_async_copy(w_ref.at[:, at(b, width)], w1.at[:, at(2 * y + b, width)], lsem.at[b])

        def bn_vectors(m):
            return remote(gbf.at[:, at(m, half)], gbf.at[:, at(m, half)], gs, gr, flip(here, Y_PEER))

        def begin():
            arrive()
            local(0).start()
            local(1).start()
            all_arrived()
            one.start()
            two.start()
            for r, (one_ref, two_ref) in enumerate(((g1_ref, g2_ref), (b1_ref, b2_ref))):
                row = pl.ds(r, 1)
                gbf[row, at(y, half)] = one_ref[...]
                gb2_ref[row] = two_ref[...]
            local(0).wait()

        def late_half():
            one.pass_x(0)
            one.pass_y(n - 1)
            one.wait_core(0)

        hooks = [(0, begin), (1, lambda: bn_vectors(y).start()), (per_block, lambda: local(1).wait()), (2 * per_block, late_half)]
        hooks += [(2 * p + 3, functools.partial(one.pass_y, p)) for p in range(n - 1)]
        hooks += [(p + 2 * per_block, functools.partial(one.pass_x, p)) for p in range(1, n)]
        hooks += [(3 * per_block, lambda: one.wait_core(1))]
        hooks += [(p + 9, functools.partial(two.pass_y, p)) for p in range(n2 - 1)]
        hooks += [(13 + (p + 1) // 2, functools.partial(two.pass_x, p)) for p in range(n2 // 2)]
        for s, hook in hooks:
            pl.when(step == s)(hook)
        for b in range(3):
            pl.when(step == (b + 1) * per_block)(lambda b=b: share.start(block(b)))

        tile_at = tile_of(j, i)
        first_view = tile_at < steps
        cols = at(j, width)
        ht_ref[...] = lax.select(first_view, ha_ref[:, cols], hb_ref[:, cols]).T
        for r in runs(tile, TM):
            u_ref[r] = mm(lax.select(first_view, ha_ref[r], hb_ref[r]), w1[:, at(block(j), width)])
        sums = jnp.concatenate([moments(u_ref, cols) for cols in runs(width, LANES)], axis=1)
        v = tile_at // steps
        share.acc[block(j), v] = jnp.where(i % steps == 0, 0.0, share.acc[block(j), v]) + sums

        @pl.when(step == 4 * per_block - 1)
        def _():
            share.start(block(3))
            two.pass_y(n2 - 1)
            for p in range(n2 // 2, n2):
                two.pass_x(p)
            bn_vectors(other(y)).wait_recv()
            bn_vectors(y).wait_send()
            gbo_ref[...] = gbf[...]
            for b in range(4):
                s_ref[:, :, b * width:(b + 1) * width] = share.total(b)
            one.drain()
            two.drain()
            two.wait_core(0)
            two.wait_core(1)

    return call(
        kernel, "fwd_first", 0, (4, per_block),
        [pl.BlockSpec((tile, depth), lambda j, i: (coords()[0] * steps + jnp.minimum(tile_of(j, i), steps - 1), 0)),
         pl.BlockSpec((tile, depth), lambda j, i: (coords()[0] * steps + jnp.maximum(tile_of(j, i) - steps, 0), 0)),
         ANY, ANY] + [whole(*t.shape) for t in vectors],
        [pl.BlockSpec((tile, width), lambda j, i: (tile_of(j, i), block(j))), whole(2, 2, dim),
         whole(2, dim), whole(2, dim), ANY, pl.BlockSpec((width, tile), lambda j, i: (j, tile_of(j, i)))],
        [sds((2 * rows, dim), F32), sds((2, 2, dim), F32), sds((2, dim), F32), sds((2, dim), F32),
         sds((half, dim), BF16), sds((depth, 2 * rows), BF16)],
        [pltpu.VMEM((depth, dim), BF16), pltpu.VMEM((2, dim), F32)] + Share.scratch(4, 2, 2, width)
        + [DMA, DMA, TWO_DMA] + Gather.scratch(n) + Gather.scratch(n2),
        4 * rows * depth * dim, 2 * rows * (8 * depth + 4 * dim), (h_a, h_b, w_one, w_two, *vectors))


def fwd_next(u, sums, gb, w_own, w_other, by_rows, total, cid, w_next=None):
    all_rows, depth = u.shape
    dim = w_own.shape[1] if by_rows else 2 * w_own.shape[1]
    half = dim // 2
    quarter = half // 4
    steps = all_rows // 2 // TM
    last = 2 * steps - 1
    slab = dim // (2 * steps)
    n = 4
    more = w_next is not None

    def kernel(u_ref, s_ref, gb_ref, wo_ref, wt_ref, *refs):
        if more:
            wn_ref, refs = refs[0], refs[1:]
        x_ref, o_ref, so_ref, wtr_ref, *refs = refs
        if more:
            wno_ref, *refs = refs
        w, act, acc, got, ssem, rsem, lsem, *refs = refs
        share = Share(acc, got, ssem, rsem)
        i = pl.program_id(0)
        y = coords()[0]

        def local(ref, model, b):
            where = at(model, half)
            return pltpu.make_async_copy(ref, w.at[where] if by_rows else w.at[:, where], lsem.at[b])

        if more:
            gather = Gather(lambda q, p: wn_ref.at[at(p, depth // n), at(q, quarter)],
                            lambda m, q, p: wno_ref.at[at(p, depth // n), at(q, quarter)], n, refs)

        @pl.when(i == 0)
        def _():
            arrive()
            acc[...] = jnp.zeros_like(acc)
            local(wo_ref, y, 0).start()
            local(wt_ref, other(y), 1).start()
            all_arrived()
            if more:
                gather.start()
            local(wo_ref, y, 0).wait()
            local(wt_ref, other(y), 1).wait()

        if more:
            for p in range(n):
                pl.when(i == p + 2)(lambda p=p: gather.pass_y(p))
                pl.when(i == p + 4)(lambda p=p: gather.pass_x(p))
        pl.when(i == steps)(lambda: share.start(0))

        mean, inv = mean_inv(s_ref[0], total)
        for k, cols in enumerate(runs(depth, LANES)):
            m, r, g, b = (t[:, k * LANES:(k + 1) * LANES] for t in (mean, inv, gb_ref[:1], gb_ref[1:]))
            for piece in runs(TM, PIECE):
                act[piece, cols] = jnp.maximum((u_ref[piece, cols] - m) * r * g + b, 0.0).astype(BF16)
        x_ref[...] = act[...].T
        wtr_ref[...] = w[:, at(i, slab)].T
        v = i // steps
        keep = jnp.where(i % steps == 0, 0.0, 1.0)
        for some in runs(dim, TM):
            o_ref[:, some] = mm(act[...], w[:, some])
            for cols in runs(TM, LANES):
                cols = pl.ds(some.start + cols.start, LANES)
                share.acc[v, :, cols] = keep * share.acc[v, :, cols] + moments(o_ref, cols)

        @pl.when(i == last)
        def _():
            share.start(1)
            for b in BOTH:
                so_ref[b] = share.total(b)
            if more:
                gather.drain()
                gather.wait_core(0)
                gather.wait_core(1)

    return call(
        kernel, "fwd_next", cid, (2 * steps,),
        [pl.BlockSpec((TM, depth), lambda i: (i, 0)), pl.BlockSpec((1, 2, depth), lambda i: (i // steps, 0, 0)),
         whole(2, depth), ANY, ANY] + [ANY] * more,
        [pl.BlockSpec((depth, TM), lambda i: (0, i)), pl.BlockSpec((TM, dim), lambda i: (i, 0)),
         whole(2, 2, dim), pl.BlockSpec((slab, depth), lambda i: (i, 0))] + [ANY] * more,
        [sds((depth, all_rows), BF16), sds((all_rows, dim), F32), sds((2, 2, dim), F32), sds((dim, depth), BF16)]
        + ([sds(w_next.shape, BF16)] if more else []),
        [pltpu.VMEM((depth, dim), BF16), pltpu.VMEM((TM, depth), BF16)] + Share.scratch(2, 2, dim) + [TWO_DMA] + (Gather.scratch(n) if more else []),
        2 * all_rows * depth * dim, all_rows * (6 * depth + 4 * dim),
        (u, sums, gb, w_own, w_other) + ((w_next,) if more else ()))


def corr_grad(z, sums, lam, total):
    all_rows, dim = z.shape
    rows = all_rows // 2
    half = dim // 2
    quart = half // 2
    n_chunk = 8
    width = half // n_chunk
    pair = 2 * width
    mt = TM
    zt = TM // 2
    ahead = 3
    lead = 3
    z_steps = all_rows // zt
    m_steps = rows // mt
    scale = 1.0 / total

    def kernel(z_ref, s_ref, lam_ref, zho_ref, d_ref, so_ref, lo_ref, zh, da, ck, r1, r2, g, stage, dsend, drecv, acc, got, ssem, rsem, loss_acc, loss_got, lsem, lrsem, zs, zos,
               d1s, d1r, s1s, s1r, s2s, s2r, a2s, a2r, a1s, a1r, ads, adr, dbs, das):
        share = Share(acc, got, ssem, rsem)
        share_loss = Share(loss_acc, loss_got, lsem, lrsem)
        here = coords()
        y, x, c = here
        on_x = c == 0
        by_core = lambda one, two: tuple(jnp.where(on_x, a, b) for a, b in zip(one, two))
        first = by_core(flip(here, X_PEER), flip(here, Y_PEER))
        second = by_core(flip(here, Y_PEER), flip(here, X_PEER))
        cpeer = flip(here, C_PEER)
        bit1, bit2 = by_core((x, y), (y, x))
        arrive()
        acc[...] = jnp.zeros_like(acc)
        loss_acc[...] = jnp.zeros_like(loss_acc)

        def load(i, slot):
            return pltpu.make_async_copy(z_ref.at[at(i, zt)], ck.at[at(slot, zt)], zs.at[slot])

        def zh_out(i):
            v, r = lax.div(i, n_chunk // 2), lax.rem(i, n_chunk // 2)
            return pltpu.make_async_copy(zh.at[v, at(r, TM)], zho_ref.at[v, at(r, TM)], zos.at[i])

        z_slots = half // zt
        for i in range(ahead):
            load(i, i).start()

        def normalise(i):
            slot = lax.rem(i, z_slots)
            v, r = lax.div(i, z_steps // 2), lax.rem(i, z_steps // 2)
            pl.when(i + ahead < z_steps)(lambda: load(i + ahead, lax.rem(i + ahead, z_slots)).start())
            load(i, slot).wait()
            mean, inv = mean_inv(s_ref[v], total)
            for k, cols in enumerate(runs(dim, LANES)):
                m, s = (t[:, k * LANES:(k + 1) * LANES] for t in (mean, inv))
                for p in range(zt // PIECE):
                    zh[v, at(r * (zt // PIECE) + p, PIECE), cols] = (
                        (ck[at(slot * (zt // PIECE) + p, PIECE), cols] - m) * s).astype(BF16)
            da[at(i, rows // z_steps)] = jnp.zeros((rows // z_steps, dim), F32)

        loop(z_steps, normalise)
        all_arrived()

        def both(v, rows_at, t):
            return jnp.concatenate([zh[v, rows_at, at(b * n_chunk + t, width)] for b in BOTH], axis=1)

        group = lambda t, b: at(2 * t + b, width)

        def to_core(t):
            return remote(dsend.at[odd(t)], drecv.at[odd(t)], d1s.at[t], d1r.at[t], cpeer)

        def to_first(t):
            return remote(ck.at[:, group(t, other(bit1))], r1.at[t], s1s.at[t], s1r.at[t], first)

        def to_second(t):
            return remote(ck.at[at(other(bit2), quart), group(t, bit1)], r2.at[t], s2s.at[t], s2r.at[t], second)

        def g_second(t, b):
            block = g.at[t, at(2 * c + b, quart), at(bit1, width)]
            return remote(block, block, a2s.at[t], a2r.at[t], second)

        def g_first(t, b):
            block = g.at[t, at(c, half), at(b, width)]
            return remote(block, block, a1s.at[t], a1r.at[t], first)

        def g_core(t, core):
            block = g.at[t, at(core, half)]
            return remote(block, block, ads.at[t], adr.at[t], cpeer)

        def chip_sum(t):
            to_core(t).wait_recv()
            to_core(t).wait_send()
            ck[:, at(t, pair)] += drecv[odd(t)]
            to_first(t).start()

        def corr_part(t):
            zh_out(t).start()
            right = both(1, pl.ds(0, rows), t)
            dsend[odd(t)] = mm_at(zh[0, :, at(other(c), half)], right)
            ck[:, at(t, pair)] = mm_at(zh[0, :, at(c, half)], right)
            to_core(t).start()

        def db_out(t, m, slot, b):
            return pltpu.make_async_copy(
                stage.at[slot, :, at(b, width)], d_ref.at[1, at(m, mt), at(b * n_chunk + t, width)], dbs.at[slot, b])

        def da_out(m):
            return pltpu.make_async_copy(da.at[at(m, mt)], d_ref.at[0, at(m, mt)], das.at[m])

        def finish(m):
            def scaled(cols):
                for p in range(mt // PIECE):
                    some = at(m * (mt // PIECE) + p, PIECE)
                    d = da[some, cols] * scale
                    da[some, cols] = d
                    yield d, d * zh[0, some, cols].astype(F32)

            for cols in runs(dim, LANES):
                acc[0, :, cols] += two_sums(scaled(cols))
            da_out(m).start()

        def grads(t):
            def rows_of(m):
                slot = odd(m)

                @pl.when(t * m_steps + m >= 2)
                def _():
                    for b in BOTH:
                        db_out(t, m, slot, b).wait()

                own = both(1, at(m, mt), t)
                stage[slot] = mm(zh[0, at(m, mt)], g[t]) * scale
                sums = two_sums((stage[slot, r], stage[slot, r] * both(1, at(m * (mt // PIECE) + p, PIECE), t).astype(F32))
                                for p, r in enumerate(runs(mt, PIECE)))
                for b in BOTH:
                    acc[1, :, at(b * n_chunk + t, width)] += sums[:, b * width:(b + 1) * width]
                    db_out(t, m, slot, b).start()
                for cols in runs(dim, LANES):
                    da[at(m, mt), cols] += mm_bt(own, g[t, cols])
                pl.when(t == n_chunk - 1)(lambda: finish(m))

            loop(m_steps, rows_of)

        def at_first(t):
            to_first(t).wait_recv()
            ck[:, group(t, bit1)] += r1[t]
            to_second(t).start()

        def at_second(t):
            to_second(t).wait_recv()
            corr_mat = (ck[at(bit2, quart), group(t, bit1)] + r2[t]) * scale
            row_ids = (2 * c + bit2) * quart + lax.broadcasted_iota(jnp.int32, (quart, width), 0)
            col_ids = (bit1 * n_chunk + t) * width + lax.broadcasted_iota(jnp.int32, (quart, width), 1)
            is_diag = row_ids == col_ids
            lam_val = lam_ref[0]
            loss = jnp.where(is_diag, (1.0 - corr_mat) * (1.0 - corr_mat), lam_val * corr_mat * corr_mat)
            loss_acc[0] += jnp.sum(loss, axis=0, keepdims=True)
            pl.when(t == n_chunk - 1)(lambda: share_loss.start(0))
            grad = jnp.where(is_diag, -2.0 * (1.0 - corr_mat), 2.0 * lam_val * corr_mat).astype(BF16)
            g[t, at(2 * c + bit2, quart), at(bit1, width)] = grad
            g_second(t, bit2).start()

        def back_second(t):
            g_second(t, other(bit2)).wait_recv()
            g_first(t, bit1).start()

        def back_first(t):
            g_first(t, other(bit1)).wait_recv()
            g_core(t, c).start()

        def back_core(t):
            g_core(t, other(c)).wait_recv()
            grads(t)

        def advance(tau):
            for lag, stage_fn in ((lead, at_first), (lead + 1, back_second), (lead + 2, back_first), (lead + 3, back_core),
                                  (lead, at_second), (1, chip_sum), (0, corr_part)):
                t = tau - lag
                pl.when(jnp.logical_and(t >= 0, t < n_chunk))(lambda t=t, stage_fn=stage_fn: stage_fn(t))

        loop(n_chunk + lead + 3, advance)
        share.start(1)
        share.start(0)
        for t in range(n_chunk):
            for copy in (to_first(t), to_second(t), g_second(t, bit2), g_first(t, bit1), g_core(t, c)):
                copy.wait_send()
        for b in BOTH:
            so_ref[b] = share.total(b)
            for slot in BOTH:
                db_out(0, 0, slot, b).wait()
        lo_ref[...] = share_loss.total(0)
        for i in range(n_chunk):
            zh_out(i).wait()
        for m in range(m_steps):
            da_out(m).wait()

    return call(
        kernel, "corr_grad", 3, (), [ANY, VMEM, pl.BlockSpec(memory_space=pltpu.SMEM)], [ANY, ANY, VMEM, VMEM],
        [sds((2, rows, dim), BF16), sds((2, rows, dim), F32), sds((2, 2, dim), F32), sds((1, width), F32)],
        [pltpu.VMEM((2, rows, dim), BF16), pltpu.VMEM((rows, dim), F32), pltpu.VMEM((half, dim), F32),
         pltpu.VMEM((n_chunk, half, width), F32), pltpu.VMEM((n_chunk, quart, width), F32),
         pltpu.VMEM((n_chunk, dim, pair), BF16), pltpu.VMEM((2, mt, pair), F32)]
        + [pltpu.VMEM((2, half, pair), F32)] * 2 + Share.scratch(2, 2, dim) + Share.scratch(1, 1, width)
        + [DMA((half // zt,)), DMA((n_chunk,))] + [DMA((n_chunk,))] * 12 + [DMA((2, 2)), DMA((m_steps,))],
        all_rows * dim * dim * 3, all_rows * dim * 12, (z, sums, lam))


def backward(d_emb, zh, sz, s_emb, layers, x2_t, total):
    all_rows, dim = zh.shape
    rows, half = all_rows // 2, dim // 2
    width = 256
    slabs = dim // width
    items = 2 * slabs
    piece = width
    side = half // 2 // piece
    per_slab = half // piece
    n_layer = len(layers) + 1
    n_slab = n_layer * slabs
    per_layer = slabs * side
    n_chunk = n_layer * per_layer
    ahead = 3
    (u2, s2, gb2, w3_t, x1_t), (u1, s1, gb1, w2_t, h_t) = layers

    def kernel(d_ref, zh_ref, sz_ref, sd_ref, x2_ref, x1_ref, h_ref, u2_ref, u1_ref, w3_ref, w2_ref,
               s2_ref, s1_ref, gb2_ref, gb1_ref, dw3_ref, dw2_ref, dw1_ref, sum_ref, dy_ref, part_ref, ry_ref, rx_ref,
               dbuf, xbuf, wbuf, ubuf, dybuf, dyout, psend, pkeep, dr, ebuf, mbuf, fbuf, acc, got, ssem, rsem,
               us, ws, ds, dos, xl, ps, pr, pm, ys, yr, xs, xr, es, fs, fcs, fcr, credit):
        share = Share(acc, got, ssem, rsem)
        here = coords()
        y, x, c = here
        ypeer, xpeer, cpeer = flip(here, Y_PEER), flip(here, X_PEER), flip(here, C_PEER)
        arrive()

        def column(k, n):
            model = odd(n + jnp.where(k == 0, other(y), 0))
            return jnp.where(k == 1, n, model * (slabs // 2) + lax.div(n, 2))

        def turn(k):
            return jnp.where(k == 0, 0, other(y))

        def m_slot(j):
            return lax.rem(j, 4)

        def copy(src, dst, sem):
            return pltpu.make_async_copy(src, dst, sem)

        def sent_by(q):
            first = jnp.minimum(per_slab * lax.div(q, 4), per_layer)
            middle = jnp.clip(side * lax.div(q - 2 * items - 2, 2), 0, per_layer)
            last = jnp.clip(per_slab * lax.div(q - 4 * items - 2, 4), 0, per_layer)
            return first + middle + last

        def begun(q):
            return jnp.maximum(lax.div(q - 6, 2), 0)

        def to_core(s):
            return remote(psend.at[odd(s)], dr.at[odd(s)], ps.at[s], pr.at[s], cpeer)

        def keep_out(s):
            return copy(pkeep.at[odd(s)], part_ref.at[s], pm)

        def chip_sum(s):
            to_core(s).wait_recv()
            pkeep[odd(s)] += dr[odd(s)]

            @pl.when(s + 2 < n_slab)
            def _():
                pl.semaphore_signal(credit, inc=1, device_id=device(cpeer), device_id_type=pl.DeviceIdType.MESH)

            to_core(s).wait_send()
            keep_out(s).start()

        def home(j, own):
            k = lax.div(j, per_layer)
            i = lax.rem(j, per_layer)
            model = y if own else other(y)
            turned = other(turn(k)) if own else turn(k)
            s = jnp.where(k == 1, lax.div(i, side), 2 * lax.div(i, per_slab) + turned)
            place = jnp.where(k == 1, model * side + lax.rem(i, side), lax.rem(i, per_slab))
            return part_ref.at[k * slabs + s, at(place, piece)]

        def to_y(j):
            return remote(home(j, False), ry_ref.at[j], ys.at[lax.div(j, per_layer)], yr.at[j], ypeer)

        def issue(s, q):
            keep_out(s).wait()
            k, n = lax.div(s, slabs), lax.rem(s, slabs)
            for mine, fire, first, count in (
                    (k == 1, True, n * side, side), (k != 1, odd(n) == jnp.where(k == 0, 0, 1), lax.div(n, 2) * per_slab, per_slab)):
                for r in range(count):
                    j = k * per_layer + first + r
                    pl.when(mine & fire & (j < begun(q) + ahead))(lambda j=j: to_y(j).start())

        def to_x(j):
            return remote(mbuf.at[m_slot(j)], rx_ref.at[j], xs.at[m_slot(j)], xr.at[j], xpeer)

        def result(j, k):
            i = lax.rem(j, per_layer)
            if k == 1:
                return dw2_ref.at[at(c * side + lax.rem(i, side), piece), at(lax.div(i, side), width)]
            return (dw1_ref if k else dw3_ref).at[at(c * per_slab + lax.rem(i, per_slab), piece), at(lax.div(i, per_slab), width)]

        def put(j, k):
            slot = odd(j)
            return (copy(fbuf.at[slot], result(j, k), fs.at[slot]),
                    remote(fbuf.at[slot], result(j, k), fcs.at[slot], fcr.at[k], cpeer))

        def put_done(j):
            here_copy, there_copy = put(j, 0)
            here_copy.wait()
            there_copy.wait_send()

        def load_part(j, which):
            src = (lambda: ry_ref.at[j], lambda: home(j, True), lambda: rx_ref.at[j])[which]()
            return copy(src, ebuf.at[which], es.at[which])

        def fetch_x(j):
            to_x(j).wait_recv()
            load_part(j, 2).start()

        def begin(j, q):
            remote(ry_ref.at[j], ry_ref.at[j], ys.at[0], yr.at[j], ypeer).wait_recv()
            load_part(j, 0).start()
            load_part(j, 1).start()
            pl.when(j + ahead < sent_by(q))(lambda: to_y(j + ahead).start())
            pl.when(j >= 2)(lambda: fetch_x(j - 2))

        def deliver(j):
            load_part(j, 2).wait()
            pl.when(j >= 2)(lambda: put_done(j))
            fbuf[odd(j)] = mbuf[m_slot(j)] + ebuf[2]
            for k in range(n_layer):
                @pl.when(lax.div(j, per_layer) == k)
                def _(k=k):
                    for one in put(j, k):
                        one.start()

        def end(j):
            load_part(j, 0).wait()
            load_part(j, 1).wait()
            pl.when(j >= 4)(lambda: to_x(j).wait_send())
            mbuf[m_slot(j)] = ebuf[0] + ebuf[1]
            to_x(j).start()
            pl.when(j >= 2)(lambda: deliver(j - 2))

        def events(q):
            now, before, earlier = begun(q), begun(q - 1), begun(q - 2)
            pl.when(before > earlier)(lambda: end(before - 1))
            pl.when(now > before)(lambda: begin(now - 1, q))

        def weight_slab(k, n, v, d):
            slot = odd(k * slabs + n)
            for buf, part in ((psend, other(c)), (pkeep, c)):
                first = jnp.where(k == 1, part, 2 * part)
                for b in BOTH:
                    left = xbuf[at(first + b * jnp.where(k == 1, 2, 1), half // 2), pl.ds(v * rows, rows)]
                    here_at = at(b, half // 2)
                    prod = mm(left, d)
                    buf[slot, here_at] = buf[slot, here_at] + prod if v else prod

        def after(k, n, v, q):
            s = k * slabs + n
            if v == 0:
                pl.when(n > 0)(lambda: chip_sum(s - 1))
            else:
                pl.when(s >= 2)(lambda: pl.semaphore_wait(credit, 1))
                to_core(s).start()
                pl.when(n > 0)(lambda: issue(s - 1, q))

        def dw_pass(k, q, ready, fetch, pre, ahead_of_next):
            def slab(n):
                for v in BOTH:
                    i = 2 * n + v
                    pl.when(i + 1 < items)(lambda: fetch(i + 1))
                    ready(i)
                    pl.when(n == 0)(lambda: x_load(x2_ref, v).wait())
                    events(q + i)
                    cols = at(column(k, n), width)
                    pre(v * rows, cols, v)
                    weight_slab(k, n, v, dbuf[pl.ds(v * rows, rows), cols])
                    after(k, n, v, q + i)
                pl.when(n == slabs - 1)(ahead_of_next)

            loop(slabs, slab)

        def emb_loads(i):
            n, v = split(i)
            cols = at(column(0, n), width)
            return (copy(d_ref.at[at(v, rows), cols], ubuf.at[v], us.at[v]),
                    copy(zh_ref.at[at(v, rows), cols], wbuf.at[v], ws.at[v]))

        def emb_fetch(i):
            for one in emb_loads(i):
                one.start()

        def emb_ready(i):
            for one in emb_loads(i):
                one.wait()

        def emb_pre(row, cols, v):
            _, inv = mean_inv(sz_ref[v, :, cols], total)
            sd = sd_ref[v, :, cols] / total
            for r in runs(rows, PIECE):
                dbuf[pl.ds(row + r.start, PIECE), cols] = (
                    inv * (ubuf[v, r] - sd[:1] - wbuf[v, r].astype(F32) * sd[1:])).astype(BF16)

        def x_load(src, v, rows_at=pl.ds(0, dim)):
            return copy(src.at[rows_at, at(v, rows)], xbuf.at[rows_at, at(v, rows)], xl.at[v])

        def u_slot(layer, v):
            return jnp.where(layer == 0, other(v), v)

        def slab_of(ref, layer, i, buf, sem, slot):
            n, v = split(i)
            return copy(ref.at[at(v, rows), at(column(layer + 1, n), width)], buf.at[slot], sem.at[slot])

        def u_load(layer, i, ref=u2_ref):
            return slab_of(ref, layer, i, ubuf, us, u_slot(layer, odd(i)))

        def dy_load(layer, i):
            return slab_of(dy_ref, layer, i, dybuf, ds, odd(i))

        def dy_out(layer, i):
            n, v = split(i)
            return copy(dyout.at[v], dy_ref.at[at(v, rows), at(column(layer + 1, n), width)], dos.at[v])

        def w_load(layer, n, ref=w3_ref):
            slot = odd(n + 1)
            return copy(ref.at[:, at(column(layer + 1, n), width)], wbuf.at[slot], ws.at[slot])

        def by_layer(layer, make, refs):
            for k, ref in enumerate(refs):
                pl.when(layer == k)(lambda ref=ref: make(ref).start())

        def start_u(layer, i):
            by_layer(layer, lambda ref: u_load(layer, i, ref), (u2_ref, u1_ref))

        def start_w(layer, n):
            by_layer(layer, lambda ref: w_load(layer, n, ref), (w3_ref, w2_ref))

        def next_layer(layer):
            start_u(layer, 0)
            start_w(layer, 0)

        for one in (x_load(x2_ref, 0), *emb_loads(0), x_load(x2_ref, 1)):
            one.start()
        all_arrived()
        dw_pass(0, 0, emb_ready, emb_fetch, emb_pre, lambda: next_layer(0))

        def stats(layer, v, cols):
            pick = lambda one, two: jnp.where(layer == 0, one, two)
            mean, inv = mean_inv(pick(s2_ref[v, :, cols], s1_ref[v, :, cols]), total)
            gb = pick(gb2_ref[:, cols], gb1_ref[:, cols])
            return mean, inv, gb[:1], gb[1:]

        def bn_layer(layer):
            start = (2 * layer + 1) * items

            def dx_item(i):
                n, v = split(i)
                slot = u_slot(layer, v)
                cols = at(column(layer + 1, n), width)

                @pl.when(i + 1 < items)
                def _():
                    start_u(layer, i + 1)
                    pl.when((v == 0) & (n + 1 < slabs))(lambda: start_w(layer, n + 1))

                @pl.when(i + 1 == items)
                def _():
                    start_u(layer, 0)
                    dy_load(layer, 0).start()

                u_load(layer, i).wait()
                pl.when(v == 0)(lambda: w_load(layer, n).wait())
                events(start + i)
                pl.when((i > 2) & (i < 11))(lambda: by_layer(
                    layer, lambda ref: x_load(ref, v, at(lax.div(i - 3, 2), half // 2)), (x1_ref, h_ref)))
                pl.when(n > 0)(lambda: dy_out(layer, i).wait())
                mean, inv, gamma, beta = stats(layer, v, cols)

                def pieces():
                    for b in BOTH:
                        dx = mm(dbuf[at(2 * v + b, rows // 2)], wbuf[odd(n + 1)])
                        for p in range(0, rows // 2, PIECE):
                            some = pl.ds(b * (rows // 2) + p, PIECE)
                            norm = (ubuf[slot, some] - mean) * inv
                            dy = jnp.where(norm * gamma + beta > 0, dx[p:p + PIECE], 0.0)
                            dyout[v, some] = dy
                            yield dy, dy * norm

                g = layer * items + i
                acc[g] = two_sums(pieces())
                dy_out(layer, i).start()
                share.start(g)
                before = (layer + 1) * slabs - 1
                pl.when(i == 0)(lambda: chip_sum(before))
                pl.when(i == 1)(lambda: issue(before, start + i))

            def fetch(i):
                start_u(layer, i)
                dy_load(layer, i).start()

            def ready(i):
                n, v = split(i)
                u_load(layer, i).wait()
                dy_load(layer, i).wait()
                sum_ref[layer, v, :, at(column(layer + 1, n), width)] = share.total(layer * items + i)

            def pre(row, cols, v):
                tot = sum_ref[layer, v, :, cols] / total
                mean, inv, gamma, _ = stats(layer, v, cols)
                slope, front, slot = inv * tot[1:], gamma * inv, u_slot(layer, v)
                for r in runs(rows, PIECE):
                    dbuf[pl.ds(row + r.start, PIECE), cols] = (
                        front * (dybuf[v, r] - (tot[:1] + (ubuf[slot, r] - mean) * slope))).astype(BF16)

            loop(items, dx_item)
            for v in BOTH:
                dy_out(layer, v).wait()
            dw_pass(layer + 1, start + items, ready, fetch, pre, lambda: pl.when(layer == 0)(lambda: next_layer(1)))

        loop(len(layers), bn_layer)

        ticks = (2 * n_layer - 1) * items
        chip_sum(n_slab - 1)
        issue(n_slab - 1, ticks)
        ended = 36

        def tail(j):
            begin(j, ticks + 2)
            end(j)

        loop(n_chunk, tail, ended)
        for j in range(n_chunk - 2, n_chunk):
            fetch_x(j)
            deliver(j)
        for j in BOTH:
            put_done(j)
        for k in range(n_layer):
            theirs = dw2_ref.at[at(other(c), half // 2)] if k == 1 else (dw1_ref if k else dw3_ref).at[at(other(c), half)]
            remote(theirs, theirs, fcs.at[0], fcr.at[k], cpeer).wait_recv()
            sent = ry_ref.at[at(k, per_layer)]
            remote(sent, sent, ys.at[k], yr.at[0], ypeer).wait_send()
        for j in range(n_chunk - 4, n_chunk):
            to_x(j).wait_send()

    n_item = len(layers) * items
    vm = lambda *shape: pltpu.VMEM(shape, F32)
    bf = lambda *shape: pltpu.VMEM(shape, BF16)
    outs = call(
        kernel, "backward", 4, (),
        [ANY, ANY, VMEM, VMEM] + [ANY] * 7 + [VMEM] * 4, [ANY] * 3 + [VMEM] + [ANY] * 4,
        [sds((dim, half), F32), sds((half, dim), F32), sds((dim, half), F32), sds((len(layers), 2, 2, dim), F32),
         sds((all_rows, dim), F32), sds((n_slab, half, width), F32), sds((n_chunk, piece, width), F32),
         sds((n_chunk, piece, width), F32)],
        [bf(all_rows, dim), bf(dim, all_rows), bf(2, dim, width), vm(2, rows, width), vm(2, rows, width), vm(2, rows, width),
         vm(2, half, width), vm(2, half, width), vm(2, half, width), vm(3, piece, width), vm(4, piece, width),
         vm(2, piece, width)] + Share.scratch(n_item, 2, width)
        + [TWO_DMA, TWO_DMA, TWO_DMA, TWO_DMA, TWO_DMA, DMA((n_slab,)), DMA((n_slab,)), DMA, DMA((n_layer,)),
           DMA((n_chunk,)), DMA((4,)), DMA((n_chunk,)), DMA((3,)), TWO_DMA, TWO_DMA, DMA((n_layer,)),
           pltpu.SemaphoreType.REGULAR],
        all_rows * dim * dim * 10, all_rows * dim * 40,
        (d_emb, zh, sz, s_emb, x2_t, x1_t, h_t, u2, u1, w3_t, w2_t, s2, s1, gb2, gb1))
    return outs[:n_layer + 1]


def settle(grads, sums, loss):
    steps = 4
    dim = sums.shape[-1]
    half = dim // 2

    def kernel(sum_ref, loss_ref, src3, src2, src1, g2_ref, b2_ref, g1_ref, b1_ref, total_ref, *dsts):
        for src, dst in zip((src3, src2, src1), dsts):
            dst[...] = src[...]

        @pl.when(pl.program_id(0) == 0)
        def _():
            y, _, _ = coords()
            for layer, (cols, g_ref, b_ref) in enumerate(((pl.ds(0, dim), g2_ref, b2_ref), (at(y, half), g1_ref, b1_ref))):
                both = jnp.sum(sum_ref[layer, :, :, cols], axis=0)
                g_ref[...] = both[1:]
                b_ref[...] = both[:1]
            total_ref[...] = jnp.sum(loss_ref[...], axis=1, keepdims=True)

    specs = [pl.BlockSpec((g.shape[0] // steps, g.shape[1]), lambda i: (i, 0)) for g in grads]
    small = [(1, n) for n in (dim, dim, half, half, 1)]
    return call(kernel, "settle", None, (steps,), [whole(*sums.shape), whole(*loss.shape)] + specs,
                [whole(*t) for t in small] + specs, [sds(t, F32) for t in small] + [sds(g.shape, F32) for g in grads], [], 0,
                sum(g.size for g in grads) * 8, (sums, loss, *grads))


def solution(mesh):
    def shard_body(h_a, h_b, w_one, w_two, w_three, g_one, b_one, g_two, b_two, lam_off):
        total = float(h_a.shape[0] * mesh.shape['data'])
        rowed = [t.reshape(1, -1) for t in (g_one, b_one, g_two, b_two)]
        u1, s1, gb1, gb2, w_two_o, h_t = fwd_first(h_a, h_b, w_one, w_two, *rowed)
        x1_t, u2, s2, w2_t, w_three_o = fwd_next(u1, s1, gb1, w_two, w_two_o, True, total, 1, w_three)
        x2_t, z, sz, w3_t = fwd_next(u2, s2, gb2, w_three, w_three_o, False, total, 2)
        zh, d_emb, s_emb, loss = corr_grad(z, sz, lam_off, total)
        *grads, sums = backward(
            d_emb.reshape(z.shape), zh.reshape(z.shape), sz, s_emb,
            ((u2, s2, gb2, w3_t, x1_t), (u1, s1, gb1, w2_t, h_t)), x2_t, total)
        *small, dw_three, dw_two, dw_one = settle(grads, sums, loss)
        dg_two, db_two, dg_one, db_one, loss = (t.reshape(-1) for t in small)
        return loss, dw_one, dw_two, dw_three, dg_one, db_one, dg_two, db_two

    in_specs = (P('data', None), P('data', None), P(None, 'model'), P('model', None), P(None, 'model'),
                P('model'), P('model'), P(), P(), P())
    out_specs = (P(), P(None, 'model'), P('model', None), P(None, 'model'), P('model'), P('model'), P(), P())
    return jax.shard_map(shard_body, mesh=mesh, in_specs=in_specs, out_specs=out_specs, check_vma=False)
```

```python
import functools

import jax
import jax.numpy as jnp
from jax import lax
from jax.experimental import pallas as pl
from jax.experimental.pallas import tpu as pltpu
from jax.sharding import PartitionSpec as P

BN_EPS = 1e-5
F32 = jnp.float32
BF16 = jnp.bfloat16
PIECE = 64
LANES = 256
SUBLANES = 8
TM = 512
MAX_VMEM = 67043328
ANY = pl.BlockSpec(memory_space=pl.ANY)
VMEM = pl.BlockSpec(memory_space=pltpu.VMEM)
DMA = pltpu.SemaphoreType.DMA
TWO_DMA = DMA((2,))
BOTH = (0, 1)
PEERS = [(ky, kx, kc) for ky in BOTH for kx in BOTH for kc in BOTH][1:]
C_PEER, X_PEER, Y_PEER = PEERS[0], PEERS[1], PEERS[3]
N_DEV = len(PEERS) + 1


def mm(left, right):
    return jnp.dot(left, right, preferred_element_type=F32)


def mm_bt(left, right):
    return lax.dot_general(left, right, (((1,), (1,)), ((), ())), preferred_element_type=F32)


def mm_at(left, right):
    return lax.dot_general(left, right, (((0,), (0,)), ((), ())), preferred_element_type=F32)


def other(p):
    return 1 - p


def odd(i):
    return lax.rem(i, 2)


def split(i):
    return lax.div(i, 2), odd(i)


def loop(n, body, start=0):
    def one(i, carry):
        body(i)
        return carry

    lax.fori_loop(start, n, one, 0)


def whole(*shape):
    return pl.BlockSpec(shape, lambda *_: (0,) * len(shape))


def at(i, n):
    return pl.ds(pl.multiple_of(i * n, n), n)


def sds(shape, dtype):
    return jax.ShapeDtypeStruct(shape, dtype)


def mean_inv(sums, total):
    mean = sums[:1] / total
    var = sums[1:2] / total - mean * mean
    return mean, lax.rsqrt(var + BN_EPS)


def fold(v):
    return jnp.sum(v.reshape(-1, SUBLANES, v.shape[1]), axis=0)


def runs(n, size):
    return [pl.ds(r, size) for r in range(0, n, size)]


def two_sums(pairs):
    one = two = 0.0
    for a, b in pairs:
        one, two = one + fold(a), two + fold(b)
    return jnp.concatenate([jnp.sum(t, axis=0, keepdims=True) for t in (one, two)], axis=0)


def moments(ref, cols):
    pieces = (ref[r, cols] for r in runs(ref.shape[0], PIECE))
    return two_sums((u, u * u) for u in pieces)


def coords():
    y, d = lax.axis_index('model'), lax.axis_index('data')
    return y, lax.div(d, 2), odd(d)


def flip(here, which):
    return tuple(other(p) if f else p for p, f in zip(here, which))


def flat(here):
    y, x, c = here
    return 4 * y + 2 * x + c


def device(here):
    y, x, c = here
    return (y, 2 * x + c)


def remote(src, dst, send_sem, recv_sem, there):
    return pltpu.make_async_remote_copy(
        src_ref=src, dst_ref=dst, send_sem=send_sem, recv_sem=recv_sem, device_id=device(there),
        device_id_type=pl.DeviceIdType.MESH)


def arrive():
    here = coords()
    for k in PEERS:
        pl.semaphore_signal(pltpu.get_barrier_semaphore(), inc=1, device_id=device(flip(here, k)),
                            device_id_type=pl.DeviceIdType.MESH)


def all_arrived():
    pl.semaphore_wait(pltpu.get_barrier_semaphore(), len(PEERS))


class Share:
    def __init__(self, acc, got, send_sem, recv_sem):
        self.acc, self.got, self.send_sem, self.recv_sem = acc, got, send_sem, recv_sem

    @staticmethod
    def scratch(n, *shape):
        return [pltpu.VMEM((n, *shape), F32), pltpu.VMEM((n, N_DEV, *shape), F32), DMA((n,)), DMA((n,))]

    def start(self, b):
        here = coords()
        me = flat(here)
        self.got[b, me] = self.acc[b]
        for which in PEERS:
            remote(self.acc.at[b], self.got.at[b, me], self.send_sem.at[b], self.recv_sem.at[b],
                   flip(here, which)).start()

    def total(self, b):
        all_of = self.got.at[b, pl.ds(0, len(PEERS))]
        copies = remote(all_of, all_of, self.send_sem.at[b], self.recv_sem.at[b], coords())
        copies.wait_send()
        copies.wait_recv()
        out = self.got[b, 0]
        for f in range(1, N_DEV):
            out += self.got[b, f]
        return out


class Gather:
    def __init__(self, own, dest, n, sems):
        self.own, self.dest, self.n = own, dest, n
        self.ys, self.yr, self.xs, self.xr, self.cs, self.cr = sems
        self.here = coords()
        _, x, c = self.here
        self.mine, self.across = 2 * x + c, 2 * (other(x)) + c
        self.core = (2 * x + other(c), 2 * (other(x)) + other(c))

    @staticmethod
    def scratch(n):
        return [DMA((n,))] * 4 + [DMA((2, n))] * 2

    def y(self, p):
        model = self.here[0]
        return remote(self.own(self.mine, p), self.dest(model, self.mine, p), self.ys.at[p], self.yr.at[p],
                      flip(self.here, Y_PEER))

    def moved(self, q, p, send_sem, recv_sem, which):
        ref = self.dest(1 - self.here[0], q, p)
        return remote(ref, ref, send_sem, recv_sem, flip(self.here, which))

    def x(self, p, q):
        return self.moved(q, p, self.xs.at[p], self.xr.at[p], X_PEER)

    def c(self, p, late, q):
        return self.moved(q, p, self.cs.at[late, p], self.cr.at[late, p], C_PEER)

    def start(self):
        for p in range(self.n):
            self.y(p).start()

    def pass_y(self, p):
        self.moved(self.mine, p, self.ys.at[p], self.yr.at[p], Y_PEER).wait_recv()
        self.x(p, self.mine).start()
        self.c(p, 0, self.mine).start()

    def pass_x(self, p):
        self.x(p, self.across).wait_recv()
        self.c(p, 1, self.across).start()

    def wait_core(self, late):
        for p in range(self.n):
            self.c(p, late, self.core[late]).wait_recv()

    def drain(self):
        for p in range(self.n):
            self.y(p).wait_send()
            self.x(p, self.mine).wait_send()
            self.c(p, 0, self.mine).wait_send()
            self.c(p, 1, self.across).wait_send()


def call(kernel, name, cid, grid, in_specs, out_specs, out_shape, scratch, flops, nbytes, args):
    return pl.pallas_call(
        kernel, name=name, grid=grid, in_specs=in_specs, out_specs=out_specs, out_shape=out_shape, scratch_shapes=scratch,
        compiler_params=pltpu.CompilerParams(vmem_limit_bytes=MAX_VMEM, collective_id=cid, has_side_effects=cid is not None),
        cost_estimate=pl.CostEstimate(flops=flops, bytes_accessed=nbytes, transcendentals=0))(*args)


def fwd_first(h_a, h_b, w_one, w_two, *vectors):
    depth, half = w_one.shape
    dim = 2 * half
    rows = h_a.shape[0] // 2
    tile, width, quarter = 2 * TM, half // 2, half // 4
    steps = rows // tile
    per_block = 2 * steps
    n, n2 = 4, 8

    def block(j):
        y, x, _ = coords()
        return jnp.where(j < 2, 2 * y + j, 2 * (other(y)) + jnp.where(j == 2, x, other(x)))

    def tile_of(j, i):
        return jnp.where(odd(j) == 0, i, per_block - 1 - i)

    def kernel(ha_ref, hb_ref, w_ref, w2_ref, g1_ref, b1_ref, g2_ref, b2_ref, u_ref, s_ref, gbo_ref, gb2_ref, w2o_ref, ht_ref,
               w1, gbf, *sems):
        share, sems = Share(*sems[:4]), sems[4:]
        gs, gr, lsem = sems[:3]
        sems = sems[3:]
        j, i = pl.program_id(0), pl.program_id(1)
        step = j * per_block + i
        here = coords()
        y = here[0]
        one = Gather(lambda q, p: w_ref.at[at(p, depth // n), at(q, quarter)],
                     lambda m, q, p: w1.at[at(p, depth // n), at(m * 4 + q, quarter)], n, sems[:6])
        two = Gather(lambda q, p: w2_ref.at[at(q * n2 + p, quarter // n2)],
                     lambda m, q, p: w2o_ref.at[at(q * n2 + p, quarter // n2)], n2, sems[6:])

        def local(b):
            return pltpu.make_async_copy(w_ref.at[:, at(b, width)], w1.at[:, at(2 * y + b, width)], lsem.at[b])

        def bn_vectors(m):
            return remote(gbf.at[:, at(m, half)], gbf.at[:, at(m, half)], gs, gr, flip(here, Y_PEER))

        def begin():
            arrive()
            local(0).start()
            local(1).start()
            all_arrived()
            one.start()
            two.start()
            for r, (one_ref, two_ref) in enumerate(((g1_ref, g2_ref), (b1_ref, b2_ref))):
                row = pl.ds(r, 1)
                gbf[row, at(y, half)] = one_ref[...]
                gb2_ref[row] = two_ref[...]
            local(0).wait()

        def late_half():
            one.pass_x(0)
            one.pass_y(n - 1)
            one.wait_core(0)

        hooks = [(0, begin), (1, lambda: bn_vectors(y).start()), (per_block, lambda: local(1).wait()), (2 * per_block, late_half)]
        hooks += [(2 * p + 3, functools.partial(one.pass_y, p)) for p in range(n - 1)]
        hooks += [(p + 2 * per_block, functools.partial(one.pass_x, p)) for p in range(1, n)]
        hooks += [(3 * per_block, lambda: one.wait_core(1))]
        hooks += [(p + 9, functools.partial(two.pass_y, p)) for p in range(n2 - 1)]
        hooks += [(13 + (p + 1) // 2, functools.partial(two.pass_x, p)) for p in range(n2 // 2)]
        for s, hook in hooks:
            pl.when(step == s)(hook)
        for b in range(3):
            pl.when(step == (b + 1) * per_block)(lambda b=b: share.start(block(b)))

        tile_at = tile_of(j, i)
        first_view = tile_at < steps
        cols = at(j, width)
        ht_ref[...] = lax.select(first_view, ha_ref[:, cols], hb_ref[:, cols]).T
        for r in runs(tile, TM):
            u_ref[r] = mm(lax.select(first_view, ha_ref[r], hb_ref[r]), w1[:, at(block(j), width)])
        sums = jnp.concatenate([moments(u_ref, cols) for cols in runs(width, LANES)], axis=1)
        v = tile_at // steps
        share.acc[block(j), v] = jnp.where(i % steps == 0, 0.0, share.acc[block(j), v]) + sums

        @pl.when(step == 4 * per_block - 1)
        def _():
            share.start(block(3))
            two.pass_y(n2 - 1)
            for p in range(n2 // 2, n2):
                two.pass_x(p)
            bn_vectors(other(y)).wait_recv()
            bn_vectors(y).wait_send()
            gbo_ref[...] = gbf[...]
            for b in range(4):
                s_ref[:, :, b * width:(b + 1) * width] = share.total(b)
            one.drain()
            two.drain()
            two.wait_core(0)
            two.wait_core(1)

    return call(
        kernel, "fwd_first", 0, (4, per_block),
        [pl.BlockSpec((tile, depth), lambda j, i: (coords()[0] * steps + jnp.minimum(tile_of(j, i), steps - 1), 0)),
         pl.BlockSpec((tile, depth), lambda j, i: (coords()[0] * steps + jnp.maximum(tile_of(j, i) - steps, 0), 0)),
         ANY, ANY] + [whole(*t.shape) for t in vectors],
        [pl.BlockSpec((tile, width), lambda j, i: (tile_of(j, i), block(j))), whole(2, 2, dim),
         whole(2, dim), whole(2, dim), ANY, pl.BlockSpec((width, tile), lambda j, i: (j, tile_of(j, i)))],
        [sds((2 * rows, dim), F32), sds((2, 2, dim), F32), sds((2, dim), F32), sds((2, dim), F32),
         sds((half, dim), BF16), sds((depth, 2 * rows), BF16)],
        [pltpu.VMEM((depth, dim), BF16), pltpu.VMEM((2, dim), F32)] + Share.scratch(4, 2, 2, width)
        + [DMA, DMA, TWO_DMA] + Gather.scratch(n) + Gather.scratch(n2),
        4 * rows * depth * dim, 2 * rows * (8 * depth + 4 * dim), (h_a, h_b, w_one, w_two, *vectors))


def fwd_next(u, sums, gb, w_own, w_other, by_rows, total, cid, w_next=None):
    all_rows, depth = u.shape
    dim = w_own.shape[1] if by_rows else 2 * w_own.shape[1]
    half = dim // 2
    quarter = half // 4
    steps = all_rows // 2 // TM
    last = 2 * steps - 1
    slab = dim // (2 * steps)
    n = 4
    more = w_next is not None

    def kernel(u_ref, s_ref, gb_ref, wo_ref, wt_ref, *refs):
        if more:
            wn_ref, refs = refs[0], refs[1:]
        x_ref, o_ref, so_ref, wtr_ref, *refs = refs
        if more:
            wno_ref, *refs = refs
        w, act, acc, got, ssem, rsem, lsem, *refs = refs
        share = Share(acc, got, ssem, rsem)
        i = pl.program_id(0)
        y = coords()[0]

        def local(ref, model, b):
            where = at(model, half)
            return pltpu.make_async_copy(ref, w.at[where] if by_rows else w.at[:, where], lsem.at[b])

        if more:
            gather = Gather(lambda q, p: wn_ref.at[at(p, depth // n), at(q, quarter)],
                            lambda m, q, p: wno_ref.at[at(p, depth // n), at(q, quarter)], n, refs)

        @pl.when(i == 0)
        def _():
            arrive()
            acc[...] = jnp.zeros_like(acc)
            local(wo_ref, y, 0).start()
            local(wt_ref, other(y), 1).start()
            all_arrived()
            if more:
                gather.start()
            local(wo_ref, y, 0).wait()
            local(wt_ref, other(y), 1).wait()

        if more:
            for p in range(n):
                pl.when(i == p + 2)(lambda p=p: gather.pass_y(p))
                pl.when(i == p + 4)(lambda p=p: gather.pass_x(p))
        pl.when(i == steps)(lambda: share.start(0))

        mean, inv = mean_inv(s_ref[0], total)
        for k, cols in enumerate(runs(depth, LANES)):
            m, r, g, b = (t[:, k * LANES:(k + 1) * LANES] for t in (mean, inv, gb_ref[:1], gb_ref[1:]))
            for piece in runs(TM, PIECE):
                act[piece, cols] = jnp.maximum((u_ref[piece, cols] - m) * r * g + b, 0.0).astype(BF16)
        x_ref[...] = act[...].T
        wtr_ref[...] = w[:, at(i, slab)].T
        v = i // steps
        keep = jnp.where(i % steps == 0, 0.0, 1.0)
        for some in runs(dim, TM):
            o_ref[:, some] = mm(act[...], w[:, some])
            for cols in runs(TM, LANES):
                cols = pl.ds(some.start + cols.start, LANES)
                share.acc[v, :, cols] = keep * share.acc[v, :, cols] + moments(o_ref, cols)

        @pl.when(i == last)
        def _():
            share.start(1)
            for b in BOTH:
                so_ref[b] = share.total(b)
            if more:
                gather.drain()
                gather.wait_core(0)
                gather.wait_core(1)

    return call(
        kernel, "fwd_next", cid, (2 * steps,),
        [pl.BlockSpec((TM, depth), lambda i: (i, 0)), pl.BlockSpec((1, 2, depth), lambda i: (i // steps, 0, 0)),
         whole(2, depth), ANY, ANY] + [ANY] * more,
        [pl.BlockSpec((depth, TM), lambda i: (0, i)), pl.BlockSpec((TM, dim), lambda i: (i, 0)),
         whole(2, 2, dim), pl.BlockSpec((slab, depth), lambda i: (i, 0))] + [ANY] * more,
        [sds((depth, all_rows), BF16), sds((all_rows, dim), F32), sds((2, 2, dim), F32), sds((dim, depth), BF16)]
        + ([sds(w_next.shape, BF16)] if more else []),
        [pltpu.VMEM((depth, dim), BF16), pltpu.VMEM((TM, depth), BF16)] + Share.scratch(2, 2, dim) + [TWO_DMA] + (Gather.scratch(n) if more else []),
        2 * all_rows * depth * dim, all_rows * (6 * depth + 4 * dim),
        (u, sums, gb, w_own, w_other) + ((w_next,) if more else ()))


def corr_grad(z, sums, lam, total):
    all_rows, dim = z.shape
    rows = all_rows // 2
    half = dim // 2
    quart = half // 2
    n_chunk = 8
    width = half // n_chunk
    pair = 2 * width
    mt = half
    zt = LANES
    ahead = 3
    lead = 3
    z_steps = all_rows // zt
    m_steps = rows // mt
    scale = 1.0 / total

    def kernel(z_ref, s_ref, lam_ref, zho_ref, d_ref, so_ref, lo_ref, zh, da, ck, r1, r2, g, stage, dsend, drecv, acc, got, ssem, rsem, loss_acc, loss_got, lsem, lrsem, zs, zos,
               d1s, d1r, s1s, s1r, s2s, s2r, a2s, a2r, a1s, a1r, ads, adr, dbs, das):
        share = Share(acc, got, ssem, rsem)
        share_loss = Share(loss_acc, loss_got, lsem, lrsem)
        here = coords()
        y, x, c = here
        on_x = c == 0
        by_core = lambda one, two: tuple(jnp.where(on_x, a, b) for a, b in zip(one, two))
        first = by_core(flip(here, X_PEER), flip(here, Y_PEER))
        second = by_core(flip(here, Y_PEER), flip(here, X_PEER))
        cpeer = flip(here, C_PEER)
        bit1, bit2 = by_core((x, y), (y, x))
        arrive()
        acc[...] = jnp.zeros_like(acc)
        loss_acc[...] = jnp.zeros_like(loss_acc)

        def load(i, slot):
            return pltpu.make_async_copy(z_ref.at[at(i, zt)], ck.at[at(slot, zt)], zs.at[slot])

        def zh_out(i):
            v, r = lax.div(i, n_chunk // 2), lax.rem(i, n_chunk // 2)
            return pltpu.make_async_copy(zh.at[v, at(r, TM)], zho_ref.at[v, at(r, TM)], zos.at[i])

        z_slots = half // zt
        for i in range(ahead):
            load(i, i).start()

        def normalise(i):
            slot = lax.rem(i, z_slots)
            v, r = lax.div(i, z_steps // 2), lax.rem(i, z_steps // 2)
            pl.when(i + ahead < z_steps)(lambda: load(i + ahead, lax.rem(i + ahead, z_slots)).start())
            load(i, slot).wait()
            mean, inv = mean_inv(s_ref[v], total)
            for k, cols in enumerate(runs(dim, LANES)):
                m, s = (t[:, k * LANES:(k + 1) * LANES] for t in (mean, inv))
                for p in range(zt // PIECE):
                    zh[v, at(r * (zt // PIECE) + p, PIECE), cols] = (
                        (ck[at(slot * (zt // PIECE) + p, PIECE), cols] - m) * s).astype(BF16)
            da[at(i, rows // z_steps)] = jnp.zeros((rows // z_steps, dim), F32)

        loop(z_steps, normalise)
        all_arrived()

        def both(v, rows_at, t):
            return jnp.concatenate([zh[v, rows_at, at(b * n_chunk + t, width)] for b in BOTH], axis=1)

        group = lambda t, b: at(2 * t + b, width)

        def to_core(t):
            return remote(dsend.at[odd(t)], drecv.at[odd(t)], d1s.at[t], d1r.at[t], cpeer)

        def to_first(t):
            return remote(ck.at[:, group(t, other(bit1))], r1.at[t], s1s.at[t], s1r.at[t], first)

        def to_second(t):
            return remote(ck.at[at(other(bit2), quart), group(t, bit1)], r2.at[t], s2s.at[t], s2r.at[t], second)

        def g_second(t, b):
            block = g.at[t, at(2 * c + b, quart), at(bit1, width)]
            return remote(block, block, a2s.at[t], a2r.at[t], second)

        def g_first(t, b):
            block = g.at[t, at(c, half), at(b, width)]
            return remote(block, block, a1s.at[t], a1r.at[t], first)

        def g_core(t, core):
            block = g.at[t, at(core, half)]
            return remote(block, block, ads.at[t], adr.at[t], cpeer)

        def chip_sum(t):
            to_core(t).wait_recv()
            to_core(t).wait_send()
            ck[:, at(t, pair)] += drecv[odd(t)]
            to_first(t).start()

        def corr_part(t):
            zh_out(t).start()
            right = both(1, pl.ds(0, rows), t)
            dsend[odd(t)] = mm_at(zh[0, :, at(other(c), half)], right)
            ck[:, at(t, pair)] = mm_at(zh[0, :, at(c, half)], right)
            to_core(t).start()

        def db_out(t, m, slot, b):
            return pltpu.make_async_copy(
                stage.at[slot, :, at(b, width)], d_ref.at[1, at(m, mt), at(b * n_chunk + t, width)], dbs.at[slot, b])

        def da_out(m):
            return pltpu.make_async_copy(da.at[at(m, mt)], d_ref.at[0, at(m, mt)], das.at[m])

        def finish(m):
            def scaled(cols):
                for p in range(mt // PIECE):
                    some = at(m * (mt // PIECE) + p, PIECE)
                    d = da[some, cols] * scale
                    da[some, cols] = d
                    yield d, d * zh[0, some, cols].astype(F32)

            for cols in runs(dim, LANES):
                acc[0, :, cols] += two_sums(scaled(cols))
            da_out(m).start()

        def grads(t):
            def rows_of(m):
                slot = odd(m)

                @pl.when(t * m_steps + m >= 2)
                def _():
                    for b in BOTH:
                        db_out(t, m, slot, b).wait()

                own = both(1, at(m, mt), t)
                stage[slot] = mm(zh[0, at(m, mt)], g[t]) * scale
                sums = two_sums((stage[slot, r], stage[slot, r] * both(1, at(m * (mt // PIECE) + p, PIECE), t).astype(F32))
                                for p, r in enumerate(runs(mt, PIECE)))
                for b in BOTH:
                    acc[1, :, at(b * n_chunk + t, width)] += sums[:, b * width:(b + 1) * width]
                    db_out(t, m, slot, b).start()
                for cols in runs(dim, LANES):
                    da[at(m, mt), cols] += mm_bt(own, g[t, cols])
                pl.when(t == n_chunk - 1)(lambda: finish(m))

            loop(m_steps, rows_of)

        def at_first(t):
            to_first(t).wait_recv()
            ck[:, group(t, bit1)] += r1[t]
            to_second(t).start()

        def at_second(t):
            to_second(t).wait_recv()
            corr_mat = (ck[at(bit2, quart), group(t, bit1)] + r2[t]) * scale
            row_ids = (2 * c + bit2) * quart + lax.broadcasted_iota(jnp.int32, (quart, width), 0)
            col_ids = (bit1 * n_chunk + t) * width + lax.broadcasted_iota(jnp.int32, (quart, width), 1)
            is_diag = row_ids == col_ids
            lam_val = lam_ref[0]
            loss = jnp.where(is_diag, (1.0 - corr_mat) * (1.0 - corr_mat), lam_val * corr_mat * corr_mat)
            loss_acc[0] += jnp.sum(loss, axis=0, keepdims=True)
            pl.when(t == n_chunk - 1)(lambda: share_loss.start(0))
            grad = jnp.where(is_diag, -2.0 * (1.0 - corr_mat), 2.0 * lam_val * corr_mat).astype(BF16)
            g[t, at(2 * c + bit2, quart), at(bit1, width)] = grad
            g_second(t, bit2).start()

        def back_second(t):
            g_second(t, other(bit2)).wait_recv()
            g_first(t, bit1).start()

        def back_first(t):
            g_first(t, other(bit1)).wait_recv()
            g_core(t, c).start()

        def back_core(t):
            g_core(t, other(c)).wait_recv()
            grads(t)

        def advance(tau):
            for lag, stage_fn in ((lead, at_first), (lead + 1, back_second), (lead + 2, back_first), (lead + 3, back_core),
                                  (lead, at_second), (1, chip_sum), (0, corr_part)):
                t = tau - lag
                pl.when(jnp.logical_and(t >= 0, t < n_chunk))(lambda t=t, stage_fn=stage_fn: stage_fn(t))

        loop(n_chunk + lead + 3, advance)
        share.start(1)
        share.start(0)
        for t in range(n_chunk):
            for copy in (to_first(t), to_second(t), g_second(t, bit2), g_first(t, bit1), g_core(t, c)):
                copy.wait_send()
        for b in BOTH:
            so_ref[b] = share.total(b)
            for slot in BOTH:
                db_out(0, 0, slot, b).wait()
        lo_ref[...] = share_loss.total(0)
        for i in range(n_chunk):
            zh_out(i).wait()
        for m in range(m_steps):
            da_out(m).wait()

    return call(
        kernel, "corr_grad", 3, (), [ANY, VMEM, pl.BlockSpec(memory_space=pltpu.SMEM)], [ANY, ANY, VMEM, VMEM],
        [sds((2, rows, dim), BF16), sds((2, rows, dim), F32), sds((2, 2, dim), F32), sds((1, width), F32)],
        [pltpu.VMEM((2, rows, dim), BF16), pltpu.VMEM((rows, dim), F32), pltpu.VMEM((half, dim), F32),
         pltpu.VMEM((n_chunk, half, width), F32), pltpu.VMEM((n_chunk, quart, width), F32),
         pltpu.VMEM((n_chunk, dim, pair), BF16), pltpu.VMEM((2, mt, pair), F32)]
        + [pltpu.VMEM((2, half, pair), F32)] * 2 + Share.scratch(2, 2, dim) + Share.scratch(1, 1, width)
        + [DMA((half // zt,)), DMA((n_chunk,))] + [DMA((n_chunk,))] * 12 + [DMA((2, 2)), DMA((m_steps,))],
        all_rows * dim * dim * 3, all_rows * dim * 12, (z, sums, lam))


def backward(d_emb, zh, sz, s_emb, layers, x2_t, total):
    all_rows, dim = zh.shape
    rows, half = all_rows // 2, dim // 2
    width = 256
    slabs = dim // width
    items = 2 * slabs
    piece = width
    side = half // 2 // piece
    per_slab = half // piece
    n_layer = len(layers) + 1
    n_slab = n_layer * slabs
    per_layer = slabs * side
    n_chunk = n_layer * per_layer
    ahead = 3
    (u2, s2, gb2, w3_t, x1_t), (u1, s1, gb1, w2_t, h_t) = layers

    def kernel(d_ref, zh_ref, sz_ref, sd_ref, x2_ref, x1_ref, h_ref, u2_ref, u1_ref, w3_ref, w2_ref,
               s2_ref, s1_ref, gb2_ref, gb1_ref, dw3_ref, dw2_ref, dw1_ref, sum_ref, dy_ref, part_ref, ry_ref, rx_ref,
               dbuf, xbuf, wbuf, ubuf, dybuf, dyout, psend, pkeep, dr, ebuf, mbuf, fbuf, acc, got, ssem, rsem,
               us, ws, ds, dos, xl, ps, pr, pm, ys, yr, xs, xr, es, fs, fcs, fcr, credit):
        share = Share(acc, got, ssem, rsem)
        here = coords()
        y, x, c = here
        ypeer, xpeer, cpeer = flip(here, Y_PEER), flip(here, X_PEER), flip(here, C_PEER)
        arrive()

        def column(k, n):
            model = odd(n + jnp.where(k == 0, other(y), 0))
            return jnp.where(k == 1, n, model * (slabs // 2) + lax.div(n, 2))

        def turn(k):
            return jnp.where(k == 0, 0, other(y))

        def m_slot(j):
            return lax.rem(j, 4)

        def copy(src, dst, sem):
            return pltpu.make_async_copy(src, dst, sem)

        def sent_by(q):
            first = jnp.minimum(per_slab * lax.div(q, 4), per_layer)
            middle = jnp.clip(side * lax.div(q - 2 * items - 2, 2), 0, per_layer)
            last = jnp.clip(per_slab * lax.div(q - 4 * items - 2, 4), 0, per_layer)
            return first + middle + last

        def begun(q):
            return jnp.maximum(lax.div(q - 6, 2), 0)

        def to_core(s):
            return remote(psend.at[odd(s)], dr.at[odd(s)], ps.at[s], pr.at[s], cpeer)

        def keep_out(s):
            return copy(pkeep.at[odd(s)], part_ref.at[s], pm)

        def chip_sum(s):
            to_core(s).wait_recv()
            pkeep[odd(s)] += dr[odd(s)]

            @pl.when(s + 2 < n_slab)
            def _():
                pl.semaphore_signal(credit, inc=1, device_id=device(cpeer), device_id_type=pl.DeviceIdType.MESH)

            to_core(s).wait_send()
            keep_out(s).start()

        def home(j, own):
            k = lax.div(j, per_layer)
            i = lax.rem(j, per_layer)
            model = y if own else other(y)
            turned = other(turn(k)) if own else turn(k)
            s = jnp.where(k == 1, lax.div(i, side), 2 * lax.div(i, per_slab) + turned)
            place = jnp.where(k == 1, model * side + lax.rem(i, side), lax.rem(i, per_slab))
            return part_ref.at[k * slabs + s, at(place, piece)]

        def to_y(j):
            return remote(home(j, False), ry_ref.at[j], ys.at[lax.div(j, per_layer)], yr.at[j], ypeer)

        def issue(s, q):
            keep_out(s).wait()
            k, n = lax.div(s, slabs), lax.rem(s, slabs)
            for mine, fire, first, count in (
                    (k == 1, True, n * side, side), (k != 1, odd(n) == jnp.where(k == 0, 0, 1), lax.div(n, 2) * per_slab, per_slab)):
                for r in range(count):
                    j = k * per_layer + first + r
                    pl.when(mine & fire & (j < begun(q) + ahead))(lambda j=j: to_y(j).start())

        def to_x(j):
            return remote(mbuf.at[m_slot(j)], rx_ref.at[j], xs.at[m_slot(j)], xr.at[j], xpeer)

        def result(j, k):
            i = lax.rem(j, per_layer)
            if k == 1:
                return dw2_ref.at[at(c * side + lax.rem(i, side), piece), at(lax.div(i, side), width)]
            return (dw1_ref if k else dw3_ref).at[at(c * per_slab + lax.rem(i, per_slab), piece), at(lax.div(i, per_slab), width)]

        def put(j, k):
            slot = odd(j)
            return (copy(fbuf.at[slot], result(j, k), fs.at[slot]),
                    remote(fbuf.at[slot], result(j, k), fcs.at[slot], fcr.at[k], cpeer))

        def put_done(j):
            here_copy, there_copy = put(j, 0)
            here_copy.wait()
            there_copy.wait_send()

        def load_part(j, which):
            src = (lambda: ry_ref.at[j], lambda: home(j, True), lambda: rx_ref.at[j])[which]()
            return copy(src, ebuf.at[which], es.at[which])

        def fetch_x(j):
            to_x(j).wait_recv()
            load_part(j, 2).start()

        def begin(j, q):
            remote(ry_ref.at[j], ry_ref.at[j], ys.at[0], yr.at[j], ypeer).wait_recv()
            load_part(j, 0).start()
            load_part(j, 1).start()
            pl.when(j + ahead < sent_by(q))(lambda: to_y(j + ahead).start())
            pl.when(j >= 2)(lambda: fetch_x(j - 2))

        def deliver(j):
            load_part(j, 2).wait()
            pl.when(j >= 2)(lambda: put_done(j))
            fbuf[odd(j)] = mbuf[m_slot(j)] + ebuf[2]
            for k in range(n_layer):
                @pl.when(lax.div(j, per_layer) == k)
                def _(k=k):
                    for one in put(j, k):
                        one.start()

        def end(j):
            load_part(j, 0).wait()
            load_part(j, 1).wait()
            pl.when(j >= 4)(lambda: to_x(j).wait_send())
            mbuf[m_slot(j)] = ebuf[0] + ebuf[1]
            to_x(j).start()
            pl.when(j >= 2)(lambda: deliver(j - 2))

        def events(q):
            now, before, earlier = begun(q), begun(q - 1), begun(q - 2)
            pl.when(before > earlier)(lambda: end(before - 1))
            pl.when(now > before)(lambda: begin(now - 1, q))

        def weight_slab(k, n, v, d):
            slot = odd(k * slabs + n)
            for buf, part in ((psend, other(c)), (pkeep, c)):
                first = jnp.where(k == 1, part, 2 * part)
                for b in BOTH:
                    left = xbuf[at(first + b * jnp.where(k == 1, 2, 1), half // 2), pl.ds(v * rows, rows)]
                    here_at = at(b, half // 2)
                    prod = mm(left, d)
                    buf[slot, here_at] = buf[slot, here_at] + prod if v else prod

        def after(k, n, v, q):
            s = k * slabs + n
            if v == 0:
                pl.when(n > 0)(lambda: chip_sum(s - 1))
            else:
                pl.when(s >= 2)(lambda: pl.semaphore_wait(credit, 1))
                to_core(s).start()
                pl.when(n > 0)(lambda: issue(s - 1, q))

        def dw_pass(k, q, ready, fetch, pre, ahead_of_next):
            def slab(n):
                for v in BOTH:
                    i = 2 * n + v
                    pl.when(i + 1 < items)(lambda: fetch(i + 1))
                    ready(i)
                    pl.when(n == 0)(lambda: x_load(x2_ref, v).wait())
                    events(q + i)
                    cols = at(column(k, n), width)
                    pre(v * rows, cols, v)
                    weight_slab(k, n, v, dbuf[pl.ds(v * rows, rows), cols])
                    after(k, n, v, q + i)
                pl.when(n == slabs - 1)(ahead_of_next)

            loop(slabs, slab)

        def emb_loads(i):
            n, v = split(i)
            cols = at(column(0, n), width)
            return (copy(d_ref.at[at(v, rows), cols], ubuf.at[v], us.at[v]),
                    copy(zh_ref.at[at(v, rows), cols], wbuf.at[v], ws.at[v]))

        def emb_fetch(i):
            for one in emb_loads(i):
                one.start()

        def emb_ready(i):
            for one in emb_loads(i):
                one.wait()

        def emb_pre(row, cols, v):
            _, inv = mean_inv(sz_ref[v, :, cols], total)
            sd = sd_ref[v, :, cols] / total
            for r in runs(rows, PIECE):
                dbuf[pl.ds(row + r.start, PIECE), cols] = (
                    inv * (ubuf[v, r] - sd[:1] - wbuf[v, r].astype(F32) * sd[1:])).astype(BF16)

        def x_load(src, v, rows_at=pl.ds(0, dim)):
            return copy(src.at[rows_at, at(v, rows)], xbuf.at[rows_at, at(v, rows)], xl.at[v])

        def u_slot(layer, v):
            return jnp.where(layer == 0, other(v), v)

        def slab_of(ref, layer, i, buf, sem, slot):
            n, v = split(i)
            return copy(ref.at[at(v, rows), at(column(layer + 1, n), width)], buf.at[slot], sem.at[slot])

        def u_load(layer, i, ref=u2_ref):
            return slab_of(ref, layer, i, ubuf, us, u_slot(layer, odd(i)))

        def dy_load(layer, i):
            return slab_of(dy_ref, layer, i, dybuf, ds, odd(i))

        def dy_out(layer, i):
            n, v = split(i)
            return copy(dyout.at[v], dy_ref.at[at(v, rows), at(column(layer + 1, n), width)], dos.at[v])

        def w_load(layer, n, ref=w3_ref):
            slot = odd(n + 1)
            return copy(ref.at[:, at(column(layer + 1, n), width)], wbuf.at[slot], ws.at[slot])

        def by_layer(layer, make, refs):
            for k, ref in enumerate(refs):
                pl.when(layer == k)(lambda ref=ref: make(ref).start())

        def start_u(layer, i):
            by_layer(layer, lambda ref: u_load(layer, i, ref), (u2_ref, u1_ref))

        def start_w(layer, n):
            by_layer(layer, lambda ref: w_load(layer, n, ref), (w3_ref, w2_ref))

        def next_layer(layer):
            start_u(layer, 0)
            start_w(layer, 0)

        for one in (x_load(x2_ref, 0), *emb_loads(0), x_load(x2_ref, 1)):
            one.start()
        all_arrived()
        dw_pass(0, 0, emb_ready, emb_fetch, emb_pre, lambda: next_layer(0))

        def stats(layer, v, cols):
            pick = lambda one, two: jnp.where(layer == 0, one, two)
            mean, inv = mean_inv(pick(s2_ref[v, :, cols], s1_ref[v, :, cols]), total)
            gb = pick(gb2_ref[:, cols], gb1_ref[:, cols])
            return mean, inv, gb[:1], gb[1:]

        def bn_layer(layer):
            start = (2 * layer + 1) * items

            def dx_item(i):
                n, v = split(i)
                slot = u_slot(layer, v)
                cols = at(column(layer + 1, n), width)

                @pl.when(i + 1 < items)
                def _():
                    start_u(layer, i + 1)
                    pl.when((v == 0) & (n + 1 < slabs))(lambda: start_w(layer, n + 1))

                @pl.when(i + 1 == items)
                def _():
                    start_u(layer, 0)
                    dy_load(layer, 0).start()

                u_load(layer, i).wait()
                pl.when(v == 0)(lambda: w_load(layer, n).wait())
                events(start + i)
                pl.when((i > 2) & (i < 11))(lambda: by_layer(
                    layer, lambda ref: x_load(ref, v, at(lax.div(i - 3, 2), half // 2)), (x1_ref, h_ref)))
                pl.when(n > 0)(lambda: dy_out(layer, i).wait())
                mean, inv, gamma, beta = stats(layer, v, cols)

                def pieces():
                    first = 0
                    for size in (rows // 2, 3 * rows // 8, rows // 8):
                        dx = mm(dbuf[pl.ds(pl.multiple_of(v * rows + first, LANES), size)], wbuf[odd(n + 1)])
                        for p in range(0, size, PIECE):
                            some = pl.ds(first + p, PIECE)
                            norm = (ubuf[slot, some] - mean) * inv
                            dy = jnp.where(norm * gamma + beta > 0, dx[p:p + PIECE], 0.0)
                            dyout[v, some] = dy
                            yield dy, dy * norm
                        first += size

                g = layer * items + i
                acc[g] = two_sums(pieces())
                dy_out(layer, i).start()
                share.start(g)
                before = (layer + 1) * slabs - 1
                pl.when(i == 0)(lambda: chip_sum(before))
                pl.when(i == 1)(lambda: issue(before, start + i))

            def fetch(i):
                start_u(layer, i)
                dy_load(layer, i).start()

            def ready(i):
                n, v = split(i)
                u_load(layer, i).wait()
                dy_load(layer, i).wait()
                sum_ref[layer, v, :, at(column(layer + 1, n), width)] = share.total(layer * items + i)

            def pre(row, cols, v):
                tot = sum_ref[layer, v, :, cols] / total
                mean, inv, gamma, _ = stats(layer, v, cols)
                slope, front, slot = inv * tot[1:], gamma * inv, u_slot(layer, v)
                for r in runs(rows, PIECE):
                    dbuf[pl.ds(row + r.start, PIECE), cols] = (
                        front * (dybuf[v, r] - (tot[:1] + (ubuf[slot, r] - mean) * slope))).astype(BF16)

            loop(items, dx_item)
            for v in BOTH:
                dy_out(layer, v).wait()
            dw_pass(layer + 1, start + items, ready, fetch, pre, lambda: pl.when(layer == 0)(lambda: next_layer(1)))

        loop(len(layers), bn_layer)

        ticks = (2 * n_layer - 1) * items
        chip_sum(n_slab - 1)
        issue(n_slab - 1, ticks)
        ended = 36

        def tail(j):
            begin(j, ticks + 2)
            end(j)

        loop(n_chunk, tail, ended)
        for j in range(n_chunk - 2, n_chunk):
            fetch_x(j)
            deliver(j)
        for j in BOTH:
            put_done(j)
        for k in range(n_layer):
            theirs = dw2_ref.at[at(other(c), half // 2)] if k == 1 else (dw1_ref if k else dw3_ref).at[at(other(c), half)]
            remote(theirs, theirs, fcs.at[0], fcr.at[k], cpeer).wait_recv()
            sent = ry_ref.at[at(k, per_layer)]
            remote(sent, sent, ys.at[k], yr.at[0], ypeer).wait_send()
        for j in range(n_chunk - 4, n_chunk):
            to_x(j).wait_send()

    n_item = len(layers) * items
    vm = lambda *shape: pltpu.VMEM(shape, F32)
    bf = lambda *shape: pltpu.VMEM(shape, BF16)
    outs = call(
        kernel, "backward", 4, (),
        [ANY, ANY, VMEM, VMEM] + [ANY] * 7 + [VMEM] * 4, [ANY] * 3 + [VMEM] + [ANY] * 4,
        [sds((dim, half), F32), sds((half, dim), F32), sds((dim, half), F32), sds((len(layers), 2, 2, dim), F32),
         sds((all_rows, dim), F32), sds((n_slab, half, width), F32), sds((n_chunk, piece, width), F32),
         sds((n_chunk, piece, width), F32)],
        [bf(all_rows, dim), bf(dim, all_rows), bf(2, dim, width), vm(2, rows, width), vm(2, rows, width), vm(2, rows, width),
         vm(2, half, width), vm(2, half, width), vm(2, half, width), vm(3, piece, width), vm(4, piece, width),
         vm(2, piece, width)] + Share.scratch(n_item, 2, width)
        + [TWO_DMA, TWO_DMA, TWO_DMA, TWO_DMA, TWO_DMA, DMA((n_slab,)), DMA((n_slab,)), DMA, DMA((n_layer,)),
           DMA((n_chunk,)), DMA((4,)), DMA((n_chunk,)), DMA((3,)), TWO_DMA, TWO_DMA, DMA((n_layer,)),
           pltpu.SemaphoreType.REGULAR],
        all_rows * dim * dim * 10, all_rows * dim * 40,
        (d_emb, zh, sz, s_emb, x2_t, x1_t, h_t, u2, u1, w3_t, w2_t, s2, s1, gb2, gb1))
    return outs[:n_layer + 1]


def settle(grads, sums, loss):
    steps = 4
    dim = sums.shape[-1]
    half = dim // 2

    def kernel(sum_ref, loss_ref, src3, src2, src1, g2_ref, b2_ref, g1_ref, b1_ref, total_ref, *dsts):
        for src, dst in zip((src3, src2, src1), dsts):
            dst[...] = src[...]

        @pl.when(pl.program_id(0) == 0)
        def _():
            y, _, _ = coords()
            for layer, (cols, g_ref, b_ref) in enumerate(((pl.ds(0, dim), g2_ref, b2_ref), (at(y, half), g1_ref, b1_ref))):
                both = jnp.sum(sum_ref[layer, :, :, cols], axis=0)
                g_ref[...] = both[1:]
                b_ref[...] = both[:1]
            total_ref[...] = jnp.sum(loss_ref[...], axis=1, keepdims=True)

    specs = [pl.BlockSpec((g.shape[0] // steps, g.shape[1]), lambda i: (i, 0)) for g in grads]
    small = [(1, n) for n in (dim, dim, half, half, 1)]
    return call(kernel, "settle", None, (steps,), [whole(*sums.shape), whole(*loss.shape)] + specs,
                [whole(*t) for t in small] + specs, [sds(t, F32) for t in small] + [sds(g.shape, F32) for g in grads], [], 0,
                sum(g.size for g in grads) * 8, (sums, loss, *grads))


def solution(mesh):
    def shard_body(h_a, h_b, w_one, w_two, w_three, g_one, b_one, g_two, b_two, lam_off):
        total = float(h_a.shape[0] * mesh.shape['data'])
        rowed = [t.reshape(1, -1) for t in (g_one, b_one, g_two, b_two)]
        u1, s1, gb1, gb2, w_two_o, h_t = fwd_first(h_a, h_b, w_one, w_two, *rowed)
        x1_t, u2, s2, w2_t, w_three_o = fwd_next(u1, s1, gb1, w_two, w_two_o, True, total, 1, w_three)
        x2_t, z, sz, w3_t = fwd_next(u2, s2, gb2, w_three, w_three_o, False, total, 2)
        zh, d_emb, s_emb, loss = corr_grad(z, sz, lam_off, total)
        *grads, sums = backward(
            d_emb.reshape(z.shape), zh.reshape(z.shape), sz, s_emb,
            ((u2, s2, gb2, w3_t, x1_t), (u1, s1, gb1, w2_t, h_t)), x2_t, total)
        *small, dw_three, dw_two, dw_one = settle(grads, sums, loss)
        dg_two, db_two, dg_one, db_one, loss = (t.reshape(-1) for t in small)
        return loss, dw_one, dw_two, dw_three, dg_one, db_one, dg_two, db_two

    in_specs = (P('data', None), P('data', None), P(None, 'model'), P('model', None), P(None, 'model'),
                P('model'), P('model'), P(), P(), P())
    out_specs = (P(), P(None, 'model'), P('model', None), P(None, 'model'), P('model'), P('model'), P(), P())
    return jax.shard_map(shard_body, mesh=mesh, in_specs=in_specs, out_specs=out_specs, check_vma=False)
```

```python
import functools

import jax
import jax.numpy as jnp
from jax import lax
from jax.experimental import pallas as pl
from jax.experimental.pallas import tpu as pltpu
from jax.sharding import PartitionSpec as P

BN_EPS = 1e-5
F32 = jnp.float32
BF16 = jnp.bfloat16
PIECE = 64
LANES = 256
SUBLANES = 8
TM = 512
MAX_VMEM = 67043328
ANY = pl.BlockSpec(memory_space=pl.ANY)
VMEM = pl.BlockSpec(memory_space=pltpu.VMEM)
DMA = pltpu.SemaphoreType.DMA
TWO_DMA = DMA((2,))
BOTH = (0, 1)
PEERS = [(ky, kx, kc) for ky in BOTH for kx in BOTH for kc in BOTH][1:]
C_PEER, X_PEER, Y_PEER = PEERS[0], PEERS[1], PEERS[3]
N_DEV = len(PEERS) + 1


def mm(left, right):
    return jnp.dot(left, right, preferred_element_type=F32)


def mm_bt(left, right):
    return lax.dot_general(left, right, (((1,), (1,)), ((), ())), preferred_element_type=F32)


def mm_at(left, right):
    return lax.dot_general(left, right, (((0,), (0,)), ((), ())), preferred_element_type=F32)


def other(p):
    return 1 - p


def odd(i):
    return lax.rem(i, 2)


def split(i):
    return lax.div(i, 2), odd(i)


def loop(n, body, start=0):
    def one(i, carry):
        body(i)
        return carry

    lax.fori_loop(start, n, one, 0)


def whole(*shape):
    return pl.BlockSpec(shape, lambda *_: (0,) * len(shape))


def at(i, n):
    return pl.ds(pl.multiple_of(i * n, n), n)


def sds(shape, dtype):
    return jax.ShapeDtypeStruct(shape, dtype)


def mean_inv(sums, total):
    mean = sums[:1] / total
    var = sums[1:2] / total - mean * mean
    return mean, lax.rsqrt(var + BN_EPS)


def fold(v):
    return jnp.sum(v.reshape(-1, SUBLANES, v.shape[1]), axis=0)


def runs(n, size):
    return [pl.ds(r, size) for r in range(0, n, size)]


def two_sums(pairs):
    one = two = 0.0
    for a, b in pairs:
        one, two = one + fold(a), two + fold(b)
    return jnp.concatenate([jnp.sum(t, axis=0, keepdims=True) for t in (one, two)], axis=0)


def moments(ref, cols):
    pieces = (ref[r, cols] for r in runs(ref.shape[0], PIECE))
    return two_sums((u, u * u) for u in pieces)


def coords():
    y, d = lax.axis_index('model'), lax.axis_index('data')
    return y, lax.div(d, 2), odd(d)


def flip(here, which):
    return tuple(other(p) if f else p for p, f in zip(here, which))


def flat(here):
    y, x, c = here
    return 4 * y + 2 * x + c


def device(here):
    y, x, c = here
    return (y, 2 * x + c)


def remote(src, dst, send_sem, recv_sem, there):
    return pltpu.make_async_remote_copy(
        src_ref=src, dst_ref=dst, send_sem=send_sem, recv_sem=recv_sem, device_id=device(there),
        device_id_type=pl.DeviceIdType.MESH)


def arrive():
    here = coords()
    for k in PEERS:
        pl.semaphore_signal(pltpu.get_barrier_semaphore(), inc=1, device_id=device(flip(here, k)),
                            device_id_type=pl.DeviceIdType.MESH)


def all_arrived():
    pl.semaphore_wait(pltpu.get_barrier_semaphore(), len(PEERS))


class Share:
    def __init__(self, acc, got, send_sem, recv_sem):
        self.acc, self.got, self.send_sem, self.recv_sem = acc, got, send_sem, recv_sem

    @staticmethod
    def scratch(n, *shape):
        return [pltpu.VMEM((n, *shape), F32), pltpu.VMEM((n, N_DEV, *shape), F32), DMA((n,)), DMA((n,))]

    def start(self, b):
        here = coords()
        me = flat(here)
        self.got[b, me] = self.acc[b]
        for which in PEERS:
            remote(self.acc.at[b], self.got.at[b, me], self.send_sem.at[b], self.recv_sem.at[b],
                   flip(here, which)).start()

    def total(self, b):
        all_of = self.got.at[b, pl.ds(0, len(PEERS))]
        copies = remote(all_of, all_of, self.send_sem.at[b], self.recv_sem.at[b], coords())
        copies.wait_send()
        copies.wait_recv()
        out = self.got[b, 0]
        for f in range(1, N_DEV):
            out += self.got[b, f]
        return out


class Gather:
    def __init__(self, own, dest, n, sems):
        self.own, self.dest, self.n = own, dest, n
        self.ys, self.yr, self.xs, self.xr, self.cs, self.cr = sems
        self.here = coords()
        _, x, c = self.here
        self.mine, self.across = 2 * x + c, 2 * (other(x)) + c
        self.core = (2 * x + other(c), 2 * (other(x)) + other(c))

    @staticmethod
    def scratch(n):
        return [DMA((n,))] * 4 + [DMA((2, n))] * 2

    def y(self, p):
        model = self.here[0]
        return remote(self.own(self.mine, p), self.dest(model, self.mine, p), self.ys.at[p], self.yr.at[p],
                      flip(self.here, Y_PEER))

    def moved(self, q, p, send_sem, recv_sem, which):
        ref = self.dest(1 - self.here[0], q, p)
        return remote(ref, ref, send_sem, recv_sem, flip(self.here, which))

    def x(self, p, q):
        return self.moved(q, p, self.xs.at[p], self.xr.at[p], X_PEER)

    def c(self, p, late, q):
        return self.moved(q, p, self.cs.at[late, p], self.cr.at[late, p], C_PEER)

    def start(self):
        for p in range(self.n):
            self.y(p).start()

    def pass_y(self, p):
        self.moved(self.mine, p, self.ys.at[p], self.yr.at[p], Y_PEER).wait_recv()
        self.x(p, self.mine).start()
        self.c(p, 0, self.mine).start()

    def pass_x(self, p):
        self.x(p, self.across).wait_recv()
        self.c(p, 1, self.across).start()

    def wait_core(self, late):
        for p in range(self.n):
            self.c(p, late, self.core[late]).wait_recv()

    def drain(self):
        for p in range(self.n):
            self.y(p).wait_send()
            self.x(p, self.mine).wait_send()
            self.c(p, 0, self.mine).wait_send()
            self.c(p, 1, self.across).wait_send()


def call(kernel, name, cid, grid, in_specs, out_specs, out_shape, scratch, flops, nbytes, args):
    return pl.pallas_call(
        kernel, name=name, grid=grid, in_specs=in_specs, out_specs=out_specs, out_shape=out_shape, scratch_shapes=scratch,
        compiler_params=pltpu.CompilerParams(vmem_limit_bytes=MAX_VMEM, collective_id=cid, has_side_effects=cid is not None),
        cost_estimate=pl.CostEstimate(flops=flops, bytes_accessed=nbytes, transcendentals=0))(*args)


def fwd_first(h_a, h_b, w_one, w_two, *vectors):
    depth, half = w_one.shape
    dim = 2 * half
    rows = h_a.shape[0] // 2
    tile, width, quarter = 2 * TM, half // 2, half // 4
    steps = rows // tile
    per_block = 2 * steps
    n, n2 = 4, 8

    def block(j):
        y, x, _ = coords()
        return jnp.where(j < 2, 2 * y + j, 2 * (other(y)) + jnp.where(j == 2, x, other(x)))

    def tile_of(j, i):
        return jnp.where(odd(j) == 0, i, per_block - 1 - i)

    def kernel(ha_ref, hb_ref, w_ref, w2_ref, g1_ref, b1_ref, g2_ref, b2_ref, u_ref, s_ref, gbo_ref, gb2_ref, w2o_ref, ht_ref,
               w1, gbf, *sems):
        share, sems = Share(*sems[:4]), sems[4:]
        gs, gr, lsem = sems[:3]
        sems = sems[3:]
        j, i = pl.program_id(0), pl.program_id(1)
        step = j * per_block + i
        here = coords()
        y = here[0]
        one = Gather(lambda q, p: w_ref.at[at(p, depth // n), at(q, quarter)],
                     lambda m, q, p: w1.at[at(p, depth // n), at(m * 4 + q, quarter)], n, sems[:6])
        two = Gather(lambda q, p: w2_ref.at[at(q * n2 + p, quarter // n2)],
                     lambda m, q, p: w2o_ref.at[at(q * n2 + p, quarter // n2)], n2, sems[6:])

        def local(b):
            return pltpu.make_async_copy(w_ref.at[:, at(b, width)], w1.at[:, at(2 * y + b, width)], lsem.at[b])

        def bn_vectors(m):
            return remote(gbf.at[:, at(m, half)], gbf.at[:, at(m, half)], gs, gr, flip(here, Y_PEER))

        def begin():
            arrive()
            local(0).start()
            local(1).start()
            all_arrived()
            one.start()
            two.start()
            for r, (one_ref, two_ref) in enumerate(((g1_ref, g2_ref), (b1_ref, b2_ref))):
                row = pl.ds(r, 1)
                gbf[row, at(y, half)] = one_ref[...]
                gb2_ref[row] = two_ref[...]
            local(0).wait()

        def late_half():
            one.pass_x(0)
            one.pass_y(n - 1)
            one.wait_core(0)

        hooks = [(0, begin), (1, lambda: bn_vectors(y).start()), (per_block, lambda: local(1).wait()), (2 * per_block, late_half)]
        hooks += [(2 * p + 3, functools.partial(one.pass_y, p)) for p in range(n - 1)]
        hooks += [(p + 2 * per_block, functools.partial(one.pass_x, p)) for p in range(1, n)]
        hooks += [(3 * per_block, lambda: one.wait_core(1))]
        hooks += [(p + 9, functools.partial(two.pass_y, p)) for p in range(n2 - 1)]
        hooks += [(13 + (p + 1) // 2, functools.partial(two.pass_x, p)) for p in range(n2 // 2)]
        for s, hook in hooks:
            pl.when(step == s)(hook)
        for b in range(3):
            pl.when(step == (b + 1) * per_block)(lambda b=b: share.start(block(b)))

        tile_at = tile_of(j, i)
        first_view = tile_at < steps
        cols = at(j, width)
        ht_ref[...] = lax.select(first_view, ha_ref[:, cols], hb_ref[:, cols]).T
        for r in runs(tile, TM):
            u_ref[r] = mm(lax.select(first_view, ha_ref[r], hb_ref[r]), w1[:, at(block(j), width)])
        sums = jnp.concatenate([moments(u_ref, cols) for cols in runs(width, LANES)], axis=1)
        v = tile_at // steps
        share.acc[block(j), v] = jnp.where(i % steps == 0, 0.0, share.acc[block(j), v]) + sums

        @pl.when(step == 4 * per_block - 1)
        def _():
            share.start(block(3))
            two.pass_y(n2 - 1)
            for p in range(n2 // 2, n2):
                two.pass_x(p)
            bn_vectors(other(y)).wait_recv()
            bn_vectors(y).wait_send()
            gbo_ref[...] = gbf[...]
            for b in range(4):
                s_ref[:, :, b * width:(b + 1) * width] = share.total(b)
            one.drain()
            two.drain()
            two.wait_core(0)
            two.wait_core(1)

    return call(
        kernel, "fwd_first", 0, (4, per_block),
        [pl.BlockSpec((tile, depth), lambda j, i: (coords()[0] * steps + jnp.minimum(tile_of(j, i), steps - 1), 0)),
         pl.BlockSpec((tile, depth), lambda j, i: (coords()[0] * steps + jnp.maximum(tile_of(j, i) - steps, 0), 0)),
         ANY, ANY] + [whole(*t.shape) for t in vectors],
        [pl.BlockSpec((tile, width), lambda j, i: (tile_of(j, i), block(j))), whole(2, 2, dim),
         whole(2, dim), whole(2, dim), ANY, pl.BlockSpec((width, tile), lambda j, i: (j, tile_of(j, i)))],
        [sds((2 * rows, dim), F32), sds((2, 2, dim), F32), sds((2, dim), F32), sds((2, dim), F32),
         sds((half, dim), BF16), sds((depth, 2 * rows), BF16)],
        [pltpu.VMEM((depth, dim), BF16), pltpu.VMEM((2, dim), F32)] + Share.scratch(4, 2, 2, width)
        + [DMA, DMA, TWO_DMA] + Gather.scratch(n) + Gather.scratch(n2),
        4 * rows * depth * dim, 2 * rows * (8 * depth + 4 * dim), (h_a, h_b, w_one, w_two, *vectors))


def fwd_next(u, sums, gb, w_own, w_other, by_rows, total, cid, w_next=None):
    all_rows, depth = u.shape
    dim = w_own.shape[1] if by_rows else 2 * w_own.shape[1]
    half = dim // 2
    quarter = half // 4
    steps = all_rows // 2 // TM
    last = 2 * steps - 1
    slab = dim // (2 * steps)
    n = 4
    more = w_next is not None

    def kernel(u_ref, s_ref, gb_ref, wo_ref, wt_ref, *refs):
        if more:
            wn_ref, refs = refs[0], refs[1:]
        x_ref, o_ref, so_ref, wtr_ref, *refs = refs
        if more:
            wno_ref, *refs = refs
        w, act, acc, got, ssem, rsem, lsem, *refs = refs
        share = Share(acc, got, ssem, rsem)
        i = pl.program_id(0)
        y = coords()[0]

        def local(ref, model, b):
            where = at(model, half)
            return pltpu.make_async_copy(ref, w.at[where] if by_rows else w.at[:, where], lsem.at[b])

        if more:
            gather = Gather(lambda q, p: wn_ref.at[at(p, depth // n), at(q, quarter)],
                            lambda m, q, p: wno_ref.at[at(p, depth // n), at(q, quarter)], n, refs)

        @pl.when(i == 0)
        def _():
            arrive()
            acc[...] = jnp.zeros_like(acc)
            local(wo_ref, y, 0).start()
            local(wt_ref, other(y), 1).start()
            all_arrived()
            if more:
                gather.start()
            local(wo_ref, y, 0).wait()
            local(wt_ref, other(y), 1).wait()

        if more:
            for p in range(n):
                pl.when(i == p + 2)(lambda p=p: gather.pass_y(p))
                pl.when(i == p + 4)(lambda p=p: gather.pass_x(p))
        pl.when(i == steps)(lambda: share.start(0))

        mean, inv = mean_inv(s_ref[0], total)
        for k, cols in enumerate(runs(depth, LANES)):
            m, r, g, b = (t[:, k * LANES:(k + 1) * LANES] for t in (mean, inv, gb_ref[:1], gb_ref[1:]))
            for piece in runs(TM, PIECE):
                act[piece, cols] = jnp.maximum((u_ref[piece, cols] - m) * r * g + b, 0.0).astype(BF16)
        x_ref[...] = act[...].T
        wtr_ref[...] = w[:, at(i, slab)].T
        v = i // steps
        keep = jnp.where(i % steps == 0, 0.0, 1.0)
        for some in runs(dim, TM):
            o_ref[:, some] = mm(act[...], w[:, some])
            for cols in runs(TM, LANES):
                cols = pl.ds(some.start + cols.start, LANES)
                share.acc[v, :, cols] = keep * share.acc[v, :, cols] + moments(o_ref, cols)

        @pl.when(i == last)
        def _():
            share.start(1)
            for b in BOTH:
                so_ref[b] = share.total(b)
            if more:
                gather.drain()
                gather.wait_core(0)
                gather.wait_core(1)

    return call(
        kernel, "fwd_next", cid, (2 * steps,),
        [pl.BlockSpec((TM, depth), lambda i: (i, 0)), pl.BlockSpec((1, 2, depth), lambda i: (i // steps, 0, 0)),
         whole(2, depth), ANY, ANY] + [ANY] * more,
        [pl.BlockSpec((depth, TM), lambda i: (0, i)), pl.BlockSpec((TM, dim), lambda i: (i, 0)),
         whole(2, 2, dim), pl.BlockSpec((slab, depth), lambda i: (i, 0))] + [ANY] * more,
        [sds((depth, all_rows), BF16), sds((all_rows, dim), F32), sds((2, 2, dim), F32), sds((dim, depth), BF16)]
        + ([sds(w_next.shape, BF16)] if more else []),
        [pltpu.VMEM((depth, dim), BF16), pltpu.VMEM((TM, depth), BF16)] + Share.scratch(2, 2, dim) + [TWO_DMA] + (Gather.scratch(n) if more else []),
        2 * all_rows * depth * dim, all_rows * (6 * depth + 4 * dim),
        (u, sums, gb, w_own, w_other) + ((w_next,) if more else ()))


def corr_grad(z, sums, lam, total):
    all_rows, dim = z.shape
    rows = all_rows // 2
    half = dim // 2
    quart = half // 2
    n_chunk = 8
    width = half // n_chunk
    pair = 2 * width
    mt = half
    zt = LANES
    ahead = 3
    lead = 3
    z_steps = all_rows // zt
    m_steps = rows // mt
    scale = 1.0 / total

    def kernel(z_ref, s_ref, lam_ref, zho_ref, d_ref, so_ref, lo_ref, zh, da, ck, r1, r2, g, stage, dsend, drecv, acc, got, ssem, rsem, loss_acc, loss_got, lsem, lrsem, zs, zos,
               d1s, d1r, s1s, s1r, s2s, s2r, a2s, a2r, a1s, a1r, ads, adr, dbs, das):
        share = Share(acc, got, ssem, rsem)
        share_loss = Share(loss_acc, loss_got, lsem, lrsem)
        here = coords()
        y, x, c = here
        on_x = c == 0
        by_core = lambda one, two: tuple(jnp.where(on_x, a, b) for a, b in zip(one, two))
        first = by_core(flip(here, X_PEER), flip(here, Y_PEER))
        second = by_core(flip(here, Y_PEER), flip(here, X_PEER))
        cpeer = flip(here, C_PEER)
        bit1, bit2 = by_core((x, y), (y, x))
        arrive()
        acc[...] = jnp.zeros_like(acc)
        loss_acc[...] = jnp.zeros_like(loss_acc)

        def load(i, slot):
            return pltpu.make_async_copy(z_ref.at[at(i, zt)], ck.at[at(slot, zt)], zs.at[slot])

        def zh_out(i):
            v, r = lax.div(i, n_chunk // 2), lax.rem(i, n_chunk // 2)
            return pltpu.make_async_copy(zh.at[v, at(r, TM)], zho_ref.at[v, at(r, TM)], zos.at[i])

        z_slots = half // zt
        for i in range(ahead):
            load(i, i).start()

        def normalise(i):
            slot = lax.rem(i, z_slots)
            v, r = lax.div(i, z_steps // 2), lax.rem(i, z_steps // 2)
            pl.when(i + ahead < z_steps)(lambda: load(i + ahead, lax.rem(i + ahead, z_slots)).start())
            load(i, slot).wait()
            mean, inv = mean_inv(s_ref[v], total)
            for k, cols in enumerate(runs(dim, LANES)):
                m, s = (t[:, k * LANES:(k + 1) * LANES] for t in (mean, inv))
                for p in range(zt // PIECE):
                    zh[v, at(r * (zt // PIECE) + p, PIECE), cols] = (
                        (ck[at(slot * (zt // PIECE) + p, PIECE), cols] - m) * s).astype(BF16)
            da[at(i, rows // z_steps)] = jnp.zeros((rows // z_steps, dim), F32)

        loop(z_steps, normalise)
        all_arrived()

        def both(v, rows_at, t):
            return jnp.concatenate([zh[v, rows_at, at(b * n_chunk + t, width)] for b in BOTH], axis=1)

        group = lambda t, b: at(2 * t + b, width)

        def to_core(t):
            return remote(dsend.at[odd(t)], drecv.at[odd(t)], d1s.at[t], d1r.at[t], cpeer)

        def to_first(t):
            return remote(ck.at[:, group(t, other(bit1))], r1.at[t], s1s.at[t], s1r.at[t], first)

        def to_second(t):
            return remote(ck.at[at(other(bit2), quart), group(t, bit1)], r2.at[t], s2s.at[t], s2r.at[t], second)

        def g_second(t, b):
            block = g.at[t, at(2 * c + b, quart), at(bit1, width)]
            return remote(block, block, a2s.at[t], a2r.at[t], second)

        def g_first(t, b):
            block = g.at[t, at(c, half), at(b, width)]
            return remote(block, block, a1s.at[t], a1r.at[t], first)

        def g_core(t, core):
            block = g.at[t, at(core, half)]
            return remote(block, block, ads.at[t], adr.at[t], cpeer)

        def chip_sum(t):
            to_core(t).wait_recv()
            to_core(t).wait_send()
            ck[:, at(t, pair)] += drecv[odd(t)]
            to_first(t).start()

        def corr_part(t):
            zh_out(t).start()
            right = both(1, pl.ds(0, rows), t)
            dsend[odd(t)] = mm_at(zh[0, :, at(other(c), half)], right)
            ck[:, at(t, pair)] = mm_at(zh[0, :, at(c, half)], right)
            to_core(t).start()

        def db_out(t, m, slot, b):
            return pltpu.make_async_copy(
                stage.at[slot, :, at(b, width)], d_ref.at[1, at(m, mt), at(b * n_chunk + t, width)], dbs.at[slot, b])

        def da_out(m):
            return pltpu.make_async_copy(da.at[at(m, mt)], d_ref.at[0, at(m, mt)], das.at[m])

        def finish(m):
            def scaled(cols):
                for p in range(mt // PIECE):
                    some = at(m * (mt // PIECE) + p, PIECE)
                    d = da[some, cols] * scale
                    da[some, cols] = d
                    yield d, d * zh[0, some, cols].astype(F32)

            for cols in runs(dim, LANES):
                acc[0, :, cols] += two_sums(scaled(cols))
            da_out(m).start()

        def grads(t):
            def rows_of(m):
                slot = odd(m)

                @pl.when(t * m_steps + m >= 2)
                def _():
                    for b in BOTH:
                        db_out(t, m, slot, b).wait()

                own = both(1, at(m, mt), t)
                stage[slot] = mm(zh[0, at(m, mt)], g[t]) * scale
                sums = two_sums((stage[slot, r], stage[slot, r] * both(1, at(m * (mt // PIECE) + p, PIECE), t).astype(F32))
                                for p, r in enumerate(runs(mt, PIECE)))
                for b in BOTH:
                    acc[1, :, at(b * n_chunk + t, width)] += sums[:, b * width:(b + 1) * width]
                    db_out(t, m, slot, b).start()
                pl.when((t == n_chunk - 1) & (m == m_steps - 1))(lambda: share.start(1))
                for cols in runs(dim, LANES):
                    da[at(m, mt), cols] += mm_bt(own, g[t, cols])
                pl.when(t == n_chunk - 1)(lambda: finish(m))

            loop(m_steps, rows_of)

        def at_first(t):
            to_first(t).wait_recv()
            ck[:, group(t, bit1)] += r1[t]
            to_second(t).start()

        def at_second(t):
            to_second(t).wait_recv()
            corr_mat = (ck[at(bit2, quart), group(t, bit1)] + r2[t]) * scale
            row_ids = (2 * c + bit2) * quart + lax.broadcasted_iota(jnp.int32, (quart, width), 0)
            col_ids = (bit1 * n_chunk + t) * width + lax.broadcasted_iota(jnp.int32, (quart, width), 1)
            is_diag = row_ids == col_ids
            lam_val = lam_ref[0]
            loss = jnp.where(is_diag, (1.0 - corr_mat) * (1.0 - corr_mat), lam_val * corr_mat * corr_mat)
            loss_acc[0] += jnp.sum(loss, axis=0, keepdims=True)
            pl.when(t == n_chunk - 1)(lambda: share_loss.start(0))
            grad = jnp.where(is_diag, -2.0 * (1.0 - corr_mat), 2.0 * lam_val * corr_mat).astype(BF16)
            g[t, at(2 * c + bit2, quart), at(bit1, width)] = grad
            g_second(t, bit2).start()

        def back_second(t):
            g_second(t, other(bit2)).wait_recv()
            g_first(t, bit1).start()

        def back_first(t):
            g_first(t, other(bit1)).wait_recv()
            g_core(t, c).start()

        def back_core(t):
            g_core(t, other(c)).wait_recv()
            grads(t)

        def advance(tau):
            for lag, stage_fn in ((lead, at_first), (lead + 1, back_second), (lead + 2, back_first), (lead + 3, back_core),
                                  (lead, at_second), (1, chip_sum), (0, corr_part)):
                t = tau - lag
                pl.when(jnp.logical_and(t >= 0, t < n_chunk))(lambda t=t, stage_fn=stage_fn: stage_fn(t))

        loop(n_chunk + lead + 3, advance)
        share.start(0)
        for t in range(n_chunk):
            for copy in (to_first(t), to_second(t), g_second(t, bit2), g_first(t, bit1), g_core(t, c)):
                copy.wait_send()
        for b in BOTH:
            so_ref[b] = share.total(b)
            for slot in BOTH:
                db_out(0, 0, slot, b).wait()
        lo_ref[...] = share_loss.total(0)
        for i in range(n_chunk):
            zh_out(i).wait()
        for m in range(m_steps):
            da_out(m).wait()

    return call(
        kernel, "corr_grad", 3, (), [ANY, VMEM, pl.BlockSpec(memory_space=pltpu.SMEM)], [ANY, ANY, VMEM, VMEM],
        [sds((2, rows, dim), BF16), sds((2, rows, dim), F32), sds((2, 2, dim), F32), sds((1, width), F32)],
        [pltpu.VMEM((2, rows, dim), BF16), pltpu.VMEM((rows, dim), F32), pltpu.VMEM((half, dim), F32),
         pltpu.VMEM((n_chunk, half, width), F32), pltpu.VMEM((n_chunk, quart, width), F32),
         pltpu.VMEM((n_chunk, dim, pair), BF16), pltpu.VMEM((2, mt, pair), F32)]
        + [pltpu.VMEM((2, half, pair), F32)] * 2 + Share.scratch(2, 2, dim) + Share.scratch(1, 1, width)
        + [DMA((half // zt,)), DMA((n_chunk,))] + [DMA((n_chunk,))] * 12 + [DMA((2, 2)), DMA((m_steps,))],
        all_rows * dim * dim * 3, all_rows * dim * 12, (z, sums, lam))


def backward(d_emb, zh, sz, s_emb, layers, x2_t, total):
    all_rows, dim = zh.shape
    rows, half = all_rows // 2, dim // 2
    width = 256
    slabs = dim // width
    items = 2 * slabs
    piece = width
    side = half // 2 // piece
    per_slab = half // piece
    n_layer = len(layers) + 1
    n_slab = n_layer * slabs
    per_layer = slabs * side
    n_chunk = n_layer * per_layer
    ahead = 3
    n_mid = 4
    (u2, s2, gb2, w3_t, x1_t), (u1, s1, gb1, w2_t, h_t) = layers

    def kernel(d_ref, zh_ref, sz_ref, sd_ref, x2_ref, x1_ref, h_ref, u2_ref, u1_ref, w3_ref, w2_ref,
               s2_ref, s1_ref, gb2_ref, gb1_ref, dw3_ref, dw2_ref, dw1_ref, sum_ref, dy_ref, part_ref, ry_ref, rx_ref,
               dbuf, xbuf, wbuf, ubuf, dybuf, dyout, psend, pkeep, dr, ebuf, mbuf, fbuf, acc, got, ssem, rsem,
               us, ws, ds, dos, xl, ps, pr, pm, ys, yr, xs, xr, es, fs, fcs, fcr, credit):
        share = Share(acc, got, ssem, rsem)
        here = coords()
        y, x, c = here
        ypeer, xpeer, cpeer = flip(here, Y_PEER), flip(here, X_PEER), flip(here, C_PEER)
        arrive()

        def column(k, n):
            model = odd(n + jnp.where(k == 0, other(y), 0))
            return jnp.where(k == 1, n, model * (slabs // 2) + lax.div(n, 2))

        def turn(k):
            return jnp.where(k == 0, 0, other(y))

        def m_slot(j):
            return lax.rem(j, n_mid)

        def copy(src, dst, sem):
            return pltpu.make_async_copy(src, dst, sem)

        def sent_by(q):
            first = jnp.minimum(per_slab * lax.div(q, 4), per_layer)
            middle = jnp.clip(side * lax.div(q - 2 * items - 2, 2), 0, per_layer)
            last = jnp.clip(per_slab * lax.div(q - 4 * items - 2, 4), 0, per_layer)
            return first + middle + last

        def begun(q):
            return jnp.maximum(lax.div(q - 5, 2), 0)

        def to_core(s):
            return remote(psend.at[odd(s)], dr.at[odd(s)], ps.at[s], pr.at[s], cpeer)

        def keep_out(s):
            return copy(pkeep.at[odd(s)], part_ref.at[s], pm)

        def chip_sum(s):
            to_core(s).wait_recv()
            pkeep[odd(s)] += dr[odd(s)]

            @pl.when(s + 2 < n_slab)
            def _():
                pl.semaphore_signal(credit, inc=1, device_id=device(cpeer), device_id_type=pl.DeviceIdType.MESH)

            to_core(s).wait_send()
            keep_out(s).start()

        def home(j, own):
            k = lax.div(j, per_layer)
            i = lax.rem(j, per_layer)
            model = y if own else other(y)
            turned = other(turn(k)) if own else turn(k)
            s = jnp.where(k == 1, lax.div(i, side), 2 * lax.div(i, per_slab) + turned)
            place = jnp.where(k == 1, model * side + lax.rem(i, side), lax.rem(i, per_slab))
            return part_ref.at[k * slabs + s, at(place, piece)]

        def to_y(j):
            return remote(home(j, False), ry_ref.at[j], ys.at[lax.div(j, per_layer)], yr.at[j], ypeer)

        def issue(s, q):
            keep_out(s).wait()
            k, n = lax.div(s, slabs), lax.rem(s, slabs)
            for mine, fire, first, count in (
                    (k == 1, True, n * side, side), (k != 1, odd(n) == jnp.where(k == 0, 0, 1), lax.div(n, 2) * per_slab, per_slab)):
                for r in range(count):
                    j = k * per_layer + first + r
                    pl.when(mine & fire & (j < begun(q) + ahead))(lambda j=j: to_y(j).start())

        def to_x(j):
            return remote(mbuf.at[m_slot(j)], rx_ref.at[j], xs.at[m_slot(j)], xr.at[j], xpeer)

        def result(j, k):
            i = lax.rem(j, per_layer)
            if k == 1:
                return dw2_ref.at[at(c * side + lax.rem(i, side), piece), at(lax.div(i, side), width)]
            return (dw1_ref if k else dw3_ref).at[at(c * per_slab + lax.rem(i, per_slab), piece), at(lax.div(i, per_slab), width)]

        def put(j, k):
            slot = odd(j)
            return (copy(fbuf.at[slot], result(j, k), fs.at[slot]),
                    remote(fbuf.at[slot], result(j, k), fcs.at[slot], fcr.at[k], cpeer))

        def put_done(j):
            here_copy, there_copy = put(j, 0)
            here_copy.wait()
            there_copy.wait_send()

        def load_part(j, which):
            src = (lambda: ry_ref.at[j], lambda: home(j, True), lambda: rx_ref.at[j])[which]()
            return copy(src, ebuf.at[which], es.at[which])

        def fetch_x(j):
            to_x(j).wait_recv()
            load_part(j, 2).start()

        def begin(j, q):
            remote(ry_ref.at[j], ry_ref.at[j], ys.at[0], yr.at[j], ypeer).wait_recv()
            load_part(j, 0).start()
            load_part(j, 1).start()
            pl.when(j + ahead < sent_by(q))(lambda: to_y(j + ahead).start())
            pl.when(j >= 2)(lambda: fetch_x(j - 2))

        def deliver(j):
            load_part(j, 2).wait()
            pl.when(j >= 2)(lambda: put_done(j))
            fbuf[odd(j)] = mbuf[m_slot(j)] + ebuf[2]
            for k in range(n_layer):
                @pl.when(lax.div(j, per_layer) == k)
                def _(k=k):
                    for one in put(j, k):
                        one.start()

        def end(j):
            load_part(j, 0).wait()
            load_part(j, 1).wait()
            pl.when(j >= n_mid)(lambda: to_x(j).wait_send())
            mbuf[m_slot(j)] = ebuf[0] + ebuf[1]
            to_x(j).start()
            pl.when(j >= 2)(lambda: deliver(j - 2))

        def events(q):
            now, before, earlier = begun(q), begun(q - 1), begun(q - 2)
            pl.when(before > earlier)(lambda: end(before - 1))
            pl.when(now > before)(lambda: begin(now - 1, q))

        def weight_slab(k, n, v, d):
            slot = odd(k * slabs + n)
            for buf, part in ((psend, other(c)), (pkeep, c)):
                first = jnp.where(k == 1, part, 2 * part)
                for b in BOTH:
                    left = xbuf[at(first + b * jnp.where(k == 1, 2, 1), half // 2), pl.ds(v * rows, rows)]
                    here_at = at(b, half // 2)
                    prod = mm(left, d)
                    buf[slot, here_at] = buf[slot, here_at] + prod if v else prod

        def after(k, n, v, q):
            s = k * slabs + n
            if v == 0:
                pl.when(n > 0)(lambda: chip_sum(s - 1))
            else:
                pl.when(s >= 2)(lambda: pl.semaphore_wait(credit, 1))
                to_core(s).start()
                pl.when(n > 0)(lambda: issue(s - 1, q))

        def dw_pass(k, q, ready, fetch, pre, ahead_of_next):
            def slab(n):
                for v in BOTH:
                    i = 2 * n + v
                    pl.when(i + 1 < items)(lambda: fetch(i + 1))
                    ready(i)
                    pl.when(n == 0)(lambda: x_load(x2_ref, v).wait())
                    events(q + i)
                    cols = at(column(k, n), width)
                    pre(v * rows, cols, v)
                    weight_slab(k, n, v, dbuf[pl.ds(v * rows, rows), cols])
                    after(k, n, v, q + i)
                pl.when(n == slabs - 1)(ahead_of_next)

            loop(slabs, slab)

        def emb_loads(i):
            n, v = split(i)
            cols = at(column(0, n), width)
            return (copy(d_ref.at[at(v, rows), cols], ubuf.at[v], us.at[v]),
                    copy(zh_ref.at[at(v, rows), cols], wbuf.at[v], ws.at[v]))

        def emb_fetch(i):
            for one in emb_loads(i):
                one.start()

        def emb_ready(i):
            for one in emb_loads(i):
                one.wait()

        def emb_pre(row, cols, v):
            _, inv = mean_inv(sz_ref[v, :, cols], total)
            sd = sd_ref[v, :, cols] / total
            for r in runs(rows, PIECE):
                dbuf[pl.ds(row + r.start, PIECE), cols] = (
                    inv * (ubuf[v, r] - sd[:1] - wbuf[v, r].astype(F32) * sd[1:])).astype(BF16)

        def x_load(src, v, rows_at=pl.ds(0, dim)):
            return copy(src.at[rows_at, at(v, rows)], xbuf.at[rows_at, at(v, rows)], xl.at[v])

        def u_slot(layer, v):
            return jnp.where(layer == 0, other(v), v)

        def slab_of(ref, layer, i, buf, sem, slot):
            n, v = split(i)
            return copy(ref.at[at(v, rows), at(column(layer + 1, n), width)], buf.at[slot], sem.at[slot])

        def u_load(layer, i, ref=u2_ref):
            return slab_of(ref, layer, i, ubuf, us, u_slot(layer, odd(i)))

        def dy_load(layer, i):
            return slab_of(dy_ref, layer, i, dybuf, ds, odd(i))

        def dy_out(layer, i):
            n, v = split(i)
            return copy(dyout.at[v], dy_ref.at[at(v, rows), at(column(layer + 1, n), width)], dos.at[v])

        def w_load(layer, n, ref=w3_ref):
            slot = odd(n + 1)
            return copy(ref.at[:, at(column(layer + 1, n), width)], wbuf.at[slot], ws.at[slot])

        def by_layer(layer, make, refs):
            for k, ref in enumerate(refs):
                pl.when(layer == k)(lambda ref=ref: make(ref).start())

        def start_u(layer, i):
            by_layer(layer, lambda ref: u_load(layer, i, ref), (u2_ref, u1_ref))

        def start_w(layer, n):
            by_layer(layer, lambda ref: w_load(layer, n, ref), (w3_ref, w2_ref))

        def next_layer(layer):
            start_u(layer, 0)
            start_w(layer, 0)

        for one in (x_load(x2_ref, 0), *emb_loads(0), x_load(x2_ref, 1)):
            one.start()
        all_arrived()
        dw_pass(0, 0, emb_ready, emb_fetch, emb_pre, lambda: next_layer(0))

        def stats(layer, v, cols):
            pick = lambda one, two: jnp.where(layer == 0, one, two)
            mean, inv = mean_inv(pick(s2_ref[v, :, cols], s1_ref[v, :, cols]), total)
            gb = pick(gb2_ref[:, cols], gb1_ref[:, cols])
            return mean, inv, gb[:1], gb[1:]

        def bn_layer(layer):
            start = (2 * layer + 1) * items

            def dx_item(i):
                n, v = split(i)
                slot = u_slot(layer, v)
                cols = at(column(layer + 1, n), width)

                @pl.when(i + 1 < items)
                def _():
                    start_u(layer, i + 1)
                    pl.when((v == 0) & (n + 1 < slabs))(lambda: start_w(layer, n + 1))

                @pl.when(i + 1 == items)
                def _():
                    start_u(layer, 0)
                    dy_load(layer, 0).start()

                u_load(layer, i).wait()
                pl.when(v == 0)(lambda: w_load(layer, n).wait())
                events(start + i)
                pl.when((i > 2) & (i < 11))(lambda: by_layer(
                    layer, lambda ref: x_load(ref, v, at(lax.div(i - 3, 2), half // 2)), (x1_ref, h_ref)))
                pl.when(n > 0)(lambda: dy_out(layer, i).wait())
                mean, inv, gamma, beta = stats(layer, v, cols)

                def pieces():
                    first = 0
                    for size in (rows // 2, 3 * rows // 8, rows // 8):
                        dx = mm(dbuf[pl.ds(pl.multiple_of(v * rows + first, LANES), size)], wbuf[odd(n + 1)])
                        for p in range(0, size, PIECE):
                            some = pl.ds(first + p, PIECE)
                            norm = (ubuf[slot, some] - mean) * inv
                            dy = jnp.where(norm * gamma + beta > 0, dx[p:p + PIECE], 0.0)
                            dyout[v, some] = dy
                            yield dy, dy * norm
                        first += size

                g = layer * items + i
                acc[g] = two_sums(pieces())
                dy_out(layer, i).start()
                share.start(g)
                before = (layer + 1) * slabs - 1
                pl.when(i == 0)(lambda: chip_sum(before))
                pl.when(i == 1)(lambda: issue(before, start + i))

            def fetch(i):
                start_u(layer, i)
                dy_load(layer, i).start()

            def ready(i):
                n, v = split(i)
                u_load(layer, i).wait()
                dy_load(layer, i).wait()
                sum_ref[layer, v, :, at(column(layer + 1, n), width)] = share.total(layer * items + i)

            def pre(row, cols, v):
                tot = sum_ref[layer, v, :, cols] / total
                mean, inv, gamma, _ = stats(layer, v, cols)
                slope, front, slot = inv * tot[1:], gamma * inv, u_slot(layer, v)
                for r in runs(rows, PIECE):
                    dbuf[pl.ds(row + r.start, PIECE), cols] = (
                        front * (dybuf[v, r] - (tot[:1] + (ubuf[slot, r] - mean) * slope))).astype(BF16)

            loop(items, dx_item)
            for v in BOTH:
                dy_out(layer, v).wait()
            dw_pass(layer + 1, start + items, ready, fetch, pre, lambda: pl.when(layer == 0)(lambda: next_layer(1)))

        loop(len(layers), bn_layer)

        ticks = (2 * n_layer - 1) * items
        chip_sum(n_slab - 1)
        issue(n_slab - 1, ticks)
        ended = 37
        end(ended - 1)

        def tail(j):
            begin(j, ticks + 2)
            end(j)

        loop(n_chunk, tail, ended)
        for j in range(n_chunk - 2, n_chunk):
            fetch_x(j)
            deliver(j)
        for j in BOTH:
            put_done(j)
        for k in range(n_layer):
            theirs = dw2_ref.at[at(other(c), half // 2)] if k == 1 else (dw1_ref if k else dw3_ref).at[at(other(c), half)]
            remote(theirs, theirs, fcs.at[0], fcr.at[k], cpeer).wait_recv()
            sent = ry_ref.at[at(k, per_layer)]
            remote(sent, sent, ys.at[k], yr.at[0], ypeer).wait_send()
        for j in range(n_chunk - n_mid, n_chunk):
            to_x(j).wait_send()

    n_item = len(layers) * items
    vm = lambda *shape: pltpu.VMEM(shape, F32)
    bf = lambda *shape: pltpu.VMEM(shape, BF16)
    outs = call(
        kernel, "backward", 4, (),
        [ANY, ANY, VMEM, VMEM] + [ANY] * 7 + [VMEM] * 4, [ANY] * 3 + [VMEM] + [ANY] * 4,
        [sds((dim, half), F32), sds((half, dim), F32), sds((dim, half), F32), sds((len(layers), 2, 2, dim), F32),
         sds((all_rows, dim), F32), sds((n_slab, half, width), F32), sds((n_chunk, piece, width), F32),
         sds((n_chunk, piece, width), F32)],
        [bf(all_rows, dim), bf(dim, all_rows), bf(2, dim, width), vm(2, rows, width), vm(2, rows, width), vm(2, rows, width),
         vm(2, half, width), vm(2, half, width), vm(2, half, width), vm(3, piece, width), vm(n_mid, piece, width),
         vm(2, piece, width)] + Share.scratch(n_item, 2, width)
        + [TWO_DMA, TWO_DMA, TWO_DMA, TWO_DMA, TWO_DMA, DMA((n_slab,)), DMA((n_slab,)), DMA, DMA((n_layer,)),
           DMA((n_chunk,)), DMA((n_mid,)), DMA((n_chunk,)), DMA((3,)), TWO_DMA, TWO_DMA, DMA((n_layer,)),
           pltpu.SemaphoreType.REGULAR],
        all_rows * dim * dim * 10, all_rows * dim * 40,
        (d_emb, zh, sz, s_emb, x2_t, x1_t, h_t, u2, u1, w3_t, w2_t, s2, s1, gb2, gb1))
    return outs[:n_layer + 1]


def settle(grads, sums, loss):
    steps = 4
    dim = sums.shape[-1]
    half = dim // 2

    def kernel(sum_ref, loss_ref, src3, src2, src1, g2_ref, b2_ref, g1_ref, b1_ref, total_ref, *dsts):
        for src, dst in zip((src3, src2, src1), dsts):
            dst[...] = src[...]

        @pl.when(pl.program_id(0) == 0)
        def _():
            y, _, _ = coords()
            for layer, (cols, g_ref, b_ref) in enumerate(((pl.ds(0, dim), g2_ref, b2_ref), (at(y, half), g1_ref, b1_ref))):
                both = jnp.sum(sum_ref[layer, :, :, cols], axis=0)
                g_ref[...] = both[1:]
                b_ref[...] = both[:1]
            total_ref[...] = jnp.sum(loss_ref[...], axis=1, keepdims=True)

    specs = [pl.BlockSpec((g.shape[0] // steps, g.shape[1]), lambda i: (i, 0)) for g in grads]
    small = [(1, n) for n in (dim, dim, half, half, 1)]
    return call(kernel, "settle", None, (steps,), [whole(*sums.shape), whole(*loss.shape)] + specs,
                [whole(*t) for t in small] + specs, [sds(t, F32) for t in small] + [sds(g.shape, F32) for g in grads], [], 0,
                sum(g.size for g in grads) * 8, (sums, loss, *grads))


def solution(mesh):
    def shard_body(h_a, h_b, w_one, w_two, w_three, g_one, b_one, g_two, b_two, lam_off):
        total = float(h_a.shape[0] * mesh.shape['data'])
        rowed = [t.reshape(1, -1) for t in (g_one, b_one, g_two, b_two)]
        u1, s1, gb1, gb2, w_two_o, h_t = fwd_first(h_a, h_b, w_one, w_two, *rowed)
        x1_t, u2, s2, w2_t, w_three_o = fwd_next(u1, s1, gb1, w_two, w_two_o, True, total, 1, w_three)
        x2_t, z, sz, w3_t = fwd_next(u2, s2, gb2, w_three, w_three_o, False, total, 2)
        zh, d_emb, s_emb, loss = corr_grad(z, sz, lam_off, total)
        *grads, sums = backward(
            d_emb.reshape(z.shape), zh.reshape(z.shape), sz, s_emb,
            ((u2, s2, gb2, w3_t, x1_t), (u1, s1, gb1, w2_t, h_t)), x2_t, total)
        *small, dw_three, dw_two, dw_one = settle(grads, sums, loss)
        dg_two, db_two, dg_one, db_one, loss = (t.reshape(-1) for t in small)
        return loss, dw_one, dw_two, dw_three, dg_one, db_one, dg_two, db_two

    in_specs = (P('data', None), P('data', None), P(None, 'model'), P('model', None), P(None, 'model'),
                P('model'), P('model'), P(), P(), P())
    out_specs = (P(), P(None, 'model'), P('model', None), P(None, 'model'), P('model'), P('model'), P(), P())
    return jax.shard_map(shard_body, mesh=mesh, in_specs=in_specs, out_specs=out_specs, check_vma=False)
```

```python
import functools

import jax
import jax.numpy as jnp
from jax import lax
from jax.experimental import pallas as pl
from jax.experimental.pallas import tpu as pltpu
from jax.sharding import PartitionSpec as P

BN_EPS = 1e-5
F32 = jnp.float32
BF16 = jnp.bfloat16
PIECE = 64
LANES = 256
SUBLANES = 8
TM = 512
MAX_VMEM = 67043328
ANY = pl.BlockSpec(memory_space=pl.ANY)
VMEM = pl.BlockSpec(memory_space=pltpu.VMEM)
DMA = pltpu.SemaphoreType.DMA
TWO_DMA = DMA((2,))
BOTH = (0, 1)
PEERS = [(ky, kx, kc) for ky in BOTH for kx in BOTH for kc in BOTH][1:]
C_PEER, X_PEER, Y_PEER = PEERS[0], PEERS[1], PEERS[3]
N_DEV = len(PEERS) + 1


def mm(left, right):
    return jnp.dot(left, right, preferred_element_type=F32)


def mm_bt(left, right):
    return lax.dot_general(left, right, (((1,), (1,)), ((), ())), preferred_element_type=F32)


def mm_at(left, right):
    return lax.dot_general(left, right, (((0,), (0,)), ((), ())), preferred_element_type=F32)


def other(p):
    return 1 - p


def odd(i):
    return lax.rem(i, 2)


def split(i):
    return lax.div(i, 2), odd(i)


def loop(n, body, start=0):
    def one(i, carry):
        body(i)
        return carry

    lax.fori_loop(start, n, one, 0)


def whole(*shape):
    return pl.BlockSpec(shape, lambda *_: (0,) * len(shape))


def at(i, n):
    return pl.ds(pl.multiple_of(i * n, n), n)


def sds(shape, dtype):
    return jax.ShapeDtypeStruct(shape, dtype)


def mean_inv(sums, total):
    mean = sums[:1] / total
    var = sums[1:2] / total - mean * mean
    return mean, lax.rsqrt(var + BN_EPS)


def fold(v):
    return jnp.sum(v.reshape(-1, SUBLANES, v.shape[1]), axis=0)


def runs(n, size):
    return [pl.ds(r, size) for r in range(0, n, size)]


def two_sums(pairs):
    one = two = 0.0
    for a, b in pairs:
        one, two = one + fold(a), two + fold(b)
    return jnp.concatenate([jnp.sum(t, axis=0, keepdims=True) for t in (one, two)], axis=0)


def moments(ref, cols):
    pieces = (ref[r, cols] for r in runs(ref.shape[0], PIECE))
    return two_sums((u, u * u) for u in pieces)


def coords():
    y, d = lax.axis_index('model'), lax.axis_index('data')
    return y, lax.div(d, 2), odd(d)


def flip(here, which):
    return tuple(other(p) if f else p for p, f in zip(here, which))


def flat(here):
    y, x, c = here
    return 4 * y + 2 * x + c


def device(here):
    y, x, c = here
    return (y, 2 * x + c)


def remote(src, dst, send_sem, recv_sem, there):
    return pltpu.make_async_remote_copy(
        src_ref=src, dst_ref=dst, send_sem=send_sem, recv_sem=recv_sem, device_id=device(there),
        device_id_type=pl.DeviceIdType.MESH)


def arrive():
    here = coords()
    for k in PEERS:
        pl.semaphore_signal(pltpu.get_barrier_semaphore(), inc=1, device_id=device(flip(here, k)),
                            device_id_type=pl.DeviceIdType.MESH)


def all_arrived():
    pl.semaphore_wait(pltpu.get_barrier_semaphore(), len(PEERS))


class Share:
    def __init__(self, acc, got, send_sem, recv_sem):
        self.acc, self.got, self.send_sem, self.recv_sem = acc, got, send_sem, recv_sem

    @staticmethod
    def scratch(n, *shape):
        return [pltpu.VMEM((n, *shape), F32), pltpu.VMEM((n, N_DEV, *shape), F32), DMA((n,)), DMA((n,))]

    def start(self, b):
        here = coords()
        me = flat(here)
        self.got[b, me] = self.acc[b]
        for which in PEERS:
            remote(self.acc.at[b], self.got.at[b, me], self.send_sem.at[b], self.recv_sem.at[b],
                   flip(here, which)).start()

    def total(self, b):
        all_of = self.got.at[b, pl.ds(0, len(PEERS))]
        copies = remote(all_of, all_of, self.send_sem.at[b], self.recv_sem.at[b], coords())
        copies.wait_send()
        copies.wait_recv()
        out = self.got[b, 0]
        for f in range(1, N_DEV):
            out += self.got[b, f]
        return out


class Gather:
    def __init__(self, own, dest, n, sems):
        self.own, self.dest, self.n = own, dest, n
        self.ys, self.yr, self.xs, self.xr, self.cs, self.cr = sems
        self.here = coords()
        _, x, c = self.here
        self.mine, self.across = 2 * x + c, 2 * (other(x)) + c
        self.core = (2 * x + other(c), 2 * (other(x)) + other(c))

    @staticmethod
    def scratch(n):
        return [DMA((n,))] * 4 + [DMA((2, n))] * 2

    def y(self, p):
        model = self.here[0]
        return remote(self.own(self.mine, p), self.dest(model, self.mine, p), self.ys.at[p], self.yr.at[p],
                      flip(self.here, Y_PEER))

    def moved(self, q, p, send_sem, recv_sem, which):
        ref = self.dest(1 - self.here[0], q, p)
        return remote(ref, ref, send_sem, recv_sem, flip(self.here, which))

    def x(self, p, q):
        return self.moved(q, p, self.xs.at[p], self.xr.at[p], X_PEER)

    def c(self, p, late, q):
        return self.moved(q, p, self.cs.at[late, p], self.cr.at[late, p], C_PEER)

    def start(self):
        for p in range(self.n):
            self.y(p).start()

    def pass_y(self, p):
        self.moved(self.mine, p, self.ys.at[p], self.yr.at[p], Y_PEER).wait_recv()
        self.x(p, self.mine).start()
        self.c(p, 0, self.mine).start()

    def pass_x(self, p):
        self.x(p, self.across).wait_recv()
        self.c(p, 1, self.across).start()

    def wait_core(self, late):
        for p in range(self.n):
            self.c(p, late, self.core[late]).wait_recv()

    def drain(self):
        for p in range(self.n):
            self.y(p).wait_send()
            self.x(p, self.mine).wait_send()
            self.c(p, 0, self.mine).wait_send()
            self.c(p, 1, self.across).wait_send()


def call(kernel, name, cid, grid, in_specs, out_specs, out_shape, scratch, flops, nbytes, args):
    return pl.pallas_call(
        kernel, name=name, grid=grid, in_specs=in_specs, out_specs=out_specs, out_shape=out_shape, scratch_shapes=scratch,
        compiler_params=pltpu.CompilerParams(vmem_limit_bytes=MAX_VMEM, collective_id=cid, has_side_effects=cid is not None),
        cost_estimate=pl.CostEstimate(flops=flops, bytes_accessed=nbytes, transcendentals=0))(*args)


def fwd_first(h_a, h_b, w_one, w_two, *vectors):
    depth, half = w_one.shape
    dim = 2 * half
    rows = h_a.shape[0] // 2
    tile, width, quarter = 2 * TM, half // 2, half // 4
    steps = rows // tile
    per_block = 2 * steps
    n, n2 = 4, 8

    def block(j):
        y, x, _ = coords()
        return jnp.where(j < 2, 2 * y + j, 2 * (other(y)) + jnp.where(j == 2, x, other(x)))

    def tile_of(j, i):
        return jnp.where(odd(j) == 0, i, per_block - 1 - i)

    def kernel(ha_ref, hb_ref, w_ref, w2_ref, g1_ref, b1_ref, g2_ref, b2_ref, u_ref, s_ref, gbo_ref, gb2_ref, w2o_ref, ht_ref,
               w1, gbf, *sems):
        share, sems = Share(*sems[:4]), sems[4:]
        gs, gr, lsem = sems[:3]
        sems = sems[3:]
        j, i = pl.program_id(0), pl.program_id(1)
        step = j * per_block + i
        here = coords()
        y = here[0]
        one = Gather(lambda q, p: w_ref.at[at(p, depth // n), at(q, quarter)],
                     lambda m, q, p: w1.at[at(p, depth // n), at(m * 4 + q, quarter)], n, sems[:6])
        two = Gather(lambda q, p: w2_ref.at[at(q * n2 + p, quarter // n2)],
                     lambda m, q, p: w2o_ref.at[at(q * n2 + p, quarter // n2)], n2, sems[6:])

        def local(b):
            return pltpu.make_async_copy(w_ref.at[:, at(b, width)], w1.at[:, at(2 * y + b, width)], lsem.at[b])

        def bn_vectors(m):
            return remote(gbf.at[:, at(m, half)], gbf.at[:, at(m, half)], gs, gr, flip(here, Y_PEER))

        def begin():
            arrive()
            local(0).start()
            local(1).start()
            all_arrived()
            one.start()
            two.start()
            for r, (one_ref, two_ref) in enumerate(((g1_ref, g2_ref), (b1_ref, b2_ref))):
                row = pl.ds(r, 1)
                gbf[row, at(y, half)] = one_ref[...]
                gb2_ref[row] = two_ref[...]
            local(0).wait()

        def late_half():
            one.pass_x(0)
            one.pass_y(n - 1)
            one.wait_core(0)

        hooks = [(0, begin), (1, lambda: bn_vectors(y).start()), (per_block, lambda: local(1).wait()), (2 * per_block, late_half)]
        hooks += [(2 * p + 3, functools.partial(one.pass_y, p)) for p in range(n - 1)]
        hooks += [(p + 2 * per_block, functools.partial(one.pass_x, p)) for p in range(1, n)]
        hooks += [(3 * per_block, lambda: one.wait_core(1))]
        hooks += [(p + 9, functools.partial(two.pass_y, p)) for p in range(n2 - 1)]
        hooks += [(13 + (p + 1) // 2, functools.partial(two.pass_x, p)) for p in range(n2 // 2)]
        for s, hook in hooks:
            pl.when(step == s)(hook)
        for b in range(3):
            pl.when(step == (b + 1) * per_block)(lambda b=b: share.start(block(b)))

        tile_at = tile_of(j, i)
        first_view = tile_at < steps
        cols = at(j, width)
        ht_ref[...] = lax.select(first_view, ha_ref[:, cols], hb_ref[:, cols]).T
        for r in runs(tile, TM):
            u_ref[r] = mm(lax.select(first_view, ha_ref[r], hb_ref[r]), w1[:, at(block(j), width)])
        sums = jnp.concatenate([moments(u_ref, cols) for cols in runs(width, LANES)], axis=1)
        v = tile_at // steps
        share.acc[block(j), v] = jnp.where(i % steps == 0, 0.0, share.acc[block(j), v]) + sums

        @pl.when(step == 4 * per_block - 1)
        def _():
            share.start(block(3))
            two.pass_y(n2 - 1)
            for p in range(n2 // 2, n2):
                two.pass_x(p)
            bn_vectors(other(y)).wait_recv()
            bn_vectors(y).wait_send()
            gbo_ref[...] = gbf[...]
            for b in range(4):
                s_ref[:, :, b * width:(b + 1) * width] = share.total(b)
            one.drain()
            two.drain()
            two.wait_core(0)
            two.wait_core(1)

    return call(
        kernel, "fwd_first", 0, (4, per_block),
        [pl.BlockSpec((tile, depth), lambda j, i: (coords()[0] * steps + jnp.minimum(tile_of(j, i), steps - 1), 0)),
         pl.BlockSpec((tile, depth), lambda j, i: (coords()[0] * steps + jnp.maximum(tile_of(j, i) - steps, 0), 0)),
         ANY, ANY] + [whole(*t.shape) for t in vectors],
        [pl.BlockSpec((tile, width), lambda j, i: (tile_of(j, i), block(j))), whole(2, 2, dim),
         whole(2, dim), whole(2, dim), ANY, pl.BlockSpec((width, tile), lambda j, i: (j, tile_of(j, i)))],
        [sds((2 * rows, dim), F32), sds((2, 2, dim), F32), sds((2, dim), F32), sds((2, dim), F32),
         sds((half, dim), BF16), sds((depth, 2 * rows), BF16)],
        [pltpu.VMEM((depth, dim), BF16), pltpu.VMEM((2, dim), F32)] + Share.scratch(4, 2, 2, width)
        + [DMA, DMA, TWO_DMA] + Gather.scratch(n) + Gather.scratch(n2),
        4 * rows * depth * dim, 2 * rows * (8 * depth + 4 * dim), (h_a, h_b, w_one, w_two, *vectors))


def fwd_next(u, sums, gb, w_own, w_other, by_rows, total, cid, w_next=None):
    all_rows, depth = u.shape
    dim = w_own.shape[1] if by_rows else 2 * w_own.shape[1]
    half = dim // 2
    quarter = half // 4
    steps = all_rows // 2 // TM
    last = 2 * steps - 1
    slab = dim // (2 * steps)
    n = 4
    more = w_next is not None

    def kernel(u_ref, s_ref, gb_ref, wo_ref, wt_ref, *refs):
        if more:
            wn_ref, refs = refs[0], refs[1:]
        x_ref, o_ref, so_ref, wtr_ref, *refs = refs
        if more:
            wno_ref, *refs = refs
        w, act, acc, got, ssem, rsem, lsem, *refs = refs
        share = Share(acc, got, ssem, rsem)
        i = pl.program_id(0)
        y = coords()[0]

        def local(ref, model, b):
            where = at(model, half)
            return pltpu.make_async_copy(ref, w.at[where] if by_rows else w.at[:, where], lsem.at[b])

        if more:
            gather = Gather(lambda q, p: wn_ref.at[at(p, depth // n), at(q, quarter)],
                            lambda m, q, p: wno_ref.at[at(p, depth // n), at(q, quarter)], n, refs)

        @pl.when(i == 0)
        def _():
            arrive()
            acc[...] = jnp.zeros_like(acc)
            local(wo_ref, y, 0).start()
            local(wt_ref, other(y), 1).start()
            all_arrived()
            if more:
                gather.start()
            local(wo_ref, y, 0).wait()
            local(wt_ref, other(y), 1).wait()

        if more:
            for p in range(n):
                pl.when(i == p + 2)(lambda p=p: gather.pass_y(p))
                pl.when(i == p + 4)(lambda p=p: gather.pass_x(p))
        pl.when(i == steps)(lambda: share.start(0))

        mean, inv = mean_inv(s_ref[0], total)
        for k, cols in enumerate(runs(depth, LANES)):
            m, r, g, b = (t[:, k * LANES:(k + 1) * LANES] for t in (mean, inv, gb_ref[:1], gb_ref[1:]))
            for piece in runs(TM, PIECE):
                act[piece, cols] = jnp.maximum((u_ref[piece, cols] - m) * r * g + b, 0.0).astype(BF16)
        x_ref[...] = act[...].T
        wtr_ref[...] = w[:, at(i, slab)].T
        v = i // steps
        keep = jnp.where(i % steps == 0, 0.0, 1.0)
        for some in runs(dim, half):
            o_ref[:, some] = mm(act[...], w[:, some])
            for cols in runs(half, LANES):
                cols = pl.ds(some.start + cols.start, LANES)
                share.acc[v, :, cols] = keep * share.acc[v, :, cols] + moments(o_ref, cols)

        @pl.when(i == last)
        def _():
            share.start(1)
            for b in BOTH:
                so_ref[b] = share.total(b)
            if more:
                gather.drain()
                gather.wait_core(0)
                gather.wait_core(1)

    return call(
        kernel, "fwd_next", cid, (2 * steps,),
        [pl.BlockSpec((TM, depth), lambda i: (i, 0)), pl.BlockSpec((1, 2, depth), lambda i: (i // steps, 0, 0)),
         whole(2, depth), ANY, ANY] + [ANY] * more,
        [pl.BlockSpec((depth, TM), lambda i: (0, i)), pl.BlockSpec((TM, dim), lambda i: (i, 0)),
         whole(2, 2, dim), pl.BlockSpec((slab, depth), lambda i: (i, 0))] + [ANY] * more,
        [sds((depth, all_rows), BF16), sds((all_rows, dim), F32), sds((2, 2, dim), F32), sds((dim, depth), BF16)]
        + ([sds(w_next.shape, BF16)] if more else []),
        [pltpu.VMEM((depth, dim), BF16), pltpu.VMEM((TM, depth), BF16)] + Share.scratch(2, 2, dim) + [TWO_DMA] + (Gather.scratch(n) if more else []),
        2 * all_rows * depth * dim, all_rows * (6 * depth + 4 * dim),
        (u, sums, gb, w_own, w_other) + ((w_next,) if more else ()))


def corr_grad(z, sums, lam, total):
    all_rows, dim = z.shape
    rows = all_rows // 2
    half = dim // 2
    quart = half // 2
    n_chunk = 8
    width = half // n_chunk
    pair = 2 * width
    mt = half
    zt = LANES
    ahead = 3
    lead = 3
    z_steps = all_rows // zt
    m_steps = rows // mt
    scale = 1.0 / total

    def kernel(z_ref, s_ref, lam_ref, zho_ref, d_ref, so_ref, lo_ref, zh, da, ck, r1, r2, g, stage, dsend, drecv, acc, got, ssem, rsem, loss_acc, loss_got, lsem, lrsem, zs, zos,
               d1s, d1r, s1s, s1r, s2s, s2r, a2s, a2r, a1s, a1r, ads, adr, dbs, das):
        share = Share(acc, got, ssem, rsem)
        share_loss = Share(loss_acc, loss_got, lsem, lrsem)
        here = coords()
        y, x, c = here
        on_x = c == 0
        by_core = lambda one, two: tuple(jnp.where(on_x, a, b) for a, b in zip(one, two))
        first = by_core(flip(here, X_PEER), flip(here, Y_PEER))
        second = by_core(flip(here, Y_PEER), flip(here, X_PEER))
        cpeer = flip(here, C_PEER)
        bit1, bit2 = by_core((x, y), (y, x))
        arrive()
        acc[...] = jnp.zeros_like(acc)
        loss_acc[...] = jnp.zeros_like(loss_acc)

        def load(i, slot):
            return pltpu.make_async_copy(z_ref.at[at(i, zt)], ck.at[at(slot, zt)], zs.at[slot])

        def zh_out(i):
            v, r = lax.div(i, n_chunk // 2), lax.rem(i, n_chunk // 2)
            return pltpu.make_async_copy(zh.at[v, at(r, TM)], zho_ref.at[v, at(r, TM)], zos.at[i])

        z_slots = half // zt
        for i in range(ahead):
            load(i, i).start()

        def normalise(i):
            slot = lax.rem(i, z_slots)
            v, r = lax.div(i, z_steps // 2), lax.rem(i, z_steps // 2)
            pl.when(i + ahead < z_steps)(lambda: load(i + ahead, lax.rem(i + ahead, z_slots)).start())
            load(i, slot).wait()
            mean, inv = mean_inv(s_ref[v], total)
            for k, cols in enumerate(runs(dim, LANES)):
                m, s = (t[:, k * LANES:(k + 1) * LANES] for t in (mean, inv))
                for p in range(zt // PIECE):
                    zh[v, at(r * (zt // PIECE) + p, PIECE), cols] = (
                        (ck[at(slot * (zt // PIECE) + p, PIECE), cols] - m) * s).astype(BF16)
            da[at(i, rows // z_steps)] = jnp.zeros((rows // z_steps, dim), F32)

        loop(z_steps, normalise)
        all_arrived()

        def both(v, rows_at, t):
            return jnp.concatenate([zh[v, rows_at, at(b * n_chunk + t, width)] for b in BOTH], axis=1)

        group = lambda t, b: at(2 * t + b, width)

        def to_core(t):
            return remote(dsend.at[odd(t)], drecv.at[odd(t)], d1s.at[t], d1r.at[t], cpeer)

        def to_first(t):
            return remote(ck.at[:, group(t, other(bit1))], r1.at[t], s1s.at[t], s1r.at[t], first)

        def to_second(t):
            return remote(ck.at[at(other(bit2), quart), group(t, bit1)], r2.at[t], s2s.at[t], s2r.at[t], second)

        def g_second(t, b):
            block = g.at[t, at(2 * c + b, quart), at(bit1, width)]
            return remote(block, block, a2s.at[t], a2r.at[t], second)

        def g_first(t, b):
            block = g.at[t, at(c, half), at(b, width)]
            return remote(block, block, a1s.at[t], a1r.at[t], first)

        def g_core(t, core):
            block = g.at[t, at(core, half)]
            return remote(block, block, ads.at[t], adr.at[t], cpeer)

        def chip_sum(t):
            to_core(t).wait_recv()
            to_core(t).wait_send()
            ck[:, at(t, pair)] += drecv[odd(t)]
            to_first(t).start()

        def corr_part(t):
            zh_out(t).start()
            right = both(1, pl.ds(0, rows), t)
            dsend[odd(t)] = mm_at(zh[0, :, at(other(c), half)], right)
            ck[:, at(t, pair)] = mm_at(zh[0, :, at(c, half)], right)
            to_core(t).start()

        def db_out(t, m, slot, b):
            return pltpu.make_async_copy(
                stage.at[slot, :, at(b, width)], d_ref.at[1, at(m, mt), at(b * n_chunk + t, width)], dbs.at[slot, b])

        def da_out(m):
            return pltpu.make_async_copy(da.at[at(m, mt)], d_ref.at[0, at(m, mt)], das.at[m])

        def finish(m):
            def scaled(cols):
                for p in range(mt // PIECE):
                    some = at(m * (mt // PIECE) + p, PIECE)
                    d = da[some, cols] * scale
                    da[some, cols] = d
                    yield d, d * zh[0, some, cols].astype(F32)

            for cols in runs(dim, LANES):
                acc[0, :, cols] += two_sums(scaled(cols))
            da_out(m).start()

        def grads(t):
            def rows_of(m):
                slot = odd(m)

                @pl.when(t * m_steps + m >= 2)
                def _():
                    for b in BOTH:
                        db_out(t, m, slot, b).wait()

                own = both(1, at(m, mt), t)
                stage[slot] = mm(zh[0, at(m, mt)], g[t]) * scale
                sums = two_sums((stage[slot, r], stage[slot, r] * both(1, at(m * (mt // PIECE) + p, PIECE), t).astype(F32))
                                for p, r in enumerate(runs(mt, PIECE)))
                for b in BOTH:
                    acc[1, :, at(b * n_chunk + t, width)] += sums[:, b * width:(b + 1) * width]
                    db_out(t, m, slot, b).start()
                for cols in runs(dim, LANES):
                    da[at(m, mt), cols] += mm_bt(own, g[t, cols])
                pl.when(t == n_chunk - 1)(lambda: finish(m))

            loop(m_steps, rows_of)

        def at_first(t):
            to_first(t).wait_recv()
            ck[:, group(t, bit1)] += r1[t]
            to_second(t).start()

        def at_second(t):
            to_second(t).wait_recv()
            corr_mat = (ck[at(bit2, quart), group(t, bit1)] + r2[t]) * scale
            row_ids = (2 * c + bit2) * quart + lax.broadcasted_iota(jnp.int32, (quart, width), 0)
            col_ids = (bit1 * n_chunk + t) * width + lax.broadcasted_iota(jnp.int32, (quart, width), 1)
            is_diag = row_ids == col_ids
            lam_val = lam_ref[0]
            loss = jnp.where(is_diag, (1.0 - corr_mat) * (1.0 - corr_mat), lam_val * corr_mat * corr_mat)
            loss_acc[0] += jnp.sum(loss, axis=0, keepdims=True)
            pl.when(t == n_chunk - 1)(lambda: share_loss.start(0))
            grad = jnp.where(is_diag, -2.0 * (1.0 - corr_mat), 2.0 * lam_val * corr_mat).astype(BF16)
            g[t, at(2 * c + bit2, quart), at(bit1, width)] = grad
            g_second(t, bit2).start()

        def back_second(t):
            g_second(t, other(bit2)).wait_recv()
            g_first(t, bit1).start()

        def back_first(t):
            g_first(t, other(bit1)).wait_recv()
            g_core(t, c).start()

        def back_core(t):
            g_core(t, other(c)).wait_recv()
            grads(t)

        def advance(tau):
            for lag, stage_fn in ((lead, at_first), (lead + 1, back_second), (lead + 2, back_first), (lead + 3, back_core),
                                  (lead, at_second), (1, chip_sum), (0, corr_part)):
                t = tau - lag
                pl.when(jnp.logical_and(t >= 0, t < n_chunk))(lambda t=t, stage_fn=stage_fn: stage_fn(t))

        loop(n_chunk + lead + 3, advance)
        share.start(1)
        share.start(0)
        for t in range(n_chunk):
            for copy in (to_first(t), to_second(t), g_second(t, bit2), g_first(t, bit1), g_core(t, c)):
                copy.wait_send()
        for b in BOTH:
            so_ref[b] = share.total(b)
            for slot in BOTH:
                db_out(0, 0, slot, b).wait()
        lo_ref[...] = share_loss.total(0)
        for i in range(n_chunk):
            zh_out(i).wait()
        for m in range(m_steps):
            da_out(m).wait()

    return call(
        kernel, "corr_grad", 3, (), [ANY, VMEM, pl.BlockSpec(memory_space=pltpu.SMEM)], [ANY, ANY, VMEM, VMEM],
        [sds((2, rows, dim), BF16), sds((2, rows, dim), F32), sds((2, 2, dim), F32), sds((1, width), F32)],
        [pltpu.VMEM((2, rows, dim), BF16), pltpu.VMEM((rows, dim), F32), pltpu.VMEM((half, dim), F32),
         pltpu.VMEM((n_chunk, half, width), F32), pltpu.VMEM((n_chunk, quart, width), F32),
         pltpu.VMEM((n_chunk, dim, pair), BF16), pltpu.VMEM((2, mt, pair), F32)]
        + [pltpu.VMEM((2, half, pair), F32)] * 2 + Share.scratch(2, 2, dim) + Share.scratch(1, 1, width)
        + [DMA((half // zt,)), DMA((n_chunk,))] + [DMA((n_chunk,))] * 12 + [DMA((2, 2)), DMA((m_steps,))],
        all_rows * dim * dim * 3, all_rows * dim * 12, (z, sums, lam))


def backward(d_emb, zh, sz, s_emb, layers, x2_t, total):
    all_rows, dim = zh.shape
    rows, half = all_rows // 2, dim // 2
    width = 256
    slabs = dim // width
    items = 2 * slabs
    piece = width
    side = half // 2 // piece
    per_slab = half // piece
    n_layer = len(layers) + 1
    n_slab = n_layer * slabs
    per_layer = slabs * side
    n_chunk = n_layer * per_layer
    ahead = 3
    (u2, s2, gb2, w3_t, x1_t), (u1, s1, gb1, w2_t, h_t) = layers

    def kernel(d_ref, zh_ref, sz_ref, sd_ref, x2_ref, x1_ref, h_ref, u2_ref, u1_ref, w3_ref, w2_ref,
               s2_ref, s1_ref, gb2_ref, gb1_ref, dw3_ref, dw2_ref, dw1_ref, sum_ref, dy_ref, part_ref, ry_ref, rx_ref,
               dbuf, xbuf, wbuf, ubuf, dybuf, dyout, psend, pkeep, dr, ebuf, mbuf, fbuf, acc, got, ssem, rsem,
               us, ws, ds, dos, xl, ps, pr, pm, ys, yr, xs, xr, es, fs, fcs, fcr, credit):
        share = Share(acc, got, ssem, rsem)
        here = coords()
        y, x, c = here
        ypeer, xpeer, cpeer = flip(here, Y_PEER), flip(here, X_PEER), flip(here, C_PEER)
        arrive()

        def column(k, n):
            model = odd(n + jnp.where(k == 0, other(y), 0))
            return jnp.where(k == 1, n, model * (slabs // 2) + lax.div(n, 2))

        def turn(k):
            return jnp.where(k == 0, 0, other(y))

        def m_slot(j):
            return lax.rem(j, 4)

        def copy(src, dst, sem):
            return pltpu.make_async_copy(src, dst, sem)

        def sent_by(q):
            first = jnp.minimum(per_slab * lax.div(q, 4), per_layer)
            middle = jnp.clip(side * lax.div(q - 2 * items - 2, 2), 0, per_layer)
            last = jnp.clip(per_slab * lax.div(q - 4 * items - 2, 4), 0, per_layer)
            return first + middle + last

        def begun(q):
            return jnp.maximum(lax.div(q - 6, 2), 0)

        def to_core(s):
            return remote(psend.at[odd(s)], dr.at[odd(s)], ps.at[s], pr.at[s], cpeer)

        def keep_out(s):
            return copy(pkeep.at[odd(s)], part_ref.at[s], pm)

        def chip_sum(s):
            to_core(s).wait_recv()
            pkeep[odd(s)] += dr[odd(s)]

            @pl.when(s + 2 < n_slab)
            def _():
                pl.semaphore_signal(credit, inc=1, device_id=device(cpeer), device_id_type=pl.DeviceIdType.MESH)

            to_core(s).wait_send()
            keep_out(s).start()

        def home(j, own):
            k = lax.div(j, per_layer)
            i = lax.rem(j, per_layer)
            model = y if own else other(y)
            turned = other(turn(k)) if own else turn(k)
            s = jnp.where(k == 1, lax.div(i, side), 2 * lax.div(i, per_slab) + turned)
            place = jnp.where(k == 1, model * side + lax.rem(i, side), lax.rem(i, per_slab))
            return part_ref.at[k * slabs + s, at(place, piece)]

        def to_y(j):
            return remote(home(j, False), ry_ref.at[j], ys.at[lax.div(j, per_layer)], yr.at[j], ypeer)

        def issue(s, q):
            keep_out(s).wait()
            k, n = lax.div(s, slabs), lax.rem(s, slabs)
            for mine, fire, first, count in (
                    (k == 1, True, n * side, side), (k != 1, odd(n) == jnp.where(k == 0, 0, 1), lax.div(n, 2) * per_slab, per_slab)):
                for r in range(count):
                    j = k * per_layer + first + r
                    pl.when(mine & fire & (j < begun(q) + ahead))(lambda j=j: to_y(j).start())

        def to_x(j):
            return remote(mbuf.at[m_slot(j)], rx_ref.at[j], xs.at[m_slot(j)], xr.at[j], xpeer)

        def result(j, k):
            i = lax.rem(j, per_layer)
            if k == 1:
                return dw2_ref.at[at(c * side + lax.rem(i, side), piece), at(lax.div(i, side), width)]
            return (dw1_ref if k else dw3_ref).at[at(c * per_slab + lax.rem(i, per_slab), piece), at(lax.div(i, per_slab), width)]

        def put(j, k):
            slot = odd(j)
            return (copy(fbuf.at[slot], result(j, k), fs.at[slot]),
                    remote(fbuf.at[slot], result(j, k), fcs.at[slot], fcr.at[k], cpeer))

        def put_done(j):
            here_copy, there_copy = put(j, 0)
            here_copy.wait()
            there_copy.wait_send()

        def load_part(j, which):
            src = (lambda: ry_ref.at[j], lambda: home(j, True), lambda: rx_ref.at[j])[which]()
            return copy(src, ebuf.at[which], es.at[which])

        def fetch_x(j):
            to_x(j).wait_recv()
            load_part(j, 2).start()

        def begin(j, q):
            remote(ry_ref.at[j], ry_ref.at[j], ys.at[0], yr.at[j], ypeer).wait_recv()
            load_part(j, 0).start()
            load_part(j, 1).start()
            pl.when(j + ahead < sent_by(q))(lambda: to_y(j + ahead).start())
            pl.when(j >= 2)(lambda: fetch_x(j - 2))

        def deliver(j):
            load_part(j, 2).wait()
            pl.when(j >= 2)(lambda: put_done(j))
            fbuf[odd(j)] = mbuf[m_slot(j)] + ebuf[2]
            for k in range(n_layer):
                @pl.when(lax.div(j, per_layer) == k)
                def _(k=k):
                    for one in put(j, k):
                        one.start()

        def end(j):
            load_part(j, 0).wait()
            load_part(j, 1).wait()
            pl.when(j >= 4)(lambda: to_x(j).wait_send())
            mbuf[m_slot(j)] = ebuf[0] + ebuf[1]
            to_x(j).start()
            pl.when(j >= 2)(lambda: deliver(j - 2))

        def events(q):
            now, before, earlier = begun(q), begun(q - 1), begun(q - 2)
            pl.when(before > earlier)(lambda: end(before - 1))
            pl.when(now > before)(lambda: begin(now - 1, q))

        def weight_slab(k, n, v, d):
            slot = odd(k * slabs + n)
            for buf, part in ((psend, other(c)), (pkeep, c)):
                first = jnp.where(k == 1, part, 2 * part)
                for b in BOTH:
                    left = xbuf[at(first + b * jnp.where(k == 1, 2, 1), half // 2), pl.ds(v * rows, rows)]
                    here_at = at(b, half // 2)
                    prod = mm(left, d)
                    buf[slot, here_at] = buf[slot, here_at] + prod if v else prod

        def after(k, n, v, q):
            s = k * slabs + n
            if v == 0:
                pl.when(n > 0)(lambda: chip_sum(s - 1))
            else:
                pl.when(s >= 2)(lambda: pl.semaphore_wait(credit, 1))
                to_core(s).start()
                pl.when(n > 0)(lambda: issue(s - 1, q))

        def dw_pass(k, q, ready, fetch, pre, ahead_of_next):
            def slab(n):
                for v in BOTH:
                    i = 2 * n + v
                    pl.when(i + 1 < items)(lambda: fetch(i + 1))
                    ready(i)
                    pl.when(n == 0)(lambda: x_load(x2_ref, v).wait())
                    events(q + i)
                    cols = at(column(k, n), width)
                    pre(v * rows, cols, v)
                    weight_slab(k, n, v, dbuf[pl.ds(v * rows, rows), cols])
                    after(k, n, v, q + i)
                pl.when(n == slabs - 1)(ahead_of_next)

            loop(slabs, slab)

        def emb_loads(i):
            n, v = split(i)
            cols = at(column(0, n), width)
            return (copy(d_ref.at[at(v, rows), cols], ubuf.at[v], us.at[v]),
                    copy(zh_ref.at[at(v, rows), cols], wbuf.at[v], ws.at[v]))

        def emb_fetch(i):
            for one in emb_loads(i):
                one.start()

        def emb_ready(i):
            for one in emb_loads(i):
                one.wait()

        def emb_pre(row, cols, v):
            _, inv = mean_inv(sz_ref[v, :, cols], total)
            sd = sd_ref[v, :, cols] / total
            for r in runs(rows, PIECE):
                dbuf[pl.ds(row + r.start, PIECE), cols] = (
                    inv * (ubuf[v, r] - sd[:1] - wbuf[v, r].astype(F32) * sd[1:])).astype(BF16)

        def x_load(src, v, rows_at=pl.ds(0, dim)):
            return copy(src.at[rows_at, at(v, rows)], xbuf.at[rows_at, at(v, rows)], xl.at[v])

        def u_slot(layer, v):
            return jnp.where(layer == 0, other(v), v)

        def slab_of(ref, layer, i, buf, sem, slot):
            n, v = split(i)
            return copy(ref.at[at(v, rows), at(column(layer + 1, n), width)], buf.at[slot], sem.at[slot])

        def u_load(layer, i, ref=u2_ref):
            return slab_of(ref, layer, i, ubuf, us, u_slot(layer, odd(i)))

        def dy_load(layer, i):
            return slab_of(dy_ref, layer, i, dybuf, ds, odd(i))

        def dy_out(layer, i):
            n, v = split(i)
            return copy(dyout.at[v], dy_ref.at[at(v, rows), at(column(layer + 1, n), width)], dos.at[v])

        def w_load(layer, n, ref=w3_ref):
            slot = odd(n + 1)
            return copy(ref.at[:, at(column(layer + 1, n), width)], wbuf.at[slot], ws.at[slot])

        def by_layer(layer, make, refs):
            for k, ref in enumerate(refs):
                pl.when(layer == k)(lambda ref=ref: make(ref).start())

        def start_u(layer, i):
            by_layer(layer, lambda ref: u_load(layer, i, ref), (u2_ref, u1_ref))

        def start_w(layer, n):
            by_layer(layer, lambda ref: w_load(layer, n, ref), (w3_ref, w2_ref))

        def next_layer(layer):
            start_u(layer, 0)
            start_w(layer, 0)

        for one in (x_load(x2_ref, 0), *emb_loads(0), x_load(x2_ref, 1)):
            one.start()
        all_arrived()
        dw_pass(0, 0, emb_ready, emb_fetch, emb_pre, lambda: next_layer(0))

        def stats(layer, v, cols):
            pick = lambda one, two: jnp.where(layer == 0, one, two)
            mean, inv = mean_inv(pick(s2_ref[v, :, cols], s1_ref[v, :, cols]), total)
            gb = pick(gb2_ref[:, cols], gb1_ref[:, cols])
            return mean, inv, gb[:1], gb[1:]

        def bn_layer(layer):
            start = (2 * layer + 1) * items

            def dx_item(i):
                n, v = split(i)
                slot = u_slot(layer, v)
                cols = at(column(layer + 1, n), width)

                @pl.when(i + 1 < items)
                def _():
                    start_u(layer, i + 1)
                    pl.when((v == 0) & (n + 1 < slabs))(lambda: start_w(layer, n + 1))

                @pl.when(i + 1 == items)
                def _():
                    start_u(layer, 0)
                    dy_load(layer, 0).start()

                u_load(layer, i).wait()
                pl.when(v == 0)(lambda: w_load(layer, n).wait())
                events(start + i)
                pl.when((i > 2) & (i < 11))(lambda: by_layer(
                    layer, lambda ref: x_load(ref, v, at(lax.div(i - 3, 2), half // 2)), (x1_ref, h_ref)))
                pl.when(n > 0)(lambda: dy_out(layer, i).wait())
                mean, inv, gamma, beta = stats(layer, v, cols)

                def pieces():
                    first = 0
                    for size in (rows // 2, 3 * rows // 8, rows // 8):
                        dx = mm(dbuf[pl.ds(pl.multiple_of(v * rows + first, LANES), size)], wbuf[odd(n + 1)])
                        for p in range(0, size, PIECE):
                            some = pl.ds(first + p, PIECE)
                            norm = (ubuf[slot, some] - mean) * inv
                            dy = jnp.where(norm * gamma + beta > 0, dx[p:p + PIECE], 0.0)
                            dyout[v, some] = dy
                            yield dy, dy * norm
                        first += size

                g = layer * items + i
                acc[g] = two_sums(pieces())
                dy_out(layer, i).start()
                share.start(g)
                before = (layer + 1) * slabs - 1
                pl.when(i == 0)(lambda: chip_sum(before))
                pl.when(i == 1)(lambda: issue(before, start + i))

            def fetch(i):
                start_u(layer, i)
                dy_load(layer, i).start()

            def ready(i):
                n, v = split(i)
                u_load(layer, i).wait()
                dy_load(layer, i).wait()
                sum_ref[layer, v, :, at(column(layer + 1, n), width)] = share.total(layer * items + i)

            def pre(row, cols, v):
                tot = sum_ref[layer, v, :, cols] / total
                mean, inv, gamma, _ = stats(layer, v, cols)
                slope, front, slot = inv * tot[1:], gamma * inv, u_slot(layer, v)
                for r in runs(rows, PIECE):
                    dbuf[pl.ds(row + r.start, PIECE), cols] = (
                        front * (dybuf[v, r] - (tot[:1] + (ubuf[slot, r] - mean) * slope))).astype(BF16)

            loop(items, dx_item)
            for v in BOTH:
                dy_out(layer, v).wait()
            dw_pass(layer + 1, start + items, ready, fetch, pre, lambda: pl.when(layer == 0)(lambda: next_layer(1)))

        loop(len(layers), bn_layer)

        ticks = (2 * n_layer - 1) * items
        chip_sum(n_slab - 1)
        issue(n_slab - 1, ticks)
        ended = 36

        def tail(j):
            begin(j, ticks + 2)
            end(j)

        loop(n_chunk, tail, ended)
        for j in range(n_chunk - 2, n_chunk):
            fetch_x(j)
            deliver(j)
        for j in BOTH:
            put_done(j)
        for k in range(n_layer):
            theirs = dw2_ref.at[at(other(c), half // 2)] if k == 1 else (dw1_ref if k else dw3_ref).at[at(other(c), half)]
            remote(theirs, theirs, fcs.at[0], fcr.at[k], cpeer).wait_recv()
            sent = ry_ref.at[at(k, per_layer)]
            remote(sent, sent, ys.at[k], yr.at[0], ypeer).wait_send()
        for j in range(n_chunk - 4, n_chunk):
            to_x(j).wait_send()

    n_item = len(layers) * items
    vm = lambda *shape: pltpu.VMEM(shape, F32)
    bf = lambda *shape: pltpu.VMEM(shape, BF16)
    outs = call(
        kernel, "backward", 4, (),
        [ANY, ANY, VMEM, VMEM] + [ANY] * 7 + [VMEM] * 4, [ANY] * 3 + [VMEM] + [ANY] * 4,
        [sds((dim, half), F32), sds((half, dim), F32), sds((dim, half), F32), sds((len(layers), 2, 2, dim), F32),
         sds((all_rows, dim), F32), sds((n_slab, half, width), F32), sds((n_chunk, piece, width), F32),
         sds((n_chunk, piece, width), F32)],
        [bf(all_rows, dim), bf(dim, all_rows), bf(2, dim, width), vm(2, rows, width), vm(2, rows, width), vm(2, rows, width),
         vm(2, half, width), vm(2, half, width), vm(2, half, width), vm(3, piece, width), vm(4, piece, width),
         vm(2, piece, width)] + Share.scratch(n_item, 2, width)
        + [TWO_DMA, TWO_DMA, TWO_DMA, TWO_DMA, TWO_DMA, DMA((n_slab,)), DMA((n_slab,)), DMA, DMA((n_layer,)),
           DMA((n_chunk,)), DMA((4,)), DMA((n_chunk,)), DMA((3,)), TWO_DMA, TWO_DMA, DMA((n_layer,)),
           pltpu.SemaphoreType.REGULAR],
        all_rows * dim * dim * 10, all_rows * dim * 40,
        (d_emb, zh, sz, s_emb, x2_t, x1_t, h_t, u2, u1, w3_t, w2_t, s2, s1, gb2, gb1))
    return outs[:n_layer + 1]


def settle(grads, sums, loss):
    steps = 4
    dim = sums.shape[-1]
    half = dim // 2

    def kernel(sum_ref, loss_ref, src3, src2, src1, g2_ref, b2_ref, g1_ref, b1_ref, total_ref, *dsts):
        for src, dst in zip((src3, src2, src1), dsts):
            dst[...] = src[...]

        @pl.when(pl.program_id(0) == 0)
        def _():
            y, _, _ = coords()
            for layer, (cols, g_ref, b_ref) in enumerate(((pl.ds(0, dim), g2_ref, b2_ref), (at(y, half), g1_ref, b1_ref))):
                both = jnp.sum(sum_ref[layer, :, :, cols], axis=0)
                g_ref[...] = both[1:]
                b_ref[...] = both[:1]
            total_ref[...] = jnp.sum(loss_ref[...], axis=1, keepdims=True)

    specs = [pl.BlockSpec((g.shape[0] // steps, g.shape[1]), lambda i: (i, 0)) for g in grads]
    small = [(1, n) for n in (dim, dim, half, half, 1)]
    return call(kernel, "settle", None, (steps,), [whole(*sums.shape), whole(*loss.shape)] + specs,
                [whole(*t) for t in small] + specs, [sds(t, F32) for t in small] + [sds(g.shape, F32) for g in grads], [], 0,
                sum(g.size for g in grads) * 8, (sums, loss, *grads))


def solution(mesh):
    def shard_body(h_a, h_b, w_one, w_two, w_three, g_one, b_one, g_two, b_two, lam_off):
        total = float(h_a.shape[0] * mesh.shape['data'])
        rowed = [t.reshape(1, -1) for t in (g_one, b_one, g_two, b_two)]
        u1, s1, gb1, gb2, w_two_o, h_t = fwd_first(h_a, h_b, w_one, w_two, *rowed)
        x1_t, u2, s2, w2_t, w_three_o = fwd_next(u1, s1, gb1, w_two, w_two_o, True, total, 1, w_three)
        x2_t, z, sz, w3_t = fwd_next(u2, s2, gb2, w_three, w_three_o, False, total, 2)
        zh, d_emb, s_emb, loss = corr_grad(z, sz, lam_off, total)
        *grads, sums = backward(
            d_emb.reshape(z.shape), zh.reshape(z.shape), sz, s_emb,
            ((u2, s2, gb2, w3_t, x1_t), (u1, s1, gb1, w2_t, h_t)), x2_t, total)
        *small, dw_three, dw_two, dw_one = settle(grads, sums, loss)
        dg_two, db_two, dg_one, db_one, loss = (t.reshape(-1) for t in small)
        return loss, dw_one, dw_two, dw_three, dg_one, db_one, dg_two, db_two

    in_specs = (P('data', None), P('data', None), P(None, 'model'), P('model', None), P(None, 'model'),
                P('model'), P('model'), P(), P(), P())
    out_specs = (P(), P(None, 'model'), P('model', None), P(None, 'model'), P('model'), P('model'), P(), P())
    return jax.shard_map(shard_body, mesh=mesh, in_specs=in_specs, out_specs=out_specs, check_vma=False)
```
